128 devices in a mesh: kpt: 1, col: 16 (over z, y), row: 8 (over x, core).
Axes of the slice: x: 4, y: 4, z: 4, core: 2. Of those that a mesh axis runs over, the one named last changes fastest.
Arguments:
- v_panels: float32 [8192, 8192], P(('kpt', 'row'), 'col')
- t_fac: float32 [128, 64, 64], P('kpt')
- z_in: float32 [8192, 8192], P(('kpt', 'row'), 'col')
- l_chol: float32 [8192, 8192], P(('kpt', 'row'), 'col')
Outputs:
- output: float32 [8192, 8192], P(('kpt', 'row'), 'col')
All inputs are finite; a program needn't handle non-finite values.
Results may differ from the reference program's by a relative error of at most 0.001.
Values sent between devices are 32-bit elements.
A program may use at most 1 GiB of HBM per device.

```python
import jax
import jax.numpy as jnp
from jax import lax

MAT_ORDER = 8192
BLOCK_SIZE = 64
EIG_COLS = 8192
ROW_DEVS = 8
COL_DEVS = 16

NUM_PANELS = MAT_ORDER // BLOCK_SIZE
PREC_HIGH = lax.Precision.HIGHEST


def rows_to_logical(stored):
    blocks = stored.reshape((ROW_DEVS, NUM_PANELS // ROW_DEVS, BLOCK_SIZE) + stored.shape[1:])
    return jnp.swapaxes(blocks, 0, 1).reshape(stored.shape)


def rows_to_stored(logical):
    blocks = logical.reshape((NUM_PANELS // ROW_DEVS, ROW_DEVS, BLOCK_SIZE) + logical.shape[1:])
    return jnp.swapaxes(blocks, 0, 1).reshape(logical.shape)


def cols_to_logical(stored):
    blocks = stored.reshape(stored.shape[0], COL_DEVS, NUM_PANELS // COL_DEVS, BLOCK_SIZE)
    return jnp.swapaxes(blocks, 1, 2).reshape(stored.shape)


def cols_to_stored(logical):
    blocks = logical.reshape(logical.shape[0], NUM_PANELS // COL_DEVS, COL_DEVS, BLOCK_SIZE)
    return jnp.swapaxes(blocks, 1, 2).reshape(logical.shape)


def wy_factors(v_log):
    v_pan = v_log.reshape(MAT_ORDER, NUM_PANELS, BLOCK_SIZE)
    gram_mat = jnp.einsum('nkb,nkc->kbc', v_pan, v_pan, precision=PREC_HIGH)
    t_inv = jnp.triu(gram_mat, 1) + 0.5 * gram_mat * jnp.eye(BLOCK_SIZE, dtype=jnp.float32)
    return jnp.triu(jnp.linalg.inv(t_inv))


def setup_inputs(seed: int = 0, part: int = 0) -> dict:
    part_key = jax.random.fold_in(jax.random.key(seed), part)
    key_v, key_z, key_l, key_d = jax.random.split(part_key, 4)
    vec_scale = MAT_ORDER ** -0.5
    eye_full = jnp.eye(MAT_ORDER, dtype=jnp.float32)
    v_raw = jax.random.normal(key_v, (MAT_ORDER, MAT_ORDER), jnp.float32) * vec_scale
    v_log = jnp.tril(v_raw, -1) + eye_full
    t_fac = wy_factors(v_log)
    z_log = jax.random.normal(key_z, (MAT_ORDER, EIG_COLS), jnp.float32)
    l_raw = jax.random.normal(key_l, (MAT_ORDER, MAT_ORDER), jnp.float32) * (0.5 * vec_scale)
    l_diag = jax.random.uniform(key_d, (MAT_ORDER,), jnp.float32, 1.0, 2.0)
    l_log = jnp.tril(l_raw, -1) + jnp.diag(l_diag)
    return {
        'v_panels': rows_to_stored(cols_to_stored(v_log)),
        't_fac': t_fac,
        'z_in': rows_to_stored(z_log),
        'l_chol': rows_to_stored(cols_to_stored(l_log)),
    }


def reference(v_panels, t_fac, z_in, l_chol):
    v_log = cols_to_logical(rows_to_logical(v_panels))

    def house_step(z_cur, panel_id):
        v_cur = lax.dynamic_slice_in_dim(v_log, panel_id * BLOCK_SIZE, BLOCK_SIZE, axis=1)
        t_cur = lax.dynamic_index_in_dim(t_fac, panel_id, keepdims=False)
        s_part = jnp.dot(v_cur.T, z_cur, precision=PREC_HIGH, preferred_element_type=jnp.float32)
        w_part = jnp.dot(t_cur.T, s_part, precision=PREC_HIGH, preferred_element_type=jnp.float32)
        return z_cur - jnp.dot(v_cur, w_part, precision=PREC_HIGH, preferred_element_type=jnp.float32), None

    y_log, _ = lax.scan(house_step, rows_to_logical(z_in), jnp.arange(NUM_PANELS - 1, -1, -1))
    l_log = cols_to_logical(rows_to_logical(l_chol))
    x_log = lax.linalg.triangular_solve(l_log, y_log, left_side=True, lower=True, transpose_a=True)
    return rows_to_stored(x_log)
```

```python
import functools

import jax
import jax.numpy as jnp
from jax import lax
from jax.experimental import pallas as pl
from jax.experimental.pallas import tpu as pltpu
from jax.sharding import PartitionSpec as P

PREC_HIGH = lax.Precision.HIGHEST
MESH = pl.DeviceIdType.MESH
EDGE = 64
LANES = 128
STEP = 256


def _dot_nt(a, b):
    return lax.dot_general(a, b, (((1,), (1,)), ((), ())), precision=PREC_HIGH, preferred_element_type=jnp.float32)


def _dot_nn(a, b):
    return lax.dot_general(a, b, (((1,), (0,)), ((), ())), precision=PREC_HIGH, preferred_element_type=jnp.float32)


def _place():
    row, col = lax.axis_index("row"), lax.axis_index("col")
    return row, col, row // 2, row % 2


def _deal_kernel(dims, v_ref, l_ref, vb_ref, ld_ref, v_send, v_recv, d_send, d_recv):
    rows, cols, half = dims
    row, col, x, k = _place()
    chips = rows // 2
    groups = cols // rows
    mine, part = col // rows, col % rows
    sent = []
    for qp in range(half):
        blk = groups * (2 * qp + k) + mine
        here = blk == col
        sent.append((jnp.logical_not(here), pltpu.make_async_remote_copy(
            v_ref.at[qp], vb_ref.at[part], v_send.at[qp], v_recv.at[part],
            device_id={"col": blk, "row": row}, device_id_type=MESH,
        )))

        @pl.when(here)
        def _(qp=qp):
            pltpu.make_async_copy(v_ref.at[qp], vb_ref.at[part], v_recv.at[part]).start()

        src = l_ref.at[qp, :, pl.ds(pl.multiple_of(blk * LANES, LANES), LANES)]
        dst = ld_ref.at[part, :, pl.ds(pl.multiple_of(x * LANES, LANES), LANES)]

        @pl.when(here)
        def _(src=src, dst=dst):
            pltpu.make_async_copy(src, dst, d_recv.at[part, x]).start()

        for d in range(chips):
            x2 = lax.rem(x + d, chips)
            sent.append((jnp.logical_not(here) if d == 0 else None, pltpu.make_async_remote_copy(
                src, dst, d_send.at[qp, d], d_recv.at[part, x],
                device_id={"col": blk, "row": 2 * x2 + k}, device_id_type=MESH,
            )))

    def over_sent(act):
        for cond, copy in sent:
            if cond is None:
                act(copy)
            else:
                pl.when(cond)(functools.partial(act, copy))

    over_sent(lambda c: c.start())

    @pl.when((col // groups) % 2 == k)
    def _():
        for p in range(rows):
            pltpu.make_async_copy(v_ref.at[0], vb_ref.at[p], v_recv.at[p]).wait()
            for x2 in range(chips):
                there = ld_ref.at[p, :, pl.ds(x2 * LANES, LANES)]
                pltpu.make_async_copy(there, there, d_recv.at[p, x2]).wait()

    over_sent(lambda c: c.wait_send())


def _deal(v_own, l_own, rows, cols):
    half, _, lanes = v_own.shape
    chips = rows // 2
    return pl.pallas_call(
        functools.partial(_deal_kernel, (rows, cols, half)),
        out_shape=[
            jax.ShapeDtypeStruct((rows, EDGE, lanes), jnp.float32),
            jax.ShapeDtypeStruct((rows, EDGE, chips * LANES), jnp.float32),
        ],
        in_specs=[pl.BlockSpec(memory_space=pl.ANY)] * 2,
        out_specs=[pl.BlockSpec(memory_space=pl.ANY)] * 2,
        scratch_shapes=[
            pltpu.SemaphoreType.DMA((half,)),
            pltpu.SemaphoreType.DMA((rows,)),
            pltpu.SemaphoreType.DMA((half, chips)),
            pltpu.SemaphoreType.DMA((rows, chips)),
        ],
        compiler_params=pltpu.CompilerParams(has_side_effects=True),
        name="deal",
    )(v_own, l_own)


def _phase_kernel(solve, dims, own_ref, m_ref, in_ref, out_ref, gath, mg, *scratch):
    (blk, mbuf, sbuf, rs, wb, xr, v_send, v_recv, m_send, m_recv, blk_local, blk_send, blk_recv,
     mat_local, mat_send, mat_recv, free, rs_send, rs_recv, ag_send, ag_recv) = scratch
    rows, cols, half, nb, ncol = dims
    row, col, x, k = _place()
    chips = rows // 2
    groups = cols // rows
    size = rows * EDGE
    lanes = nb * LANES
    gcol = ncol // 2
    sl = gcol // chips
    mate = {"row": row + 1 - 2 * k, "col": col}

    def peer(d):
        return lax.rem(x + d, chips)

    def low(qp):
        return 2 * groups * qp * LANES

    def piece(qp, to):
        return own_ref.at[qp, :, pl.ds(low(qp), lanes - low(qp))], gath.at[to, qp, :, pl.ds(low(qp), lanes - low(qp))]

    my_q = col // groups
    my_m = (my_q // 2) * groups + col % groups
    m_mine = my_q % 2 == k

    for qp in reversed(range(half)):
        src, dst = piece(qp, col)
        pltpu.make_async_copy(src, dst, v_recv.at[qp, col]).start()

        def send_slot(d, carry, src=src, dst=dst, qp=qp):
            pltpu.make_async_remote_copy(
                src, dst, v_send.at[qp, d], v_recv.at[qp, col],
                device_id={"row": row, "col": lax.rem(col + d, cols)}, device_id_type=MESH,
            ).start()
            return carry

        lax.fori_loop(1, cols, send_slot, 0)
        if qp == half - 1:

            @pl.when(m_mine)
            def _():
                pltpu.make_async_copy(m_ref, mg.at[my_m], m_recv.at[my_m]).start()

                def send_mat(d, carry):
                    pltpu.make_async_remote_copy(
                        m_ref, mg.at[my_m], m_send.at[d], m_recv.at[my_m],
                        device_id={"row": row, "col": lax.rem(col + d, cols)}, device_id_type=MESH,
                    ).start()
                    return carry

                lax.fori_loop(1, cols, send_mat, 0)

    def owner_of(j):
        return (j // groups) % 2

    def by_class(j, body):
        for qp in range(half):
            pl.when((j // groups) // 2 == qp)(functools.partial(body, qp))

    def blk_copies(j, qp):
        s, h = j % 2, j % groups
        src = gath.at[pl.ds(h * rows, rows), qp, :, pl.ds(low(qp), lanes - low(qp))]
        dst = blk.at[s, :, :, pl.ds(low(qp), lanes - low(qp))]
        here = pltpu.make_async_copy(src, dst, blk_local.at[s])
        there = pltpu.make_async_remote_copy(
            src, dst, blk_send.at[s], blk_recv.at[s], device_id=mate, device_id_type=MESH
        )
        return here, there

    def mat_copies(j):
        s = j % 2
        src = mg.at[((j // groups) // 2) * groups + j % groups]
        here = pltpu.make_async_copy(src, mbuf.at[s], mat_local.at[s])
        there = pltpu.make_async_remote_copy(
            src, mbuf.at[s], mat_send.at[s], mat_recv.at[s], device_id=mate, device_id_type=MESH
        )
        return here, there

    def prefetch(j, first):
        @pl.when(owner_of(j) == k)
        def _():
            h, q = j % groups, j // groups

            def arrived(qp):
                def one(p, carry):
                    _, dst = piece(qp, h * rows + p)
                    pltpu.make_async_copy(dst, dst, v_recv.at[qp, h * rows + p]).wait()
                    return carry

                lax.fori_loop(0, rows, one, 0)

            by_class(j, arrived)
            slot = (q // 2) * groups + h
            pltpu.make_async_copy(mg.at[slot], mg.at[slot], m_recv.at[slot]).wait()
            if not first:

                @pl.when(owner_of(j) == k)
                def _():
                    pl.semaphore_wait(free.at[j % 2], 1)

            def go(qp):
                here, there = blk_copies(j, qp)
                here.start()
                there.start()

            by_class(j, go)
            here, there = mat_copies(j)
            here.start()
            there.start()

    def wait_blk(j):
        mine = owner_of(j) == k

        def one(qp):
            here, there = blk_copies(j, qp)

            @pl.when(mine)
            def _():
                here.wait()

            @pl.when(jnp.logical_not(mine))
            def _():
                there.wait_recv()

        by_class(j, one)
        here, there = mat_copies(j)

        @pl.when(mine)
        def _():
            here.wait()

        @pl.when(jnp.logical_not(mine))
        def _():
            there.wait_recv()

    def release(j):
        @pl.when(owner_of(j) == k)
        def _():
            by_class(j, lambda qp: blk_copies(j, qp)[1].wait_send())
            mat_copies(j)[1].wait_send()

        @pl.when(j >= 2)
        def _():
            @pl.when(owner_of(j - 2) != k)
            def _():
                pl.semaphore_signal(free.at[j % 2], inc=1, device_id=mate, device_id_type=MESH)

            prefetch(j - 2, False)

    def cut(s, i):
        return blk[s, :, :, pl.ds(pl.multiple_of(i * STEP, STEP), STEP)].reshape(size, STEP)

    def rs_copy(par, g, d):
        x2 = peer(d)
        return pltpu.make_async_remote_copy(
            sbuf.at[par, g, pl.ds(pl.multiple_of(x2 * sl, sl), sl)], rs.at[g, d - 1],
            rs_send.at[g, d - 1], rs_recv.at[g, d - 1],
            device_id={"row": 2 * x2 + k, "col": col}, device_id_type=MESH,
        )

    def send_partial(par, g):
        for d in range(1, chips):
            rs_copy(par, g, d).start()

    def gather_sum(par, g):
        for d in range(1, chips):
            rs_copy(par, g, d).wait_recv()
        total = sbuf[par, g, pl.ds(pl.multiple_of(x * sl, sl), sl)]
        for d in range(1, chips):
            total = total + rs[g, d - 1]
        for d in range(1, chips):
            rs_copy(par, g, d).wait_send()
        return total

    def state(ref, g, i):
        return ref[pl.ds(g * gcol, gcol), pl.ds(pl.multiple_of(i * STEP, STEP), STEP)]

    def project(par, g, s, ref, first, limit):
        sbuf[par, g] = jnp.zeros((gcol, size), jnp.float32)

        def one(i, carry):
            sbuf[par, g] += _dot_nt(state(ref, g, i), cut(s, i))
            return carry

        lax.fori_loop(first, limit, one, 0)

    top = nb - 1
    whole = nb * LANES // STEP
    prefetch(top, True)
    prefetch(top - 1, True)

    if not solve:
        out_ref[...] = in_ref[...]
        mine_rows = pl.ds(pl.multiple_of(x * sl, sl), sl)

        def ag_copy(g, d):
            return pltpu.make_async_remote_copy(
                wb.at[g, mine_rows], wb.at[g, mine_rows], ag_send.at[g, d - 1], ag_recv.at[g, d - 1],
                device_id={"row": 2 * peer(d) + k, "col": col}, device_id_type=MESH,
            )

        def ag_wait(g, d):
            rows_of = pl.ds(pl.multiple_of(peer(chips - d) * sl, sl), sl)
            pltpu.make_async_copy(wb.at[g, rows_of], wb.at[g, rows_of], ag_recv.at[g, d - 1]).wait()

        wait_blk(top)
        for g in range(2):
            project(0, g, top % 2, out_ref, top // 2, whole)
            send_partial(0, g)

        def step(i, carry):
            j = top - i
            s = j % 2
            for g in range(2):
                wb[g, mine_rows] = _dot_nn(gather_sum(0, g), mbuf[s])
                for d in range(1, chips):
                    ag_copy(g, d).start()

            @pl.when(j > 0)
            def _():
                wait_blk(j - 1)

            for g in range(2):
                for d in range(1, chips):
                    ag_wait(g, d)

                def apply(n, carry, g=g, s=s):
                    at = pl.ds(g * gcol, gcol), pl.ds(pl.multiple_of(n * STEP, STEP), STEP)
                    out_ref[at] = out_ref[at] - _dot_nn(wb[g], cut(s, n))
                    return carry

                lax.fori_loop(j // 2, whole, apply, 0)
                for d in range(1, chips):
                    ag_copy(g, d).wait_send()

                @pl.when(j > 0)
                def _(g=g):
                    project(0, g, (j - 1) % 2, out_ref, (j - 1) // 2, whole)
                    send_partial(0, g)

            release(j)
            return carry

        lax.fori_loop(0, nb, step, 0)
    else:
        out_ref[...] = jnp.zeros_like(out_ref)

        def right_side(par, g, j):
            sbuf[par, g] = -sbuf[par, g]
            at = pl.ds(pl.multiple_of(x * LANES, LANES), LANES)
            sbuf[par, g, :, at] += in_ref[pl.ds(g * gcol, gcol), pl.ds(pl.multiple_of(j * LANES, LANES), LANES)]

        def aa_copy(g, d):
            x2 = peer(d)
            return pltpu.make_async_remote_copy(
                wb.at[g, pl.ds(0, sl), pl.ds(pl.multiple_of(x2 * LANES, LANES), LANES)],
                xr.at[g, pl.ds(pl.multiple_of(x * sl, sl), sl)], ag_send.at[g, d - 1], ag_recv.at[g, d - 1],
                device_id={"row": 2 * x2 + k, "col": col}, device_id_type=MESH,
            )

        def aa_wait(g, d):
            there = xr.at[g, pl.ds(pl.multiple_of(peer(chips - d) * sl, sl), sl)]
            pltpu.make_async_copy(there, there, ag_recv.at[g, d - 1]).wait()

        wait_blk(top)
        for g in range(2):
            sbuf[top % 2, g] = jnp.zeros((gcol, size), jnp.float32)
            right_side(top % 2, g, top)
            send_partial(top % 2, g)

        def step(i, carry):
            j = top - i
            par, nxt = j % 2, (j + 1) % 2

            @pl.when(j > 0)
            def _():
                wait_blk(j - 1)

            for g in range(2):

                @pl.when(j > 0)
                def _(g=g):
                    project(nxt, g, nxt, out_ref, (j + 1) // 2, whole)

                wb[g, pl.ds(0, sl)] = _dot_nn(gather_sum(par, g), mbuf[par])
                for d in range(1, chips):
                    aa_copy(g, d).start()
                xr[g, pl.ds(pl.multiple_of(x * sl, sl), sl)] = wb[
                    g, pl.ds(0, sl), pl.ds(pl.multiple_of(x * LANES, LANES), LANES)
                ]

            here = pl.ds(pl.multiple_of(j * LANES, LANES), LANES)
            for g in range(2):
                for d in range(1, chips):
                    aa_wait(g, d)
                out_ref[pl.ds(g * gcol, gcol), here] = xr[g]

                @pl.when(j > 0)
                def _(g=g):
                    sbuf[nxt, g] += _dot_nt(xr[g], blk[nxt, :, :, here].reshape(size, LANES))
                    right_side(nxt, g, j - 1)
                    send_partial(nxt, g)

                for d in range(1, chips):
                    aa_copy(g, d).wait_send()

            release(j)
            return carry

        lax.fori_loop(0, nb, step, 0)

    for qp in range(half):
        src, dst = piece(qp, col)

        def sent(d, carry, src=src, dst=dst, qp=qp):
            pltpu.make_async_remote_copy(
                src, dst, v_send.at[qp, d], v_recv.at[qp, col],
                device_id={"row": row, "col": lax.rem(col + d, cols)}, device_id_type=MESH,
            ).wait_send()
            return carry

        lax.fori_loop(1, cols, sent, 0)

    @pl.when(m_mine)
    def _():
        def sent(d, carry):
            pltpu.make_async_remote_copy(
                m_ref, mg.at[my_m], m_send.at[d], m_recv.at[my_m],
                device_id={"row": row, "col": lax.rem(col + d, cols)}, device_id_type=MESH,
            ).wait_send()
            return carry

        lax.fori_loop(1, cols, sent, 0)


def _phase(solve, own, factor, state, rows, cols):
    half, _, lanes = own.shape
    nb = lanes // LANES
    ncol = state.shape[0]
    chips, size, gcol = rows // 2, rows * EDGE, ncol // 2
    sl = gcol // chips
    dma = pltpu.SemaphoreType.DMA
    hbm, vmem = pl.BlockSpec(memory_space=pl.ANY), pl.BlockSpec(memory_space=pltpu.VMEM)
    outs = pl.pallas_call(
        functools.partial(_phase_kernel, solve, (rows, cols, half, nb, ncol)),
        out_shape=[
            jax.ShapeDtypeStruct(state.shape, jnp.float32),
            jax.ShapeDtypeStruct((cols, half, EDGE, lanes), jnp.float32),
            jax.ShapeDtypeStruct((nb // 2, size, size), jnp.float32),
        ],
        in_specs=[hbm, hbm, vmem],
        out_specs=[vmem, hbm, hbm],
        scratch_shapes=[
            pltpu.VMEM((2, rows, EDGE, lanes), jnp.float32),
            pltpu.VMEM((2, size, size), jnp.float32),
            pltpu.VMEM((2 if solve else 1, 2, gcol, size), jnp.float32),
            pltpu.VMEM((2, chips - 1, sl, size), jnp.float32),
            pltpu.VMEM((2, gcol, size), jnp.float32),
            pltpu.VMEM((2, gcol, LANES), jnp.float32),
            dma((half, cols)), dma((half, cols)), dma((cols,)), dma((nb // 2,)),
            dma((2,)), dma((2,)), dma((2,)), dma((2,)), dma((2,)), dma((2,)),
            pltpu.SemaphoreType.REGULAR((2,)),
            dma((2, chips - 1)), dma((2, chips - 1)), dma((2, chips - 1)), dma((2, chips - 1)),
        ],
        compiler_params=pltpu.CompilerParams(has_side_effects=True, vmem_limit_bytes=48 * 1024 * 1024),
        name="solve" if solve else "reflect",
    )(own, factor, state)
    return outs[0]


def _merge(diag, full):
    two, n, b, _ = diag.shape
    while n > 1:
        pairs = diag.reshape(two, n // 2, 2, b, b)
        d1, d2 = pairs[:, :, 0], pairs[:, :, 1]
        c21 = jnp.stack([full[:, (2 * i + 1) * b : (2 * i + 2) * b, 2 * i * b : (2 * i + 1) * b] for i in range(n // 2)], axis=1)
        mid = jnp.einsum("pnij,pnjk->pnik", d2, c21, precision=PREC_HIGH)
        off = -jnp.einsum("pnij,pnjk->pnik", mid, d1, precision=PREC_HIGH)
        zero = jnp.zeros_like(off)
        diag = jnp.concatenate([jnp.concatenate([d1, zero], axis=3), jnp.concatenate([off, d2], axis=3)], axis=2)
        n, b = n // 2, 2 * b
    return diag[:, 0]


def solution(mesh):
    rows, cols = mesh.shape["row"], mesh.shape["col"]
    groups = cols // rows
    mat_spec = P(("kpt", "row"), "col")
    fac_spec = P("kpt", None, None)
    swap = [(r, r + 1 - 2 * (r % 2)) for r in range(rows)]

    def local_work(v_loc, t_loc, z_loc, l_loc):
        nb = v_loc.shape[0] // EDGE
        size = rows * EDGE
        lanes = nb * LANES
        slots = v_loc.shape[1] // EDGE
        row, col = lax.axis_index("row"), lax.axis_index("col")
        k = row % 2

        def chip_rows(keep, send, axis):
            got = lax.ppermute(send, "row", swap)
            return jnp.stack([jnp.where(k == 0, keep, got), jnp.where(k == 0, got, keep)], axis=axis)

        def slots_of(m_loc):
            mt = m_loc.T.reshape(slots // 2, 2, EDGE, nb, EDGE)
            keep = lax.dynamic_index_in_dim(mt, k, 1, keepdims=False)
            send = lax.dynamic_index_in_dim(mt, 1 - k, 1, keepdims=False)
            return chip_rows(keep, send, 3).reshape(slots // 2, EDGE, lanes)

        v_own, l_own = slots_of(v_loc), slots_of(l_loc)
        half_cols = z_loc.shape[1] // 2
        zt = z_loc.T.reshape(2, half_cols, nb, EDGE)
        z_state = chip_rows(
            lax.dynamic_index_in_dim(zt, k, 0, keepdims=False), lax.dynamic_index_in_dim(zt, 1 - k, 0, keepdims=False), 2
        ).reshape(half_cols, lanes)

        v_blk, l_diag = _deal(v_own, l_own, rows, cols)
        held = (col // groups) % 2 == k
        vb = jnp.where(held, v_blk.reshape(size, lanes), 0.0)
        gram = lax.psum(_dot_nt(vb, vb), "row")
        l_blk = jnp.where(held, l_diag.reshape(size, size), jnp.eye(size, dtype=jnp.float32)).T
        t_blk = lax.dynamic_slice_in_dim(t_loc, col * rows, rows, axis=0)
        l_pan = jnp.stack([l_blk[i * EDGE : (i + 1) * EDGE, i * EDGE : (i + 1) * EDGE] for i in range(rows)])
        eye = jnp.broadcast_to(jnp.eye(EDGE, dtype=jnp.float32), l_pan.shape)
        l_inv = lax.linalg.triangular_solve(l_pan, eye, left_side=True, lower=True)
        factors = _merge(jnp.stack([t_blk, l_inv]), jnp.stack([gram, l_blk]))

        y_state = _phase(False, v_own, factors[0], z_state, rows, cols)
        x_state = _phase(True, l_own, factors[1], y_state, rows, cols)

        xs = x_state.reshape(half_cols, nb, 2, EDGE)
        keep = lax.dynamic_index_in_dim(xs, k, 2, keepdims=False).reshape(half_cols, nb * EDGE)
        send = lax.dynamic_index_in_dim(xs, 1 - k, 2, keepdims=False).reshape(half_cols, nb * EDGE)
        got = lax.ppermute(send, "row", swap)
        return jnp.concatenate([jnp.where(k == 0, keep, got), jnp.where(k == 0, got, keep)], axis=0).T

    return jax.shard_map(local_work, mesh=mesh, in_specs=(mat_spec, fac_spec, mat_spec, mat_spec), out_specs=mat_spec, check_vma=False)
```

```python
import functools

import jax
import jax.numpy as jnp
from jax import lax
from jax.experimental import pallas as pl
from jax.experimental.pallas import tpu as pltpu
from jax.sharding import PartitionSpec as P

PREC_HIGH = lax.Precision.HIGHEST
MESH = pl.DeviceIdType.MESH
EDGE = 64
HALF = EDGE // 2
LANES = 128
STEP = 256
RING = 4


def _dot_nt(a, b):
    return lax.dot_general(a, b, (((1,), (1,)), ((), ())), precision=PREC_HIGH, preferred_element_type=jnp.float32)


def _dot_nn(a, b):
    return lax.dot_general(a, b, (((1,), (0,)), ((), ())), precision=PREC_HIGH, preferred_element_type=jnp.float32)


def _place():
    row, col = lax.axis_index("row"), lax.axis_index("col")
    return row, col, row // 2, row % 2


def _at(i, n):
    return pl.ds(pl.multiple_of(i * n, n), n)


def _prep_kernel(dims, v_ref, l_ref, z_ref, own, zs, vb, ld, vt, zt, loc, swap_s, swap_r, v_s, v_r, l_s, l_r):
    rows, cols, slots, pairs = dims
    row, col, x, k = _place()
    chips, groups = rows // 2, cols // rows
    part, grp = col % rows, col // rows
    mate = {"row": row + 1 - 2 * k, "col": col}
    width = pairs * STEP // 2

    def swaps(m, i):
        there = _at(2 * i + k, LANES)
        if m < 2:
            mine, theirs = vt.at[m, :, k, :, _at(i, LANES)], vt.at[m, :, 1 - k, :, _at(i, LANES)]
            dst = own.at[m, :, :, there]
        else:
            mine, theirs = zt.at[k, :, _at(i, LANES)], zt.at[1 - k, :, _at(i, LANES)]
            dst = zs.at[:, there]
        return (
            pltpu.make_async_copy(mine, dst, loc.at[m, i]),
            pltpu.make_async_remote_copy(
                theirs, dst, swap_s.at[m, i], swap_r.at[m, i], device_id=mate, device_id_type=MESH
            ),
        )

    for m, ref in enumerate((v_ref, l_ref, z_ref)):

        def turn(i, carry, m=m, ref=ref):
            block = ref[_at(i, LANES), :].T
            if m < 2:
                vt[m, :, :, :, _at(i, LANES)] = block.reshape(slots, 2, HALF, LANES)
            else:
                zt[:, :, _at(i, LANES)] = block.reshape(2, -1, LANES)
            for c in swaps(m, i):
                c.start()
            return carry

        lax.fori_loop(0, pairs, turn, 0)

    def swapped(m):
        def one(i, carry):
            here, there = swaps(m, i)
            here.wait()
            there.wait_recv()
            return carry

        lax.fori_loop(0, pairs, one, 0)

    def deal_v(q, kk):
        blk = groups * q + grp
        src = own.at[0, q, :, pl.ds(kk * width, width)]
        dst = vb.at[part, pl.ds(pl.multiple_of(k * HALF, HALF), HALF)]
        self_ = jnp.logical_and(blk == col, k == kk)
        here = pltpu.make_async_copy(src, dst, v_r.at[part, k])
        there = pltpu.make_async_remote_copy(
            src, dst, v_s.at[q, kk], v_r.at[part, k], device_id={"col": blk, "row": 2 * x + kk}, device_id_type=MESH
        )
        return self_, here, there

    def deal_l(q, d):
        blk = groups * q + grp
        src = own.at[1, q, :, _at(blk // 2, STEP)]
        dst = ld.at[part, pl.ds(pl.multiple_of(k * HALF, HALF), HALF), _at(x, STEP)]
        self_ = jnp.logical_and(blk == col, d == 0)
        here = pltpu.make_async_copy(src, dst, l_r.at[part, k, x])
        there = pltpu.make_async_remote_copy(
            src, dst, l_s.at[q, d], l_r.at[part, k, x],
            device_id={"col": blk, "row": lax.rem(row + d, rows)}, device_id_type=MESH,
        )
        return self_, here, there

    def send(self_, here, there):
        @pl.when(self_)
        def _():
            here.start()

        @pl.when(jnp.logical_not(self_))
        def _():
            there.start()

    def sent(self_, here, there):
        @pl.when(jnp.logical_not(self_))
        def _():
            there.wait_send()

    def over_v(act):
        def one(q, carry):
            for kk in range(2):
                act(*deal_v(q, kk))
            return carry

        lax.fori_loop(0, slots, one, 0)

    def over_l(act):
        def one(n, carry):
            act(*deal_l(n // rows, n % rows))
            return carry

        lax.fori_loop(0, slots * rows, one, 0)

    swapped(0)
    over_v(send)
    swapped(1)
    over_l(send)
    swapped(2)

    def got(n, carry):
        p, kk = n // 2, n % 2
        there = vb.at[p, pl.ds(pl.multiple_of(kk * HALF, HALF), HALF)]
        pltpu.make_async_copy(there, there, v_r.at[p, kk]).wait()
        for x2 in range(chips):
            there = ld.at[p, pl.ds(pl.multiple_of(kk * HALF, HALF), HALF), pl.ds(x2 * STEP, STEP)]
            pltpu.make_async_copy(there, there, l_r.at[p, kk, x2]).wait()
        return carry

    lax.fori_loop(0, 2 * rows, got, 0)
    over_v(sent)
    over_l(sent)

    def left(i, carry):
        for m in range(3):
            swaps(m, i)[1].wait_send()
        return carry

    lax.fori_loop(0, pairs, left, 0)


def _prep(v_loc, l_loc, z_loc, rows, cols):
    n_row, n_col = v_loc.shape
    slots, pairs = n_col // EDGE, n_row // LANES
    lanes, chips, ncol = 2 * n_row, rows // 2, z_loc.shape[1] // 2
    dma = pltpu.SemaphoreType.DMA
    hbm, vmem = pl.BlockSpec(memory_space=pl.ANY), pl.BlockSpec(memory_space=pltpu.VMEM)
    return pl.pallas_call(
        functools.partial(_prep_kernel, (rows, cols, slots, pairs)),
        out_shape=[
            jax.ShapeDtypeStruct((2, slots, HALF, lanes), jnp.float32),
            jax.ShapeDtypeStruct((ncol, lanes), jnp.float32),
            jax.ShapeDtypeStruct((rows, EDGE, lanes // 2), jnp.float32),
            jax.ShapeDtypeStruct((rows, EDGE, chips * STEP), jnp.float32),
        ],
        in_specs=[vmem] * 3,
        out_specs=[hbm] * 4,
        scratch_shapes=[
            pltpu.VMEM((2, slots, 2, HALF, n_row), jnp.float32),
            pltpu.VMEM((2, ncol, n_row), jnp.float32),
            dma((3, pairs)), dma((3, pairs)), dma((3, pairs)),
            dma((slots, 2)), dma((rows, 2)), dma((slots, rows)), dma((rows, 2, chips)),
        ],
        compiler_params=pltpu.CompilerParams(has_side_effects=True, vmem_limit_bytes=32 * 1024 * 1024),
        name="prep",
    )(v_loc, l_loc, z_loc)


def _main_kernel(dims, own_ref, m_ref, z_ref, out_ref, gath, mg, *scratch):
    (ys, blk, mbuf, sbuf, rs, wb, xr, ag_loc, ag_s, ag_r, blk_loc, blk_s, blk_r, mat_loc, mat_s, mat_r, free,
     rs_s, rs_r, ex_s, ex_r) = scratch
    rows, cols, slots, nb, ncol = dims
    row, col, x, k = _place()
    chips, groups = rows // 2, cols // rows
    size, lanes = rows * EDGE, nb * LANES
    gcol = ncol // 2
    sl = gcol // chips
    mate = {"row": row + 1 - 2 * k, "col": col}
    top, whole = nb - 1, nb // 2
    per = slots + 1
    s_a, s_b = 1 + (RING - 1) * k, RING - (RING - 1) * k
    a, b = (col // s_a) % RING, (col // s_b) % RING

    def plane(da, db):
        aa, bb = lax.rem(a + da, RING), lax.rem(b + db, RING)
        return {"row": row, "col": aa * s_a + bb * s_b}

    def low(q):
        return (groups * q // 2) * STEP

    class Slot:
        def __init__(self, kind, w, n):
            self.kind, self.w, self.n = kind, w, n

        def own(self):
            if self.kind == "m":
                return m_ref.at[self.w]
            return own_ref.at[self.w, self.kind, :, pl.ds(low(self.kind), lanes - low(self.kind))]

        def piece(self, bb, aa, part=None):
            if self.kind == "m":
                return mg.at[self.w, bb, aa] if part is None else mg.at[self.w, bb, aa, pl.ds(part * (size // 4), size // 4)]
            at = pl.ds(low(self.kind), lanes - low(self.kind))
            e = slice(None) if part is None else pl.ds(part * (HALF // 2), HALF // 2)
            return gath.at[self.w, self.kind, bb, aa, e, at]

        def bundle(self, bb, part=None):
            e = slice(None) if part is None else pl.ds(part * (RING // 2), RING // 2)
            if self.kind == "m":
                return mg.at[self.w, bb, e]
            return gath.at[self.w, self.kind, bb, e, :, pl.ds(low(self.kind), lanes - low(self.kind))]

        def copy(self, i):
            plus = i % 2 == 0
            d = 1 if plus else RING - 1
            back = RING - d
            if i < 2:
                src, dst, to = self.own(), self.piece(b, a), plane(d, 0)
            elif i < 4:
                src = dst = self.piece(b, lax.rem(a + back, RING), i % 2)
                to = plane(d, 0)
            elif i < 6:
                src = dst = self.bundle(b)
                to = plane(0, d)
            else:
                src = dst = self.bundle(lax.rem(b + back, RING), i % 2)
                to = plane(0, d)
            return pltpu.make_async_remote_copy(
                src, dst, ag_s.at[self.n, i], ag_r.at[self.n, i], device_id=to, device_id_type=MESH
            )

        def arrived(self, i):
            back = RING - 1 if i % 2 == 0 else 1
            if i < 2:
                dst = self.piece(b, lax.rem(a + back, RING))
            elif i < 4:
                dst = self.piece(b, lax.rem(a + 2, RING), i % 2)
            elif i < 6:
                dst = self.bundle(lax.rem(b + back, RING))
            else:
                dst = self.bundle(lax.rem(b + 2, RING), i % 2)
            pltpu.make_async_copy(dst, dst, ag_r.at[self.n, i]).wait()

        def kept(self):
            return pltpu.make_async_copy(self.own(), self.piece(b, a), ag_loc.at[self.n])

        def stage(self, s):
            if s == 0:
                self.kept().start()
                self.copy(0).start()
                self.copy(1).start()
            elif s == 1:
                for i in range(2):
                    self.arrived(i)
                    self.copy(2 + i).start()
            elif s == 2:
                self.arrived(2)
                self.arrived(3)
                self.kept().wait()
                self.copy(4).start()
                self.copy(5).start()
            elif s == 3:
                for i in range(4, 6):
                    self.arrived(i)
                    self.copy(2 + i).start()
            elif s == 4:
                self.arrived(6)
                self.arrived(7)
            else:
                for i in range(8):
                    self.copy(i).wait_send()

    def tick(t):
        for s in (5, 4, 3, 2, 1, 0):
            n = t - s

            @pl.when(jnp.logical_and(n >= 0, n < 2 * per))
            def _(s=s, n=n):
                w, pos = n // per, n % per
                for q in list(range(slots)) + ["m"]:
                    here = 1 if q == "m" else (0 if q == slots - 1 else slots - q)
                    pl.when(pos == here)(lambda q=q: Slot(q, w, n).stage(s))

    def block_of(n):
        w = n // nb
        j = top - n % nb
        return w, j, j // groups, j % groups, n % 2

    def blk_copies(n, q, p):
        w, j, _, h, s = block_of(n)
        c = h * rows + p
        src = gath.at[w, q, (c // s_b) % RING, (c // s_a) % RING, :, pl.ds(low(q), lanes - low(q))]
        dst = blk.at[s, p, pl.ds(pl.multiple_of(k * HALF, HALF), HALF), pl.ds(low(q), lanes - low(q))]
        here = pltpu.make_async_copy(src, dst, blk_loc.at[s, p])
        there = pltpu.make_async_remote_copy(
            src, dst, blk_s.at[s, p], blk_r.at[s, p], device_id=mate, device_id_type=MESH
        )
        return here, there

    def from_mate(n, q, p):
        s = n % 2
        dst = blk.at[s, p, pl.ds(pl.multiple_of((1 - k) * HALF, HALF), HALF), pl.ds(low(q), lanes - low(q))]
        pltpu.make_async_copy(dst, dst, blk_r.at[s, p]).wait()

    def mat_copies(n):
        w, j, _, _, s = block_of(n)
        src = mg.at[w, (j // s_b) % RING, (j // s_a) % RING]
        dst = mbuf.at[s, _at(k, size // 2)]
        here = pltpu.make_async_copy(src, dst, mat_loc.at[s])
        there = pltpu.make_async_remote_copy(
            src, dst, mat_s.at[s], mat_r.at[s], device_id=mate, device_id_type=MESH
        )
        return here, there

    def per_piece(n, act):
        _, _, q_now, _, _ = block_of(n)
        for q in range(slots):

            @pl.when(q_now == q)
            def _(q=q):
                def one(p, carry):
                    act(q, p)
                    return carry

                lax.fori_loop(0, rows, one, 0)

    def prefetch(n, first):
        if not first:
            pl.semaphore_wait(free.at[n % 2], 1)

        def go(q, p):
            here, there = blk_copies(n, q, p)
            here.start()
            there.start()

        per_piece(n, go)
        for c in mat_copies(n):
            c.start()

    def wait_blk(n):
        def one(q, p):
            blk_copies(n, q, p)[0].wait()
            from_mate(n, q, p)

        per_piece(n, one)
        mat_copies(n)[0].wait()
        there = mbuf.at[n % 2, _at(1 - k, size // 2)]
        pltpu.make_async_copy(there, there, mat_r.at[n % 2]).wait()

    def release(n):
        per_piece(n, lambda q, p: blk_copies(n, q, p)[1].wait_send())
        mat_copies(n)[1].wait_send()

        @pl.when(n + 2 < 2 * nb)
        def _():
            pl.semaphore_signal(free.at[n % 2], inc=1, device_id=mate, device_id_type=MESH)
            prefetch(n + 2, False)

    def cut(s, i):
        return blk[s, :, :, _at(i, STEP)].reshape(size, STEP)

    def peer(d):
        return lax.rem(x + d, chips)

    def at_peer(d):
        return {"row": 2 * peer(d) + k, "col": col}

    def rs_copy(par, g, d):
        return pltpu.make_async_remote_copy(
            sbuf.at[par, g, _at(peer(d), sl)], rs.at[g, d - 1], rs_s.at[g, d - 1], rs_r.at[g, d - 1],
            device_id=at_peer(d), device_id_type=MESH,
        )

    def send_partial(par, g):
        for d in range(1, chips):
            rs_copy(par, g, d).start()

    def gather_sum(par, g):
        for d in range(1, chips):
            rs_copy(par, g, d).wait_recv()
        total = sbuf[par, g, _at(x, sl)]
        for d in range(1, chips):
            total = total + rs[g, d - 1]
        for d in range(1, chips):
            rs_copy(par, g, d).wait_send()
        return total

    def cols_of(g):
        return pl.ds(g * gcol, gcol)

    def project(par, g, s, ref, first):
        sbuf[par, g] = jnp.zeros((gcol, size), jnp.float32)

        def one(i, carry):
            sbuf[par, g] += _dot_nt(ref[cols_of(g), _at(i, STEP)], cut(s, i))
            return carry

        lax.fori_loop(first, whole, one, 0)

    def ex_wait(g, d, ref):
        there = ref.at[g, _at(peer(chips - d), sl)]
        pltpu.make_async_copy(there, there, ex_r.at[g, d - 1]).wait()

    ys[...] = z_ref[...]
    out_ref[...] = jnp.zeros_like(out_ref)
    lead = 6

    def start(t, carry):
        tick(t)
        return carry

    lax.fori_loop(0, lead, start, 0)
    prefetch(0, True)
    prefetch(1, True)

    def w_copy(g, d):
        mine = wb.at[g, _at(x, sl)]
        return pltpu.make_async_remote_copy(
            mine, mine, ex_s.at[g, d - 1], ex_r.at[g, d - 1], device_id=at_peer(d), device_id_type=MESH
        )

    wait_blk(0)
    for g in range(2):
        project(0, g, 0, ys, top // 2)
        send_partial(0, g)

    def reflect(n, carry):
        j, s = top - n, n % 2
        for g in range(2):
            wb[g, _at(x, sl)] = _dot_nn(gather_sum(0, g), mbuf[s])
            for d in range(1, chips):
                w_copy(g, d).start()

        tick(n + lead)

        @pl.when(j > 0)
        def _():
            wait_blk(n + 1)

        for g in range(2):
            for d in range(1, chips):
                ex_wait(g, d, wb)

            def apply(i, carry, g=g):
                at = cols_of(g), _at(i, STEP)
                ys[at] = ys[at] - _dot_nn(wb[g], cut(s, i))
                return carry

            lax.fori_loop(j // 2, whole, apply, 0)
            for d in range(1, chips):
                w_copy(g, d).wait_send()

            @pl.when(j > 0)
            def _(g=g):
                project(0, g, 1 - s, ys, (j - 1) // 2)
                send_partial(0, g)

        release(n)
        return carry

    lax.fori_loop(0, nb, reflect, 0)
    lax.fori_loop(nb + lead, 2 * per + 5, start, 0)

    first_half = lax.broadcasted_iota(jnp.int32, (gcol, LANES), 1) < EDGE

    def take(ref, g, j):
        lo = ref[cols_of(g), pl.ds(pl.multiple_of((j // 2) * STEP, LANES), LANES)]
        hi = ref[cols_of(g), pl.ds(pl.multiple_of((j // 2) * STEP + LANES, LANES), LANES)]
        even = j % 2 == 0
        return jnp.where(
            first_half,
            jnp.where(even, lo, pltpu.roll(lo, EDGE, 1)),
            jnp.where(even, pltpu.roll(hi, EDGE, 1), hi),
        )

    def spread(val, j):
        even = j % 2 == 0
        other = pltpu.roll(val, EDGE, 1)
        zero = jnp.zeros_like(val)
        lo = jnp.where(even, jnp.where(first_half, val, zero), jnp.where(first_half, zero, other))
        hi = jnp.where(even, jnp.where(first_half, other, zero), jnp.where(first_half, zero, val))
        return jnp.concatenate([lo, hi], axis=1)

    def right_side(par, g, j):
        sbuf[par, g] = -sbuf[par, g]
        sbuf[par, g, :, _at(x, LANES)] += take(ys, g, j)

    def x_copy(g, d):
        return pltpu.make_async_remote_copy(
            wb.at[g, pl.ds(0, sl), _at(peer(d), LANES)], xr.at[g, _at(x, sl)], ex_s.at[g, d - 1], ex_r.at[g, d - 1],
            device_id=at_peer(d), device_id_type=MESH,
        )

    wait_blk(nb)
    for g in range(2):
        sbuf[0, g] = jnp.zeros((gcol, size), jnp.float32)
        right_side(0, g, top)
        send_partial(0, g)

    def solve(i, carry):
        n = nb + i
        j = top - i
        par, nxt = n % 2, (n + 1) % 2

        @pl.when(j > 0)
        def _():
            wait_blk(n + 1)

        for g in range(2):

            @pl.when(j > 0)
            def _(g=g):
                project(nxt, g, nxt, out_ref, (j + 1) // 2)

            wb[g, pl.ds(0, sl)] = _dot_nn(gather_sum(par, g), mbuf[par])
            for d in range(1, chips):
                x_copy(g, d).start()
            xr[g, _at(x, sl)] = wb[g, pl.ds(0, sl), _at(x, LANES)]

        for g in range(2):
            for d in range(1, chips):
                ex_wait(g, d, xr)
            solved = spread(xr[g], j)
            out_ref[cols_of(g), _at(j // 2, STEP)] += solved

            @pl.when(j > 0)
            def _(g=g, solved=solved):
                sbuf[nxt, g] += _dot_nt(solved, cut(nxt, j // 2))
                right_side(nxt, g, j - 1)
                send_partial(nxt, g)

            for d in range(1, chips):
                x_copy(g, d).wait_send()

        release(n)
        return carry

    lax.fori_loop(0, nb, solve, 0)


def _main(own, factors, state, rows, cols):
    _, slots, _, lanes = own.shape
    nb, ncol = lanes // LANES, state.shape[0]
    chips, size, gcol = rows // 2, rows * EDGE, ncol // 2
    sl = gcol // chips
    dma = pltpu.SemaphoreType.DMA
    hbm, vmem = pl.BlockSpec(memory_space=pl.ANY), pl.BlockSpec(memory_space=pltpu.VMEM)
    peers = max(chips - 1, 1)
    gathers = 2 * (slots + 1)
    outs = pl.pallas_call(
        functools.partial(_main_kernel, (rows, cols, slots, nb, ncol)),
        out_shape=[
            jax.ShapeDtypeStruct(state.shape, jnp.float32),
            jax.ShapeDtypeStruct((2, slots, RING, RING, HALF, lanes), jnp.float32),
            jax.ShapeDtypeStruct((2, RING, RING, size // 2, size), jnp.float32),
        ],
        in_specs=[vmem] * 3,
        out_specs=[vmem, hbm, hbm],
        scratch_shapes=[
            pltpu.VMEM((ncol, lanes), jnp.float32),
            pltpu.VMEM((2, rows, EDGE, lanes), jnp.float32),
            pltpu.VMEM((2, size, size), jnp.float32),
            pltpu.VMEM((2, 2, gcol, size), jnp.float32),
            pltpu.VMEM((2, peers, sl, size), jnp.float32),
            pltpu.VMEM((2, gcol, size), jnp.float32),
            pltpu.VMEM((2, gcol, LANES), jnp.float32),
            dma((gathers,)), dma((gathers, 8)), dma((gathers, 8)),
            dma((2, rows)), dma((2, rows)), dma((2, rows)), dma((2,)), dma((2,)), dma((2,)),
            pltpu.SemaphoreType.REGULAR((2,)),
            dma((2, peers)), dma((2, peers)), dma((2, peers)), dma((2, peers)),
        ],
        compiler_params=pltpu.CompilerParams(has_side_effects=True, vmem_limit_bytes=56 * 1024 * 1024),
        name="main",
    )(own, factors, state)
    return outs[0]


def _merge(diag, full):
    two, n, b, _ = diag.shape
    while n > 1:
        pairs = diag.reshape(two, n // 2, 2, b, b)
        d1, d2 = pairs[:, :, 0], pairs[:, :, 1]
        c21 = jnp.stack([full[:, (2 * i + 1) * b : (2 * i + 2) * b, 2 * i * b : (2 * i + 1) * b] for i in range(n // 2)], axis=1)
        mid = jnp.einsum("pnij,pnjk->pnik", d2, c21, precision=PREC_HIGH)
        off = -jnp.einsum("pnij,pnjk->pnik", mid, d1, precision=PREC_HIGH)
        zero = jnp.zeros_like(off)
        diag = jnp.concatenate([jnp.concatenate([d1, zero], axis=3), jnp.concatenate([off, d2], axis=3)], axis=2)
        n, b = n // 2, 2 * b
    return diag[:, 0]


def solution(mesh):
    rows, cols = mesh.shape["row"], mesh.shape["col"]
    mat_spec = P(("kpt", "row"), "col")
    fac_spec = P("kpt", None, None)
    swap = [(r, r + 1 - 2 * (r % 2)) for r in range(rows)]

    def local_work(v_loc, t_loc, z_loc, l_loc):
        size, chips = rows * EDGE, rows // 2
        row, col = lax.axis_index("row"), lax.axis_index("col")
        k = row % 2
        own, state, v_blk, l_diag = _prep(v_loc, l_loc, z_loc, rows, cols)

        vb = v_blk.reshape(size, -1)
        gram = lax.psum(_dot_nt(vb, vb), "row")
        l_blk = lax.dynamic_index_in_dim(l_diag.reshape(size, chips, 2, 2, EDGE), col % 2, 3, keepdims=False)
        l_blk = l_blk.reshape(size, size).T
        t_blk = lax.dynamic_slice_in_dim(t_loc, col * rows, rows, axis=0)
        l_pan = jnp.stack([l_blk[i * EDGE : (i + 1) * EDGE, i * EDGE : (i + 1) * EDGE] for i in range(rows)])
        eye = jnp.broadcast_to(jnp.eye(EDGE, dtype=jnp.float32), l_pan.shape)
        l_inv = lax.linalg.triangular_solve(l_pan, eye, left_side=True, lower=True)
        factors = _merge(jnp.stack([t_blk, l_inv]), jnp.stack([gram, l_blk]))
        mine = lax.dynamic_slice_in_dim(factors, k * (size // 2), size // 2, axis=1)

        x_state = _main(own, mine, state, rows, cols)

        ncol, lanes = x_state.shape
        xs = x_state.reshape(ncol, lanes // STEP, 2, LANES)
        keep = lax.dynamic_index_in_dim(xs, k, 2, keepdims=False).reshape(ncol, lanes // 2)
        send = lax.dynamic_index_in_dim(xs, 1 - k, 2, keepdims=False).reshape(ncol, lanes // 2)
        got = lax.ppermute(send, "row", swap)
        return jnp.concatenate([jnp.where(k == 0, keep, got), jnp.where(k == 0, got, keep)], axis=0).T

    return jax.shard_map(local_work, mesh=mesh, in_specs=(mat_spec, fac_spec, mat_spec, mat_spec), out_specs=mat_spec, check_vma=False)
```

```python
import functools

import jax
import jax.numpy as jnp
from jax import lax
from jax.experimental import pallas as pl
from jax.experimental.pallas import tpu as pltpu
from jax.sharding import PartitionSpec as P

PREC_HIGH = lax.Precision.HIGHEST
MESH = pl.DeviceIdType.MESH
EDGE = 64
HALF = EDGE // 2
LANES = 128
STEP = 256
RING = 4
LEAD = 11


def _dot_nt(a, b):
    return lax.dot_general(a, b, (((1,), (1,)), ((), ())), precision=PREC_HIGH, preferred_element_type=jnp.float32)


def _dot_nn(a, b):
    return lax.dot_general(a, b, (((1,), (0,)), ((), ())), precision=PREC_HIGH, preferred_element_type=jnp.float32)


def _at(i, n):
    return pl.ds(pl.multiple_of(i * n, n), n)


def _loop(lo, hi, body):
    def one(i, carry):
        body(i)
        return carry

    lax.fori_loop(lo, hi, one, 0)


def _gathers(slots):
    early = [(q, 0) for q in range(slots - 1, max(slots - 5, -1), -1)]
    late = [(q, 0) for q in range(slots - 5, -1, -1)]
    rest = [(slots - 1, 1), ("m", 1)] + [(q, 1) for q in range(slots - 2, -1, -1)]
    first = early + [None] * (6 - len(early)) + [("m", 0)] + late
    return first + [None] * (LEAD - len(first)) + rest


def _kernel(dims, v_in, t_in, z_in, l_in, out_ref, gath, mg, *scratch):
    (stage, vt, zt, tb, own, ys, xs, vb, ld, lx, gm, gx, r2, ga, xm, blk, mbuf, sbuf, rs, wb, xr, xf,
     in_sem, swap_l, swap_s, swap_r, v_s, v_r, l_s, l_r, lx_s, lx_r, gx_sem, r2_s, r2_r, ga_s, ga_r, fin_s, fin_r,
     ag_loc, ag_s, ag_r, blk_loc, blk_s, blk_r, mat_loc, mat_s, mat_r, free, rs_s, rs_r, ex_s, ex_r) = scratch
    rows, cols, slots, nb, ncol = dims
    row, col = lax.axis_index("row"), lax.axis_index("col")
    x, k = row // 2, row % 2
    chips, groups = rows // 2, cols // rows
    size, lanes = rows * EDGE, nb * LANES
    hsize = size // 2
    pairs = nb // 2
    gcol = ncol // 2
    sl = gcol // chips
    mate = {"row": row + 1 - 2 * k, "col": col}
    top, whole = nb - 1, nb // 2
    part, grp = col % rows, col // rows
    k_half, m_half = _at(k, HALF), _at(1 - k, HALF)
    s_a, s_b = 1 + (RING - 1) * k, RING - (RING - 1) * k
    a, b = (col // s_a) % RING, (col // s_b) % RING

    def remote(src, dst, ss, rr, to):
        return pltpu.make_async_remote_copy(src, dst, ss, rr, device_id=to, device_id_type=MESH)

    def await_(ref, sem):
        pltpu.make_async_copy(ref, ref, sem).wait()

    def peer(d):
        return lax.rem(x + d, chips)

    def at_peer(d):
        return {"row": 2 * peer(d) + k, "col": col}

    def plane(da, db):
        return {"row": row, "col": lax.rem(a + da, RING) * s_a + lax.rem(b + db, RING) * s_b}

    def low(q):
        return (groups * q // 2) * STEP

    order = _gathers(slots)

    class Slot:
        def __init__(self, kind, w, n):
            self.kind, self.w, self.n = kind, w, n

        def own(self):
            if self.kind == "m":
                return xm.at[self.w, _at(k, hsize)]
            return own.at[self.w, self.kind, :, pl.ds(low(self.kind), lanes - low(self.kind))]

        def piece(self, bb, aa, part=None):
            if self.kind == "m":
                return mg.at[self.w, bb, aa] if part is None else mg.at[self.w, bb, aa, pl.ds(part * (size // 4), size // 4)]
            at = pl.ds(low(self.kind), lanes - low(self.kind))
            e = slice(None) if part is None else pl.ds(part * (HALF // 2), HALF // 2)
            return gath.at[self.w, self.kind, bb, aa, e, at]

        def bundle(self, bb, part=None):
            e = slice(None) if part is None else pl.ds(part * (RING // 2), RING // 2)
            if self.kind == "m":
                return mg.at[self.w, bb, e]
            return gath.at[self.w, self.kind, bb, e, :, pl.ds(low(self.kind), lanes - low(self.kind))]

        def copy(self, i):
            d = 1 if i % 2 == 0 else RING - 1
            back = RING - d
            if i < 2:
                src, dst, to = self.own(), self.piece(b, a), plane(d, 0)
            elif i < 4:
                src = dst = self.piece(b, lax.rem(a + back, RING), i % 2)
                to = plane(d, 0)
            elif i < 6:
                src = dst = self.bundle(b)
                to = plane(0, d)
            else:
                src = dst = self.bundle(lax.rem(b + back, RING), i % 2)
                to = plane(0, d)
            return remote(src, dst, ag_s.at[self.n, i], ag_r.at[self.n, i], to)

        def arrived(self, i):
            back = RING - 1 if i % 2 == 0 else 1
            if i < 2:
                dst = self.piece(b, lax.rem(a + back, RING))
            elif i < 4:
                dst = self.piece(b, lax.rem(a + 2, RING), i % 2)
            elif i < 6:
                dst = self.bundle(lax.rem(b + back, RING))
            else:
                dst = self.bundle(lax.rem(b + 2, RING), i % 2)
            await_(dst, ag_r.at[self.n, i])

        def kept(self):
            return pltpu.make_async_copy(self.own(), self.piece(b, a), ag_loc.at[self.n])

        def stage(self, s):
            if s == 0:
                self.copy(0).start()
                self.copy(1).start()
                self.kept().start()
            elif s == 1:
                for i in range(2):
                    self.arrived(i)
                    self.copy(2 + i).start()
            elif s == 2:
                self.kept().wait()
                self.arrived(2)
                self.arrived(3)
                self.copy(4).start()
                self.copy(5).start()
            elif s == 3:
                for i in range(4, 6):
                    self.arrived(i)
                    self.copy(2 + i).start()
            elif s == 4:
                self.arrived(6)
                self.arrived(7)
            else:
                for i in range(8):
                    self.copy(i).wait_send()

    def tick(t):
        for s in (4, 3, 2, 1, 0, 5):
            n = t - s
            if isinstance(n, int):
                if 0 <= n < len(order) and order[n] is not None:
                    Slot(*order[n], n).stage(s)
                continue
            for kind in list(range(slots)) + ["m"]:
                at_v, at_l = order.index((kind, 0)), order.index((kind, 1))

                @pl.when(jnp.logical_or(n == at_v, n == at_l))
                def _(s=s, n=n, kind=kind, at_l=at_l):
                    Slot(kind, jnp.where(n == at_l, 1, 0), n).stage(s)

    def block_of(n):
        j = top - n % nb
        return n // nb, j, j // groups, j % groups, n % 2

    def blk_copies(n, q, p):
        w, _, _, h, s = block_of(n)
        c = h * rows + p
        at = pl.ds(low(q), lanes - low(q))
        src = gath.at[w, q, (c // s_b) % RING, (c // s_a) % RING, :, at]
        dst = blk.at[s, p, k_half, at]
        return pltpu.make_async_copy(src, dst, blk_loc.at[s, p]), remote(src, dst, blk_s.at[s, p], blk_r.at[s, p], mate)

    def from_mate(n, q, p):
        await_(blk.at[n % 2, p, m_half, pl.ds(low(q), lanes - low(q))], blk_r.at[n % 2, p])

    def mat_copies(n):
        w, j, _, _, s = block_of(n)
        src = mg.at[w, (j // s_b) % RING, (j // s_a) % RING]
        dst = mbuf.at[s, _at(k, hsize)]
        return pltpu.make_async_copy(src, dst, mat_loc.at[s]), remote(src, dst, mat_s.at[s], mat_r.at[s], mate)

    def per_piece(n, act):
        q_now = block_of(n)[2]
        for q in range(slots):

            @pl.when(q_now == q)
            def _(q=q):
                _loop(0, rows, functools.partial(act, q))

    def fetch_blk(n):
        def go(q, p):
            for c in blk_copies(n, q, p):
                c.start()

        per_piece(n, go)

    def fetch_mat(n):
        for c in mat_copies(n):
            c.start()

    def wait_blk(n):
        def one(q, p):
            blk_copies(n, q, p)[0].wait()
            from_mate(n, q, p)

        per_piece(n, one)

    def wait_mat(n):
        mat_copies(n)[0].wait()
        await_(mbuf.at[n % 2, _at(1 - k, hsize)], mat_r.at[n % 2])

    def release(n):
        per_piece(n, lambda q, p: blk_copies(n, q, p)[1].wait_send())
        mat_copies(n)[1].wait_send()

        @pl.when(n + 2 < 2 * nb)
        def _():
            pl.semaphore_signal(free.at[n % 2], inc=1, device_id=mate, device_id_type=MESH)
            pl.semaphore_wait(free.at[n % 2], 1)
            fetch_blk(n + 2)
            fetch_mat(n + 2)

    ins = [
        pltpu.make_async_copy(src, stage.at[i], in_sem.at[i]) for i, src in enumerate((v_in, l_in, z_in))
    ] + [pltpu.make_async_copy(t_in.at[_at(col, rows)], tb, in_sem.at[3])]
    for c in ins:
        c.start()

    def swaps(m, i):
        there = _at(2 * i + k, LANES)
        if m < 2:
            mine, theirs = vt.at[m, :, k, :, _at(i, LANES)], vt.at[m, :, 1 - k, :, _at(i, LANES)]
            dst = own.at[m, :, :, there]
        else:
            mine, theirs = zt.at[k, :, _at(i, LANES)], zt.at[1 - k, :, _at(i, LANES)]
            dst = ys.at[:, there]
        return (
            pltpu.make_async_copy(mine, dst, swap_l.at[m, i]),
            remote(theirs, dst, swap_s.at[m, i], swap_r.at[m, i], mate),
        )

    def arriving(m, i):
        there = _at(2 * i + 1 - k, LANES)
        await_(own.at[m, :, :, there] if m < 2 else ys.at[:, there], swap_r.at[m, i])

    def turn(m):
        ins[m].wait()

        def one(i):
            block = stage[m, _at(i, LANES), :].T
            if m < 2:
                vt[m, :, :, :, _at(i, LANES)] = block.reshape(slots, 2, HALF, LANES)
            else:
                zt[:, :, _at(i, LANES)] = block.reshape(2, ncol, LANES)
            for c in swaps(m, i):
                c.start()

        _loop(0, pairs, one)

    def swapped(m):
        def one(i):
            swaps(m, i)[0].wait()
            arriving(m, i)

        _loop(0, pairs, one)

    width = lanes // 2

    def deal_v(q, kk, act):
        to = groups * q + grp
        src = own.at[0, q, :, pl.ds(kk * width, width)]
        dst = vb.at[part, k_half]
        self_ = jnp.logical_and(to == col, k == kk)
        act(
            self_,
            pltpu.make_async_copy(src, dst, v_r.at[part, k]),
            remote(src, dst, v_s.at[q, kk], v_r.at[part, k], {"col": to, "row": 2 * x + kk}),
        )

    def deal_l(q, kk, act):
        to = groups * q + grp
        src = own.at[1, q, :, _at(to // 2, STEP)]
        dst = ld.at[part, k_half]
        self_ = jnp.logical_and(to == col, k == kk)
        act(
            self_,
            pltpu.make_async_copy(src, dst, l_r.at[part, k]),
            remote(src, dst, l_s.at[q, kk], l_r.at[part, k], {"col": to, "row": 2 * x + kk}),
        )

    def send(self_, here, there):
        pl.when(self_)(here.start)
        pl.when(jnp.logical_not(self_))(there.start)

    def sent(self_, here, there):
        pl.when(jnp.logical_not(self_))(there.wait_send)

    def over_v(act):
        def one(q):
            pl.when(groups * q + grp < nb // 2)(lambda: deal_v(q, 0, act))
            deal_v(q, 1, act)

        _loop(0, slots, one)

    def over_l(act):
        def one(q):
            deal_l(q, 0, act)
            deal_l(q, 1, act)

        _loop(0, slots, one)

    has_v = jnp.logical_or(k == 1, col < nb // 2)

    turn(0)
    swapped(0)
    over_v(send)
    tick(0)
    turn(1)
    tick(1)
    swapped(1)
    over_l(send)
    turn(2)
    tick(2)

    gm[...] = jnp.zeros_like(gm)

    @pl.when(has_v)
    def _():
        def got(n):
            await_(vb.at[n // 2, _at(n % 2, HALF)], v_r.at[n // 2, n % 2])

        _loop(0, 2 * rows, got)

        def chunk(i):
            all_ = vb[:, :, _at(i, STEP)].reshape(size, STEP)
            gm[pl.ds(0, hsize), pl.ds(0, hsize)] += _dot_nt(all_[:hsize], all_[:hsize])
            gm[pl.ds(hsize, hsize), :] += _dot_nt(all_[hsize:], all_)

        _loop(0, width // STEP, chunk)

    mine, theirs = _at(k, hsize), _at(1 - k, hsize)
    to_mate = remote(gm.at[theirs], gx, gx_sem.at[0], gx_sem.at[1], mate)
    to_mate.start()
    tick(3)
    to_mate.wait_recv()
    gm[mine] += gx[...]
    rl = hsize // chips

    def r2_copy(d):
        src = gm.at[pl.ds(pl.multiple_of(k * hsize + peer(d) * rl, rl), rl)]
        return remote(src, r2.at[d - 1], r2_s.at[d - 1], r2_r.at[d - 1], at_peer(d))

    for d in range(1, chips):
        r2_copy(d).start()

    def got_l(n):
        await_(ld.at[n // 2, _at(n % 2, HALF)], l_r.at[n // 2, n % 2])

    _loop(0, 2 * rows, got_l)
    ev = col % 2 == 0
    lo_half = lax.broadcasted_iota(jnp.int32, (size, LANES), 1) < EDGE
    l_lo, l_hi = ld[:, :, pl.ds(0, LANES)].reshape(size, LANES), ld[:, :, pl.ds(LANES, LANES)].reshape(size, LANES)
    lx[x] = jnp.where(
        lo_half,
        jnp.where(ev, l_lo, pltpu.roll(l_lo, EDGE, 1)),
        jnp.where(ev, pltpu.roll(l_hi, EDGE, 1), l_hi),
    )

    def lx_copy(d):
        return remote(lx.at[x], lx.at[x], lx_s.at[d - 1], lx_r.at[d - 1], at_peer(d))

    tick(4)
    for d in range(1, chips):
        r2_copy(d).wait_recv()
    my_rows = pl.ds(pl.multiple_of(k * hsize + x * rl, rl), rl)
    total = gm[my_rows]
    for d in range(1, chips):
        total = total + r2[d - 1]
    ga[my_rows] = total

    def ga_copy(d):
        return remote(ga.at[my_rows], ga.at[my_rows], ga_s.at[d - 1], ga_r.at[d - 1], at_peer(d))

    for d in range(1, chips):
        ga_copy(d).start()
    for d in range(1, chips):
        lx_copy(d).start()
    tick(5)
    for d in range(1, chips):
        await_(ga.at[pl.ds(pl.multiple_of(k * hsize + peer(chips - d) * rl, rl), rl)], ga_r.at[d - 1])
    half_to_mate = remote(ga.at[mine], ga.at[mine], gx_sem.at[2], gx_sem.at[3], mate)
    half_to_mate.start()

    n128 = size // LANES
    r_i = lax.broadcasted_iota(jnp.int32, (LANES, LANES), 0)
    c_i = lax.broadcasted_iota(jnp.int32, (LANES, LANES), 1)

    def tile(i):
        return _at(i, LANES), _at(i, LANES)

    def level_small(w, c_ref, lev):
        pick = jnp.logical_and(
            lax.shift_right_logical(r_i, lev) % 2 == 1,
            lax.shift_right_logical(c_i, lev) + 1 == lax.shift_right_logical(r_i, lev),
        )

        def one(i):
            at = tile(i)
            cur = xm[(w, *at)]
            low_part = jnp.where(pick, c_ref[at], 0.0)
            xm[(w, *at)] = cur - _dot_nn(_dot_nn(cur, low_part), cur)

        _loop(0, n128, one)

    def level_big(w, c_ref):
        width_ = LANES
        while width_ < size:
            for i in range(size // (2 * width_)):
                d1 = pl.ds(2 * i * width_, width_)
                d2 = pl.ds((2 * i + 1) * width_, width_)
                xm[w, d2, d1] = -_dot_nn(_dot_nn(xm[w, d2, d2], c_ref[d2, d1]), xm[w, d1, d1])
            width_ *= 2

    xm[...] = jnp.zeros_like(xm)
    ins[3].wait()
    for p in range(0, rows, 2):
        zero = jnp.zeros((EDGE, EDGE), jnp.float32)
        both = jnp.concatenate(
            [jnp.concatenate([tb[p], zero], axis=1), jnp.concatenate([zero, tb[p + 1]], axis=1)], axis=0
        )
        xm[0, pl.ds(p * EDGE, LANES), pl.ds(p * EDGE, LANES)] = both
    await_(ga.at[theirs], gx_sem.at[3])
    level_small(0, ga, 6)
    level_big(0, ga)
    tick(6)

    fetch_blk(0)
    fetch_blk(1)
    for d in range(1, chips):
        await_(lx.at[peer(chips - d)], lx_r.at[d - 1])
    to_mate.wait_send()
    for d in range(1, chips):
        r2_copy(d).wait_send()
    for i in range(chips):
        gm[_at(i, LANES), :] = lx[i].T
    same = r_i == c_i

    def diag(i):
        d = gm[tile(i)]
        xm[(1, *tile(i))] = jnp.where(same, 1.0 / jnp.where(same, d, 1.0), 0.0)

    _loop(0, n128, diag)
    swapped(2)
    tick(7)
    _loop(0, 3, lambda i: level_small(1, gm, i))
    tick(8)
    _loop(3, 7, lambda i: level_small(1, gm, i))
    tick(9)
    level_big(1, gm)
    tick(10)
    fetch_mat(0)
    fetch_mat(1)

    def cut(s, i):
        return blk[s, :, :, _at(i, STEP)].reshape(size, STEP)

    def rs_copy(par, g, d):
        return remote(sbuf.at[par, g, _at(peer(d), sl)], rs.at[g, d - 1], rs_s.at[g, d - 1], rs_r.at[g, d - 1], at_peer(d))

    def send_partial(par, g):
        for d in range(1, chips):
            rs_copy(par, g, d).start()

    def gather_sum(par, g):
        for d in range(1, chips):
            rs_copy(par, g, d).wait_recv()
        total = sbuf[par, g, _at(x, sl)]
        for d in range(1, chips):
            total = total + rs[g, d - 1]
        for d in range(1, chips):
            rs_copy(par, g, d).wait_send()
        return total

    def cols_of(g):
        return pl.ds(g * gcol, gcol)

    def project(par, g, s, ref, first):
        sbuf[par, g] = jnp.zeros((gcol, size), jnp.float32)

        def one(i):
            sbuf[par, g] += _dot_nt(ref[cols_of(g), _at(i, STEP)], cut(s, i))

        _loop(first, whole, one)

    def ex_wait(g, d, ref):
        await_(ref.at[g, _at(peer(chips - d), sl)], ex_r.at[g, d - 1])

    def w_copy(g, d):
        mine = wb.at[g, _at(x, sl)]
        return remote(mine, mine, ex_s.at[g, d - 1], ex_r.at[g, d - 1], at_peer(d))

    wait_blk(0)
    for g in range(2):
        project(0, g, 0, ys, top // 2)
        send_partial(0, g)
    wait_mat(0)

    def reflect(n):
        j, s = top - n, n % 2
        for g in range(2):
            wb[g, _at(x, sl)] = _dot_nn(gather_sum(0, g), mbuf[s])
            for d in range(1, chips):
                w_copy(g, d).start()

        @pl.when(s == 0)
        def _():
            tick(LEAD + n // 2)

        @pl.when(j > 0)
        def _():
            wait_blk(n + 1)
            wait_mat(n + 1)

        for g in range(2):
            for d in range(1, chips):
                ex_wait(g, d, wb)

            def apply(i, g=g):
                at = cols_of(g), _at(i, STEP)
                ys[at] = ys[at] - _dot_nn(wb[g], cut(s, i))

            _loop(j // 2, whole, apply)
            for d in range(1, chips):
                w_copy(g, d).wait_send()

            @pl.when(j > 0)
            def _(g=g):
                project(0, g, 1 - s, ys, (j - 1) // 2)
                send_partial(0, g)

        release(n)

    _loop(0, nb, reflect)

    xs[...] = jnp.zeros_like(xs)
    first_half = lax.broadcasted_iota(jnp.int32, (gcol, LANES), 1) < EDGE

    def take(ref, g, j):
        lo = ref[cols_of(g), pl.ds(pl.multiple_of((j // 2) * STEP, LANES), LANES)]
        hi = ref[cols_of(g), pl.ds(pl.multiple_of((j // 2) * STEP + LANES, LANES), LANES)]
        even = j % 2 == 0
        return jnp.where(
            first_half,
            jnp.where(even, lo, pltpu.roll(lo, EDGE, 1)),
            jnp.where(even, pltpu.roll(hi, EDGE, 1), hi),
        )

    def spread(val, j):
        even = j % 2 == 0
        other = pltpu.roll(val, EDGE, 1)
        zero = jnp.zeros_like(val)
        lo = jnp.where(even, jnp.where(first_half, val, zero), jnp.where(first_half, zero, other))
        hi = jnp.where(even, jnp.where(first_half, other, zero), jnp.where(first_half, zero, val))
        return jnp.concatenate([lo, hi], axis=1)

    def right_side(par, g, j):
        sbuf[par, g] = -sbuf[par, g]
        sbuf[par, g, :, _at(x, LANES)] += take(ys, g, j)

    def x_copy(g, d):
        src = wb.at[g, pl.ds(0, sl), _at(peer(d), LANES)]
        return remote(src, xr.at[g, _at(x, sl)], ex_s.at[g, d - 1], ex_r.at[g, d - 1], at_peer(d))

    wait_blk(nb)
    wait_mat(nb)
    for g in range(2):
        sbuf[0, g] = jnp.zeros((gcol, size), jnp.float32)
        right_side(0, g, top)
        send_partial(0, g)

    def solve(i):
        n = nb + i
        j = top - i
        par, nxt = n % 2, (n + 1) % 2

        @pl.when(j > 0)
        def _():
            wait_blk(n + 1)
            wait_mat(n + 1)

        for g in range(2):

            @pl.when(j > 0)
            def _(g=g):
                project(nxt, g, nxt, xs, (j + 1) // 2)

            wb[g, pl.ds(0, sl)] = _dot_nn(gather_sum(par, g), mbuf[par])
            for d in range(1, chips):
                x_copy(g, d).start()
            xr[g, _at(x, sl)] = wb[g, pl.ds(0, sl), _at(x, LANES)]

        @pl.when(par == 0)
        def _():
            tick(LEAD + n // 2)

        for g in range(2):
            for d in range(1, chips):
                ex_wait(g, d, xr)
            solved = spread(xr[g], j)
            xs[cols_of(g), _at(j // 2, STEP)] += solved

            @pl.when(j > 0)
            def _(g=g, solved=solved):
                sbuf[nxt, g] += _dot_nt(solved, cut(nxt, j // 2))
                right_side(nxt, g, j - 1)
                send_partial(nxt, g)

            for d in range(1, chips):
                x_copy(g, d).wait_send()

        release(n)

    _loop(0, nb, solve)

    def fin_copy(i):
        return remote(
            xs.at[:, _at(2 * i + 1 - k, LANES)], xf.at[_at(k, ncol), _at(i, LANES)], fin_s.at[i], fin_r.at[i], mate
        )

    _loop(0, pairs, lambda i: fin_copy(i).start())

    def own_cols(i):
        xf[_at(k, ncol), _at(i, LANES)] = xs[:, _at(2 * i + k, LANES)]

    _loop(0, pairs, own_cols)

    def give(i):
        await_(xf.at[_at(1 - k, ncol), _at(i, LANES)], fin_r.at[i])
        out_ref[_at(i, LANES), :] = xf[:, _at(i, LANES)].T

    _loop(0, pairs, give)

    _loop(0, pairs, lambda i: fin_copy(i).wait_send())
    for m in range(3):
        _loop(0, pairs, lambda i, m=m: swaps(m, i)[1].wait_send())
    over_v(sent)
    over_l(sent)
    half_to_mate.wait_send()
    for d in range(1, chips):
        ga_copy(d).wait_send()
        lx_copy(d).wait_send()


def solution(mesh):
    rows, cols = mesh.shape["row"], mesh.shape["col"]
    mat_spec = P(("kpt", "row"), "col")
    fac_spec = P("kpt", None, None)

    def local_work(v_loc, t_loc, z_loc, l_loc):
        n_row, n_col = v_loc.shape
        slots, lanes, chips, size = n_col // EDGE, 2 * n_row, rows // 2, rows * EDGE
        nb, ncol = lanes // LANES, z_loc.shape[1] // 2
        pairs, gcol, peers = nb // 2, ncol // 2, max(chips - 1, 1)
        sl, gathers = gcol // chips, len(_gathers(slots))
        dma = pltpu.SemaphoreType.DMA
        hbm, vmem = pl.BlockSpec(memory_space=pl.ANY), pl.BlockSpec(memory_space=pltpu.VMEM)

        def buf(*shape):
            return pltpu.VMEM(shape, jnp.float32)

        return pl.pallas_call(
            functools.partial(_kernel, (rows, cols, slots, nb, ncol)),
            out_shape=[
                jax.ShapeDtypeStruct(z_loc.shape, jnp.float32),
                jax.ShapeDtypeStruct((2, slots, RING, RING, HALF, lanes), jnp.float32),
                jax.ShapeDtypeStruct((2, RING, RING, size // 2, size), jnp.float32),
            ],
            in_specs=[hbm] * 4,
            out_specs=[vmem, hbm, hbm],
            scratch_shapes=[
                buf(3, n_row, n_col),
                buf(2, slots, 2, HALF, n_row),
                buf(2, ncol, n_row),
                buf(rows, EDGE, EDGE),
                buf(2, slots, HALF, lanes),
                buf(ncol, lanes),
                buf(ncol, lanes),
                buf(rows, EDGE, lanes // 2),
                buf(rows, EDGE, STEP),
                buf(chips, size, LANES),
                buf(size, size),
                buf(size // 2, size),
                buf(peers, size // 2 // chips, size),
                buf(size, size),
                buf(2, size, size),
                buf(2, rows, EDGE, lanes),
                buf(2, size, size),
                buf(2, 2, gcol, size),
                buf(2, peers, sl, size),
                buf(2, gcol, size),
                buf(2, gcol, LANES),
                buf(2 * ncol, n_row),
                dma((4,)),
                dma((3, pairs)), dma((3, pairs)), dma((3, pairs)),
                dma((slots, 2)), dma((rows, 2)),
                dma((slots, 2)), dma((rows, 2)),
                dma((peers,)), dma((peers,)),
                dma((4,)),
                dma((peers,)), dma((peers,)), dma((peers,)), dma((peers,)),
                dma((pairs,)), dma((pairs,)),
                dma((gathers,)), dma((gathers, 8)), dma((gathers, 8)),
                dma((2, rows)), dma((2, rows)), dma((2, rows)),
                dma((2,)), dma((2,)), dma((2,)),
                pltpu.SemaphoreType.REGULAR((2,)),
                dma((2, peers)), dma((2, peers)), dma((2, peers)), dma((2, peers)),
            ],
            compiler_params=pltpu.CompilerParams(has_side_effects=True, vmem_limit_bytes=60 * 1024 * 1024),
            name="eigvec",
        )(v_loc, t_loc, z_loc, l_loc)[0]

    return jax.shard_map(local_work, mesh=mesh, in_specs=(mat_spec, fac_spec, mat_spec, mat_spec), out_specs=mat_spec, check_vma=False)
```

```python
import functools

import jax
import jax.numpy as jnp
from jax import lax
from jax.experimental import pallas as pl
from jax.experimental.pallas import tpu as pltpu
from jax.sharding import PartitionSpec as P

PREC_HIGH = lax.Precision.HIGHEST
MESH = pl.DeviceIdType.MESH
EDGE = 64
HALF = EDGE // 2
LANES = 128
STEP = 256
RING = 4
LEAD = 9


def _dot_nt(a, b):
    return lax.dot_general(a, b, (((1,), (1,)), ((), ())), precision=PREC_HIGH, preferred_element_type=jnp.float32)


def _dot_nn(a, b):
    return lax.dot_general(a, b, (((1,), (0,)), ((), ())), precision=PREC_HIGH, preferred_element_type=jnp.float32)


def _at(i, n):
    return pl.ds(pl.multiple_of(i * n, n), n)


def _loop(lo, hi, body):
    def one(i, carry):
        body(i)
        return carry

    lax.fori_loop(lo, hi, one, 0)


def _gathers(slots):
    early = [(slots - 1, 0), (slots - 2, 0), None, None, ("m", 0)]
    first = early + [(q, 0) for q in range(slots - 3, -1, -1)]
    rest = [(slots - 1, 1), ("m", 1)] + [(q, 1) for q in range(slots - 2, -1, -1)]
    return first + [None] * (LEAD - len(first)) + rest


def _kernel(dims, v_in, t_in, z_in, l_in, out_ref, gath, *scratch):
    (stage, vt, zt, tb, own, ys, xs, vb, ld, lx, gm, pk, gx, r2, ga, xm, pm, mg, blk, mbuf, sbuf, rs, wb, xr,
     in_sem, swap_l, swap_s, swap_r, v_s, v_r, l_s, l_r, lx_s, lx_r, gx_sem, r2_s, r2_r, ga_s, ga_r, fin_s, fin_r,
     ag_loc, ag_s, ag_r, blk_loc, blk_s, blk_r, mat_loc, mat_s, mat_r, free, rs_s, rs_r, ex_s, ex_r) = scratch
    rows, cols, slots, nb, ncol = dims
    row, col = lax.axis_index("row"), lax.axis_index("col")
    x, k = row // 2, row % 2
    chips, groups = rows // 2, cols // rows
    size, lanes = rows * EDGE, nb * LANES
    hsize, qsize, n128 = size // 2, size // 4, size // LANES
    pairs = nb // 2
    gcol = ncol // 2
    sl = gcol // chips
    mate = {"row": row + 1 - 2 * k, "col": col}
    top, whole = nb - 1, nb // 2
    part, grp = col % rows, col // rows
    k_half, m_half = _at(k, HALF), _at(1 - k, HALF)
    s_a, s_b = 1 + (RING - 1) * k, RING - (RING - 1) * k
    a, b = (col // s_a) % RING, (col // s_b) % RING

    def remote(src, dst, ss, rr, to):
        return pltpu.make_async_remote_copy(src, dst, ss, rr, device_id=to, device_id_type=MESH)

    def await_(ref, sem):
        pltpu.make_async_copy(ref, ref, sem).wait()

    def peer(d):
        return lax.rem(x + d, chips)

    def at_peer(d):
        return {"row": 2 * peer(d) + k, "col": col}

    def plane(da, db):
        return {"row": row, "col": lax.rem(a + da, RING) * s_a + lax.rem(b + db, RING) * s_b}

    def low(q):
        return (groups * q // 2) * STEP

    order = _gathers(slots)

    class Slot:
        def __init__(self, kind, w, n):
            self.kind, self.w, self.n = kind, w, n

        def own(self):
            if self.kind == "m":
                return pm.at[self.w]
            return own.at[self.w, self.kind, :, pl.ds(low(self.kind), lanes - low(self.kind))]

        def piece(self, bb, aa, part=None):
            if self.kind == "m":
                return mg.at[self.w, bb, aa] if part is None else mg.at[self.w, bb, aa, pl.ds(part * HALF, HALF)]
            at = pl.ds(low(self.kind), lanes - low(self.kind))
            e = slice(None) if part is None else pl.ds(part * (HALF // 2), HALF // 2)
            return gath.at[self.w, self.kind, bb, aa, e, at]

        def bundle(self, bb, part=None):
            e = slice(None) if part is None else pl.ds(part * (RING // 2), RING // 2)
            if self.kind == "m":
                return mg.at[self.w, bb, e]
            return gath.at[self.w, self.kind, bb, e, :, pl.ds(low(self.kind), lanes - low(self.kind))]

        def copy(self, i):
            d = 1 if i % 2 == 0 else RING - 1
            back = RING - d
            if i < 2:
                src, dst, to = self.own(), self.piece(b, a), plane(d, 0)
            elif i < 4:
                src = dst = self.piece(b, lax.rem(a + back, RING), i % 2)
                to = plane(d, 0)
            elif i < 6:
                src = dst = self.bundle(b)
                to = plane(0, d)
            else:
                src = dst = self.bundle(lax.rem(b + back, RING), i % 2)
                to = plane(0, d)
            return remote(src, dst, ag_s.at[self.n, i], ag_r.at[self.n, i], to)

        def arrived(self, i):
            back = RING - 1 if i % 2 == 0 else 1
            if i < 2:
                dst = self.piece(b, lax.rem(a + back, RING))
            elif i < 4:
                dst = self.piece(b, lax.rem(a + 2, RING), i % 2)
            elif i < 6:
                dst = self.bundle(lax.rem(b + back, RING))
            else:
                dst = self.bundle(lax.rem(b + 2, RING), i % 2)
            await_(dst, ag_r.at[self.n, i])

        def kept(self):
            return pltpu.make_async_copy(self.own(), self.piece(b, a), ag_loc.at[self.n])

        def stage(self, s):
            if s == 0:
                self.copy(0).start()
                self.copy(1).start()
                self.kept().start()
            elif s == 1:
                for i in range(2):
                    self.arrived(i)
                    self.copy(2 + i).start()
            elif s == 2:
                self.kept().wait()
                self.arrived(2)
                self.arrived(3)
                self.copy(4).start()
                self.copy(5).start()
            elif s == 3:
                for i in range(4, 6):
                    self.arrived(i)
                    self.copy(2 + i).start()
            elif s == 4:
                self.arrived(6)
                self.arrived(7)
            else:
                for i in range(8):
                    self.copy(i).wait_send()

    def tick(t):
        for s in (4, 3, 2, 1, 0, 5):
            n = t - s
            if isinstance(n, int):
                if 0 <= n < len(order) and order[n] is not None:
                    Slot(*order[n], n).stage(s)
                continue
            for kind in list(range(slots)) + ["m"]:
                at_v, at_l = order.index((kind, 0)), order.index((kind, 1))

                @pl.when(jnp.logical_or(n == at_v, n == at_l))
                def _(s=s, n=n, kind=kind, at_l=at_l):
                    Slot(kind, jnp.where(n == at_l, 1, 0), n).stage(s)

    def block_of(n):
        j = top - n % nb
        return n // nb, j, j // groups, j % groups, n % 2

    def blk_copies(n, q, p):
        w, _, _, h, s = block_of(n)
        c = h * rows + p
        at = pl.ds(low(q), lanes - low(q))
        src = gath.at[w, q, (c // s_b) % RING, (c // s_a) % RING, :, at]
        dst = blk.at[s, p, k_half, at]
        return pltpu.make_async_copy(src, dst, blk_loc.at[s, p]), remote(src, dst, blk_s.at[s, p], blk_r.at[s, p], mate)

    def from_mate(n, q, p):
        await_(blk.at[n % 2, p, m_half, pl.ds(low(q), lanes - low(q))], blk_r.at[n % 2, p])

    def mat_copies(n, i):
        w, j, q, h, s = block_of(n)
        c = h * rows + q
        src = mg.at[w, (c // s_b) % RING, (c // s_a) % RING, :, pl.ds(LANES * (i * (i + 1) // 2), LANES * (i + 1))]
        dst = mbuf.at[s, pl.ds(pl.multiple_of(i * LANES + k * EDGE, EDGE), EDGE), pl.ds(0, LANES * (i + 1))]
        return (
            pltpu.make_async_copy(src, dst, mat_loc.at[s, i]),
            remote(src, dst, mat_s.at[s, i], mat_r.at[s, i], mate),
        )

    def per_piece(n, act):
        q_now = block_of(n)[2]
        for q in range(slots):

            @pl.when(q_now == q)
            def _(q=q):
                _loop(0, rows, functools.partial(act, q))

    def fetch_blk(n):
        def go(q, p):
            for c in blk_copies(n, q, p):
                c.start()

        per_piece(n, go)

    def fetch_mat(n):
        for i in range(n128):
            for c in mat_copies(n, i):
                c.start()

    def wait_blk(n):
        def one(q, p):
            blk_copies(n, q, p)[0].wait()
            from_mate(n, q, p)

        per_piece(n, one)

    def wait_mat(n):
        for i in range(n128):
            mat_copies(n, i)[0].wait()
            there = pl.ds(pl.multiple_of(i * LANES + (1 - k) * EDGE, EDGE), EDGE), pl.ds(0, LANES * (i + 1))
            await_(mbuf.at[(n % 2, *there)], mat_r.at[n % 2, i])

    def release(n):
        per_piece(n, lambda q, p: blk_copies(n, q, p)[1].wait_send())
        for i in range(n128):
            mat_copies(n, i)[1].wait_send()

        @pl.when(n + 2 < 2 * nb)
        def _():
            pl.semaphore_signal(free.at[n % 2], inc=1, device_id=mate, device_id_type=MESH)
            pl.semaphore_wait(free.at[n % 2], 1)
            fetch_blk(n + 2)
            fetch_mat(n + 2)

    ins = [
        pltpu.make_async_copy(src, stage.at[i], in_sem.at[i]) for i, src in enumerate((v_in, l_in, z_in))
    ] + [pltpu.make_async_copy(t_in.at[_at(groups * part + grp, rows)], tb, in_sem.at[3])]
    for c in ins:
        c.start()

    def swaps(m, i):
        there = _at(2 * i + k, LANES)
        if m < 2:
            mine, theirs = vt.at[m, :, k, :, _at(i, LANES)], vt.at[m, :, 1 - k, :, _at(i, LANES)]
            dst = own.at[m, :, :, there]
        else:
            mine, theirs = zt.at[k, :, _at(i, LANES)], zt.at[1 - k, :, _at(i, LANES)]
            dst = ys.at[:, there]
        return (
            pltpu.make_async_copy(mine, dst, swap_l.at[m, i]),
            remote(theirs, dst, swap_s.at[m, i], swap_r.at[m, i], mate),
        )

    def arriving(m, i):
        there = _at(2 * i + 1 - k, LANES)
        await_(own.at[m, :, :, there] if m < 2 else ys.at[:, there], swap_r.at[m, i])

    def turn(m):
        ins[m].wait()

        def one(i):
            block = stage[m, _at(i, LANES), :].T
            if m < 2:
                vt[m, :, :, :, _at(i, LANES)] = block.reshape(slots, 2, HALF, LANES)
            else:
                zt[:, :, _at(i, LANES)] = block.reshape(2, ncol, LANES)
            for c in swaps(m, i):
                c.start()

        _loop(0, pairs, one)

    def swapped(m):
        def one(i):
            swaps(m, i)[0].wait()
            arriving(m, i)

        _loop(0, pairs, one)

    my_q, my_h = part, grp
    my_j = groups * my_q + my_h
    first_t = my_j // 2

    def deal_v(q, t, act):
        to, kk = grp * rows + q, t % 2
        src = own.at[0, q, :, _at(t, STEP)]
        dst = vb.at[t // 2, part, k_half]
        self_ = jnp.logical_and(to == col, k == kk)
        act(
            self_,
            pltpu.make_async_copy(src, dst, v_r.at[t // 2, part, k]),
            remote(src, dst, v_s.at[q, t], v_r.at[t // 2, part, k], {"col": to, "row": 2 * x + kk}),
        )

    def deal_l(q, kk, act):
        to = grp * rows + q
        src = own.at[1, q, :, _at((groups * q + grp) // 2, STEP)]
        dst = ld.at[part, k_half]
        self_ = jnp.logical_and(to == col, k == kk)
        act(
            self_,
            pltpu.make_async_copy(src, dst, l_r.at[part, k]),
            remote(src, dst, l_s.at[q, kk], l_r.at[part, k], {"col": to, "row": 2 * x + kk}),
        )

    def send(self_, here, there):
        pl.when(self_)(here.start)
        pl.when(jnp.logical_not(self_))(there.start)

    def sent(self_, here, there):
        pl.when(jnp.logical_not(self_))(there.wait_send)

    def over_v(act):
        def one(q):
            _loop((groups * q + grp) // 2, pairs, lambda t: deal_v(q, t, act))

        _loop(0, slots, one)

    def over_l(act):
        def one(q):
            deal_l(q, 0, act)
            deal_l(q, 1, act)

        _loop(0, slots, one)

    turn(0)
    swapped(0)
    over_v(send)
    turn(1)
    swapped(1)
    over_l(send)
    turn(2)
    mbuf[...] = jnp.zeros_like(mbuf)

    gm[...] = jnp.zeros_like(gm)

    def chunk(i):
        def got(n):
            await_(vb.at[i, n // 2, _at(n % 2, HALF)], v_r.at[i, n // 2, n % 2])

        _loop(0, 2 * rows, got)
        all_ = vb[i].reshape(size, STEP)
        gm[pl.ds(0, hsize), pl.ds(0, hsize)] += _dot_nt(all_[:hsize], all_[:hsize])
        gm[pl.ds(hsize, hsize), :] += _dot_nt(all_[hsize:], all_)

    _loop((first_t + 1 - k) // 2, pairs // 2, chunk)
    tick(0)

    widths = []
    w_ = hsize
    while w_ >= EDGE:
        widths.append(w_)
        w_ //= 2

    def packed(w_):
        return pl.ds(size - 2 * w_, w_)

    pk[...] = jnp.zeros_like(pk)
    for w_ in widths:
        for i in range(hsize // w_):
            pk[pl.ds(i * w_, w_), packed(w_)] = gm[pl.ds((2 * i + 1) * w_, w_), pl.ds(2 * i * w_, w_)]

    mine, theirs = _at(k, qsize), _at(1 - k, qsize)
    to_mate = remote(pk.at[theirs], gx, gx_sem.at[0], gx_sem.at[1], mate)
    to_mate.start()
    tick(1)
    to_mate.wait_recv()
    pk[mine] += gx[...]
    rl = qsize // chips

    def r2_copy(d):
        src = pk.at[pl.ds(pl.multiple_of(k * qsize + peer(d) * rl, rl), rl)]
        return remote(src, r2.at[d - 1], r2_s.at[d - 1], r2_r.at[d - 1], at_peer(d))

    for d in range(1, chips):
        r2_copy(d).start()

    def got_l(n):
        await_(ld.at[n // 2, _at(n % 2, HALF)], l_r.at[n // 2, n % 2])

    _loop(0, 2 * rows, got_l)
    ev = my_j % 2 == 0
    lo_half = lax.broadcasted_iota(jnp.int32, (size, LANES), 1) < EDGE
    l_lo, l_hi = ld[:, :, pl.ds(0, LANES)].reshape(size, LANES), ld[:, :, pl.ds(LANES, LANES)].reshape(size, LANES)
    lx[x] = jnp.where(
        lo_half,
        jnp.where(ev, l_lo, pltpu.roll(l_lo, EDGE, 1)),
        jnp.where(ev, pltpu.roll(l_hi, EDGE, 1), l_hi),
    )

    def lx_copy(d):
        return remote(lx.at[x], lx.at[x], lx_s.at[d - 1], lx_r.at[d - 1], at_peer(d))

    tick(2)
    for d in range(1, chips):
        r2_copy(d).wait_recv()
    my_rows = pl.ds(pl.multiple_of(k * qsize + x * rl, rl), rl)
    total = pk[my_rows]
    for d in range(1, chips):
        total = total + r2[d - 1]
    ga[my_rows] = total

    def ga_copy(d):
        return remote(ga.at[my_rows], ga.at[my_rows], ga_s.at[d - 1], ga_r.at[d - 1], at_peer(d))

    for d in range(1, chips):
        ga_copy(d).start()
    for d in range(1, chips):
        lx_copy(d).start()
    tick(3)
    for d in range(1, chips):
        await_(ga.at[pl.ds(pl.multiple_of(k * qsize + peer(chips - d) * rl, rl), rl)], ga_r.at[d - 1])
    half_to_mate = remote(ga.at[mine], ga.at[mine], gx_sem.at[2], gx_sem.at[3], mate)
    half_to_mate.start()

    r_i = lax.broadcasted_iota(jnp.int32, (LANES, LANES), 0)
    c_i = lax.broadcasted_iota(jnp.int32, (LANES, LANES), 1)

    def tile(i):
        return _at(i, LANES), _at(i, LANES)

    def merge_tile(w, i, low_part):
        cur = xm[(w, *tile(i))]
        xm[(w, *tile(i))] = cur - _dot_nn(_dot_nn(cur, low_part), cur)

    def level_l(lev):
        pick = jnp.logical_and(
            lax.shift_right_logical(r_i, lev) % 2 == 1,
            lax.shift_right_logical(c_i, lev) + 1 == lax.shift_right_logical(r_i, lev),
        )
        _loop(0, n128, lambda i: merge_tile(1, i, jnp.where(pick, gm[tile(i)], 0.0)))

    def level_big(w, corner):
        for w_ in reversed(widths[:-1]):
            for i in range(hsize // w_):
                d1 = pl.ds(2 * i * w_, w_)
                d2 = pl.ds((2 * i + 1) * w_, w_)
                xm[w, d2, d1] = -_dot_nn(_dot_nn(xm[w, d2, d2], corner(w_, i)), xm[w, d1, d1])

    def pack_factor(w):
        for i in range(n128):
            pm[w, :, pl.ds(LANES * (i * (i + 1) // 2), LANES * (i + 1))] = xm[
                w, pl.ds(pl.multiple_of(i * LANES + k * EDGE, EDGE), EDGE), pl.ds(0, LANES * (i + 1))
            ]

    xm[...] = jnp.zeros_like(xm)
    ins[3].wait()
    for p in range(0, rows, 2):
        zero = jnp.zeros((EDGE, EDGE), jnp.float32)
        both = jnp.concatenate(
            [jnp.concatenate([tb[p], zero], axis=1), jnp.concatenate([zero, tb[p + 1]], axis=1)], axis=0
        )
        xm[0, pl.ds(p * EDGE, LANES), pl.ds(p * EDGE, LANES)] = both
    await_(ga.at[theirs], gx_sem.at[3])

    def corner64(i):
        block = ga[_at(i, EDGE), packed(EDGE)]
        zero = jnp.zeros((EDGE, EDGE), jnp.float32)
        low_part = jnp.concatenate([block, zero], axis=1)
        merge_tile(0, i, jnp.concatenate([jnp.zeros_like(low_part), low_part], axis=0))

    _loop(0, n128, corner64)
    level_big(0, lambda w_, i: ga[pl.ds(i * w_, w_), packed(w_)])
    pack_factor(0)
    tick(4)

    fetch_blk(0)
    fetch_blk(1)
    for d in range(1, chips):
        await_(lx.at[peer(chips - d)], lx_r.at[d - 1])
    for i in range(chips):
        gm[_at(i, LANES), :] = lx[i].T
    same = r_i == c_i

    def diag(i):
        d = gm[tile(i)]
        xm[(1, *tile(i))] = jnp.where(same, 1.0 / jnp.where(same, d, 1.0), 0.0)

    _loop(0, n128, diag)
    swapped(2)
    tick(5)
    _loop(0, 3, level_l)
    tick(6)
    _loop(3, 7, level_l)
    tick(7)
    level_big(1, lambda w_, i: gm[pl.ds((2 * i + 1) * w_, w_), pl.ds(2 * i * w_, w_)])
    pack_factor(1)
    tick(8)
    fetch_mat(0)
    fetch_mat(1)

    def cut(s, i):
        return blk[s, :, :, _at(i, STEP)].reshape(size, STEP)

    def rs_copy(par, g, d):
        return remote(sbuf.at[par, g, _at(peer(d), sl)], rs.at[g, d - 1], rs_s.at[g, d - 1], rs_r.at[g, d - 1], at_peer(d))

    def send_partial(par, g):
        for d in range(1, chips):
            rs_copy(par, g, d).start()

    def gather_sum(par, g):
        for d in range(1, chips):
            rs_copy(par, g, d).wait_recv()
        total = sbuf[par, g, _at(x, sl)]
        for d in range(1, chips):
            total = total + rs[g, d - 1]
        for d in range(1, chips):
            rs_copy(par, g, d).wait_send()
        return total

    def cols_of(g):
        return pl.ds(g * gcol, gcol)

    def project(par, g, s, ref, first):
        sbuf[par, g] = jnp.zeros((gcol, size), jnp.float32)

        def one(i):
            sbuf[par, g] += _dot_nt(ref[cols_of(g), _at(i, STEP)], cut(s, i))

        _loop(first, whole, one)

    def ex_wait(g, d, ref):
        await_(ref.at[g, _at(peer(chips - d), sl)], ex_r.at[g, d - 1])

    def w_copy(g, d):
        mine = wb.at[g, _at(x, sl)]
        return remote(mine, mine, ex_s.at[g, d - 1], ex_r.at[g, d - 1], at_peer(d))

    wait_blk(0)
    for g in range(2):
        project(0, g, 0, ys, top // 2)
        send_partial(0, g)
    wait_mat(0)

    def reflect(n):
        j, s = top - n, n % 2
        for g in range(2):
            wb[g, _at(x, sl)] = _dot_nn(gather_sum(0, g), mbuf[s])
            for d in range(1, chips):
                w_copy(g, d).start()

        @pl.when(s == 0)
        def _():
            tick(LEAD + n // 2)

        @pl.when(j > 0)
        def _():
            wait_blk(n + 1)
            wait_mat(n + 1)

        for g in range(2):
            for d in range(1, chips):
                ex_wait(g, d, wb)

            def apply(i, g=g):
                at = cols_of(g), _at(i, STEP)
                ys[at] = ys[at] - _dot_nn(wb[g], cut(s, i))

            _loop(j // 2, whole, apply)
            for d in range(1, chips):
                w_copy(g, d).wait_send()

            @pl.when(j > 0)
            def _(g=g):
                project(0, g, 1 - s, ys, (j - 1) // 2)
                send_partial(0, g)

        release(n)

    _loop(0, nb, reflect)

    xs[...] = jnp.zeros_like(xs)
    first_half = lax.broadcasted_iota(jnp.int32, (gcol, LANES), 1) < EDGE

    def take(ref, g, j):
        lo = ref[cols_of(g), pl.ds(pl.multiple_of((j // 2) * STEP, LANES), LANES)]
        hi = ref[cols_of(g), pl.ds(pl.multiple_of((j // 2) * STEP + LANES, LANES), LANES)]
        even = j % 2 == 0
        return jnp.where(
            first_half,
            jnp.where(even, lo, pltpu.roll(lo, EDGE, 1)),
            jnp.where(even, pltpu.roll(hi, EDGE, 1), hi),
        )

    def spread(val, j):
        even = j % 2 == 0
        other = pltpu.roll(val, EDGE, 1)
        zero = jnp.zeros_like(val)
        lo = jnp.where(even, jnp.where(first_half, val, zero), jnp.where(first_half, zero, other))
        hi = jnp.where(even, jnp.where(first_half, other, zero), jnp.where(first_half, zero, val))
        return jnp.concatenate([lo, hi], axis=1)

    def right_side(par, g, j):
        sbuf[par, g] = -sbuf[par, g]
        sbuf[par, g, :, _at(x, LANES)] += take(ys, g, j)

    def x_copy(g, d):
        src = wb.at[g, pl.ds(0, sl), _at(peer(d), LANES)]
        return remote(src, xr.at[g, _at(x, sl)], ex_s.at[g, d - 1], ex_r.at[g, d - 1], at_peer(d))

    for m in range(3):
        _loop(0, pairs, lambda i, m=m: swaps(m, i)[1].wait_send())
    over_v(sent)
    over_l(sent)
    to_mate.wait_send()
    half_to_mate.wait_send()
    for d in range(1, chips):
        r2_copy(d).wait_send()
        ga_copy(d).wait_send()
        lx_copy(d).wait_send()

    wait_blk(nb)
    wait_mat(nb)
    for g in range(2):
        sbuf[0, g] = jnp.zeros((gcol, size), jnp.float32)
        right_side(0, g, top)
        send_partial(0, g)

    def solve(i):
        n = nb + i
        j = top - i
        par, nxt = n % 2, (n + 1) % 2

        @pl.when(j > 0)
        def _():
            wait_blk(n + 1)
            wait_mat(n + 1)

        for g in range(2):

            @pl.when(j > 0)
            def _(g=g):
                project(nxt, g, nxt, xs, (j + 1) // 2)

            wb[g, pl.ds(0, sl)] = _dot_nn(gather_sum(par, g), mbuf[par])
            for d in range(1, chips):
                x_copy(g, d).start()
            xr[g, _at(x, sl)] = wb[g, pl.ds(0, sl), _at(x, LANES)]

        @pl.when(par == 0)
        def _():
            tick(LEAD + n // 2)

        for g in range(2):
            for d in range(1, chips):
                ex_wait(g, d, xr)
            solved = spread(xr[g], j)
            xs[cols_of(g), _at(j // 2, STEP)] += solved

            @pl.when(j > 0)
            def _(g=g, solved=solved):
                sbuf[nxt, g] += _dot_nt(solved, cut(nxt, j // 2))
                right_side(nxt, g, j - 1)
                send_partial(nxt, g)

            for d in range(1, chips):
                x_copy(g, d).wait_send()

        release(n)

    _loop(0, nb, solve)

    def fin_copy(i):
        return remote(
            xs.at[:, _at(2 * i + 1 - k, LANES)], zt.at[k, :, _at(i, LANES)], fin_s.at[i], fin_r.at[i], mate
        )

    _loop(0, pairs, lambda i: fin_copy(i).start())

    def own_cols(i):
        zt[k, :, _at(i, LANES)] = xs[:, _at(2 * i + k, LANES)]

    _loop(0, pairs, own_cols)

    def give(i):
        await_(zt.at[1 - k, :, _at(i, LANES)], fin_r.at[i])
        out_ref[_at(i, LANES), :] = zt[:, :, _at(i, LANES)].reshape(2 * ncol, LANES).T

    _loop(0, pairs, give)

    _loop(0, pairs, lambda i: fin_copy(i).wait_send())


def solution(mesh):
    rows, cols = mesh.shape["row"], mesh.shape["col"]
    mat_spec = P(("kpt", "row"), "col")
    fac_spec = P("kpt", None, None)

    def local_work(v_loc, t_loc, z_loc, l_loc):
        n_row, n_col = v_loc.shape
        slots, lanes, chips, size = n_col // EDGE, 2 * n_row, rows // 2, rows * EDGE
        nb, ncol = lanes // LANES, z_loc.shape[1] // 2
        pairs, gcol, peers = nb // 2, ncol // 2, max(chips - 1, 1)
        sl, gathers, n128 = gcol // chips, len(_gathers(slots)), size // LANES
        tri = LANES * (n128 * (n128 + 1) // 2)
        dma = pltpu.SemaphoreType.DMA
        hbm, vmem = pl.BlockSpec(memory_space=pl.ANY), pl.BlockSpec(memory_space=pltpu.VMEM)

        def buf(*shape):
            return pltpu.VMEM(shape, jnp.float32)

        return pl.pallas_call(
            functools.partial(_kernel, (rows, cols, slots, nb, ncol)),
            out_shape=[
                jax.ShapeDtypeStruct(z_loc.shape, jnp.float32),
                jax.ShapeDtypeStruct((2, slots, RING, RING, HALF, lanes), jnp.float32),
            ],
            in_specs=[hbm] * 4,
            out_specs=[vmem, hbm],
            scratch_shapes=[
                buf(3, n_row, n_col),
                buf(2, slots, 2, HALF, n_row),
                buf(2, ncol, n_row),
                buf(rows, EDGE, EDGE),
                buf(2, slots, HALF, lanes),
                buf(ncol, lanes),
                buf(ncol, lanes),
                buf(pairs // 2, rows, EDGE, STEP),
                buf(rows, EDGE, STEP),
                buf(chips, size, LANES),
                buf(size, size),
                buf(size // 2, size),
                buf(size // 4, size),
                buf(peers, size // 4 // chips, size),
                buf(size // 2, size),
                buf(2, size, size),
                buf(2, EDGE, tri),
                buf(2, RING, RING, EDGE, tri),
                buf(2, rows, EDGE, lanes),
                buf(2, size, size),
                buf(2, 2, gcol, size),
                buf(2, peers, sl, size),
                buf(2, gcol, size),
                buf(2, gcol, LANES),
                dma((4,)),
                dma((3, pairs)), dma((3, pairs)), dma((3, pairs)),
                dma((slots, pairs)), dma((pairs // 2, rows, 2)),
                dma((slots, 2)), dma((rows, 2)),
                dma((peers,)), dma((peers,)),
                dma((4,)),
                dma((peers,)), dma((peers,)), dma((peers,)), dma((peers,)),
                dma((pairs,)), dma((pairs,)),
                dma((gathers,)), dma((gathers, 8)), dma((gathers, 8)),
                dma((2, rows)), dma((2, rows)), dma((2, rows)),
                dma((2, n128)), dma((2, n128)), dma((2, n128)),
                pltpu.SemaphoreType.REGULAR((2,)),
                dma((2, peers)), dma((2, peers)), dma((2, peers)), dma((2, peers)),
            ],
            compiler_params=pltpu.CompilerParams(has_side_effects=True, vmem_limit_bytes=60 * 1024 * 1024),
            name="eigvec",
        )(v_loc, t_loc, z_loc, l_loc)[0]

    return jax.shard_map(local_work, mesh=mesh, in_specs=(mat_spec, fac_spec, mat_spec, mat_spec), out_specs=mat_spec, check_vma=False)
```

```python
import functools

import jax
import jax.numpy as jnp
from jax import lax
from jax.experimental import pallas as pl
from jax.experimental.pallas import tpu as pltpu
from jax.sharding import PartitionSpec as P

PREC_HIGH = lax.Precision.HIGHEST
MESH = pl.DeviceIdType.MESH
EDGE = 64
HALF = EDGE // 2
LANES = 128
STEP = 256
RING = 4
LEAD = 9
DEEP = 3


def _dot_nt(a, b):
    return lax.dot_general(a, b, (((1,), (1,)), ((), ())), precision=PREC_HIGH, preferred_element_type=jnp.float32)


def _dot_nn(a, b):
    return lax.dot_general(a, b, (((1,), (0,)), ((), ())), precision=PREC_HIGH, preferred_element_type=jnp.float32)


def _at(i, n):
    return pl.ds(pl.multiple_of(i * n, n), n)


def _loop(lo, hi, body):
    def one(i, carry):
        body(i)
        return carry

    lax.fori_loop(lo, hi, one, 0)


def _gathers(slots):
    early = [(slots - 1, 0), (slots - 2, 0), None, None, ("m", 0)]
    first = early + [(q, 0) for q in range(slots - 3, -1, -1)]
    rest = [(slots - 1, 1), ("m", 1)] + [(q, 1) for q in range(slots - 2, -1, -1)]
    return first + [None] * (LEAD - len(first)) + rest


def _kernel(dims, v_in, t_in, z_in, l_in, out_ref, gath, *scratch):
    (stage, vt, zt, tb, own, ys, xs, vb, ld, lx, gm, pk, gx, r2, ga, xm, pm, mg, blk, mbuf, sbuf, rs, wb, cm, rx,
     in_sem, swap_l, swap_s, swap_r, v_s, v_r, l_s, l_r, lx_s, lx_r, gx_sem, r2_s, r2_r, ga_s, ga_r, fin_s, fin_r,
     ag_loc, ag_s, ag_r, blk_loc, blk_s, blk_r, mat_loc, mat_s, mat_r, free_b, free_m, rs_s, rs_r, ex_s, ex_r, cm_s, cm_r,
     rx_s, rx_r) = scratch
    rows, cols, slots, nb, ncol = dims
    row, col = lax.axis_index("row"), lax.axis_index("col")
    x, k = row // 2, row % 2
    chips, groups = rows // 2, cols // rows
    size, lanes = rows * EDGE, nb * LANES
    hsize, qsize, n128 = size // 2, size // 4, size // LANES
    pairs = nb // 2
    gcol = ncol // 2
    sl = gcol // chips
    mate = {"row": row + 1 - 2 * k, "col": col}
    top, whole = nb - 1, nb // 2
    part, grp = col % rows, col // rows
    k_half, m_half = _at(k, HALF), _at(1 - k, HALF)
    s_a, s_b = 1 + (RING - 1) * k, RING - (RING - 1) * k
    a, b = (col // s_a) % RING, (col // s_b) % RING

    def remote(src, dst, ss, rr, to):
        return pltpu.make_async_remote_copy(src, dst, ss, rr, device_id=to, device_id_type=MESH)

    def await_(ref, sem):
        pltpu.make_async_copy(ref, ref, sem).wait()

    def peer(d):
        return lax.rem(x + d, chips)

    def at_peer(d):
        return {"row": 2 * peer(d) + k, "col": col}

    def plane(da, db):
        return {"row": row, "col": lax.rem(a + da, RING) * s_a + lax.rem(b + db, RING) * s_b}

    def low(q):
        return (groups * q // 2) * STEP

    order = _gathers(slots)

    class Slot:
        def __init__(self, kind, w, n):
            self.kind, self.w, self.n = kind, w, n

        def own(self):
            if self.kind == "m":
                return pm.at[self.w]
            return own.at[self.w, self.kind, :, pl.ds(low(self.kind), lanes - low(self.kind))]

        def piece(self, bb, aa, part=None):
            if self.kind == "m":
                return mg.at[self.w, bb, aa] if part is None else mg.at[self.w, bb, aa, pl.ds(part * HALF, HALF)]
            at = pl.ds(low(self.kind), lanes - low(self.kind))
            e = slice(None) if part is None else pl.ds(part * (HALF // 2), HALF // 2)
            return gath.at[self.w, self.kind, bb, aa, e, at]

        def bundle(self, bb, part=None):
            e = slice(None) if part is None else pl.ds(part * (RING // 2), RING // 2)
            if self.kind == "m":
                return mg.at[self.w, bb, e]
            return gath.at[self.w, self.kind, bb, e, :, pl.ds(low(self.kind), lanes - low(self.kind))]

        def copy(self, i):
            d = 1 if i % 2 == 0 else RING - 1
            back = RING - d
            if i < 2:
                src, dst, to = self.own(), self.piece(b, a), plane(d, 0)
            elif i < 4:
                src = dst = self.piece(b, lax.rem(a + back, RING), i % 2)
                to = plane(d, 0)
            elif i < 6:
                src = dst = self.bundle(b)
                to = plane(0, d)
            else:
                src = dst = self.bundle(lax.rem(b + back, RING), i % 2)
                to = plane(0, d)
            return remote(src, dst, ag_s.at[self.n, i], ag_r.at[self.n, i], to)

        def arrived(self, i):
            back = RING - 1 if i % 2 == 0 else 1
            if i < 2:
                dst = self.piece(b, lax.rem(a + back, RING))
            elif i < 4:
                dst = self.piece(b, lax.rem(a + 2, RING), i % 2)
            elif i < 6:
                dst = self.bundle(lax.rem(b + back, RING))
            else:
                dst = self.bundle(lax.rem(b + 2, RING), i % 2)
            await_(dst, ag_r.at[self.n, i])

        def kept(self):
            return pltpu.make_async_copy(self.own(), self.piece(b, a), ag_loc.at[self.n])

        def stage(self, s):
            if s == 0:
                self.copy(0).start()
                self.copy(1).start()
                self.kept().start()
            elif s == 1:
                for i in range(2):
                    self.arrived(i)
                    self.copy(2 + i).start()
            elif s == 2:
                self.kept().wait()
                self.arrived(2)
                self.arrived(3)
                self.copy(4).start()
                self.copy(5).start()
            elif s == 3:
                for i in range(4, 6):
                    self.arrived(i)
                    self.copy(2 + i).start()
            elif s == 4:
                self.arrived(6)
                self.arrived(7)
            else:
                for i in range(8):
                    self.copy(i).wait_send()

    def tick(t):
        for s in (4, 3, 2, 1, 0, 5):
            n = t - s
            if isinstance(n, int):
                if 0 <= n < len(order) and order[n] is not None:
                    Slot(*order[n], n).stage(s)
                continue
            for kind in list(range(slots)) + ["m"]:
                at_v, at_l = order.index((kind, 0)), order.index((kind, 1))

                @pl.when(jnp.logical_or(n == at_v, n == at_l))
                def _(s=s, n=n, kind=kind, at_l=at_l):
                    Slot(kind, jnp.where(n == at_l, 1, 0), n).stage(s)

    def block_of(n):
        j = top - n % nb
        return n // nb, j, j // groups, j % groups, n % 2

    def blk_copies(n, q, p):
        w, _, _, h, _ = block_of(n)
        s, c = n % DEEP, h * rows + p
        at = pl.ds(low(q), lanes - low(q))
        src = gath.at[w, q, (c // s_b) % RING, (c // s_a) % RING, :, at]
        dst = blk.at[s, p, k_half, at]
        return pltpu.make_async_copy(src, dst, blk_loc.at[s, p]), remote(src, dst, blk_s.at[s, p], blk_r.at[s, p], mate)

    def from_mate(n, q, p):
        await_(blk.at[n % DEEP, p, m_half, pl.ds(low(q), lanes - low(q))], blk_r.at[n % DEEP, p])

    def mat_copies(n, i):
        w, j, q, h, s = block_of(n)
        c = h * rows + q
        src = mg.at[w, (c // s_b) % RING, (c // s_a) % RING, :, pl.ds(LANES * (i * (i + 1) // 2), LANES * (i + 1))]
        dst = mbuf.at[s, pl.ds(pl.multiple_of(i * LANES + k * EDGE, EDGE), EDGE), pl.ds(0, LANES * (i + 1))]
        return (
            pltpu.make_async_copy(src, dst, mat_loc.at[s, i]),
            remote(src, dst, mat_s.at[s, i], mat_r.at[s, i], mate),
        )

    def per_piece(n, act):
        q_now = block_of(n)[2]
        for q in range(slots):

            @pl.when(q_now == q)
            def _(q=q):
                _loop(0, rows, functools.partial(act, q))

    def fetch_blk(n):
        def go(q, p):
            for c in blk_copies(n, q, p):
                c.start()

        per_piece(n, go)

    def fetch_mat(n):
        for i in range(n128):
            for c in mat_copies(n, i):
                c.start()

    def wait_blk(n):
        def one(q, p):
            blk_copies(n, q, p)[0].wait()
            from_mate(n, q, p)

        per_piece(n, one)

    def wait_mat(n):
        for i in range(n128):
            mat_copies(n, i)[0].wait()
            there = pl.ds(pl.multiple_of(i * LANES + (1 - k) * EDGE, EDGE), EDGE), pl.ds(0, LANES * (i + 1))
            await_(mbuf.at[(n % 2, *there)], mat_r.at[n % 2, i])

    def release_blk(n):
        per_piece(n, lambda q, p: blk_copies(n, q, p)[1].wait_send())

        @pl.when(n + DEEP < 2 * nb)
        def _():
            pl.semaphore_signal(free_b.at[n % DEEP], inc=1, device_id=mate, device_id_type=MESH)
            pl.semaphore_wait(free_b.at[n % DEEP], 1)
            fetch_blk(n + DEEP)

    def release_mat(n):
        for i in range(n128):
            mat_copies(n, i)[1].wait_send()

        @pl.when(n + 2 < 2 * nb)
        def _():
            pl.semaphore_signal(free_m.at[n % 2], inc=1, device_id=mate, device_id_type=MESH)
            pl.semaphore_wait(free_m.at[n % 2], 1)
            fetch_mat(n + 2)

    ins = [
        pltpu.make_async_copy(src, stage.at[i % 2], in_sem.at[i]) for i, src in enumerate((v_in, l_in, z_in))
    ] + [pltpu.make_async_copy(t_in.at[_at(groups * part + grp, rows)], tb, in_sem.at[3])]
    for i in (0, 1, 3):
        ins[i].start()

    def swaps(m, i):
        there = _at(2 * i + k, LANES)
        if m < 2:
            mine, theirs = vt.at[m, :, k, :, _at(i, LANES)], vt.at[m, :, 1 - k, :, _at(i, LANES)]
            dst = own.at[m, :, :, there]
        else:
            mine, theirs = zt.at[k, :, _at(i, LANES)], zt.at[1 - k, :, _at(i, LANES)]
            dst = ys.at[:, there]
        return (
            pltpu.make_async_copy(mine, dst, swap_l.at[m, i]),
            remote(theirs, dst, swap_s.at[m, i], swap_r.at[m, i], mate),
        )

    def arriving(m, i):
        there = _at(2 * i + 1 - k, LANES)
        await_(own.at[m, :, :, there] if m < 2 else ys.at[:, there], swap_r.at[m, i])

    def turn(m):
        ins[m].wait()

        def one(i):
            block = stage[m % 2, _at(i, LANES), :].T
            if m < 2:
                vt[m, :, :, :, _at(i, LANES)] = block.reshape(slots, 2, HALF, LANES)
            else:
                zt[:, :, _at(i, LANES)] = block.reshape(2, ncol, LANES)
            for c in swaps(m, i):
                c.start()

        _loop(0, pairs, one)

    def swapped(m):
        def one(i):
            swaps(m, i)[0].wait()
            arriving(m, i)

        _loop(0, pairs, one)

    my_q, my_h = part, grp
    my_j = groups * my_q + my_h
    first_t = my_j // 2

    def deal_v(q, t, act):
        to, kk = grp * rows + q, t % 2
        src = own.at[0, q, :, _at(t, STEP)]
        dst = vb.at[t // 2, part, k_half]
        self_ = jnp.logical_and(to == col, k == kk)
        act(
            self_,
            pltpu.make_async_copy(src, dst, v_r.at[t // 2, part, k]),
            remote(src, dst, v_s.at[q, t], v_r.at[t // 2, part, k], {"col": to, "row": 2 * x + kk}),
        )

    def deal_l(q, kk, act):
        to = grp * rows + q
        src = own.at[1, q, :, _at((groups * q + grp) // 2, STEP)]
        dst = ld.at[part, k_half]
        self_ = jnp.logical_and(to == col, k == kk)
        act(
            self_,
            pltpu.make_async_copy(src, dst, l_r.at[part, k]),
            remote(src, dst, l_s.at[q, kk], l_r.at[part, k], {"col": to, "row": 2 * x + kk}),
        )

    def send(self_, here, there):
        pl.when(self_)(here.start)
        pl.when(jnp.logical_not(self_))(there.start)

    def sent(self_, here, there):
        pl.when(jnp.logical_not(self_))(there.wait_send)

    def over_v(act):
        def one(q):
            _loop((groups * q + grp) // 2, pairs, lambda t: deal_v(q, t, act))

        _loop(0, slots, one)

    def over_l(act):
        def one(q):
            deal_l(q, 0, act)
            deal_l(q, 1, act)

        _loop(0, slots, one)

    turn(0)
    ins[2].start()
    swapped(0)
    over_v(send)
    turn(1)
    swapped(1)
    over_l(send)
    turn(2)
    mbuf[...] = jnp.zeros_like(mbuf)

    gm[...] = jnp.zeros_like(gm)

    def chunk(i):
        def got(n):
            await_(vb.at[i, n // 2, _at(n % 2, HALF)], v_r.at[i, n // 2, n % 2])

        _loop(0, 2 * rows, got)
        all_ = vb[i].reshape(size, STEP)
        gm[pl.ds(0, hsize), pl.ds(0, hsize)] += _dot_nt(all_[:hsize], all_[:hsize])
        gm[pl.ds(hsize, hsize), :] += _dot_nt(all_[hsize:], all_)

    _loop((first_t + 1 - k) // 2, pairs // 2, chunk)
    tick(0)

    widths = []
    w_ = hsize
    while w_ >= EDGE:
        widths.append(w_)
        w_ //= 2

    def packed(w_):
        return pl.ds(size - 2 * w_, w_)

    pk[...] = jnp.zeros_like(pk)
    for w_ in widths:
        for i in range(hsize // w_):
            pk[pl.ds(i * w_, w_), packed(w_)] = gm[pl.ds((2 * i + 1) * w_, w_), pl.ds(2 * i * w_, w_)]

    mine, theirs = _at(k, qsize), _at(1 - k, qsize)
    to_mate = remote(pk.at[theirs], gx, gx_sem.at[0], gx_sem.at[1], mate)
    to_mate.start()
    tick(1)
    to_mate.wait_recv()
    pk[mine] += gx[...]
    rl = qsize // chips

    def r2_copy(d):
        src = pk.at[pl.ds(pl.multiple_of(k * qsize + peer(d) * rl, rl), rl)]
        return remote(src, r2.at[d - 1], r2_s.at[d - 1], r2_r.at[d - 1], at_peer(d))

    for d in range(1, chips):
        r2_copy(d).start()

    def got_l(n):
        await_(ld.at[n // 2, _at(n % 2, HALF)], l_r.at[n // 2, n % 2])

    _loop(0, 2 * rows, got_l)
    ev = my_j % 2 == 0
    lo_half = lax.broadcasted_iota(jnp.int32, (size, LANES), 1) < EDGE
    l_lo, l_hi = ld[:, :, pl.ds(0, LANES)].reshape(size, LANES), ld[:, :, pl.ds(LANES, LANES)].reshape(size, LANES)
    lx[x] = jnp.where(
        lo_half,
        jnp.where(ev, l_lo, pltpu.roll(l_lo, EDGE, 1)),
        jnp.where(ev, pltpu.roll(l_hi, EDGE, 1), l_hi),
    )

    def lx_copy(d):
        return remote(lx.at[x], lx.at[x], lx_s.at[d - 1], lx_r.at[d - 1], at_peer(d))

    tick(2)
    for d in range(1, chips):
        r2_copy(d).wait_recv()
    my_rows = pl.ds(pl.multiple_of(k * qsize + x * rl, rl), rl)
    total = pk[my_rows]
    for d in range(1, chips):
        total = total + r2[d - 1]
    ga[my_rows] = total

    def ga_copy(d):
        return remote(ga.at[my_rows], ga.at[my_rows], ga_s.at[d - 1], ga_r.at[d - 1], at_peer(d))

    for d in range(1, chips):
        ga_copy(d).start()
    for d in range(1, chips):
        lx_copy(d).start()
    tick(3)
    for d in range(1, chips):
        await_(ga.at[pl.ds(pl.multiple_of(k * qsize + peer(chips - d) * rl, rl), rl)], ga_r.at[d - 1])
    half_to_mate = remote(ga.at[mine], ga.at[mine], gx_sem.at[2], gx_sem.at[3], mate)
    half_to_mate.start()

    r_i = lax.broadcasted_iota(jnp.int32, (LANES, LANES), 0)
    c_i = lax.broadcasted_iota(jnp.int32, (LANES, LANES), 1)

    def tile(i):
        return _at(i, LANES), _at(i, LANES)

    def merge_tile(w, i, low_part):
        cur = xm[(w, *tile(i))]
        xm[(w, *tile(i))] = cur - _dot_nn(_dot_nn(cur, low_part), cur)

    def level_l(lev):
        pick = jnp.logical_and(
            lax.shift_right_logical(r_i, lev) % 2 == 1,
            lax.shift_right_logical(c_i, lev) + 1 == lax.shift_right_logical(r_i, lev),
        )
        _loop(0, n128, lambda i: merge_tile(1, i, jnp.where(pick, gm[tile(i)], 0.0)))

    def level_big(w, corner):
        for w_ in reversed(widths[:-1]):
            for i in range(hsize // w_):
                d1 = pl.ds(2 * i * w_, w_)
                d2 = pl.ds((2 * i + 1) * w_, w_)
                xm[w, d2, d1] = -_dot_nn(_dot_nn(xm[w, d2, d2], corner(w_, i)), xm[w, d1, d1])

    def pack_factor(w):
        for i in range(n128):
            pm[w, :, pl.ds(LANES * (i * (i + 1) // 2), LANES * (i + 1))] = xm[
                w, pl.ds(pl.multiple_of(i * LANES + k * EDGE, EDGE), EDGE), pl.ds(0, LANES * (i + 1))
            ]

    xm[...] = jnp.zeros_like(xm)
    ins[3].wait()
    for p in range(0, rows, 2):
        zero = jnp.zeros((EDGE, EDGE), jnp.float32)
        both = jnp.concatenate(
            [jnp.concatenate([tb[p], zero], axis=1), jnp.concatenate([zero, tb[p + 1]], axis=1)], axis=0
        )
        xm[0, pl.ds(p * EDGE, LANES), pl.ds(p * EDGE, LANES)] = both
    await_(ga.at[theirs], gx_sem.at[3])

    def corner64(i):
        block = ga[_at(i, EDGE), packed(EDGE)]
        zero = jnp.zeros((EDGE, EDGE), jnp.float32)
        low_part = jnp.concatenate([block, zero], axis=1)
        merge_tile(0, i, jnp.concatenate([jnp.zeros_like(low_part), low_part], axis=0))

    _loop(0, n128, corner64)
    level_big(0, lambda w_, i: ga[pl.ds(i * w_, w_), packed(w_)])
    pack_factor(0)
    tick(4)

    fetch_blk(0)
    fetch_blk(1)
    for d in range(1, chips):
        await_(lx.at[peer(chips - d)], lx_r.at[d - 1])
    for i in range(chips):
        gm[_at(i, LANES), :] = lx[i].T
    same = r_i == c_i

    def diag(i):
        d = gm[tile(i)]
        xm[(1, *tile(i))] = jnp.where(same, 1.0 / jnp.where(same, d, 1.0), 0.0)

    _loop(0, n128, diag)
    swapped(2)
    tick(5)
    _loop(0, 3, level_l)
    tick(6)
    _loop(3, 7, level_l)
    tick(7)
    level_big(1, lambda w_, i: gm[pl.ds((2 * i + 1) * w_, w_), pl.ds(2 * i * w_, w_)])
    pack_factor(1)
    tick(8)
    fetch_mat(0)
    fetch_mat(1)
    fetch_blk(2)

    def over(first, body):
        pl.when(first % 2 == 1)(lambda: body(first * STEP, STEP))
        _loop((first + 1) // 2, whole // 2, lambda i: body(i * 2 * STEP, 2 * STEP))

    def rows_at(off, width):
        return pl.ds(pl.multiple_of(off, STEP), width)

    def cut(n, off, width):
        return blk[n % DEEP, :, :, rows_at(off, width)].reshape(size, width)

    def project(dst, ref, n, first):
        dst[...] = jnp.zeros((ncol, size), jnp.float32)

        def one(off, width):
            dst[...] += _dot_nt(ref[:, rows_at(off, width)], cut(n, off, width))

        over(first, one)

    def slice_of(g, x2):
        return pl.ds(pl.multiple_of(g * gcol + x2 * sl, sl), sl)

    def cols_of(g):
        return pl.ds(g * gcol, gcol)

    def rs_copy(par, g, d):
        return remote(sbuf.at[par, slice_of(g, peer(d))], rs.at[g, d - 1], rs_s.at[g, d - 1], rs_r.at[g, d - 1], at_peer(d))

    def w_copy(par, g, d):
        mine = wb.at[par, slice_of(g, x)]
        return remote(mine, mine, ex_s.at[g, d - 1], ex_r.at[g, d - 1], at_peer(d))

    c_half = pl.ds(pl.multiple_of(k * (rows // 2), rows // 2), rows // 2)

    def c_copy(par):
        return remote(cm.at[par, _at(k, hsize)], cm.at[par, _at(k, hsize)], cm_s.at[par], cm_r.at[par], mate)

    def apply(n):
        def one(off, width):
            ys[:, rows_at(off, width)] = ys[:, rows_at(off, width)] - _dot_nn(wb[n % 2], cut(n, off, width))

        over((top - n) // 2, one)

    wait_blk(0)
    project(sbuf.at[0], ys, 0, top // 2)
    for g in range(2):
        for d in range(1, chips):
            rs_copy(0, g, d).start()
    wait_mat(0)

    def reflect(n):
        j, par, nxt = top - n, n % 2, (n + 1) % 2

        @pl.when(n > 0)
        def _():
            apply(n - 1)
            release_blk(n - 1)

        @pl.when(j > 0)
        def _():
            wait_blk(n + 1)
            project(sbuf.at[nxt], ys, n + 1, (j - 1) // 2)

        for g in range(2):
            for d in range(1, chips):
                rs_copy(par, g, d).wait_recv()
            total = sbuf[par, slice_of(g, x)]
            for d in range(1, chips):
                total = total + rs[g, d - 1]
            wb[par, slice_of(g, x)] = _dot_nn(total, mbuf[par])
            for d in range(1, chips):
                w_copy(par, g, d).start()

        release_mat(n)

        @pl.when(j > 0)
        def _():
            cm[par, _at(k, hsize)] = jnp.zeros((hsize, size), jnp.float32)

            def one(off, width):
                here = blk[n % DEEP, c_half, :, rows_at(off, width)].reshape(hsize, width)
                cm[par, _at(k, hsize)] += _dot_nt(here, cut(n + 1, off, width))

            over(j // 2, one)
            c_copy(par).start()

        @pl.when(jnp.logical_and(n < 8, par == 0))
        def _():
            tick(LEAD + n // 2)

        @pl.when(n >= 8)
        def _():
            tick(LEAD - 4 + n)

        for g in range(2):
            for d in range(1, chips):
                rs_copy(par, g, d).wait_send()

        @pl.when(j > 0)
        def _():
            wait_mat(n + 1)
            await_(cm.at[par, _at(1 - k, hsize)], cm_r.at[par])

        for g in range(2):
            for d in range(1, chips):
                await_(wb.at[par, slice_of(g, peer(chips - d))], ex_r.at[g, d - 1])

            @pl.when(j > 0)
            def _(g=g):
                sbuf[nxt, cols_of(g)] = sbuf[nxt, cols_of(g)] - _dot_nn(wb[par, cols_of(g)], cm[par])
                for d in range(1, chips):
                    rs_copy(nxt, g, d).start()

        for g in range(2):
            for d in range(1, chips):
                w_copy(par, g, d).wait_send()

        @pl.when(j > 0)
        def _():
            c_copy(par).wait_send()

    _loop(0, nb, reflect)
    apply(top)
    release_blk(top)

    xs[...] = jnp.zeros_like(xs)
    first_half = lax.broadcasted_iota(jnp.int32, (gcol, LANES), 1) < EDGE

    def take(ref, g, j):
        lo = ref[cols_of(g), pl.ds(pl.multiple_of((j // 2) * STEP, LANES), LANES)]
        hi = ref[cols_of(g), pl.ds(pl.multiple_of((j // 2) * STEP + LANES, LANES), LANES)]
        even = j % 2 == 0
        return jnp.where(
            first_half,
            jnp.where(even, lo, pltpu.roll(lo, EDGE, 1)),
            jnp.where(even, pltpu.roll(hi, EDGE, 1), hi),
        )

    def spread(val, j):
        even = j % 2 == 0
        other = pltpu.roll(val, EDGE, 1)
        zero = jnp.zeros_like(val)
        lo = jnp.where(even, jnp.where(first_half, val, zero), jnp.where(first_half, zero, other))
        hi = jnp.where(even, jnp.where(first_half, other, zero), jnp.where(first_half, zero, val))
        return jnp.concatenate([lo, hi], axis=1)

    def x_copy(par, g, d):
        src = sbuf.at[par, cols_of(g), _at(peer(d), LANES)]
        return remote(src, rx.at[par, g, d - 1], rx_s.at[par, g, d - 1], rx_r.at[par, g, d - 1], at_peer(d))

    def solve_partial(n, g, j):
        par = n % 2
        wb[0, cols_of(g)] = -wb[0, cols_of(g)]
        wb[0, cols_of(g), _at(x, LANES)] += take(ys, g, j)
        sbuf[par, cols_of(g)] = _dot_nn(wb[0, cols_of(g)], mbuf[par])
        for d in range(1, chips):
            x_copy(par, g, d).start()

    for m in range(3):
        _loop(0, pairs, lambda i, m=m: swaps(m, i)[1].wait_send())
    over_v(sent)
    over_l(sent)
    to_mate.wait_send()
    half_to_mate.wait_send()
    for d in range(1, chips):
        r2_copy(d).wait_send()
        ga_copy(d).wait_send()
        lx_copy(d).wait_send()

    wait_blk(nb)
    wait_mat(nb)
    wb[0] = jnp.zeros((ncol, size), jnp.float32)
    for g in range(2):
        solve_partial(nb, g, top)
    release_blk(nb)
    release_mat(nb)

    def solve(i):
        n = nb + i
        j, par, nxt = top - i, n % 2, (n + 1) % 2

        @pl.when(j > 0)
        def _():
            wait_blk(n + 1)
            wait_mat(n + 1)
            project(wb.at[0], xs, n + 1, (j + 1) // 2)

        for g in range(2):
            for d in range(1, chips):
                x_copy(par, g, d).wait_recv()
            val = sbuf[par, cols_of(g), _at(x, LANES)]
            for d in range(1, chips):
                val = val + rx[par, g, d - 1]
            solved = spread(val, j)
            xs[cols_of(g), _at(j // 2, STEP)] += solved

            @pl.when(j > 0)
            def _(g=g, solved=solved):
                wb[0, cols_of(g)] += _dot_nt(solved, cut(n + 1, (j // 2) * STEP, STEP))
                solve_partial(n + 1, g, j - 1)

        for g in range(2):
            for d in range(1, chips):
                x_copy(par, g, d).wait_send()

        @pl.when(j > 0)
        def _():
            release_blk(n + 1)
            release_mat(n + 1)

        tick(LEAD - 4 + n)

    _loop(0, nb, solve)

    def fin_copy(i):
        return remote(
            xs.at[:, _at(2 * i + 1 - k, LANES)], zt.at[k, :, _at(i, LANES)], fin_s.at[i], fin_r.at[i], mate
        )

    _loop(0, pairs, lambda i: fin_copy(i).start())

    def own_cols(i):
        zt[k, :, _at(i, LANES)] = xs[:, _at(2 * i + k, LANES)]

    _loop(0, pairs, own_cols)

    def give(i):
        await_(zt.at[1 - k, :, _at(i, LANES)], fin_r.at[i])
        out_ref[_at(i, LANES), :] = zt[:, :, _at(i, LANES)].reshape(2 * ncol, LANES).T

    _loop(0, pairs, give)

    _loop(0, pairs, lambda i: fin_copy(i).wait_send())


def solution(mesh):
    rows, cols = mesh.shape["row"], mesh.shape["col"]
    mat_spec = P(("kpt", "row"), "col")
    fac_spec = P("kpt", None, None)

    def local_work(v_loc, t_loc, z_loc, l_loc):
        n_row, n_col = v_loc.shape
        slots, lanes, chips, size = n_col // EDGE, 2 * n_row, rows // 2, rows * EDGE
        nb, ncol = lanes // LANES, z_loc.shape[1] // 2
        pairs, gcol, peers = nb // 2, ncol // 2, max(chips - 1, 1)
        sl, gathers, n128 = gcol // chips, len(_gathers(slots)), size // LANES
        tri = LANES * (n128 * (n128 + 1) // 2)
        dma = pltpu.SemaphoreType.DMA
        hbm, vmem = pl.BlockSpec(memory_space=pl.ANY), pl.BlockSpec(memory_space=pltpu.VMEM)

        def buf(*shape):
            return pltpu.VMEM(shape, jnp.float32)

        return pl.pallas_call(
            functools.partial(_kernel, (rows, cols, slots, nb, ncol)),
            out_shape=[
                jax.ShapeDtypeStruct(z_loc.shape, jnp.float32),
                jax.ShapeDtypeStruct((2, slots, RING, RING, HALF, lanes), jnp.float32),
            ],
            in_specs=[hbm] * 4,
            out_specs=[vmem, hbm],
            scratch_shapes=[
                buf(2, n_row, n_col),
                buf(2, slots, 2, HALF, n_row),
                buf(2, ncol, n_row),
                buf(rows, EDGE, EDGE),
                buf(2, slots, HALF, lanes),
                buf(ncol, lanes),
                buf(ncol, lanes),
                buf(pairs // 2, rows, EDGE, STEP),
                buf(rows, EDGE, STEP),
                buf(chips, size, LANES),
                buf(size, size),
                buf(size // 2, size),
                buf(size // 4, size),
                buf(peers, size // 4 // chips, size),
                buf(size // 2, size),
                buf(2, size, size),
                buf(2, EDGE, tri),
                buf(2, RING, RING, EDGE, tri),
                buf(DEEP, rows, EDGE, lanes),
                buf(2, size, size),
                buf(2, ncol, size),
                buf(2, peers, sl, size),
                buf(2, ncol, size),
                buf(2, size, size),
                buf(2, 2, peers, gcol, LANES),
                dma((4,)),
                dma((3, pairs)), dma((3, pairs)), dma((3, pairs)),
                dma((slots, pairs)), dma((pairs // 2, rows, 2)),
                dma((slots, 2)), dma((rows, 2)),
                dma((peers,)), dma((peers,)),
                dma((4,)),
                dma((peers,)), dma((peers,)), dma((peers,)), dma((peers,)),
                dma((pairs,)), dma((pairs,)),
                dma((gathers,)), dma((gathers, 8)), dma((gathers, 8)),
                dma((DEEP, rows)), dma((DEEP, rows)), dma((DEEP, rows)),
                dma((2, n128)), dma((2, n128)), dma((2, n128)),
                pltpu.SemaphoreType.REGULAR((DEEP,)), pltpu.SemaphoreType.REGULAR((2,)),
                dma((2, peers)), dma((2, peers)), dma((2, peers)), dma((2, peers)),
                dma((2,)), dma((2,)),
                dma((2, 2, peers)), dma((2, 2, peers)),
            ],
            compiler_params=pltpu.CompilerParams(has_side_effects=True, vmem_limit_bytes=63 * 1024 * 1024),
            name="eigvec",
        )(v_loc, t_loc, z_loc, l_loc)[0]

    return jax.shard_map(local_work, mesh=mesh, in_specs=(mat_spec, fac_spec, mat_spec, mat_spec), out_specs=mat_spec, check_vma=False)
```

```python
import functools

import jax
import jax.numpy as jnp
from jax import lax
from jax.experimental import pallas as pl
from jax.experimental.pallas import tpu as pltpu
from jax.sharding import PartitionSpec as P

PREC_HIGH = lax.Precision.HIGHEST
MESH = pl.DeviceIdType.MESH
EDGE = 64
HALF = EDGE // 2
LANES = 128
STEP = 256
RING = 4
LEAD = 9
DEEP = 3


def _dot_nt(a, b):
    return lax.dot_general(a, b, (((1,), (1,)), ((), ())), precision=PREC_HIGH, preferred_element_type=jnp.float32)


def _dot_nn(a, b):
    return lax.dot_general(a, b, (((1,), (0,)), ((), ())), precision=PREC_HIGH, preferred_element_type=jnp.float32)


def _at(i, n):
    return pl.ds(pl.multiple_of(i * n, n), n)


def _loop(lo, hi, body):
    def one(i, carry):
        body(i)
        return carry

    lax.fori_loop(lo, hi, one, 0)


def _gathers(slots):
    early = [(slots - 1, 0), (slots - 2, 0), None, None, ("m", 0)]
    first = early + [(q, 0) for q in range(slots - 3, -1, -1)]
    rest = [(slots - 1, 1), ("m", 1)] + [(q, 1) for q in range(slots - 2, -1, -1)]
    return first + [None] * (LEAD - len(first)) + rest


def _kernel(dims, v_in, t_in, z_in, l_in, out_ref, gath, *scratch):
    (stage, vt, zt, tb, own, ys, xs, vb, ld, lx, gm, pk, gx, r2, ga, xm, pm, mg, blk, mbuf, sbuf, rs, wb, cm, rx,
     in_sem, swap_l, swap_s, swap_r, v_s, v_r, l_s, l_r, lx_s, lx_r, gx_sem, r2_s, r2_r, ga_s, ga_r, fin_s, fin_r,
     ag_loc, ag_s, ag_r, blk_loc, blk_s, blk_r, mat_loc, mat_s, mat_r, free_b, free_m, rs_s, rs_r, ex_s, ex_r, cm_s, cm_r,
     rx_s, rx_r) = scratch
    rows, cols, slots, nb, ncol = dims
    row, col = lax.axis_index("row"), lax.axis_index("col")
    x, k = row // 2, row % 2
    chips, groups = rows // 2, cols // rows
    size, lanes = rows * EDGE, nb * LANES
    hsize, qsize, n128 = size // 2, size // 4, size // LANES
    pairs = nb // 2
    gcol = ncol // 2
    sl = gcol // chips
    mate = {"row": row + 1 - 2 * k, "col": col}
    top, whole = nb - 1, nb // 2
    part, grp = col % rows, col // rows
    k_half, m_half = _at(k, HALF), _at(1 - k, HALF)
    s_a, s_b = 1 + (RING - 1) * k, RING - (RING - 1) * k
    a, b = (col // s_a) % RING, (col // s_b) % RING

    def remote(src, dst, ss, rr, to):
        return pltpu.make_async_remote_copy(src, dst, ss, rr, device_id=to, device_id_type=MESH)

    def await_(ref, sem):
        pltpu.make_async_copy(ref, ref, sem).wait()

    def peer(d):
        return lax.rem(x + d, chips)

    def at_peer(d):
        return {"row": 2 * peer(d) + k, "col": col}

    def plane(da, db):
        return {"row": row, "col": lax.rem(a + da, RING) * s_a + lax.rem(b + db, RING) * s_b}

    def low(q):
        return (groups * q // 2) * STEP

    order = _gathers(slots)

    class Slot:
        def __init__(self, kind, w, n):
            self.kind, self.w, self.n = kind, w, n

        def own(self):
            if self.kind == "m":
                return pm.at[self.w]
            return own.at[self.w, self.kind, :, pl.ds(low(self.kind), lanes - low(self.kind))]

        def piece(self, bb, aa, part=None):
            if self.kind == "m":
                return mg.at[self.w, bb, aa] if part is None else mg.at[self.w, bb, aa, pl.ds(part * HALF, HALF)]
            at = pl.ds(low(self.kind), lanes - low(self.kind))
            e = slice(None) if part is None else pl.ds(part * (HALF // 2), HALF // 2)
            return gath.at[self.w, self.kind, bb, aa, e, at]

        def bundle(self, bb, part=None):
            e = slice(None) if part is None else pl.ds(part * (RING // 2), RING // 2)
            if self.kind == "m":
                return mg.at[self.w, bb, e]
            return gath.at[self.w, self.kind, bb, e, :, pl.ds(low(self.kind), lanes - low(self.kind))]

        def copy(self, i):
            d = 1 if i % 2 == 0 else RING - 1
            back = RING - d
            if i < 2:
                src, dst, to = self.own(), self.piece(b, a), plane(d, 0)
            elif i < 4:
                src = dst = self.piece(b, lax.rem(a + back, RING), i % 2)
                to = plane(d, 0)
            elif i < 6:
                src = dst = self.bundle(b)
                to = plane(0, d)
            else:
                src = dst = self.bundle(lax.rem(b + back, RING), i % 2)
                to = plane(0, d)
            return remote(src, dst, ag_s.at[self.n, i], ag_r.at[self.n, i], to)

        def arrived(self, i):
            back = RING - 1 if i % 2 == 0 else 1
            if i < 2:
                dst = self.piece(b, lax.rem(a + back, RING))
            elif i < 4:
                dst = self.piece(b, lax.rem(a + 2, RING), i % 2)
            elif i < 6:
                dst = self.bundle(lax.rem(b + back, RING))
            else:
                dst = self.bundle(lax.rem(b + 2, RING), i % 2)
            await_(dst, ag_r.at[self.n, i])

        def kept(self):
            return pltpu.make_async_copy(self.own(), self.piece(b, a), ag_loc.at[self.n])

        def stage(self, s):
            if s == 0:
                self.copy(0).start()
                self.copy(1).start()
                self.kept().start()
            elif s == 1:
                for i in range(2):
                    self.arrived(i)
                    self.copy(2 + i).start()
            elif s == 2:
                self.kept().wait()
                self.arrived(2)
                self.arrived(3)
                self.copy(4).start()
                self.copy(5).start()
            elif s == 3:
                for i in range(4, 6):
                    self.arrived(i)
                    self.copy(2 + i).start()
            elif s == 4:
                self.arrived(6)
                self.arrived(7)
            else:
                for i in range(8):
                    self.copy(i).wait_send()

    def tick(t):
        for s in (4, 3, 2, 1, 0, 5):
            n = t - s
            if isinstance(n, int):
                if 0 <= n < len(order) and order[n] is not None:
                    Slot(*order[n], n).stage(s)
                continue
            for kind in list(range(slots)) + ["m"]:
                at_v, at_l = order.index((kind, 0)), order.index((kind, 1))

                @pl.when(jnp.logical_or(n == at_v, n == at_l))
                def _(s=s, n=n, kind=kind, at_l=at_l):
                    Slot(kind, jnp.where(n == at_l, 1, 0), n).stage(s)

    def block_of(n):
        j = top - n % nb
        return n // nb, j, j // groups, j % groups, n % 2

    def blk_copies(n, q, p):
        w, _, _, h, _ = block_of(n)
        s, c = n % DEEP, h * rows + p
        at = pl.ds(low(q), lanes - low(q))
        src = gath.at[w, q, (c // s_b) % RING, (c // s_a) % RING, :, at]
        dst = blk.at[s, p, k_half, at]
        return pltpu.make_async_copy(src, dst, blk_loc.at[s, p]), remote(src, dst, blk_s.at[s, p], blk_r.at[s, p], mate)

    def from_mate(n, q, p):
        await_(blk.at[n % DEEP, p, m_half, pl.ds(low(q), lanes - low(q))], blk_r.at[n % DEEP, p])

    def mat_copies(n, i):
        w, j, q, h, s = block_of(n)
        c = h * rows + q
        src = mg.at[w, (c // s_b) % RING, (c // s_a) % RING, :, pl.ds(LANES * (i * (i + 1) // 2), LANES * (i + 1))]
        dst = mbuf.at[s, pl.ds(pl.multiple_of(i * LANES + k * EDGE, EDGE), EDGE), pl.ds(0, LANES * (i + 1))]
        return (
            pltpu.make_async_copy(src, dst, mat_loc.at[s, i]),
            remote(src, dst, mat_s.at[s, i], mat_r.at[s, i], mate),
        )

    def per_piece(n, act):
        q_now = block_of(n)[2]
        for q in range(slots):

            @pl.when(q_now == q)
            def _(q=q):
                _loop(0, rows, functools.partial(act, q))

    def fetch_blk(n):
        def go(q, p):
            for c in blk_copies(n, q, p):
                c.start()

        per_piece(n, go)

    def fetch_mat(n):
        for i in range(n128):
            for c in mat_copies(n, i):
                c.start()

    def wait_blk(n):
        def one(q, p):
            blk_copies(n, q, p)[0].wait()
            from_mate(n, q, p)

        per_piece(n, one)

    def wait_mat(n):
        for i in range(n128):
            mat_copies(n, i)[0].wait()
            there = pl.ds(pl.multiple_of(i * LANES + (1 - k) * EDGE, EDGE), EDGE), pl.ds(0, LANES * (i + 1))
            await_(mbuf.at[(n % 2, *there)], mat_r.at[n % 2, i])

    def release_blk(n):
        per_piece(n, lambda q, p: blk_copies(n, q, p)[1].wait_send())

        @pl.when(n + DEEP < 2 * nb)
        def _():
            pl.semaphore_signal(free_b.at[n % DEEP], inc=1, device_id=mate, device_id_type=MESH)
            pl.semaphore_wait(free_b.at[n % DEEP], 1)
            fetch_blk(n + DEEP)

    def release_mat(n):
        for i in range(n128):
            mat_copies(n, i)[1].wait_send()

        @pl.when(n + 2 < 2 * nb)
        def _():
            pl.semaphore_signal(free_m.at[n % 2], inc=1, device_id=mate, device_id_type=MESH)
            pl.semaphore_wait(free_m.at[n % 2], 1)
            fetch_mat(n + 2)

    barrier = pltpu.get_barrier_semaphore()

    def here_i_am(device):
        pl.semaphore_signal(barrier, inc=1, device_id=device, device_id_type=MESH)

    def group_member(d):
        n = lax.rem(2 * part + k + d, 2 * rows)
        here_i_am({"col": grp * rows + n // 2, "row": 2 * x + n % 2})

    _loop(1, 2 * rows, group_member)
    for d in range(1, chips):
        here_i_am(at_peer(d))
    for d in (1, RING - 1):
        here_i_am(plane(d, 0))
        here_i_am(plane(0, d))

    ins = [
        pltpu.make_async_copy(src, stage.at[i % 2], in_sem.at[i]) for i, src in enumerate((v_in, l_in, z_in))
    ] + [pltpu.make_async_copy(t_in, tb, in_sem.at[3])]
    for i in (0, 1, 3):
        ins[i].start()
    pl.semaphore_wait(barrier, 2 * rows - 1 + chips - 1 + 4)

    def swaps(m, i):
        there = _at(2 * i + k, LANES)
        if m < 2:
            mine, theirs = vt.at[m, :, k, :, _at(i, LANES)], vt.at[m, :, 1 - k, :, _at(i, LANES)]
            dst = own.at[m, :, :, there]
        else:
            mine, theirs = zt.at[k, :, _at(i, LANES)], zt.at[1 - k, :, _at(i, LANES)]
            dst = ys.at[:, there]
        return (
            pltpu.make_async_copy(mine, dst, swap_l.at[m, i]),
            remote(theirs, dst, swap_s.at[m, i], swap_r.at[m, i], mate),
        )

    def arriving(m, i):
        there = _at(2 * i + 1 - k, LANES)
        await_(own.at[m, :, :, there] if m < 2 else ys.at[:, there], swap_r.at[m, i])

    def turn(m, then=None):
        ins[m].wait()

        def one(i):
            block = stage[m % 2, _at(i, LANES), :].T
            if m < 2:
                vt[m, :, :, :, _at(i, LANES)] = block.reshape(slots, 2, HALF, LANES)
            else:
                zt[:, :, _at(i, LANES)] = block.reshape(2, ncol, LANES)
            for c in swaps(m, i):
                c.start()
            if then is not None:
                pl.when(i > 0)(lambda: then(i - 1))

        _loop(0, pairs, one)
        if then is not None:
            then(pairs - 1)

    def swapped(m):
        def one(i):
            swaps(m, i)[0].wait()
            arriving(m, i)

        _loop(0, pairs, one)

    my_q, my_h = part, grp
    my_j = groups * my_q + my_h
    first_t = my_j // 2

    def deal_v(q, t, act):
        to, kk = grp * rows + q, t % 2
        src = own.at[0, q, :, _at(t, STEP)]
        dst = vb.at[t // 2, part, k_half]
        self_ = jnp.logical_and(to == col, k == kk)
        act(
            self_,
            pltpu.make_async_copy(src, dst, v_r.at[t // 2, part, k]),
            remote(src, dst, v_s.at[q, t], v_r.at[t // 2, part, k], {"col": to, "row": 2 * x + kk}),
        )

    def deal_l(q, kk, act):
        to = grp * rows + q
        src = own.at[1, q, :, _at((groups * q + grp) // 2, STEP)]
        dst = ld.at[part, k_half]
        self_ = jnp.logical_and(to == col, k == kk)
        act(
            self_,
            pltpu.make_async_copy(src, dst, l_r.at[part, k]),
            remote(src, dst, l_s.at[q, kk], l_r.at[part, k], {"col": to, "row": 2 * x + kk}),
        )

    def send(self_, here, there):
        pl.when(self_)(here.start)
        pl.when(jnp.logical_not(self_))(there.start)

    def sent(self_, here, there):
        pl.when(jnp.logical_not(self_))(there.wait_send)

    def over_v(act):
        def one(q):
            _loop((groups * q + grp) // 2, pairs, lambda t: deal_v(q, t, act))

        _loop(0, slots, one)

    def over_l(act):
        def one(q):
            deal_l(q, 0, act)
            deal_l(q, 1, act)

        _loop(0, slots, one)

    def deal_chunk(t):
        swaps(0, t)[0].wait()
        arriving(0, t)
        _loop(0, (2 * t + 1 - grp + groups) // groups, lambda q: deal_v(q, t, send))

    turn(0, deal_chunk)
    ins[2].start()
    turn(1)
    swapped(1)
    over_l(send)
    turn(2)
    mbuf[...] = jnp.zeros_like(mbuf)

    gm[...] = jnp.zeros_like(gm)

    def chunk(i):
        def got(n):
            await_(vb.at[i, n // 2, _at(n % 2, HALF)], v_r.at[i, n // 2, n % 2])

        _loop(0, 2 * rows, got)
        all_ = vb[i].reshape(size, STEP)
        gm[pl.ds(0, hsize), pl.ds(0, hsize)] += _dot_nt(all_[:hsize], all_[:hsize])
        gm[pl.ds(hsize, hsize), :] += _dot_nt(all_[hsize:], all_)

    _loop((first_t + 1 - k) // 2, pairs // 2, chunk)
    tick(0)

    widths = []
    w_ = hsize
    while w_ >= EDGE:
        widths.append(w_)
        w_ //= 2

    def packed(w_):
        return pl.ds(size - 2 * w_, w_)

    pk[...] = jnp.zeros_like(pk)
    for w_ in widths:
        for i in range(hsize // w_):
            pk[pl.ds(i * w_, w_), packed(w_)] = gm[pl.ds((2 * i + 1) * w_, w_), pl.ds(2 * i * w_, w_)]

    mine, theirs = _at(k, qsize), _at(1 - k, qsize)
    to_mate = remote(pk.at[theirs], gx, gx_sem.at[0], gx_sem.at[1], mate)
    to_mate.start()
    tick(1)
    to_mate.wait_recv()
    pk[mine] += gx[...]
    rl = qsize // chips

    def r2_copy(d):
        src = pk.at[pl.ds(pl.multiple_of(k * qsize + peer(d) * rl, rl), rl)]
        return remote(src, r2.at[d - 1], r2_s.at[d - 1], r2_r.at[d - 1], at_peer(d))

    for d in range(1, chips):
        r2_copy(d).start()

    def got_l(n):
        await_(ld.at[n // 2, _at(n % 2, HALF)], l_r.at[n // 2, n % 2])

    _loop(0, 2 * rows, got_l)
    ev = my_j % 2 == 0
    lo_half = lax.broadcasted_iota(jnp.int32, (size, LANES), 1) < EDGE
    l_lo, l_hi = ld[:, :, pl.ds(0, LANES)].reshape(size, LANES), ld[:, :, pl.ds(LANES, LANES)].reshape(size, LANES)
    lx[x] = jnp.where(
        lo_half,
        jnp.where(ev, l_lo, pltpu.roll(l_lo, EDGE, 1)),
        jnp.where(ev, pltpu.roll(l_hi, EDGE, 1), l_hi),
    )

    def lx_copy(d):
        return remote(lx.at[x], lx.at[x], lx_s.at[d - 1], lx_r.at[d - 1], at_peer(d))

    tick(2)
    for d in range(1, chips):
        r2_copy(d).wait_recv()
    my_rows = pl.ds(pl.multiple_of(k * qsize + x * rl, rl), rl)
    total = pk[my_rows]
    for d in range(1, chips):
        total = total + r2[d - 1]
    ga[my_rows] = total

    def ga_copy(d):
        return remote(ga.at[my_rows], ga.at[my_rows], ga_s.at[d - 1], ga_r.at[d - 1], at_peer(d))

    for d in range(1, chips):
        ga_copy(d).start()
    for d in range(1, chips):
        lx_copy(d).start()
    tick(3)
    for d in range(1, chips):
        await_(ga.at[pl.ds(pl.multiple_of(k * qsize + peer(chips - d) * rl, rl), rl)], ga_r.at[d - 1])
    half_to_mate = remote(ga.at[mine], ga.at[mine], gx_sem.at[2], gx_sem.at[3], mate)
    half_to_mate.start()

    r_i = lax.broadcasted_iota(jnp.int32, (LANES, LANES), 0)
    c_i = lax.broadcasted_iota(jnp.int32, (LANES, LANES), 1)

    def tile(i):
        return _at(i, LANES), _at(i, LANES)

    def merge_tile(w, i, low_part):
        cur = xm[(w, *tile(i))]
        xm[(w, *tile(i))] = cur - _dot_nn(_dot_nn(cur, low_part), cur)

    def level_l(lev):
        pick = jnp.logical_and(
            lax.shift_right_logical(r_i, lev) % 2 == 1,
            lax.shift_right_logical(c_i, lev) + 1 == lax.shift_right_logical(r_i, lev),
        )
        _loop(0, n128, lambda i: merge_tile(1, i, jnp.where(pick, gm[tile(i)], 0.0)))

    def level_big(w, corner):
        for w_ in reversed(widths[:-1]):
            for i in range(hsize // w_):
                d1 = pl.ds(2 * i * w_, w_)
                d2 = pl.ds((2 * i + 1) * w_, w_)
                xm[w, d2, d1] = -_dot_nn(_dot_nn(xm[w, d2, d2], corner(w_, i)), xm[w, d1, d1])

    def pack_factor(w):
        for i in range(n128):
            pm[w, :, pl.ds(LANES * (i * (i + 1) // 2), LANES * (i + 1))] = xm[
                w, pl.ds(pl.multiple_of(i * LANES + k * EDGE, EDGE), EDGE), pl.ds(0, LANES * (i + 1))
            ]

    xm[...] = jnp.zeros_like(xm)
    ins[3].wait()
    for p in range(0, rows, 2):
        zero = jnp.zeros((EDGE, EDGE), jnp.float32)
        both = jnp.concatenate(
            [jnp.concatenate([tb[p], zero], axis=1), jnp.concatenate([zero, tb[p + 1]], axis=1)], axis=0
        )
        xm[0, pl.ds(p * EDGE, LANES), pl.ds(p * EDGE, LANES)] = both
    await_(ga.at[theirs], gx_sem.at[3])

    def corner64(i):
        block = ga[_at(i, EDGE), packed(EDGE)]
        zero = jnp.zeros((EDGE, EDGE), jnp.float32)
        low_part = jnp.concatenate([block, zero], axis=1)
        merge_tile(0, i, jnp.concatenate([jnp.zeros_like(low_part), low_part], axis=0))

    _loop(0, n128, corner64)
    level_big(0, lambda w_, i: ga[pl.ds(i * w_, w_), packed(w_)])
    pack_factor(0)
    tick(4)

    fetch_blk(0)
    fetch_blk(1)
    for d in range(1, chips):
        await_(lx.at[peer(chips - d)], lx_r.at[d - 1])
    for i in range(chips):
        gm[_at(i, LANES), :] = lx[i].T
    same = r_i == c_i

    def diag(i):
        d = gm[tile(i)]
        xm[(1, *tile(i))] = jnp.where(same, 1.0 / jnp.where(same, d, 1.0), 0.0)

    _loop(0, n128, diag)
    swapped(2)
    tick(5)
    _loop(0, 3, level_l)
    tick(6)
    _loop(3, 7, level_l)
    tick(7)
    level_big(1, lambda w_, i: gm[pl.ds((2 * i + 1) * w_, w_), pl.ds(2 * i * w_, w_)])
    pack_factor(1)
    tick(8)
    fetch_mat(0)
    fetch_mat(1)
    fetch_blk(2)

    def over(first, body):
        pl.when(first % 2 == 1)(lambda: body(first * STEP, STEP))
        _loop((first + 1) // 2, whole // 2, lambda i: body(i * 2 * STEP, 2 * STEP))

    def rows_at(off, width):
        return pl.ds(pl.multiple_of(off, STEP), width)

    def cut(n, off, width):
        return blk[n % DEEP, :, :, rows_at(off, width)].reshape(size, width)

    def project(dst, ref, n, first):
        dst[...] = jnp.zeros((ncol, size), jnp.float32)

        def one(off, width):
            dst[...] += _dot_nt(ref[:, rows_at(off, width)], cut(n, off, width))

        over(first, one)

    def slice_of(g, x2):
        return pl.ds(pl.multiple_of(g * gcol + x2 * sl, sl), sl)

    def cols_of(g):
        return pl.ds(g * gcol, gcol)

    def rs_copy(par, g, d):
        return remote(sbuf.at[par, slice_of(g, peer(d))], rs.at[g, d - 1], rs_s.at[g, d - 1], rs_r.at[g, d - 1], at_peer(d))

    def w_copy(par, g, d):
        mine = wb.at[par, slice_of(g, x)]
        return remote(mine, mine, ex_s.at[g, d - 1], ex_r.at[g, d - 1], at_peer(d))

    c_half = pl.ds(pl.multiple_of(k * (rows // 2), rows // 2), rows // 2)

    def c_copy(par):
        return remote(cm.at[par, _at(k, hsize)], cm.at[par, _at(k, hsize)], cm_s.at[par], cm_r.at[par], mate)

    def apply(n):
        def one(off, width):
            ys[:, rows_at(off, width)] = ys[:, rows_at(off, width)] - _dot_nn(wb[n % 2], cut(n, off, width))

        over((top - n) // 2, one)

    wait_blk(0)
    project(sbuf.at[0], ys, 0, top // 2)
    for g in range(2):
        for d in range(1, chips):
            rs_copy(0, g, d).start()
    wait_mat(0)

    def reflect(n):
        j, par, nxt = top - n, n % 2, (n + 1) % 2
        pl.when(n > 0)(lambda: apply(n - 1))

        @pl.when(j > 0)
        def _():
            wait_blk(n + 1)
            cm[par, _at(k, hsize)] = jnp.zeros((hsize, size), jnp.float32)

            def one(off, width):
                here = blk[n % DEEP, c_half, :, rows_at(off, width)].reshape(hsize, width)
                cm[par, _at(k, hsize)] += _dot_nt(here, cut(n + 1, off, width))

            over(j // 2, one)
            c_copy(par).start()

        for g in range(2):
            for d in range(1, chips):
                rs_copy(par, g, d).wait_recv()
            total = sbuf[par, slice_of(g, x)]
            for d in range(1, chips):
                total = total + rs[g, d - 1]
            wb[par, slice_of(g, x)] = _dot_nn(total, mbuf[par])
            for d in range(1, chips):
                w_copy(par, g, d).start()

        for g in range(2):
            for d in range(1, chips):
                rs_copy(par, g, d).wait_send()

        @pl.when(jnp.logical_and(n < 8, par == 0))
        def _():
            tick(LEAD + n // 2)

        @pl.when(n >= 8)
        def _():
            tick(LEAD - 4 + n)

        pl.when(n > 0)(lambda: release_blk(n - 1))
        release_mat(n)

        @pl.when(j > 0)
        def _():
            project(sbuf.at[nxt], ys, n + 1, (j - 1) // 2)
            wait_mat(n + 1)
            await_(cm.at[par, _at(1 - k, hsize)], cm_r.at[par])

        for g in range(2):
            for d in range(1, chips):
                await_(wb.at[par, slice_of(g, peer(chips - d))], ex_r.at[g, d - 1])

            @pl.when(j > 0)
            def _(g=g):
                sbuf[nxt, cols_of(g)] = sbuf[nxt, cols_of(g)] - _dot_nn(wb[par, cols_of(g)], cm[par])
                for d in range(1, chips):
                    rs_copy(nxt, g, d).start()

        for g in range(2):
            for d in range(1, chips):
                w_copy(par, g, d).wait_send()

        @pl.when(j > 0)
        def _():
            c_copy(par).wait_send()

    _loop(0, nb, reflect)
    apply(top)
    release_blk(top)

    xs[...] = jnp.zeros_like(xs)
    first_half = lax.broadcasted_iota(jnp.int32, (gcol, LANES), 1) < EDGE

    def take(ref, g, j):
        lo = ref[cols_of(g), pl.ds(pl.multiple_of((j // 2) * STEP, LANES), LANES)]
        hi = ref[cols_of(g), pl.ds(pl.multiple_of((j // 2) * STEP + LANES, LANES), LANES)]
        even = j % 2 == 0
        return jnp.where(
            first_half,
            jnp.where(even, lo, pltpu.roll(lo, EDGE, 1)),
            jnp.where(even, pltpu.roll(hi, EDGE, 1), hi),
        )

    def spread(val, j):
        even = j % 2 == 0
        other = pltpu.roll(val, EDGE, 1)
        zero = jnp.zeros_like(val)
        lo = jnp.where(even, jnp.where(first_half, val, zero), jnp.where(first_half, zero, other))
        hi = jnp.where(even, jnp.where(first_half, other, zero), jnp.where(first_half, zero, val))
        return jnp.concatenate([lo, hi], axis=1)

    def x_copy(par, g, d):
        src = sbuf.at[par, cols_of(g), _at(peer(d), LANES)]
        return remote(src, rx.at[par, g, d - 1], rx_s.at[par, g, d - 1], rx_r.at[par, g, d - 1], at_peer(d))

    def solve_partial(n, g, j):
        par = n % 2
        wb[0, cols_of(g)] = -wb[0, cols_of(g)]
        wb[0, cols_of(g), _at(x, LANES)] += take(ys, g, j)
        sbuf[par, cols_of(g)] = _dot_nn(wb[0, cols_of(g)], mbuf[par])
        for d in range(1, chips):
            x_copy(par, g, d).start()

    def fin_copy(i):
        return remote(
            xs.at[:, _at(2 * i + 1 - k, LANES)], zt.at[k, :, _at(i, LANES)], fin_s.at[i], fin_r.at[i], mate
        )

    def give(i):
        await_(zt.at[1 - k, :, _at(i, LANES)], fin_r.at[i])
        zt[k, :, _at(i, LANES)] = xs[:, _at(2 * i + k, LANES)]
        out_ref[_at(i, LANES), :] = zt[:, :, _at(i, LANES)].reshape(2 * ncol, LANES).T

    for m in range(3):
        _loop(0, pairs, lambda i, m=m: swaps(m, i)[1].wait_send())
    over_v(sent)
    over_l(sent)
    to_mate.wait_send()
    half_to_mate.wait_send()
    for d in range(1, chips):
        r2_copy(d).wait_send()
        ga_copy(d).wait_send()
        lx_copy(d).wait_send()

    wait_blk(nb)
    wait_mat(nb)
    wb[0] = jnp.zeros((ncol, size), jnp.float32)
    for g in range(2):
        solve_partial(nb, g, top)
    release_blk(nb)
    release_mat(nb)

    def solve(i):
        n = nb + i
        j, par, nxt = top - i, n % 2, (n + 1) % 2

        @pl.when(j > 0)
        def _():
            wait_blk(n + 1)
            wait_mat(n + 1)
            project(wb.at[0], xs, n + 1, (j + 1) // 2)

        for g in range(2):
            for d in range(1, chips):
                x_copy(par, g, d).wait_recv()
            val = sbuf[par, cols_of(g), _at(x, LANES)]
            for d in range(1, chips):
                val = val + rx[par, g, d - 1]
            solved = spread(val, j)
            xs[cols_of(g), _at(j // 2, STEP)] += solved

            @pl.when(j > 0)
            def _(g=g, solved=solved):
                wb[0, cols_of(g)] += _dot_nt(solved, cut(n + 1, (j // 2) * STEP, STEP))
                solve_partial(n + 1, g, j - 1)

        pl.when(j % 2 == 0)(lambda: fin_copy(j // 2).start())
        pl.when(jnp.logical_and(j % 2 == 1, j < top))(lambda: give(j // 2 + 1))

        for g in range(2):
            for d in range(1, chips):
                x_copy(par, g, d).wait_send()

        @pl.when(j > 0)
        def _():
            release_blk(n + 1)
            release_mat(n + 1)

        tick(LEAD - 4 + n)

    _loop(0, nb, solve)

    give(0)
    _loop(0, pairs, lambda i: fin_copy(i).wait_send())


def solution(mesh):
    rows, cols = mesh.shape["row"], mesh.shape["col"]
    mat_spec = P(("kpt", "row"), "col")
    fac_spec = P("kpt", None, None)

    def local_work(v_loc, t_loc, z_loc, l_loc):
        n_row, n_col = v_loc.shape
        slots, lanes, chips, size = n_col // EDGE, 2 * n_row, rows // 2, rows * EDGE
        nb, ncol = lanes // LANES, z_loc.shape[1] // 2
        pairs, gcol, peers = nb // 2, ncol // 2, max(chips - 1, 1)
        sl, gathers, n128 = gcol // chips, len(_gathers(slots)), size // LANES
        tri = LANES * (n128 * (n128 + 1) // 2)
        dma = pltpu.SemaphoreType.DMA
        hbm, vmem = pl.BlockSpec(memory_space=pl.ANY), pl.BlockSpec(memory_space=pltpu.VMEM)

        def buf(*shape):
            return pltpu.VMEM(shape, jnp.float32)

        col = lax.axis_index("col")
        t_mine = lax.dynamic_slice_in_dim(t_loc, (cols // rows * (col % rows) + col // rows) * rows, rows, axis=0)
        return pl.pallas_call(
            functools.partial(_kernel, (rows, cols, slots, nb, ncol)),
            out_shape=[
                jax.ShapeDtypeStruct(z_loc.shape, jnp.float32),
                jax.ShapeDtypeStruct((2, slots, RING, RING, HALF, lanes), jnp.float32),
            ],
            in_specs=[hbm] * 4,
            out_specs=[vmem, hbm],
            scratch_shapes=[
                buf(2, n_row, n_col),
                buf(2, slots, 2, HALF, n_row),
                buf(2, ncol, n_row),
                buf(rows, EDGE, EDGE),
                buf(2, slots, HALF, lanes),
                buf(ncol, lanes),
                buf(ncol, lanes),
                buf(pairs // 2, rows, EDGE, STEP),
                buf(rows, EDGE, STEP),
                buf(chips, size, LANES),
                buf(size, size),
                buf(size // 2, size),
                buf(size // 4, size),
                buf(peers, size // 4 // chips, size),
                buf(size // 2, size),
                buf(2, size, size),
                buf(2, EDGE, tri),
                buf(2, RING, RING, EDGE, tri),
                buf(DEEP, rows, EDGE, lanes),
                buf(2, size, size),
                buf(2, ncol, size),
                buf(2, peers, sl, size),
                buf(2, ncol, size),
                buf(2, size, size),
                buf(2, 2, peers, gcol, LANES),
                dma((4,)),
                dma((3, pairs)), dma((3, pairs)), dma((3, pairs)),
                dma((slots, pairs)), dma((pairs // 2, rows, 2)),
                dma((slots, 2)), dma((rows, 2)),
                dma((peers,)), dma((peers,)),
                dma((4,)),
                dma((peers,)), dma((peers,)), dma((peers,)), dma((peers,)),
                dma((pairs,)), dma((pairs,)),
                dma((gathers,)), dma((gathers, 8)), dma((gathers, 8)),
                dma((DEEP, rows)), dma((DEEP, rows)), dma((DEEP, rows)),
                dma((2, n128)), dma((2, n128)), dma((2, n128)),
                pltpu.SemaphoreType.REGULAR((DEEP,)), pltpu.SemaphoreType.REGULAR((2,)),
                dma((2, peers)), dma((2, peers)), dma((2, peers)), dma((2, peers)),
                dma((2,)), dma((2,)),
                dma((2, 2, peers)), dma((2, 2, peers)),
            ],
            compiler_params=pltpu.CompilerParams(collective_id=0, has_side_effects=True, vmem_limit_bytes=63 * 1024 * 1024),
            name="eigvec",
        )(v_loc, t_mine, z_loc, l_loc)[0]

    return jax.shard_map(local_work, mesh=mesh, in_specs=(mat_spec, fac_spec, mat_spec, mat_spec), out_specs=mat_spec, check_vma=False)
```

```python
import functools

import jax
import jax.numpy as jnp
from jax import lax
from jax.experimental import pallas as pl
from jax.experimental.pallas import tpu as pltpu
from jax.sharding import PartitionSpec as P

PREC_HIGH = lax.Precision.HIGHEST
MESH = pl.DeviceIdType.MESH
EDGE = 64
HALF = EDGE // 2
LANES = 128
STEP = 256
RING = 4
LEAD = 9
DEEP = 3


def _dot_nt(a, b):
    return lax.dot_general(a, b, (((1,), (1,)), ((), ())), precision=PREC_HIGH, preferred_element_type=jnp.float32)


def _dot_nn(a, b):
    return lax.dot_general(a, b, (((1,), (0,)), ((), ())), precision=PREC_HIGH, preferred_element_type=jnp.float32)


def _at(i, n):
    return pl.ds(pl.multiple_of(i * n, n), n)


def _loop(lo, hi, body):
    def one(i, carry):
        body(i)
        return carry

    lax.fori_loop(lo, hi, one, 0)


def _gathers(slots):
    early = [(slots - 1, 0), (slots - 2, 0), None, None, ("m", 0)]
    first = early + [(q, 0) for q in range(slots - 3, -1, -1)]
    rest = [(slots - 1, 1), ("m", 1)] + [(q, 1) for q in range(slots - 2, -1, -1)]
    return first + [None] * (LEAD - len(first)) + rest


def _kernel(dims, v_in, t_in, z_in, l_in, out_ref, gath, *scratch):
    (stage, vt, zt, tb, own, ys, xs, vb, ld, lx, gm, pk, gx, r2, ga, xm, pm, mg, blk, mbuf, sbuf, rs, wb, cm, rx,
     in_sem, swap_l, swap_s, swap_r, v_s, v_r, l_s, l_r, lx_s, lx_r, gx_sem, r2_s, r2_r, ga_s, ga_r, fin_s, fin_r,
     ag_loc, ag_s, ag_r, blk_loc, blk_s, blk_r, mat_loc, mat_s, mat_r, free_b, free_m, rs_s, rs_r, ex_s, ex_r, cm_s, cm_r,
     rx_s, rx_r) = scratch
    rows, cols, slots, nb, ncol = dims
    row, col = lax.axis_index("row"), lax.axis_index("col")
    x, k = row // 2, row % 2
    chips, groups = rows // 2, cols // rows
    size, lanes = rows * EDGE, nb * LANES
    hsize, qsize, n128 = size // 2, size // 4, size // LANES
    pairs = nb // 2
    gcol = ncol // 2
    sl = gcol // chips
    mate = {"row": row + 1 - 2 * k, "col": col}
    top, whole = nb - 1, nb // 2
    part, grp = col % rows, col // rows
    k_half, m_half = _at(k, HALF), _at(1 - k, HALF)
    s_a, s_b = 1 + (RING - 1) * k, RING - (RING - 1) * k
    a, b = (col // s_a) % RING, (col // s_b) % RING

    def remote(src, dst, ss, rr, to):
        return pltpu.make_async_remote_copy(src, dst, ss, rr, device_id=to, device_id_type=MESH)

    def await_(ref, sem):
        pltpu.make_async_copy(ref, ref, sem).wait()

    def peer(d):
        return lax.rem(x + d, chips)

    def at_peer(d):
        return {"row": 2 * peer(d) + k, "col": col}

    def plane(da, db):
        return {"row": row, "col": lax.rem(a + da, RING) * s_a + lax.rem(b + db, RING) * s_b}

    def low(q):
        return (groups * q // 2) * STEP

    order = _gathers(slots)

    class Slot:
        def __init__(self, kind, w, n):
            self.kind, self.w, self.n = kind, w, n

        def own(self):
            if self.kind == "m":
                return pm.at[self.w]
            return own.at[self.w, self.kind, :, pl.ds(low(self.kind), lanes - low(self.kind))]

        def piece(self, bb, aa, part=None):
            if self.kind == "m":
                return mg.at[self.w, bb, aa] if part is None else mg.at[self.w, bb, aa, pl.ds(part * HALF, HALF)]
            at = pl.ds(low(self.kind), lanes - low(self.kind))
            e = slice(None) if part is None else pl.ds(part * (HALF // 2), HALF // 2)
            return gath.at[self.w, self.kind, bb, aa, e, at]

        def bundle(self, bb, part=None):
            e = slice(None) if part is None else pl.ds(part * (RING // 2), RING // 2)
            if self.kind == "m":
                return mg.at[self.w, bb, e]
            return gath.at[self.w, self.kind, bb, e, :, pl.ds(low(self.kind), lanes - low(self.kind))]

        def copy(self, i):
            d = 1 if i % 2 == 0 else RING - 1
            back = RING - d
            if i < 2:
                src, dst, to = self.own(), self.piece(b, a), plane(d, 0)
            elif i < 4:
                src = dst = self.piece(b, lax.rem(a + back, RING), i % 2)
                to = plane(d, 0)
            elif i < 6:
                src = dst = self.bundle(b)
                to = plane(0, d)
            else:
                src = dst = self.bundle(lax.rem(b + back, RING), i % 2)
                to = plane(0, d)
            return remote(src, dst, ag_s.at[self.n, i], ag_r.at[self.n, i], to)

        def arrived(self, i):
            back = RING - 1 if i % 2 == 0 else 1
            if i < 2:
                dst = self.piece(b, lax.rem(a + back, RING))
            elif i < 4:
                dst = self.piece(b, lax.rem(a + 2, RING), i % 2)
            elif i < 6:
                dst = self.bundle(lax.rem(b + back, RING))
            else:
                dst = self.bundle(lax.rem(b + 2, RING), i % 2)
            await_(dst, ag_r.at[self.n, i])

        def kept(self):
            return pltpu.make_async_copy(self.own(), self.piece(b, a), ag_loc.at[self.n])

        def stage(self, s):
            if s == 0:
                self.copy(0).start()
                self.copy(1).start()
                self.kept().start()
            elif s == 1:
                for i in range(2):
                    self.arrived(i)
                    self.copy(2 + i).start()
            elif s == 2:
                self.kept().wait()
                self.arrived(2)
                self.arrived(3)
                self.copy(4).start()
                self.copy(5).start()
            elif s == 3:
                for i in range(4, 6):
                    self.arrived(i)
                    self.copy(2 + i).start()
            elif s == 4:
                self.arrived(6)
                self.arrived(7)
            else:
                for i in range(8):
                    self.copy(i).wait_send()

    def tick(t):
        for s in (4, 3, 2, 1, 0, 5):
            n = t - s
            if isinstance(n, int):
                if 0 <= n < len(order) and order[n] is not None:
                    Slot(*order[n], n).stage(s)
                continue
            for kind in list(range(slots)) + ["m"]:
                at_v, at_l = order.index((kind, 0)), order.index((kind, 1))

                @pl.when(jnp.logical_or(n == at_v, n == at_l))
                def _(s=s, n=n, kind=kind, at_l=at_l):
                    Slot(kind, jnp.where(n == at_l, 1, 0), n).stage(s)

    def block_of(n):
        j = top - n % nb
        return n // nb, j, j // groups, j % groups, n % 2

    run = min(rows, RING)
    runs = rows // run

    def in_blk(n, q, i, half):
        return blk.at[n % DEEP, pl.ds(i * run, run), half, pl.ds(low(q), lanes - low(q))]

    def from_mate(n, q, i):
        await_(in_blk(n, q, i, m_half), blk_r.at[n % DEEP, i])

    def mat_copies(n, i):
        w, j, q, h, s = block_of(n)
        c = h * rows + q
        src = mg.at[w, (c // s_b) % RING, (c // s_a) % RING, :, pl.ds(LANES * (i * (i + 1) // 2), LANES * (i + 1))]
        dst = mbuf.at[s, pl.ds(pl.multiple_of(i * LANES + k * EDGE, EDGE), EDGE), pl.ds(0, LANES * (i + 1))]
        return (
            pltpu.make_async_copy(src, dst, mat_loc.at[s, i]),
            remote(src, dst, mat_s.at[s, i], mat_r.at[s, i], mate),
        )

    def per_piece(n, act):
        q_now = block_of(n)[2]
        for q in range(slots):

            @pl.when(q_now == q)
            def _(q=q):
                for i in range(runs):
                    act(q, i)

    def fetch_blk(n):
        w, _, _, h, _ = block_of(n)
        s = n % DEEP

        def go(q, i):
            c = h * rows + i * run
            z_now, y_run = c // RING, pl.ds(c % RING, run)
            at = pl.ds(low(q), lanes - low(q))
            dst = in_blk(n, q, i, k_half)

            def both(src):
                pltpu.make_async_copy(src, dst, blk_loc.at[s, i]).start()
                remote(src, dst, blk_s.at[s, i], blk_r.at[s, i], mate).start()

            pl.when(k == 0)(lambda: both(gath.at[w, q, z_now, y_run, :, at]))
            pl.when(k == 1)(lambda: both(gath.at[w, q, y_run, z_now, :, at]))

        per_piece(n, go)

    def fetch_mat(n):
        for i in range(n128):
            for c in mat_copies(n, i):
                c.start()

    def wait_blk(n):
        def one(q, i):
            await_(in_blk(n, q, i, k_half), blk_loc.at[n % DEEP, i])
            from_mate(n, q, i)

        per_piece(n, one)

    def wait_mat(n):
        for i in range(n128):
            mat_copies(n, i)[0].wait()
            there = pl.ds(pl.multiple_of(i * LANES + (1 - k) * EDGE, EDGE), EDGE), pl.ds(0, LANES * (i + 1))
            await_(mbuf.at[(n % 2, *there)], mat_r.at[n % 2, i])

    def release_blk(n):
        per_piece(n, lambda q, i: await_(in_blk(n, q, i, k_half), blk_s.at[n % DEEP, i]))

        @pl.when(n + DEEP < 2 * nb)
        def _():
            pl.semaphore_signal(free_b.at[n % DEEP], inc=1, device_id=mate, device_id_type=MESH)
            pl.semaphore_wait(free_b.at[n % DEEP], 1)
            fetch_blk(n + DEEP)

    def release_mat(n):
        for i in range(n128):
            mat_copies(n, i)[1].wait_send()

        @pl.when(n + 2 < 2 * nb)
        def _():
            pl.semaphore_signal(free_m.at[n % 2], inc=1, device_id=mate, device_id_type=MESH)
            pl.semaphore_wait(free_m.at[n % 2], 1)
            fetch_mat(n + 2)

    barrier = pltpu.get_barrier_semaphore()

    def here_i_am(device):
        pl.semaphore_signal(barrier, inc=1, device_id=device, device_id_type=MESH)

    def group_member(d):
        n = lax.rem(2 * part + k + d, 2 * rows)
        here_i_am({"col": grp * rows + n // 2, "row": 2 * x + n % 2})

    _loop(1, 2 * rows, group_member)
    for d in range(1, chips):
        here_i_am(at_peer(d))
    for d in (1, RING - 1):
        here_i_am(plane(d, 0))
        here_i_am(plane(0, d))

    ins = [
        pltpu.make_async_copy(src, stage.at[i % 2], in_sem.at[i]) for i, src in enumerate((v_in, l_in, z_in))
    ] + [pltpu.make_async_copy(t_in, tb, in_sem.at[3])]
    for i in (0, 1, 3):
        ins[i].start()
    pl.semaphore_wait(barrier, 2 * rows - 1 + chips - 1 + 4)

    def swaps(m, i):
        there = _at(2 * i + k, LANES)
        if m < 2:
            mine, theirs = vt.at[m, :, k, :, _at(i, LANES)], vt.at[m, :, 1 - k, :, _at(i, LANES)]
            dst = own.at[m, :, :, there]
        else:
            mine, theirs = zt.at[k, :, _at(i, LANES)], zt.at[1 - k, :, _at(i, LANES)]
            dst = ys.at[:, there]
        return (
            pltpu.make_async_copy(mine, dst, swap_l.at[m, i]),
            remote(theirs, dst, swap_s.at[m, i], swap_r.at[m, i], mate),
        )

    def arriving(m, i):
        there = _at(2 * i + 1 - k, LANES)
        await_(own.at[m, :, :, there] if m < 2 else ys.at[:, there], swap_r.at[m, i])

    def turn(m, then=None):
        ins[m].wait()

        def one(i):
            block = stage[m % 2, _at(i, LANES), :].T
            if m < 2:
                vt[m, :, :, :, _at(i, LANES)] = block.reshape(slots, 2, HALF, LANES)
            else:
                zt[:, :, _at(i, LANES)] = block.reshape(2, ncol, LANES)
            for c in swaps(m, i):
                c.start()
            if then is not None:
                pl.when(i > 0)(lambda: then(i - 1))

        _loop(0, pairs, one)
        if then is not None:
            then(pairs - 1)

    def swapped(m):
        def one(i):
            swaps(m, i)[0].wait()
            arriving(m, i)

        _loop(0, pairs, one)

    my_q, my_h = part, grp
    my_j = groups * my_q + my_h
    first_t = my_j // 2

    def deal_v(q, t, act):
        to, kk = grp * rows + q, t % 2
        src = own.at[0, q, :, _at(t, STEP)]
        dst = vb.at[t // 2, part, k_half]
        self_ = jnp.logical_and(to == col, k == kk)
        act(
            self_,
            pltpu.make_async_copy(src, dst, v_r.at[t // 2, part, k]),
            remote(src, dst, v_s.at[q, t], v_r.at[t // 2, part, k], {"col": to, "row": 2 * x + kk}),
        )

    def deal_l(q, kk, act):
        to = grp * rows + q
        src = own.at[1, q, :, _at((groups * q + grp) // 2, STEP)]
        dst = ld.at[part, k_half]
        self_ = jnp.logical_and(to == col, k == kk)
        act(
            self_,
            pltpu.make_async_copy(src, dst, l_r.at[part, k]),
            remote(src, dst, l_s.at[q, kk], l_r.at[part, k], {"col": to, "row": 2 * x + kk}),
        )

    def send(self_, here, there):
        pl.when(self_)(here.start)
        pl.when(jnp.logical_not(self_))(there.start)

    def sent(self_, here, there):
        pl.when(jnp.logical_not(self_))(there.wait_send)

    def over_v(act):
        def one(q):
            _loop((groups * q + grp) // 2, pairs, lambda t: deal_v(q, t, act))

        _loop(0, slots, one)

    def over_l(act):
        def one(q):
            deal_l(q, 0, act)
            deal_l(q, 1, act)

        _loop(0, slots, one)

    def deal_chunk(t):
        swaps(0, t)[0].wait()
        arriving(0, t)
        _loop(0, (2 * t + 1 - grp + groups) // groups, lambda q: deal_v(q, t, send))

    turn(0, deal_chunk)
    ins[2].start()
    turn(1)
    swapped(1)
    over_l(send)
    turn(2)
    mbuf[...] = jnp.zeros_like(mbuf)

    gm[...] = jnp.zeros_like(gm)

    def chunk(i):
        def got(n):
            await_(vb.at[i, n // 2, _at(n % 2, HALF)], v_r.at[i, n // 2, n % 2])

        _loop(0, 2 * rows, got)
        all_ = vb[i].reshape(size, STEP)
        gm[pl.ds(0, hsize), pl.ds(0, hsize)] += _dot_nt(all_[:hsize], all_[:hsize])
        gm[pl.ds(hsize, hsize), :] += _dot_nt(all_[hsize:], all_)

    _loop((first_t + 1 - k) // 2, pairs // 2, chunk)
    tick(0)

    widths = []
    w_ = hsize
    while w_ >= EDGE:
        widths.append(w_)
        w_ //= 2

    def packed(w_):
        return pl.ds(size - 2 * w_, w_)

    pk[...] = jnp.zeros_like(pk)
    for w_ in widths:
        for i in range(hsize // w_):
            pk[pl.ds(i * w_, w_), packed(w_)] = gm[pl.ds((2 * i + 1) * w_, w_), pl.ds(2 * i * w_, w_)]

    mine, theirs = _at(k, qsize), _at(1 - k, qsize)
    to_mate = remote(pk.at[theirs], gx, gx_sem.at[0], gx_sem.at[1], mate)
    to_mate.start()
    tick(1)
    to_mate.wait_recv()
    pk[mine] += gx[...]
    rl = qsize // chips

    def r2_copy(d):
        src = pk.at[pl.ds(pl.multiple_of(k * qsize + peer(d) * rl, rl), rl)]
        return remote(src, r2.at[d - 1], r2_s.at[d - 1], r2_r.at[d - 1], at_peer(d))

    for d in range(1, chips):
        r2_copy(d).start()

    def got_l(n):
        await_(ld.at[n // 2, _at(n % 2, HALF)], l_r.at[n // 2, n % 2])

    _loop(0, 2 * rows, got_l)
    ev = my_j % 2 == 0
    lo_half = lax.broadcasted_iota(jnp.int32, (size, LANES), 1) < EDGE
    l_lo, l_hi = ld[:, :, pl.ds(0, LANES)].reshape(size, LANES), ld[:, :, pl.ds(LANES, LANES)].reshape(size, LANES)
    lx[x] = jnp.where(
        lo_half,
        jnp.where(ev, l_lo, pltpu.roll(l_lo, EDGE, 1)),
        jnp.where(ev, pltpu.roll(l_hi, EDGE, 1), l_hi),
    )

    def lx_copy(d):
        return remote(lx.at[x], lx.at[x], lx_s.at[d - 1], lx_r.at[d - 1], at_peer(d))

    tick(2)
    for d in range(1, chips):
        r2_copy(d).wait_recv()
    my_rows = pl.ds(pl.multiple_of(k * qsize + x * rl, rl), rl)
    total = pk[my_rows]
    for d in range(1, chips):
        total = total + r2[d - 1]
    ga[my_rows] = total

    def ga_copy(d):
        return remote(ga.at[my_rows], ga.at[my_rows], ga_s.at[d - 1], ga_r.at[d - 1], at_peer(d))

    for d in range(1, chips):
        ga_copy(d).start()
    for d in range(1, chips):
        lx_copy(d).start()
    tick(3)
    for d in range(1, chips):
        await_(ga.at[pl.ds(pl.multiple_of(k * qsize + peer(chips - d) * rl, rl), rl)], ga_r.at[d - 1])
    half_to_mate = remote(ga.at[mine], ga.at[mine], gx_sem.at[2], gx_sem.at[3], mate)
    half_to_mate.start()

    r_i = lax.broadcasted_iota(jnp.int32, (LANES, LANES), 0)
    c_i = lax.broadcasted_iota(jnp.int32, (LANES, LANES), 1)

    def tile(i):
        return _at(i, LANES), _at(i, LANES)

    def merge_tile(w, i, low_part):
        cur = xm[(w, *tile(i))]
        xm[(w, *tile(i))] = cur - _dot_nn(_dot_nn(cur, low_part), cur)

    def level_l(lev):
        pick = jnp.logical_and(
            lax.shift_right_logical(r_i, lev) % 2 == 1,
            lax.shift_right_logical(c_i, lev) + 1 == lax.shift_right_logical(r_i, lev),
        )
        _loop(0, n128, lambda i: merge_tile(1, i, jnp.where(pick, gm[tile(i)], 0.0)))

    def level_big(w, corner):
        for w_ in reversed(widths[:-1]):
            for i in range(hsize // w_):
                d1 = pl.ds(2 * i * w_, w_)
                d2 = pl.ds((2 * i + 1) * w_, w_)
                xm[w, d2, d1] = -_dot_nn(_dot_nn(xm[w, d2, d2], corner(w_, i)), xm[w, d1, d1])

    def pack_factor(w):
        for i in range(n128):
            pm[w, :, pl.ds(LANES * (i * (i + 1) // 2), LANES * (i + 1))] = xm[
                w, pl.ds(pl.multiple_of(i * LANES + k * EDGE, EDGE), EDGE), pl.ds(0, LANES * (i + 1))
            ]

    xm[...] = jnp.zeros_like(xm)
    ins[3].wait()
    for p in range(0, rows, 2):
        zero = jnp.zeros((EDGE, EDGE), jnp.float32)
        both = jnp.concatenate(
            [jnp.concatenate([tb[p], zero], axis=1), jnp.concatenate([zero, tb[p + 1]], axis=1)], axis=0
        )
        xm[0, pl.ds(p * EDGE, LANES), pl.ds(p * EDGE, LANES)] = both
    await_(ga.at[theirs], gx_sem.at[3])

    def corner64(i):
        block = ga[_at(i, EDGE), packed(EDGE)]
        zero = jnp.zeros((EDGE, EDGE), jnp.float32)
        low_part = jnp.concatenate([block, zero], axis=1)
        merge_tile(0, i, jnp.concatenate([jnp.zeros_like(low_part), low_part], axis=0))

    _loop(0, n128, corner64)
    level_big(0, lambda w_, i: ga[pl.ds(i * w_, w_), packed(w_)])
    pack_factor(0)
    tick(4)

    fetch_blk(0)
    fetch_blk(1)
    for d in range(1, chips):
        await_(lx.at[peer(chips - d)], lx_r.at[d - 1])
    for i in range(chips):
        gm[_at(i, LANES), :] = lx[i].T
    same = r_i == c_i

    def diag(i):
        d = gm[tile(i)]
        xm[(1, *tile(i))] = jnp.where(same, 1.0 / jnp.where(same, d, 1.0), 0.0)

    _loop(0, n128, diag)
    swapped(2)
    tick(5)
    _loop(0, 3, level_l)
    tick(6)
    _loop(3, 7, level_l)
    tick(7)
    level_big(1, lambda w_, i: gm[pl.ds((2 * i + 1) * w_, w_), pl.ds(2 * i * w_, w_)])
    pack_factor(1)
    tick(8)
    fetch_mat(0)
    fetch_mat(1)
    fetch_blk(2)

    def over(first, body):
        pl.when(first % 2 == 1)(lambda: body(first * STEP, STEP))
        _loop((first + 1) // 2, whole // 2, lambda i: body(i * 2 * STEP, 2 * STEP))

    def rows_at(off, width):
        return pl.ds(pl.multiple_of(off, STEP), width)

    def cut(n, off, width):
        return blk[n % DEEP, :, :, rows_at(off, width)].reshape(size, width)

    def project(dst, ref, n, first):
        dst[...] = jnp.zeros((ncol, size), jnp.float32)

        def one(off, width):
            dst[...] += _dot_nt(ref[:, rows_at(off, width)], cut(n, off, width))

        over(first, one)

    def slice_of(g, x2):
        return pl.ds(pl.multiple_of(g * gcol + x2 * sl, sl), sl)

    def cols_of(g):
        return pl.ds(g * gcol, gcol)

    def rs_copy(par, g, d):
        return remote(sbuf.at[par, slice_of(g, peer(d))], rs.at[g, d - 1], rs_s.at[g, d - 1], rs_r.at[g, d - 1], at_peer(d))

    def w_copy(par, g, d):
        mine = wb.at[par, slice_of(g, x)]
        return remote(mine, mine, ex_s.at[g, d - 1], ex_r.at[g, d - 1], at_peer(d))

    c_half = pl.ds(pl.multiple_of(k * (rows // 2), rows // 2), rows // 2)

    def c_copy(par):
        return remote(cm.at[par, _at(k, hsize)], cm.at[par, _at(k, hsize)], cm_s.at[par], cm_r.at[par], mate)

    def apply(n, off, width):
        ys[:, rows_at(off, width)] = ys[:, rows_at(off, width)] - _dot_nn(wb[n % 2], cut(n, off, width))

    def cross(n, off, width):
        here = blk[n % DEEP, c_half, :, rows_at(off, width)].reshape(hsize, width)
        cm[n % 2, _at(k, hsize)] += _dot_nt(here, cut(n + 1, off, width))

    def by_half(j, act):
        @pl.when(j >= nb // 2)
        def _():
            act((0,))
            act((1,))

        pl.when(j < nb // 2)(lambda: act((0, 1)))

    def cols_in(gs):
        return pl.ds(gs[0] * gcol, len(gs) * gcol)

    wait_blk(0)
    project(sbuf.at[0], ys, 0, top // 2)
    for g in range(2):
        for d in range(1, chips):
            rs_copy(0, g, d).start()
    wait_mat(0)

    def reflect(n):
        j, par, nxt = top - n, n % 2, (n + 1) % 2

        @pl.when(j > 0)
        def _():
            wait_blk(n + 1)
            cm[par, _at(k, hsize)] = jnp.zeros((hsize, size), jnp.float32)
            pl.when(j % 2 == 1)(lambda: cross(n, (j // 2) * STEP, STEP))

            def one(off, width):
                apply(n - 1, off, width)
                cross(n, off, width)

            over((j + 1) // 2, one)
            c_copy(par).start()

        pl.when(j == 0)(lambda: over(0, functools.partial(apply, n - 1)))

        def factor(gs):
            totals = []
            for g in gs:
                for d in range(1, chips):
                    rs_copy(par, g, d).wait_recv()
                total = sbuf[par, slice_of(g, x)]
                for d in range(1, chips):
                    total = total + rs[g, d - 1]
                totals.append(total)
            got = _dot_nn(jnp.concatenate(totals, axis=0), mbuf[par])
            for i, g in enumerate(gs):
                wb[par, slice_of(g, x)] = got[i * sl : (i + 1) * sl]
                for d in range(1, chips):
                    w_copy(par, g, d).start()

        by_half(j, factor)

        for g in range(2):
            for d in range(1, chips):
                rs_copy(par, g, d).wait_send()

        @pl.when(jnp.logical_and(n < 8, par == 0))
        def _():
            tick(LEAD + n // 2)

        @pl.when(n >= 8)
        def _():
            tick(LEAD - 4 + n)

        pl.when(n > 0)(lambda: release_blk(n - 1))
        release_mat(n)

        @pl.when(j > 0)
        def _():
            project(sbuf.at[nxt], ys, n + 1, (j - 1) // 2)
            wait_mat(n + 1)
            await_(cm.at[par, _at(1 - k, hsize)], cm_r.at[par])

        def correct(gs):
            for g in gs:
                for d in range(1, chips):
                    await_(wb.at[par, slice_of(g, peer(chips - d))], ex_r.at[g, d - 1])

            @pl.when(j > 0)
            def _():
                sbuf[nxt, cols_in(gs)] = sbuf[nxt, cols_in(gs)] - _dot_nn(wb[par, cols_in(gs)], cm[par])
                for g in gs:
                    for d in range(1, chips):
                        rs_copy(nxt, g, d).start()

        by_half(j, correct)

        for g in range(2):
            for d in range(1, chips):
                w_copy(par, g, d).wait_send()

        @pl.when(j > 0)
        def _():
            c_copy(par).wait_send()

    _loop(0, nb, reflect)
    over(0, functools.partial(apply, top))
    release_blk(top)

    xs[...] = jnp.zeros_like(xs)
    def first_half(val):
        return lax.broadcasted_iota(jnp.int32, val.shape, 1) < EDGE


    def take(ref, cols_, j):
        lo = ref[cols_, pl.ds(pl.multiple_of((j // 2) * STEP, LANES), LANES)]
        hi = ref[cols_, pl.ds(pl.multiple_of((j // 2) * STEP + LANES, LANES), LANES)]
        even = j % 2 == 0
        return jnp.where(
            first_half(lo),
            jnp.where(even, lo, pltpu.roll(lo, EDGE, 1)),
            jnp.where(even, pltpu.roll(hi, EDGE, 1), hi),
        )

    def spread(val, j):
        even, first = j % 2 == 0, first_half(val)
        other = pltpu.roll(val, EDGE, 1)
        zero = jnp.zeros_like(val)
        lo = jnp.where(even, jnp.where(first, val, zero), jnp.where(first, zero, other))
        hi = jnp.where(even, jnp.where(first, other, zero), jnp.where(first, zero, val))
        return jnp.concatenate([lo, hi], axis=1)

    def x_copy(par, g, d):
        src = sbuf.at[par, cols_of(g), _at(peer(d), LANES)]
        return remote(src, rx.at[par, g, d - 1], rx_s.at[par, g, d - 1], rx_r.at[par, g, d - 1], at_peer(d))

    def solve_partial(n, gs, j):
        par, cols_ = n % 2, cols_in(gs)
        wb[0, cols_] = -wb[0, cols_]
        wb[0, cols_, _at(x, LANES)] += take(ys, cols_, j)
        sbuf[par, cols_] = _dot_nn(wb[0, cols_], mbuf[par])
        for g in gs:
            for d in range(1, chips):
                x_copy(par, g, d).start()

    def fin_copy(i):
        return remote(
            xs.at[:, _at(2 * i + 1 - k, LANES)], zt.at[k, :, _at(i, LANES)], fin_s.at[i], fin_r.at[i], mate
        )

    def give(i):
        await_(zt.at[1 - k, :, _at(i, LANES)], fin_r.at[i])
        zt[k, :, _at(i, LANES)] = xs[:, _at(2 * i + k, LANES)]
        out_ref[_at(i, LANES), :] = zt[:, :, _at(i, LANES)].reshape(2 * ncol, LANES).T

    for m in range(3):
        _loop(0, pairs, lambda i, m=m: swaps(m, i)[1].wait_send())
    over_v(sent)
    over_l(sent)
    to_mate.wait_send()
    half_to_mate.wait_send()
    for d in range(1, chips):
        r2_copy(d).wait_send()
        ga_copy(d).wait_send()
        lx_copy(d).wait_send()

    wait_blk(nb)
    wait_mat(nb)
    wb[0] = jnp.zeros((ncol, size), jnp.float32)
    for g in range(2):
        solve_partial(nb, (g,), top)
    release_blk(nb)
    release_mat(nb)

    def solve(i):
        n = nb + i
        j, par, nxt = top - i, n % 2, (n + 1) % 2

        @pl.when(j > 0)
        def _():
            wait_blk(n + 1)
            wait_mat(n + 1)
            project(wb.at[0], xs, n + 1, (j + 1) // 2)

        def finish(gs):
            cols_ = cols_in(gs)
            vals = []
            for g in gs:
                for d in range(1, chips):
                    x_copy(par, g, d).wait_recv()
                val = sbuf[par, cols_of(g), _at(x, LANES)]
                for d in range(1, chips):
                    val = val + rx[par, g, d - 1]
                vals.append(val)
            solved = spread(jnp.concatenate(vals, axis=0), j)
            xs[cols_, _at(j // 2, STEP)] += solved

            @pl.when(j > 0)
            def _():
                wb[0, cols_] += _dot_nt(solved, cut(n + 1, (j // 2) * STEP, STEP))
                solve_partial(n + 1, gs, j - 1)

        by_half(j, finish)

        pl.when(j % 2 == 0)(lambda: fin_copy(j // 2).start())
        pl.when(jnp.logical_and(j % 2 == 1, j < top))(lambda: give(j // 2 + 1))

        for g in range(2):
            for d in range(1, chips):
                x_copy(par, g, d).wait_send()

        @pl.when(j > 0)
        def _():
            release_blk(n + 1)
            release_mat(n + 1)

        tick(LEAD - 4 + n)

    _loop(0, nb, solve)

    give(0)
    _loop(0, pairs, lambda i: fin_copy(i).wait_send())


def solution(mesh):
    rows, cols = mesh.shape["row"], mesh.shape["col"]
    mat_spec = P(("kpt", "row"), "col")
    fac_spec = P("kpt", None, None)

    def local_work(v_loc, t_loc, z_loc, l_loc):
        n_row, n_col = v_loc.shape
        slots, lanes, chips, size = n_col // EDGE, 2 * n_row, rows // 2, rows * EDGE
        nb, ncol = lanes // LANES, z_loc.shape[1] // 2
        pairs, gcol, peers = nb // 2, ncol // 2, max(chips - 1, 1)
        sl, gathers, n128 = gcol // chips, len(_gathers(slots)), size // LANES
        tri = LANES * (n128 * (n128 + 1) // 2)
        dma = pltpu.SemaphoreType.DMA
        hbm, vmem = pl.BlockSpec(memory_space=pl.ANY), pl.BlockSpec(memory_space=pltpu.VMEM)

        def buf(*shape):
            return pltpu.VMEM(shape, jnp.float32)

        col = lax.axis_index("col")
        t_mine = lax.dynamic_slice_in_dim(t_loc, (cols // rows * (col % rows) + col // rows) * rows, rows, axis=0)
        return pl.pallas_call(
            functools.partial(_kernel, (rows, cols, slots, nb, ncol)),
            out_shape=[
                jax.ShapeDtypeStruct(z_loc.shape, jnp.float32),
                jax.ShapeDtypeStruct((2, slots, RING, RING, HALF, lanes), jnp.float32),
            ],
            in_specs=[hbm] * 4,
            out_specs=[vmem, hbm],
            scratch_shapes=[
                buf(2, n_row, n_col),
                buf(2, slots, 2, HALF, n_row),
                buf(2, ncol, n_row),
                buf(rows, EDGE, EDGE),
                buf(2, slots, HALF, lanes),
                buf(ncol, lanes),
                buf(ncol, lanes),
                buf(pairs // 2, rows, EDGE, STEP),
                buf(rows, EDGE, STEP),
                buf(chips, size, LANES),
                buf(size, size),
                buf(size // 2, size),
                buf(size // 4, size),
                buf(peers, size // 4 // chips, size),
                buf(size // 2, size),
                buf(2, size, size),
                buf(2, EDGE, tri),
                buf(2, RING, RING, EDGE, tri),
                buf(DEEP, rows, EDGE, lanes),
                buf(2, size, size),
                buf(2, ncol, size),
                buf(2, peers, sl, size),
                buf(2, ncol, size),
                buf(2, size, size),
                buf(2, 2, peers, gcol, LANES),
                dma((4,)),
                dma((3, pairs)), dma((3, pairs)), dma((3, pairs)),
                dma((slots, pairs)), dma((pairs // 2, rows, 2)),
                dma((slots, 2)), dma((rows, 2)),
                dma((peers,)), dma((peers,)),
                dma((4,)),
                dma((peers,)), dma((peers,)), dma((peers,)), dma((peers,)),
                dma((pairs,)), dma((pairs,)),
                dma((gathers,)), dma((gathers, 8)), dma((gathers, 8)),
                dma((DEEP, rows)), dma((DEEP, rows)), dma((DEEP, rows)),
                dma((2, n128)), dma((2, n128)), dma((2, n128)),
                pltpu.SemaphoreType.REGULAR((DEEP,)), pltpu.SemaphoreType.REGULAR((2,)),
                dma((2, peers)), dma((2, peers)), dma((2, peers)), dma((2, peers)),
                dma((2,)), dma((2,)),
                dma((2, 2, peers)), dma((2, 2, peers)),
            ],
            compiler_params=pltpu.CompilerParams(collective_id=0, has_side_effects=True, vmem_limit_bytes=63 * 1024 * 1024),
            name="eigvec",
        )(v_loc, t_mine, z_loc, l_loc)[0]

    return jax.shard_map(local_work, mesh=mesh, in_specs=(mat_spec, fac_spec, mat_spec, mat_spec), out_specs=mat_spec, check_vma=False)
```

```python
import functools

import jax
import jax.numpy as jnp
from jax import lax
from jax.experimental import pallas as pl
from jax.experimental.pallas import tpu as pltpu
from jax.sharding import PartitionSpec as P

PREC_HIGH = lax.Precision.HIGHEST
MESH = pl.DeviceIdType.MESH
EDGE = 64
HALF = EDGE // 2
LANES = 128
STEP = 256
RING = 4
LEAD = 9
DEEP = 3


def _dot_nt(a, b):
    return lax.dot_general(a, b, (((1,), (1,)), ((), ())), precision=PREC_HIGH, preferred_element_type=jnp.float32)


def _dot_nn(a, b):
    return lax.dot_general(a, b, (((1,), (0,)), ((), ())), precision=PREC_HIGH, preferred_element_type=jnp.float32)


def _at(i, n):
    return pl.ds(pl.multiple_of(i * n, n), n)


def _loop(lo, hi, body):
    def one(i, carry):
        body(i)
        return carry

    lax.fori_loop(lo, hi, one, 0)


def _gathers(slots):
    early = [(slots - 1, 0), (slots - 2, 0), None, None, ("m", 0)]
    first = early + [(q, 0) for q in range(slots - 3, -1, -1)]
    rest = [(slots - 1, 1), ("m", 1)] + [(q, 1) for q in range(slots - 2, -1, -1)]
    return first + [None] * (LEAD - len(first)) + rest


def _kernel(dims, v_in, t_in, z_in, l_in, out_ref, gath, *scratch):
    (stage, vt, zt, tb, own, ys, xs, vb, ld, lx, gm, pk, gx, r2, ga, xm, pm, mg, blk, mbuf, sbuf, rs, wb, cm, rx,
     in_sem, swap_l, swap_s, swap_r, v_s, v_r, l_s, l_r, lx_s, lx_r, gx_sem, r2_s, r2_r, ga_s, ga_r, fin_s, fin_r,
     ag_loc, ag_s, ag_r, blk_loc, blk_s, blk_r, mat_loc, mat_s, mat_r, free_b, free_m, rs_s, rs_r, ex_s, ex_r, cm_s, cm_r,
     rx_s, rx_r) = scratch
    rows, cols, slots, nb, ncol = dims
    row, col = lax.axis_index("row"), lax.axis_index("col")
    x, k = row // 2, row % 2
    chips, groups = rows // 2, cols // rows
    size, lanes = rows * EDGE, nb * LANES
    hsize, qsize, n128 = size // 2, size // 4, size // LANES
    pairs = nb // 2
    gcol = ncol // 2
    sl = gcol // chips
    mate = {"row": row + 1 - 2 * k, "col": col}
    top, whole = nb - 1, nb // 2
    part, grp = col % rows, col // rows
    k_half, m_half = _at(k, HALF), _at(1 - k, HALF)
    s_a, s_b = 1 + (RING - 1) * k, RING - (RING - 1) * k
    a, b = (col // s_a) % RING, (col // s_b) % RING

    def remote(src, dst, ss, rr, to):
        return pltpu.make_async_remote_copy(src, dst, ss, rr, device_id=to, device_id_type=MESH)

    def await_(ref, sem):
        pltpu.make_async_copy(ref, ref, sem).wait()

    def peer(d):
        return lax.rem(x + d, chips)

    def at_peer(d):
        return {"row": 2 * peer(d) + k, "col": col}

    def plane(da, db):
        return {"row": row, "col": lax.rem(a + da, RING) * s_a + lax.rem(b + db, RING) * s_b}

    def low(q):
        return (groups * q // 2) * STEP

    order = _gathers(slots)

    class Slot:
        def __init__(self, kind, w, n):
            self.kind, self.w, self.n = kind, w, n

        def own(self):
            if self.kind == "m":
                return pm.at[self.w]
            return own.at[self.w, self.kind, :, pl.ds(low(self.kind), lanes - low(self.kind))]

        def piece(self, bb, aa, part=None):
            if self.kind == "m":
                return mg.at[self.w, bb, aa] if part is None else mg.at[self.w, bb, aa, pl.ds(part * HALF, HALF)]
            at = pl.ds(low(self.kind), lanes - low(self.kind))
            e = slice(None) if part is None else pl.ds(part * (HALF // 2), HALF // 2)
            return gath.at[self.w, self.kind, bb, aa, e, at]

        def bundle(self, bb, part=None):
            e = slice(None) if part is None else pl.ds(part * (RING // 2), RING // 2)
            if self.kind == "m":
                return mg.at[self.w, bb, e]
            return gath.at[self.w, self.kind, bb, e, :, pl.ds(low(self.kind), lanes - low(self.kind))]

        def copy(self, i):
            d = 1 if i % 2 == 0 else RING - 1
            back = RING - d
            if i < 2:
                src, dst, to = self.own(), self.piece(b, a), plane(d, 0)
            elif i < 4:
                src = dst = self.piece(b, lax.rem(a + back, RING), i % 2)
                to = plane(d, 0)
            elif i < 6:
                src = dst = self.bundle(b)
                to = plane(0, d)
            else:
                src = dst = self.bundle(lax.rem(b + back, RING), i % 2)
                to = plane(0, d)
            return remote(src, dst, ag_s.at[self.n, i], ag_r.at[self.n, i], to)

        def arrived(self, i):
            back = RING - 1 if i % 2 == 0 else 1
            if i < 2:
                dst = self.piece(b, lax.rem(a + back, RING))
            elif i < 4:
                dst = self.piece(b, lax.rem(a + 2, RING), i % 2)
            elif i < 6:
                dst = self.bundle(lax.rem(b + back, RING))
            else:
                dst = self.bundle(lax.rem(b + 2, RING), i % 2)
            await_(dst, ag_r.at[self.n, i])

        def kept(self):
            return pltpu.make_async_copy(self.own(), self.piece(b, a), ag_loc.at[self.n])

        def stage(self, s):
            if s == 0:
                self.copy(0).start()
                self.copy(1).start()
                self.kept().start()
            elif s == 1:
                for i in range(2):
                    self.arrived(i)
                    self.copy(2 + i).start()
            elif s == 2:
                self.kept().wait()
                self.arrived(2)
                self.arrived(3)
                self.copy(4).start()
                self.copy(5).start()
            elif s == 3:
                for i in range(4, 6):
                    self.arrived(i)
                    self.copy(2 + i).start()
            elif s == 4:
                self.arrived(6)
                self.arrived(7)
            else:
                for i in range(8):
                    self.copy(i).wait_send()

    def tick(t):
        for s in (4, 3, 2, 1, 0, 5):
            n = t - s
            if isinstance(n, int):
                if 0 <= n < len(order) and order[n] is not None:
                    Slot(*order[n], n).stage(s)
                continue
            for kind in list(range(slots)) + ["m"]:
                at_v, at_l = order.index((kind, 0)), order.index((kind, 1))

                @pl.when(jnp.logical_or(n == at_v, n == at_l))
                def _(s=s, n=n, kind=kind, at_l=at_l):
                    Slot(kind, jnp.where(n == at_l, 1, 0), n).stage(s)

    def block_of(n):
        j = top - n % nb
        return n // nb, j, j // groups, j % groups, n % 2

    run = min(rows, RING)
    runs = rows // run

    def in_blk(n, q, i, half):
        return blk.at[n % DEEP, pl.ds(i * run, run), half, pl.ds(low(q), lanes - low(q))]

    def from_mate(n, q, i):
        await_(in_blk(n, q, i, m_half), blk_r.at[n % DEEP, i])

    def mat_copies(n, i):
        w, j, q, h, s = block_of(n)
        c = h * rows + q
        src = mg.at[w, (c // s_b) % RING, (c // s_a) % RING, :, pl.ds(LANES * (i * (i + 1) // 2), LANES * (i + 1))]
        dst = mbuf.at[s, pl.ds(pl.multiple_of(i * LANES + k * EDGE, EDGE), EDGE), pl.ds(0, LANES * (i + 1))]
        return (
            pltpu.make_async_copy(src, dst, mat_loc.at[s, i]),
            remote(src, dst, mat_s.at[s, i], mat_r.at[s, i], mate),
        )

    def per_piece(n, act):
        q_now = block_of(n)[2]
        for q in range(slots):

            @pl.when(q_now == q)
            def _(q=q):
                for i in range(runs):
                    act(q, i)

    def fetch_blk(n):
        w, _, _, h, _ = block_of(n)
        s = n % DEEP

        def go(q, i):
            c = h * rows + i * run
            z_now, y_run = c // RING, pl.ds(c % RING, run)
            at = pl.ds(low(q), lanes - low(q))
            dst = in_blk(n, q, i, k_half)

            def both(src):
                pltpu.make_async_copy(src, dst, blk_loc.at[s, i]).start()
                remote(src, dst, blk_s.at[s, i], blk_r.at[s, i], mate).start()

            pl.when(k == 0)(lambda: both(gath.at[w, q, z_now, y_run, :, at]))
            pl.when(k == 1)(lambda: both(gath.at[w, q, y_run, z_now, :, at]))

        per_piece(n, go)

    def fetch_mat(n):
        for i in range(n128):
            for c in mat_copies(n, i):
                c.start()

    def wait_blk(n):
        def one(q, i):
            await_(in_blk(n, q, i, k_half), blk_loc.at[n % DEEP, i])
            from_mate(n, q, i)

        per_piece(n, one)

    def wait_mat(n):
        for i in range(n128):
            mat_copies(n, i)[0].wait()
            there = pl.ds(pl.multiple_of(i * LANES + (1 - k) * EDGE, EDGE), EDGE), pl.ds(0, LANES * (i + 1))
            await_(mbuf.at[(n % 2, *there)], mat_r.at[n % 2, i])

    def release_blk(n):
        per_piece(n, lambda q, i: await_(in_blk(n, q, i, k_half), blk_s.at[n % DEEP, i]))

        @pl.when(n + DEEP < 2 * nb)
        def _():
            pl.semaphore_signal(free_b.at[n % DEEP], inc=1, device_id=mate, device_id_type=MESH)
            pl.semaphore_wait(free_b.at[n % DEEP], 1)
            fetch_blk(n + DEEP)

    def release_mat(n):
        for i in range(n128):
            mat_copies(n, i)[1].wait_send()

        @pl.when(n + 2 < 2 * nb)
        def _():
            pl.semaphore_signal(free_m.at[n % 2], inc=1, device_id=mate, device_id_type=MESH)
            pl.semaphore_wait(free_m.at[n % 2], 1)
            fetch_mat(n + 2)

    barrier = pltpu.get_barrier_semaphore()

    def here_i_am(device):
        pl.semaphore_signal(barrier, inc=1, device_id=device, device_id_type=MESH)

    def group_member(d):
        n = lax.rem(2 * part + k + d, 2 * rows)
        here_i_am({"col": grp * rows + n // 2, "row": 2 * x + n % 2})

    _loop(1, 2 * rows, group_member)
    for d in range(1, chips):
        here_i_am(at_peer(d))
    for d in (1, RING - 1):
        here_i_am(plane(d, 0))
        here_i_am(plane(0, d))

    ins = [
        pltpu.make_async_copy(src, stage.at[i % 2], in_sem.at[i]) for i, src in enumerate((v_in, l_in, z_in))
    ] + [pltpu.make_async_copy(t_in, tb, in_sem.at[3])]
    for i in (0, 1, 3):
        ins[i].start()
    pl.semaphore_wait(barrier, 2 * rows - 1 + chips - 1 + 4)

    def swaps(m, i):
        there = _at(2 * i + k, LANES)
        if m < 2:
            mine, theirs = vt.at[m, :, k, :, _at(i, LANES)], vt.at[m, :, 1 - k, :, _at(i, LANES)]
            dst = own.at[m, :, :, there]
        else:
            mine, theirs = zt.at[k, :, _at(i, LANES)], zt.at[1 - k, :, _at(i, LANES)]
            dst = ys.at[:, there]
        return (
            pltpu.make_async_copy(mine, dst, swap_l.at[m, i]),
            remote(theirs, dst, swap_s.at[m, i], swap_r.at[m, i], mate),
        )

    def arriving(m, i):
        there = _at(2 * i + 1 - k, LANES)
        await_(own.at[m, :, :, there] if m < 2 else ys.at[:, there], swap_r.at[m, i])

    def turn(m, then=None):
        ins[m].wait()

        def one(i):
            block = stage[m % 2, _at(i, LANES), :].T
            if m < 2:
                vt[m, :, :, :, _at(i, LANES)] = block.reshape(slots, 2, HALF, LANES)
            else:
                zt[:, :, _at(i, LANES)] = block.reshape(2, ncol, LANES)
            for c in swaps(m, i):
                c.start()
            if then is not None:
                pl.when(i > 0)(lambda: then(i - 1))

        _loop(0, pairs, one)
        if then is not None:
            then(pairs - 1)

    def swapped(m):
        def one(i):
            swaps(m, i)[0].wait()
            arriving(m, i)

        _loop(0, pairs, one)

    my_q, my_h = part, grp
    my_j = groups * my_q + my_h
    first_t = my_j // 2

    def deal_v(q, t, act):
        to, kk = grp * rows + q, t % 2
        src = own.at[0, q, :, _at(t, STEP)]
        dst = vb.at[t // 2, part, k_half]
        self_ = jnp.logical_and(to == col, k == kk)
        act(
            self_,
            pltpu.make_async_copy(src, dst, v_r.at[t // 2, part, k]),
            remote(src, dst, v_s.at[q, t], v_r.at[t // 2, part, k], {"col": to, "row": 2 * x + kk}),
        )

    def deal_l(q, kk, act):
        to = grp * rows + q
        src = own.at[1, q, :, _at((groups * q + grp) // 2, STEP)]
        dst = ld.at[part, k_half]
        self_ = jnp.logical_and(to == col, k == kk)
        act(
            self_,
            pltpu.make_async_copy(src, dst, l_r.at[part, k]),
            remote(src, dst, l_s.at[q, kk], l_r.at[part, k], {"col": to, "row": 2 * x + kk}),
        )

    def send(self_, here, there):
        pl.when(self_)(here.start)
        pl.when(jnp.logical_not(self_))(there.start)

    def sent(self_, here, there):
        pl.when(jnp.logical_not(self_))(there.wait_send)

    def over_v(act):
        def one(q):
            _loop((groups * q + grp) // 2, pairs, lambda t: deal_v(q, t, act))

        _loop(0, slots, one)

    def over_l(act):
        def one(q):
            deal_l(q, 0, act)
            deal_l(q, 1, act)

        _loop(0, slots, one)

    def deal_chunk(t):
        swaps(0, t)[0].wait()
        arriving(0, t)
        _loop(0, (2 * t + 1 - grp + groups) // groups, lambda q: deal_v(q, t, send))

    turn(0, deal_chunk)
    ins[2].start()
    turn(1)
    swapped(1)
    over_l(send)
    turn(2)
    mbuf[...] = jnp.zeros_like(mbuf)

    gm[...] = jnp.zeros_like(gm)

    def chunk(i):
        def got(n):
            await_(vb.at[i, n // 2, _at(n % 2, HALF)], v_r.at[i, n // 2, n % 2])

        _loop(0, 2 * rows, got)
        all_ = vb[i].reshape(size, STEP)
        gm[pl.ds(0, hsize), pl.ds(0, hsize)] += _dot_nt(all_[:hsize], all_[:hsize])
        gm[pl.ds(hsize, hsize), :] += _dot_nt(all_[hsize:], all_)

    _loop((first_t + 1 - k) // 2, pairs // 2, chunk)
    tick(0)

    widths = []
    w_ = hsize
    while w_ >= EDGE:
        widths.append(w_)
        w_ //= 2

    def packed(w_):
        return pl.ds(size - 2 * w_, w_)

    pk[...] = jnp.zeros_like(pk)
    for w_ in widths:
        for i in range(hsize // w_):
            pk[pl.ds(i * w_, w_), packed(w_)] = gm[pl.ds((2 * i + 1) * w_, w_), pl.ds(2 * i * w_, w_)]

    mine, theirs = _at(k, qsize), _at(1 - k, qsize)
    to_mate = remote(pk.at[theirs], gx, gx_sem.at[0], gx_sem.at[1], mate)
    to_mate.start()
    tick(1)
    to_mate.wait_recv()
    pk[mine] += gx[...]
    rl = qsize // chips

    def r2_copy(d):
        src = pk.at[pl.ds(pl.multiple_of(k * qsize + peer(d) * rl, rl), rl)]
        return remote(src, r2.at[d - 1], r2_s.at[d - 1], r2_r.at[d - 1], at_peer(d))

    for d in range(1, chips):
        r2_copy(d).start()

    def got_l(n):
        await_(ld.at[n // 2, _at(n % 2, HALF)], l_r.at[n // 2, n % 2])

    _loop(0, 2 * rows, got_l)
    ev = my_j % 2 == 0
    lo_half = lax.broadcasted_iota(jnp.int32, (size, LANES), 1) < EDGE
    l_lo, l_hi = ld[:, :, pl.ds(0, LANES)].reshape(size, LANES), ld[:, :, pl.ds(LANES, LANES)].reshape(size, LANES)
    lx[x] = jnp.where(
        lo_half,
        jnp.where(ev, l_lo, pltpu.roll(l_lo, EDGE, 1)),
        jnp.where(ev, pltpu.roll(l_hi, EDGE, 1), l_hi),
    )

    def lx_copy(d):
        return remote(lx.at[x], lx.at[x], lx_s.at[d - 1], lx_r.at[d - 1], at_peer(d))

    tick(2)
    for d in range(1, chips):
        r2_copy(d).wait_recv()
    my_rows = pl.ds(pl.multiple_of(k * qsize + x * rl, rl), rl)
    total = pk[my_rows]
    for d in range(1, chips):
        total = total + r2[d - 1]
    ga[my_rows] = total

    def ga_copy(d):
        return remote(ga.at[my_rows], ga.at[my_rows], ga_s.at[d - 1], ga_r.at[d - 1], at_peer(d))

    for d in range(1, chips):
        ga_copy(d).start()
    for d in range(1, chips):
        lx_copy(d).start()
    tick(3)
    for d in range(1, chips):
        await_(ga.at[pl.ds(pl.multiple_of(k * qsize + peer(chips - d) * rl, rl), rl)], ga_r.at[d - 1])
    half_to_mate = remote(ga.at[mine], ga.at[mine], gx_sem.at[2], gx_sem.at[3], mate)
    half_to_mate.start()

    r_i = lax.broadcasted_iota(jnp.int32, (LANES, LANES), 0)
    c_i = lax.broadcasted_iota(jnp.int32, (LANES, LANES), 1)

    def tile(i):
        return _at(i, LANES), _at(i, LANES)

    def merge_tile(w, i, low_part):
        cur = xm[(w, *tile(i))]
        xm[(w, *tile(i))] = cur - _dot_nn(_dot_nn(cur, low_part), cur)

    def level_l(lev):
        pick = jnp.logical_and(
            lax.shift_right_logical(r_i, lev) % 2 == 1,
            lax.shift_right_logical(c_i, lev) + 1 == lax.shift_right_logical(r_i, lev),
        )
        _loop(0, n128, lambda i: merge_tile(1, i, jnp.where(pick, gm[tile(i)], 0.0)))

    def level_big(w, corner):
        for w_ in reversed(widths[:-1]):
            for i in range(hsize // w_):
                d1 = pl.ds(2 * i * w_, w_)
                d2 = pl.ds((2 * i + 1) * w_, w_)
                xm[w, d2, d1] = -_dot_nn(_dot_nn(xm[w, d2, d2], corner(w_, i)), xm[w, d1, d1])

    def pack_factor(w):
        for i in range(n128):
            pm[w, :, pl.ds(LANES * (i * (i + 1) // 2), LANES * (i + 1))] = xm[
                w, pl.ds(pl.multiple_of(i * LANES + k * EDGE, EDGE), EDGE), pl.ds(0, LANES * (i + 1))
            ]

    xm[...] = jnp.zeros_like(xm)
    ins[3].wait()
    for p in range(0, rows, 2):
        zero = jnp.zeros((EDGE, EDGE), jnp.float32)
        both = jnp.concatenate(
            [jnp.concatenate([tb[p], zero], axis=1), jnp.concatenate([zero, tb[p + 1]], axis=1)], axis=0
        )
        xm[0, pl.ds(p * EDGE, LANES), pl.ds(p * EDGE, LANES)] = both
    await_(ga.at[theirs], gx_sem.at[3])

    def corner64(i):
        block = ga[_at(i, EDGE), packed(EDGE)]
        zero = jnp.zeros((EDGE, EDGE), jnp.float32)
        low_part = jnp.concatenate([block, zero], axis=1)
        merge_tile(0, i, jnp.concatenate([jnp.zeros_like(low_part), low_part], axis=0))

    _loop(0, n128, corner64)
    level_big(0, lambda w_, i: ga[pl.ds(i * w_, w_), packed(w_)])
    pack_factor(0)
    tick(4)

    fetch_blk(0)
    fetch_blk(1)
    for d in range(1, chips):
        await_(lx.at[peer(chips - d)], lx_r.at[d - 1])
    for i in range(chips):
        gm[_at(i, LANES), :] = lx[i].T
    same = r_i == c_i

    def diag(i):
        d = gm[tile(i)]
        xm[(1, *tile(i))] = jnp.where(same, 1.0 / jnp.where(same, d, 1.0), 0.0)

    _loop(0, n128, diag)
    swapped(2)
    tick(5)
    _loop(0, 3, level_l)
    tick(6)
    _loop(3, 7, level_l)
    tick(7)
    level_big(1, lambda w_, i: gm[pl.ds((2 * i + 1) * w_, w_), pl.ds(2 * i * w_, w_)])
    pack_factor(1)
    tick(8)
    fetch_mat(0)
    fetch_mat(1)
    fetch_blk(2)

    def over(first, body):
        pl.when(first % 2 == 1)(lambda: body(first * STEP, STEP))
        _loop((first + 1) // 2, whole // 2, lambda i: body(i * 2 * STEP, 2 * STEP))

    def rows_at(off, width):
        return pl.ds(pl.multiple_of(off, STEP), width)

    def cut(n, off, width):
        return blk[n % DEEP, :, :, rows_at(off, width)].reshape(size, width)

    def project(dst, ref, n, first):
        dst[...] = jnp.zeros((ncol, size), jnp.float32)

        def one(off, width):
            dst[...] += _dot_nt(ref[:, rows_at(off, width)], cut(n, off, width))

        over(first, one)

    def slice_of(g, x2):
        return pl.ds(pl.multiple_of(g * gcol + x2 * sl, sl), sl)

    def cols_of(g):
        return pl.ds(g * gcol, gcol)

    def rs_copy(par, g, d):
        return remote(sbuf.at[par, slice_of(g, peer(d))], rs.at[g, d - 1], rs_s.at[g, d - 1], rs_r.at[g, d - 1], at_peer(d))

    def w_copy(par, g, d):
        mine = wb.at[par, slice_of(g, x)]
        return remote(mine, mine, ex_s.at[g, d - 1], ex_r.at[g, d - 1], at_peer(d))

    c_half = pl.ds(pl.multiple_of(k * (rows // 2), rows // 2), rows // 2)

    def c_copy(par):
        return remote(cm.at[par, _at(k, hsize)], cm.at[par, _at(k, hsize)], cm_s.at[par], cm_r.at[par], mate)

    def apply(n, off, width):
        ys[:, rows_at(off, width)] = ys[:, rows_at(off, width)] - _dot_nn(wb[n % 2], cut(n, off, width))

    def cross(n, off, width):
        here = blk[n % DEEP, c_half, :, rows_at(off, width)].reshape(hsize, width)
        cm[n % 2, _at(k, hsize)] += _dot_nt(here, cut(n + 1, off, width))

    def cols_in(gs):
        return pl.ds(gs[0] * gcol, len(gs) * gcol)

    wait_blk(0)
    project(sbuf.at[0], ys, 0, top // 2)
    for g in range(2):
        for d in range(1, chips):
            rs_copy(0, g, d).start()
    wait_mat(0)

    def reflect(n):
        j, par, nxt = top - n, n % 2, (n + 1) % 2

        @pl.when(j > 0)
        def _():
            wait_blk(n + 1)
            cm[par, _at(k, hsize)] = jnp.zeros((hsize, size), jnp.float32)
            pl.when(j % 2 == 1)(lambda: cross(n, (j // 2) * STEP, STEP))

            def one(off, width):
                apply(n - 1, off, width)
                cross(n, off, width)

            over((j + 1) // 2, one)
            c_copy(par).start()

        pl.when(j == 0)(lambda: over(0, functools.partial(apply, n - 1)))

        def factor(gs):
            totals = []
            for g in gs:
                for d in range(1, chips):
                    rs_copy(par, g, d).wait_recv()
                total = sbuf[par, slice_of(g, x)]
                for d in range(1, chips):
                    total = total + rs[g, d - 1]
                totals.append(total)
            got = _dot_nn(jnp.concatenate(totals, axis=0), mbuf[par])
            for i, g in enumerate(gs):
                wb[par, slice_of(g, x)] = got[i * sl : (i + 1) * sl]
                for d in range(1, chips):
                    w_copy(par, g, d).start()

        factor((0,))
        factor((1,))

        for g in range(2):
            for d in range(1, chips):
                rs_copy(par, g, d).wait_send()

        @pl.when(jnp.logical_and(n < 8, par == 0))
        def _():
            tick(LEAD + n // 2)

        @pl.when(n >= 8)
        def _():
            tick(LEAD - 4 + n)

        pl.when(n > 0)(lambda: release_blk(n - 1))
        release_mat(n)

        @pl.when(j > 0)
        def _():
            project(sbuf.at[nxt], ys, n + 1, (j - 1) // 2)
            wait_mat(n + 1)
            await_(cm.at[par, _at(1 - k, hsize)], cm_r.at[par])

        def correct(gs):
            for g in gs:
                for d in range(1, chips):
                    await_(wb.at[par, slice_of(g, peer(chips - d))], ex_r.at[g, d - 1])

            @pl.when(j > 0)
            def _():
                sbuf[nxt, cols_in(gs)] = sbuf[nxt, cols_in(gs)] - _dot_nn(wb[par, cols_in(gs)], cm[par])
                for g in gs:
                    for d in range(1, chips):
                        rs_copy(nxt, g, d).start()

        correct((0,))
        correct((1,))

        for g in range(2):
            for d in range(1, chips):
                w_copy(par, g, d).wait_send()

        @pl.when(j > 0)
        def _():
            c_copy(par).wait_send()

    _loop(0, nb, reflect)
    over(0, functools.partial(apply, top))
    release_blk(top)

    xs[...] = jnp.zeros_like(xs)
    def first_half(val):
        return lax.broadcasted_iota(jnp.int32, val.shape, 1) < EDGE


    def take(ref, cols_, j):
        lo = ref[cols_, pl.ds(pl.multiple_of((j // 2) * STEP, LANES), LANES)]
        hi = ref[cols_, pl.ds(pl.multiple_of((j // 2) * STEP + LANES, LANES), LANES)]
        even = j % 2 == 0
        return jnp.where(
            first_half(lo),
            jnp.where(even, lo, pltpu.roll(lo, EDGE, 1)),
            jnp.where(even, pltpu.roll(hi, EDGE, 1), hi),
        )

    def spread(val, j):
        even, first = j % 2 == 0, first_half(val)
        other = pltpu.roll(val, EDGE, 1)
        zero = jnp.zeros_like(val)
        lo = jnp.where(even, jnp.where(first, val, zero), jnp.where(first, zero, other))
        hi = jnp.where(even, jnp.where(first, other, zero), jnp.where(first, zero, val))
        return jnp.concatenate([lo, hi], axis=1)

    def x_copy(par, g, d):
        src = sbuf.at[par, cols_of(g), _at(peer(d), LANES)]
        return remote(src, rx.at[par, g, d - 1], rx_s.at[par, g, d - 1], rx_r.at[par, g, d - 1], at_peer(d))

    def solve_partial(n, gs, j):
        par, cols_ = n % 2, cols_in(gs)
        wb[0, cols_] = -wb[0, cols_]
        wb[0, cols_, _at(x, LANES)] += take(ys, cols_, j)
        sbuf[par, cols_] = _dot_nn(wb[0, cols_], mbuf[par])
        for g in gs:
            for d in range(1, chips):
                x_copy(par, g, d).start()

    def fin_copy(i):
        return remote(
            xs.at[:, _at(2 * i + 1 - k, LANES)], zt.at[k, :, _at(i, LANES)], fin_s.at[i], fin_r.at[i], mate
        )

    def give(i):
        await_(zt.at[1 - k, :, _at(i, LANES)], fin_r.at[i])
        zt[k, :, _at(i, LANES)] = xs[:, _at(2 * i + k, LANES)]
        out_ref[_at(i, LANES), :] = zt[:, :, _at(i, LANES)].reshape(2 * ncol, LANES).T

    for m in range(3):
        _loop(0, pairs, lambda i, m=m: swaps(m, i)[1].wait_send())
    over_v(sent)
    over_l(sent)
    to_mate.wait_send()
    half_to_mate.wait_send()
    for d in range(1, chips):
        r2_copy(d).wait_send()
        ga_copy(d).wait_send()
        lx_copy(d).wait_send()

    wait_blk(nb)
    wait_mat(nb)
    wb[0] = jnp.zeros((ncol, size), jnp.float32)
    for g in range(2):
        solve_partial(nb, (g,), top)
    release_blk(nb)
    release_mat(nb)

    def solve(i):
        n = nb + i
        j, par, nxt = top - i, n % 2, (n + 1) % 2

        @pl.when(j > 0)
        def _():
            wait_blk(n + 1)
            wait_mat(n + 1)
            project(wb.at[0], xs, n + 1, (j + 1) // 2)

        def finish(gs):
            cols_ = cols_in(gs)
            vals = []
            for g in gs:
                for d in range(1, chips):
                    x_copy(par, g, d).wait_recv()
                val = sbuf[par, cols_of(g), _at(x, LANES)]
                for d in range(1, chips):
                    val = val + rx[par, g, d - 1]
                vals.append(val)
            solved = spread(jnp.concatenate(vals, axis=0), j)
            xs[cols_, _at(j // 2, STEP)] += solved

            @pl.when(j > 0)
            def _():
                wb[0, cols_] += _dot_nt(solved, cut(n + 1, (j // 2) * STEP, STEP))
                solve_partial(n + 1, gs, j - 1)

        finish((0,))
        finish((1,))

        pl.when(j % 2 == 0)(lambda: fin_copy(j // 2).start())
        pl.when(jnp.logical_and(j % 2 == 1, j < top))(lambda: give(j // 2 + 1))

        for g in range(2):
            for d in range(1, chips):
                x_copy(par, g, d).wait_send()

        @pl.when(j > 0)
        def _():
            release_blk(n + 1)
            release_mat(n + 1)

        tick(LEAD - 4 + n)

    _loop(0, nb, solve)

    give(0)
    _loop(0, pairs, lambda i: fin_copy(i).wait_send())


def solution(mesh):
    rows, cols = mesh.shape["row"], mesh.shape["col"]
    mat_spec = P(("kpt", "row"), "col")
    fac_spec = P("kpt", None, None)

    def local_work(v_loc, t_loc, z_loc, l_loc):
        n_row, n_col = v_loc.shape
        slots, lanes, chips, size = n_col // EDGE, 2 * n_row, rows // 2, rows * EDGE
        nb, ncol = lanes // LANES, z_loc.shape[1] // 2
        pairs, gcol, peers = nb // 2, ncol // 2, max(chips - 1, 1)
        sl, gathers, n128 = gcol // chips, len(_gathers(slots)), size // LANES
        tri = LANES * (n128 * (n128 + 1) // 2)
        dma = pltpu.SemaphoreType.DMA
        hbm, vmem = pl.BlockSpec(memory_space=pl.ANY), pl.BlockSpec(memory_space=pltpu.VMEM)

        def buf(*shape):
            return pltpu.VMEM(shape, jnp.float32)

        col = lax.axis_index("col")
        t_mine = lax.dynamic_slice_in_dim(t_loc, (cols // rows * (col % rows) + col // rows) * rows, rows, axis=0)
        return pl.pallas_call(
            functools.partial(_kernel, (rows, cols, slots, nb, ncol)),
            out_shape=[
                jax.ShapeDtypeStruct(z_loc.shape, jnp.float32),
                jax.ShapeDtypeStruct((2, slots, RING, RING, HALF, lanes), jnp.float32),
            ],
            in_specs=[hbm] * 4,
            out_specs=[vmem, hbm],
            scratch_shapes=[
                buf(2, n_row, n_col),
                buf(2, slots, 2, HALF, n_row),
                buf(2, ncol, n_row),
                buf(rows, EDGE, EDGE),
                buf(2, slots, HALF, lanes),
                buf(ncol, lanes),
                buf(ncol, lanes),
                buf(pairs // 2, rows, EDGE, STEP),
                buf(rows, EDGE, STEP),
                buf(chips, size, LANES),
                buf(size, size),
                buf(size // 2, size),
                buf(size // 4, size),
                buf(peers, size // 4 // chips, size),
                buf(size // 2, size),
                buf(2, size, size),
                buf(2, EDGE, tri),
                buf(2, RING, RING, EDGE, tri),
                buf(DEEP, rows, EDGE, lanes),
                buf(2, size, size),
                buf(2, ncol, size),
                buf(2, peers, sl, size),
                buf(2, ncol, size),
                buf(2, size, size),
                buf(2, 2, peers, gcol, LANES),
                dma((4,)),
                dma((3, pairs)), dma((3, pairs)), dma((3, pairs)),
                dma((slots, pairs)), dma((pairs // 2, rows, 2)),
                dma((slots, 2)), dma((rows, 2)),
                dma((peers,)), dma((peers,)),
                dma((4,)),
                dma((peers,)), dma((peers,)), dma((peers,)), dma((peers,)),
                dma((pairs,)), dma((pairs,)),
                dma((gathers,)), dma((gathers, 8)), dma((gathers, 8)),
                dma((DEEP, rows)), dma((DEEP, rows)), dma((DEEP, rows)),
                dma((2, n128)), dma((2, n128)), dma((2, n128)),
                pltpu.SemaphoreType.REGULAR((DEEP,)), pltpu.SemaphoreType.REGULAR((2,)),
                dma((2, peers)), dma((2, peers)), dma((2, peers)), dma((2, peers)),
                dma((2,)), dma((2,)),
                dma((2, 2, peers)), dma((2, 2, peers)),
            ],
            compiler_params=pltpu.CompilerParams(collective_id=0, has_side_effects=True, vmem_limit_bytes=67_043_328),
            name="eigvec",
        )(v_loc, t_mine, z_loc, l_loc)[0]

    return jax.shard_map(local_work, mesh=mesh, in_specs=(mat_spec, fac_spec, mat_spec, mat_spec), out_specs=mat_spec, check_vma=False)
```

```python
import functools

import jax
import jax.numpy as jnp
from jax import lax
from jax.experimental import pallas as pl
from jax.experimental.pallas import tpu as pltpu
from jax.sharding import PartitionSpec as P

PREC_HIGH = lax.Precision.HIGHEST
MESH = pl.DeviceIdType.MESH
EDGE = 64
HALF = EDGE // 2
LANES = 128
STEP = 256
RING = 4
LEAD = 9
DEEP = 3


def _dot_nt(a, b):
    return lax.dot_general(a, b, (((1,), (1,)), ((), ())), precision=PREC_HIGH, preferred_element_type=jnp.float32)


def _dot_nn(a, b):
    return lax.dot_general(a, b, (((1,), (0,)), ((), ())), precision=PREC_HIGH, preferred_element_type=jnp.float32)


def _at(i, n):
    return pl.ds(pl.multiple_of(i * n, n), n)


def _loop(lo, hi, body):
    def one(i, carry):
        body(i)
        return carry

    lax.fori_loop(lo, hi, one, 0)


def _gathers(slots):
    early = [(slots - 1, 0), (slots - 2, 0), None, None, ("m", 0)]
    first = early + [(q, 0) for q in range(slots - 3, -1, -1)]
    rest = [(slots - 1, 1), ("m", 1)] + [(q, 1) for q in range(slots - 2, -1, -1)]
    return first + [None] * (LEAD - len(first)) + rest


def _kernel(dims, v_in, t_in, z_in, l_in, out_ref, gath, *scratch):
    (stage, vt, zt, tb, own, ys, xs, vb, ld, lx, gm, pk, gx, r2, ga, xm, pm, mg, blk, mbuf, sbuf, rs, wb, cm, rx,
     in_sem, swap_l, swap_s, swap_r, v_s, v_r, l_s, l_r, lx_s, lx_r, gx_sem, r2_s, r2_r, ga_s, ga_r, fin_s, fin_r,
     ag_loc, ag_s, ag_r, blk_loc, blk_s, blk_r, mat_loc, mat_s, mat_r, free_b, free_m, rs_s, rs_r, ex_s, ex_r, cm_s, cm_r,
     rx_s, rx_r, eg_s, eg_r) = scratch
    rows, cols, slots, nb, ncol = dims
    row, col = lax.axis_index("row"), lax.axis_index("col")
    x, k = row // 2, row % 2
    chips, groups = rows // 2, cols // rows
    size, lanes = rows * EDGE, nb * LANES
    hsize, qsize, n128 = size // 2, size // 4, size // LANES
    pairs = nb // 2
    gcol = ncol // 2
    sl = gcol // chips
    mate = {"row": row + 1 - 2 * k, "col": col}
    top, whole = nb - 1, nb // 2
    part, grp = col % rows, col // rows
    k_half, m_half = _at(k, HALF), _at(1 - k, HALF)
    s_a, s_b = 1 + (RING - 1) * k, RING - (RING - 1) * k
    a, b = (col // s_a) % RING, (col // s_b) % RING

    def remote(src, dst, ss, rr, to):
        return pltpu.make_async_remote_copy(src, dst, ss, rr, device_id=to, device_id_type=MESH)

    def await_(ref, sem):
        pltpu.make_async_copy(ref, ref, sem).wait()

    def peer(d):
        return lax.rem(x + d, chips)

    def at_peer(d):
        return {"row": 2 * peer(d) + k, "col": col}

    def plane(da, db):
        return {"row": row, "col": lax.rem(a + da, RING) * s_a + lax.rem(b + db, RING) * s_b}

    def low(q):
        return (groups * q // 2) * STEP

    order = _gathers(slots)

    class Slot:
        def __init__(self, kind, w, n):
            self.kind, self.w, self.n = kind, w, n

        def own(self):
            if self.kind == "m":
                return pm.at[self.w]
            return own.at[self.w, self.kind, :, pl.ds(low(self.kind), lanes - low(self.kind))]

        def piece(self, bb, aa, part=None):
            if self.kind == "m":
                return mg.at[self.w, bb, aa] if part is None else mg.at[self.w, bb, aa, pl.ds(part * HALF, HALF)]
            at = pl.ds(low(self.kind), lanes - low(self.kind))
            e = slice(None) if part is None else pl.ds(part * (HALF // 2), HALF // 2)
            return gath.at[self.w, self.kind, bb, aa, e, at]

        def bundle(self, bb, part=None):
            e = slice(None) if part is None else pl.ds(part * (RING // 2), RING // 2)
            if self.kind == "m":
                return mg.at[self.w, bb, e]
            return gath.at[self.w, self.kind, bb, e, :, pl.ds(low(self.kind), lanes - low(self.kind))]

        def copy(self, i):
            d = 1 if i % 2 == 0 else RING - 1
            back = RING - d
            if i < 2:
                src, dst, to = self.own(), self.piece(b, a), plane(d, 0)
            elif i < 4:
                src = dst = self.piece(b, lax.rem(a + back, RING), i % 2)
                to = plane(d, 0)
            elif i < 6:
                src = dst = self.bundle(b)
                to = plane(0, d)
            else:
                src = dst = self.bundle(lax.rem(b + back, RING), i % 2)
                to = plane(0, d)
            return remote(src, dst, ag_s.at[self.n, i], ag_r.at[self.n, i], to)

        def arrived(self, i):
            back = RING - 1 if i % 2 == 0 else 1
            if i < 2:
                dst = self.piece(b, lax.rem(a + back, RING))
            elif i < 4:
                dst = self.piece(b, lax.rem(a + 2, RING), i % 2)
            elif i < 6:
                dst = self.bundle(lax.rem(b + back, RING))
            else:
                dst = self.bundle(lax.rem(b + 2, RING), i % 2)
            await_(dst, ag_r.at[self.n, i])

        def kept(self):
            return pltpu.make_async_copy(self.own(), self.piece(b, a), ag_loc.at[self.n])

        def stage(self, s):
            if s == 0:
                self.copy(0).start()
                self.copy(1).start()
                self.kept().start()
            elif s == 1:
                for i in range(2):
                    self.arrived(i)
                    self.copy(2 + i).start()
            elif s == 2:
                self.kept().wait()
                self.arrived(2)
                self.arrived(3)
                self.copy(4).start()
                self.copy(5).start()
            elif s == 3:
                for i in range(4, 6):
                    self.arrived(i)
                    self.copy(2 + i).start()
            elif s == 4:
                self.arrived(6)
                self.arrived(7)
            else:
                for i in range(8):
                    self.copy(i).wait_send()

    class Eager(Slot):
        def spot(self, db, da, part=None):
            return self.piece(lax.rem(b + db, RING), lax.rem(a + da, RING), part)

        def copy(self, i):
            back = RING - 1
            db, da, part, to_b, to_a = (
                (0, 0, None, 0, 1), (0, 0, None, 0, back), (0, 0, None, 1, 0), (0, 0, None, back, 0),
                (0, back, 0, 0, 1), (0, 1, 1, 0, back),
                (0, back, None, 1, 0), (0, back, None, back, 0), (0, 1, None, 1, 0), (0, 1, None, back, 0),
                (0, 2, None, 1, 0), (0, 2, None, back, 0),
                (back, 0, None, 1, 0), (back, back, None, 1, 0), (1, 1, None, back, 0), (1, 2, None, back, 0),
            )[i]
            dst = self.spot(db, da, part)
            src = self.own() if db == 0 and da == 0 else dst
            sent_ = remote(src, dst, eg_s.at[i], eg_r.at[i], plane(to_a, to_b))
            return sent_, self.spot(db + RING - to_b, da + RING - to_a, part)

        def go(self, *which):
            for i in which:
                self.copy(i)[0].start()

        def got(self, *which):
            for i in which:
                await_(self.copy(i)[1], eg_r.at[i])

        def stage(self, s):
            if s == 0:
                self.go(0, 1, 2, 3)
                self.kept().start()
            elif s == 1:
                self.got(0)
                self.go(4, 6, 7)
                self.got(1)
                self.go(5, 8, 9)
                self.got(2)
                self.go(12)
            elif s == 2:
                self.got(4, 5)
                self.go(10, 11)
                self.got(6)
                self.go(13)
            elif s == 3:
                self.got(9)
                self.go(14)
                self.got(11)
                self.go(15)
            elif s == 4:
                self.got(3, 7, 8, 10, 12, 13, 14, 15)
                self.kept().wait()
                for i in range(16):
                    self.copy(i)[0].wait_send()

    def tick(t):
        for s in (4, 3, 2, 1, 0, 5):
            n = t - s
            if isinstance(n, int):
                if 0 <= n < len(order) and order[n] is not None:
                    (Eager if order[n] == ("m", 0) else Slot)(*order[n], n).stage(s)
                continue
            for kind in list(range(slots)) + ["m"]:
                at_v, at_l = order.index((kind, 0)), order.index((kind, 1))

                @pl.when(n == at_l if kind == "m" else jnp.logical_or(n == at_v, n == at_l))
                def _(s=s, n=n, kind=kind, at_l=at_l):
                    Slot(kind, jnp.where(n == at_l, 1, 0), n).stage(s)

    def block_of(n):
        j = top - n % nb
        return n // nb, j, j // groups, j % groups, n % 2

    run = min(rows, RING)
    runs = rows // run

    def in_blk(n, q, i, half):
        return blk.at[n % DEEP, pl.ds(i * run, run), half, pl.ds(low(q), lanes - low(q))]

    def from_mate(n, q, i):
        await_(in_blk(n, q, i, m_half), blk_r.at[n % DEEP, i])

    def mat_copies(n, i):
        w, j, q, h, s = block_of(n)
        c = h * rows + q
        src = mg.at[w, (c // s_b) % RING, (c // s_a) % RING, :, pl.ds(LANES * (i * (i + 1) // 2), LANES * (i + 1))]
        dst = mbuf.at[s, pl.ds(pl.multiple_of(i * LANES + k * EDGE, EDGE), EDGE), pl.ds(0, LANES * (i + 1))]
        return (
            pltpu.make_async_copy(src, dst, mat_loc.at[s, i]),
            remote(src, dst, mat_s.at[s, i], mat_r.at[s, i], mate),
        )

    def per_piece(n, act):
        q_now = block_of(n)[2]
        for q in range(slots):

            @pl.when(q_now == q)
            def _(q=q):
                for i in range(runs):
                    act(q, i)

    def fetch_blk(n):
        w, _, _, h, _ = block_of(n)
        s = n % DEEP

        def go(q, i):
            c = h * rows + i * run
            z_now, y_run = c // RING, pl.ds(c % RING, run)
            at = pl.ds(low(q), lanes - low(q))
            dst = in_blk(n, q, i, k_half)

            def both(src):
                pltpu.make_async_copy(src, dst, blk_loc.at[s, i]).start()
                remote(src, dst, blk_s.at[s, i], blk_r.at[s, i], mate).start()

            pl.when(k == 0)(lambda: both(gath.at[w, q, z_now, y_run, :, at]))
            pl.when(k == 1)(lambda: both(gath.at[w, q, y_run, z_now, :, at]))

        per_piece(n, go)

    def fetch_mat(n):
        for i in range(n128):
            for c in mat_copies(n, i):
                c.start()

    def wait_blk(n):
        def one(q, i):
            await_(in_blk(n, q, i, k_half), blk_loc.at[n % DEEP, i])
            from_mate(n, q, i)

        per_piece(n, one)

    def wait_mat(n):
        for i in range(n128):
            mat_copies(n, i)[0].wait()
            there = pl.ds(pl.multiple_of(i * LANES + (1 - k) * EDGE, EDGE), EDGE), pl.ds(0, LANES * (i + 1))
            await_(mbuf.at[(n % 2, *there)], mat_r.at[n % 2, i])

    def release_blk(n):
        per_piece(n, lambda q, i: await_(in_blk(n, q, i, k_half), blk_s.at[n % DEEP, i]))

        @pl.when(n + DEEP < 2 * nb)
        def _():
            pl.semaphore_signal(free_b.at[n % DEEP], inc=1, device_id=mate, device_id_type=MESH)
            pl.semaphore_wait(free_b.at[n % DEEP], 1)
            fetch_blk(n + DEEP)

    def release_mat(n):
        for i in range(n128):
            mat_copies(n, i)[1].wait_send()

        @pl.when(n + 2 < 2 * nb)
        def _():
            pl.semaphore_signal(free_m.at[n % 2], inc=1, device_id=mate, device_id_type=MESH)
            pl.semaphore_wait(free_m.at[n % 2], 1)
            fetch_mat(n + 2)

    def over(first, body):
        pl.when(first % 2 == 1)(lambda: body(first * STEP, STEP))
        _loop((first + 1) // 2, whole // 2, lambda i: body(i * 2 * STEP, 2 * STEP))

    def rows_at(off, width):
        return pl.ds(pl.multiple_of(off, STEP), width)

    def cut(n, off, width):
        return blk[n % DEEP, :, :, rows_at(off, width)].reshape(size, width)

    def project(dst, ref, n, first):
        dst[...] = jnp.zeros((ncol, size), jnp.float32)

        def one(off, width):
            dst[...] += _dot_nt(ref[:, rows_at(off, width)], cut(n, off, width))

        over(first, one)

    def slice_of(g, x2):
        return pl.ds(pl.multiple_of(g * gcol + x2 * sl, sl), sl)

    def cols_of(g):
        return pl.ds(g * gcol, gcol)

    def rs_copy(par, g, d):
        return remote(sbuf.at[par, slice_of(g, peer(d))], rs.at[g, d - 1], rs_s.at[g, d - 1], rs_r.at[g, d - 1], at_peer(d))

    def w_copy(par, g, d):
        mine = wb.at[par, slice_of(g, x)]
        return remote(mine, mine, ex_s.at[g, d - 1], ex_r.at[g, d - 1], at_peer(d))

    c_half = pl.ds(pl.multiple_of(k * (rows // 2), rows // 2), rows // 2)

    def c_copy(par):
        return remote(cm.at[par, _at(k, hsize)], cm.at[par, _at(k, hsize)], cm_s.at[par], cm_r.at[par], mate)

    def apply(n, off, width):
        ys[:, rows_at(off, width)] = ys[:, rows_at(off, width)] - _dot_nn(wb[n % 2], cut(n, off, width))

    def cross(n, off, width):
        here = blk[n % DEEP, c_half, :, rows_at(off, width)].reshape(hsize, width)
        cm[n % 2, _at(k, hsize)] += _dot_nt(here, cut(n + 1, off, width))

    def cols_in(gs):
        return pl.ds(gs[0] * gcol, len(gs) * gcol)

    barrier = pltpu.get_barrier_semaphore()

    def here_i_am(device):
        pl.semaphore_signal(barrier, inc=1, device_id=device, device_id_type=MESH)

    def group_member(d):
        n = lax.rem(2 * part + k + d, 2 * rows)
        here_i_am({"col": grp * rows + n // 2, "row": 2 * x + n % 2})

    _loop(1, 2 * rows, group_member)
    for d in range(1, chips):
        here_i_am(at_peer(d))
    for d in (1, RING - 1):
        here_i_am(plane(d, 0))
        here_i_am(plane(0, d))

    ins = [
        pltpu.make_async_copy(src, stage.at[i % 2], in_sem.at[i]) for i, src in enumerate((v_in, l_in, z_in))
    ] + [pltpu.make_async_copy(t_in, tb, in_sem.at[3])]
    for i in (0, 1, 3):
        ins[i].start()
    pl.semaphore_wait(barrier, 2 * rows - 1 + chips - 1 + 4)

    def swaps(m, i):
        there = _at(2 * i + k, LANES)
        if m < 2:
            mine, theirs = vt.at[m, :, k, :, _at(i, LANES)], vt.at[m, :, 1 - k, :, _at(i, LANES)]
            dst = own.at[m, :, :, there]
        else:
            mine, theirs = zt.at[k, :, _at(i, LANES)], zt.at[1 - k, :, _at(i, LANES)]
            dst = ys.at[:, there]
        return (
            pltpu.make_async_copy(mine, dst, swap_l.at[m, i]),
            remote(theirs, dst, swap_s.at[m, i], swap_r.at[m, i], mate),
        )

    def arriving(m, i):
        there = _at(2 * i + 1 - k, LANES)
        await_(own.at[m, :, :, there] if m < 2 else ys.at[:, there], swap_r.at[m, i])

    def turn(m, then=None):
        ins[m].wait()

        def one(i):
            block = stage[m % 2, _at(i, LANES), :].T
            if m < 2:
                vt[m, :, :, :, _at(i, LANES)] = block.reshape(slots, 2, HALF, LANES)
            else:
                zt[:, :, _at(i, LANES)] = block.reshape(2, ncol, LANES)
            for c in swaps(m, i):
                c.start()
            if then is not None:
                pl.when(i > 0)(lambda: then(i - 1))

        _loop(0, pairs, one)
        if then is not None:
            then(pairs - 1)

    def swapped(m):
        def one(i):
            swaps(m, i)[0].wait()
            arriving(m, i)

        _loop(0, pairs, one)

    my_q, my_h = part, grp
    my_j = groups * my_q + my_h
    first_t = my_j // 2

    def deal_v(q, t, act):
        to, kk = grp * rows + q, t % 2
        src = own.at[0, q, :, _at(t, STEP)]
        dst = vb.at[t // 2, part, k_half]
        self_ = jnp.logical_and(to == col, k == kk)
        act(
            self_,
            pltpu.make_async_copy(src, dst, v_r.at[t // 2, part, k]),
            remote(src, dst, v_s.at[q, t], v_r.at[t // 2, part, k], {"col": to, "row": 2 * x + kk}),
        )

    def deal_l(q, kk, act):
        to = grp * rows + q
        src = own.at[1, q, :, _at((groups * q + grp) // 2, STEP)]
        dst = ld.at[part, k_half]
        self_ = jnp.logical_and(to == col, k == kk)
        act(
            self_,
            pltpu.make_async_copy(src, dst, l_r.at[part, k]),
            remote(src, dst, l_s.at[q, kk], l_r.at[part, k], {"col": to, "row": 2 * x + kk}),
        )

    def send(self_, here, there):
        pl.when(self_)(here.start)
        pl.when(jnp.logical_not(self_))(there.start)

    def sent(self_, here, there):
        pl.when(jnp.logical_not(self_))(there.wait_send)

    def over_v(act):
        def one(q):
            _loop((groups * q + grp) // 2, pairs, lambda t: deal_v(q, t, act))

        _loop(0, slots, one)

    def over_l(act):
        def one(q):
            deal_l(q, 0, act)
            deal_l(q, 1, act)

        _loop(0, slots, one)

    def deal_chunk(t):
        swaps(0, t)[0].wait()
        arriving(0, t)
        _loop(0, (2 * t + 1 - grp + groups) // groups, lambda q: deal_v(q, t, send))

    turn(0, deal_chunk)
    ins[2].start()
    turn(1)
    swapped(1)
    over_l(send)
    turn(2)
    mbuf[...] = jnp.zeros_like(mbuf)

    gm[...] = jnp.zeros_like(gm)

    def chunk(i):
        def got(n):
            await_(vb.at[i, n // 2, _at(n % 2, HALF)], v_r.at[i, n // 2, n % 2])

        _loop(0, 2 * rows, got)
        all_ = vb[i].reshape(size, STEP)
        gm[pl.ds(0, hsize), pl.ds(0, hsize)] += _dot_nt(all_[:hsize], all_[:hsize])
        gm[pl.ds(hsize, hsize), :] += _dot_nt(all_[hsize:], all_)

    _loop((first_t + 1 - k) // 2, pairs // 2, chunk)
    tick(0)

    widths = []
    w_ = hsize
    while w_ >= EDGE:
        widths.append(w_)
        w_ //= 2

    def packed(w_):
        return pl.ds(size - 2 * w_, w_)

    pk[...] = jnp.zeros_like(pk)
    for w_ in widths:
        for i in range(hsize // w_):
            pk[pl.ds(i * w_, w_), packed(w_)] = gm[pl.ds((2 * i + 1) * w_, w_), pl.ds(2 * i * w_, w_)]

    mine, theirs = _at(k, qsize), _at(1 - k, qsize)
    to_mate = remote(pk.at[theirs], gx, gx_sem.at[0], gx_sem.at[1], mate)
    to_mate.start()
    tick(1)
    to_mate.wait_recv()
    pk[mine] += gx[...]
    rl = qsize // chips

    def r2_copy(d):
        src = pk.at[pl.ds(pl.multiple_of(k * qsize + peer(d) * rl, rl), rl)]
        return remote(src, r2.at[d - 1], r2_s.at[d - 1], r2_r.at[d - 1], at_peer(d))

    for d in range(1, chips):
        r2_copy(d).start()

    def got_l(n):
        await_(ld.at[n // 2, _at(n % 2, HALF)], l_r.at[n // 2, n % 2])

    _loop(0, 2 * rows, got_l)
    ev = my_j % 2 == 0
    lo_half = lax.broadcasted_iota(jnp.int32, (size, LANES), 1) < EDGE
    l_lo, l_hi = ld[:, :, pl.ds(0, LANES)].reshape(size, LANES), ld[:, :, pl.ds(LANES, LANES)].reshape(size, LANES)
    lx[x] = jnp.where(
        lo_half,
        jnp.where(ev, l_lo, pltpu.roll(l_lo, EDGE, 1)),
        jnp.where(ev, pltpu.roll(l_hi, EDGE, 1), l_hi),
    )

    def lx_copy(d):
        return remote(lx.at[x], lx.at[x], lx_s.at[d - 1], lx_r.at[d - 1], at_peer(d))

    tick(2)
    for d in range(1, chips):
        r2_copy(d).wait_recv()
    my_rows = pl.ds(pl.multiple_of(k * qsize + x * rl, rl), rl)
    total = pk[my_rows]
    for d in range(1, chips):
        total = total + r2[d - 1]
    ga[my_rows] = total

    def ga_copy(d):
        return remote(ga.at[my_rows], ga.at[my_rows], ga_s.at[d - 1], ga_r.at[d - 1], at_peer(d))

    for d in range(1, chips):
        ga_copy(d).start()
    for d in range(1, chips):
        lx_copy(d).start()
    tick(3)
    for d in range(1, chips):
        await_(ga.at[pl.ds(pl.multiple_of(k * qsize + peer(chips - d) * rl, rl), rl)], ga_r.at[d - 1])
    half_to_mate = remote(ga.at[mine], ga.at[mine], gx_sem.at[2], gx_sem.at[3], mate)
    half_to_mate.start()

    r_i = lax.broadcasted_iota(jnp.int32, (LANES, LANES), 0)
    c_i = lax.broadcasted_iota(jnp.int32, (LANES, LANES), 1)

    def tile(i):
        return _at(i, LANES), _at(i, LANES)

    def merge_tile(w, i, low_part):
        cur = xm[(w, *tile(i))]
        xm[(w, *tile(i))] = cur - _dot_nn(_dot_nn(cur, low_part), cur)

    def level_l(lev):
        pick = jnp.logical_and(
            lax.shift_right_logical(r_i, lev) % 2 == 1,
            lax.shift_right_logical(c_i, lev) + 1 == lax.shift_right_logical(r_i, lev),
        )
        _loop(0, n128, lambda i: merge_tile(1, i, jnp.where(pick, gm[tile(i)], 0.0)))

    def level_big(w, corner):
        for w_ in reversed(widths[:-1]):
            for i in range(hsize // w_):
                d1 = pl.ds(2 * i * w_, w_)
                d2 = pl.ds((2 * i + 1) * w_, w_)
                xm[w, d2, d1] = -_dot_nn(_dot_nn(xm[w, d2, d2], corner(w_, i)), xm[w, d1, d1])

    def pack_factor(w):
        for i in range(n128):
            pm[w, :, pl.ds(LANES * (i * (i + 1) // 2), LANES * (i + 1))] = xm[
                w, pl.ds(pl.multiple_of(i * LANES + k * EDGE, EDGE), EDGE), pl.ds(0, LANES * (i + 1))
            ]

    xm[...] = jnp.zeros_like(xm)
    ins[3].wait()
    for p in range(0, rows, 2):
        zero = jnp.zeros((EDGE, EDGE), jnp.float32)
        both = jnp.concatenate(
            [jnp.concatenate([tb[p], zero], axis=1), jnp.concatenate([zero, tb[p + 1]], axis=1)], axis=0
        )
        xm[0, pl.ds(p * EDGE, LANES), pl.ds(p * EDGE, LANES)] = both
    await_(ga.at[theirs], gx_sem.at[3])

    def corner64(i):
        block = ga[_at(i, EDGE), packed(EDGE)]
        zero = jnp.zeros((EDGE, EDGE), jnp.float32)
        low_part = jnp.concatenate([block, zero], axis=1)
        merge_tile(0, i, jnp.concatenate([jnp.zeros_like(low_part), low_part], axis=0))

    _loop(0, n128, corner64)
    level_big(0, lambda w_, i: ga[pl.ds(i * w_, w_), packed(w_)])
    pack_factor(0)
    tick(4)

    fetch_blk(0)
    fetch_blk(1)
    for d in range(1, chips):
        await_(lx.at[peer(chips - d)], lx_r.at[d - 1])
    for i in range(chips):
        gm[_at(i, LANES), :] = lx[i].T
    same = r_i == c_i

    def diag(i):
        d = gm[tile(i)]
        xm[(1, *tile(i))] = jnp.where(same, 1.0 / jnp.where(same, d, 1.0), 0.0)

    _loop(0, n128, diag)
    swapped(2)
    tick(5)
    _loop(0, 3, level_l)
    tick(6)
    wait_blk(0)
    project(sbuf.at[0], ys, 0, top // 2)
    for g in range(2):
        for d in range(1, chips):
            rs_copy(0, g, d).start()
    _loop(3, 7, level_l)
    tick(7)
    level_big(1, lambda w_, i: gm[pl.ds((2 * i + 1) * w_, w_), pl.ds(2 * i * w_, w_)])
    pack_factor(1)
    tick(8)
    fetch_mat(0)
    fetch_mat(1)
    fetch_blk(2)

    wait_mat(0)

    def reflect(n):
        j, par, nxt = top - n, n % 2, (n + 1) % 2

        @pl.when(j > 0)
        def _():
            wait_blk(n + 1)
            cm[par, _at(k, hsize)] = jnp.zeros((hsize, size), jnp.float32)
            pl.when(j % 2 == 1)(lambda: cross(n, (j // 2) * STEP, STEP))

            def one(off, width):
                apply(n - 1, off, width)
                cross(n, off, width)

            over((j + 1) // 2, one)
            c_copy(par).start()

        pl.when(j == 0)(lambda: over(0, functools.partial(apply, n - 1)))

        def factor(gs):
            totals = []
            for g in gs:
                for d in range(1, chips):
                    rs_copy(par, g, d).wait_recv()
                total = sbuf[par, slice_of(g, x)]
                for d in range(1, chips):
                    total = total + rs[g, d - 1]
                totals.append(total)
            got = _dot_nn(jnp.concatenate(totals, axis=0), mbuf[par])
            for i, g in enumerate(gs):
                wb[par, slice_of(g, x)] = got[i * sl : (i + 1) * sl]
                for d in range(1, chips):
                    w_copy(par, g, d).start()

        factor((0,))
        factor((1,))

        for g in range(2):
            for d in range(1, chips):
                rs_copy(par, g, d).wait_send()

        @pl.when(jnp.logical_and(n < 8, par == 0))
        def _():
            tick(LEAD + n // 2)

        @pl.when(n >= 8)
        def _():
            tick(LEAD - 4 + n)

        pl.when(n > 0)(lambda: release_blk(n - 1))
        release_mat(n)

        @pl.when(j > 0)
        def _():
            project(sbuf.at[nxt], ys, n + 1, (j - 1) // 2)
            wait_mat(n + 1)
            await_(cm.at[par, _at(1 - k, hsize)], cm_r.at[par])

        def correct(gs):
            for g in gs:
                for d in range(1, chips):
                    await_(wb.at[par, slice_of(g, peer(chips - d))], ex_r.at[g, d - 1])

            @pl.when(j > 0)
            def _():
                sbuf[nxt, cols_in(gs)] = sbuf[nxt, cols_in(gs)] - _dot_nn(wb[par, cols_in(gs)], cm[par])
                for g in gs:
                    for d in range(1, chips):
                        rs_copy(nxt, g, d).start()

        correct((0,))
        correct((1,))

        for g in range(2):
            for d in range(1, chips):
                w_copy(par, g, d).wait_send()

        @pl.when(j > 0)
        def _():
            c_copy(par).wait_send()

    _loop(0, nb, reflect)
    over(0, functools.partial(apply, top))
    release_blk(top)

    xs[...] = jnp.zeros_like(xs)
    def first_half(val):
        return lax.broadcasted_iota(jnp.int32, val.shape, 1) < EDGE


    def take(ref, cols_, j):
        lo = ref[cols_, pl.ds(pl.multiple_of((j // 2) * STEP, LANES), LANES)]
        hi = ref[cols_, pl.ds(pl.multiple_of((j // 2) * STEP + LANES, LANES), LANES)]
        even = j % 2 == 0
        return jnp.where(
            first_half(lo),
            jnp.where(even, lo, pltpu.roll(lo, EDGE, 1)),
            jnp.where(even, pltpu.roll(hi, EDGE, 1), hi),
        )

    def spread(val, j):
        even, first = j % 2 == 0, first_half(val)
        other = pltpu.roll(val, EDGE, 1)
        zero = jnp.zeros_like(val)
        lo = jnp.where(even, jnp.where(first, val, zero), jnp.where(first, zero, other))
        hi = jnp.where(even, jnp.where(first, other, zero), jnp.where(first, zero, val))
        return jnp.concatenate([lo, hi], axis=1)

    def x_copy(par, g, d):
        src = sbuf.at[par, cols_of(g), _at(peer(d), LANES)]
        return remote(src, rx.at[par, g, d - 1], rx_s.at[par, g, d - 1], rx_r.at[par, g, d - 1], at_peer(d))

    def solve_partial(n, gs, j):
        par, cols_ = n % 2, cols_in(gs)
        wb[0, cols_] = -wb[0, cols_]
        wb[0, cols_, _at(x, LANES)] += take(ys, cols_, j)
        sbuf[par, cols_] = _dot_nn(wb[0, cols_], mbuf[par])
        for g in gs:
            for d in range(1, chips):
                x_copy(par, g, d).start()

    def fin_copy(i):
        return remote(
            xs.at[:, _at(2 * i + 1 - k, LANES)], zt.at[k, :, _at(i, LANES)], fin_s.at[i], fin_r.at[i], mate
        )

    def give(i):
        await_(zt.at[1 - k, :, _at(i, LANES)], fin_r.at[i])
        zt[k, :, _at(i, LANES)] = xs[:, _at(2 * i + k, LANES)]
        out_ref[_at(i, LANES), :] = zt[:, :, _at(i, LANES)].reshape(2 * ncol, LANES).T

    for m in range(3):
        _loop(0, pairs, lambda i, m=m: swaps(m, i)[1].wait_send())
    over_v(sent)
    over_l(sent)
    to_mate.wait_send()
    half_to_mate.wait_send()
    for d in range(1, chips):
        r2_copy(d).wait_send()
        ga_copy(d).wait_send()
        lx_copy(d).wait_send()

    wait_blk(nb)
    wait_mat(nb)
    wb[0] = jnp.zeros((ncol, size), jnp.float32)
    for g in range(2):
        solve_partial(nb, (g,), top)
    release_blk(nb)
    release_mat(nb)

    def solve(i):
        n = nb + i
        j, par, nxt = top - i, n % 2, (n + 1) % 2

        @pl.when(j > 0)
        def _():
            wait_blk(n + 1)
            wait_mat(n + 1)
            project(wb.at[0], xs, n + 1, (j + 1) // 2)

        def finish(gs):
            cols_ = cols_in(gs)
            vals = []
            for g in gs:
                for d in range(1, chips):
                    x_copy(par, g, d).wait_recv()
                val = sbuf[par, cols_of(g), _at(x, LANES)]
                for d in range(1, chips):
                    val = val + rx[par, g, d - 1]
                vals.append(val)
            solved = spread(jnp.concatenate(vals, axis=0), j)
            xs[cols_, _at(j // 2, STEP)] += solved

            @pl.when(j > 0)
            def _():
                wb[0, cols_] += _dot_nt(solved, cut(n + 1, (j // 2) * STEP, STEP))
                solve_partial(n + 1, gs, j - 1)

        finish((0,))
        finish((1,))

        pl.when(j % 2 == 0)(lambda: fin_copy(j // 2).start())
        pl.when(jnp.logical_and(j % 2 == 1, j < top))(lambda: give(j // 2 + 1))

        for g in range(2):
            for d in range(1, chips):
                x_copy(par, g, d).wait_send()

        @pl.when(j > 0)
        def _():
            release_blk(n + 1)
            release_mat(n + 1)

        tick(LEAD - 4 + n)

    _loop(0, nb, solve)

    give(0)
    _loop(0, pairs, lambda i: fin_copy(i).wait_send())


def solution(mesh):
    rows, cols = mesh.shape["row"], mesh.shape["col"]
    mat_spec = P(("kpt", "row"), "col")
    fac_spec = P("kpt", None, None)

    def local_work(v_loc, t_loc, z_loc, l_loc):
        n_row, n_col = v_loc.shape
        slots, lanes, chips, size = n_col // EDGE, 2 * n_row, rows // 2, rows * EDGE
        nb, ncol = lanes // LANES, z_loc.shape[1] // 2
        pairs, gcol, peers = nb // 2, ncol // 2, max(chips - 1, 1)
        sl, gathers, n128 = gcol // chips, len(_gathers(slots)), size // LANES
        tri = LANES * (n128 * (n128 + 1) // 2)
        dma = pltpu.SemaphoreType.DMA
        hbm, vmem = pl.BlockSpec(memory_space=pl.ANY), pl.BlockSpec(memory_space=pltpu.VMEM)

        def buf(*shape):
            return pltpu.VMEM(shape, jnp.float32)

        col = lax.axis_index("col")
        t_mine = lax.dynamic_slice_in_dim(t_loc, (cols // rows * (col % rows) + col // rows) * rows, rows, axis=0)
        return pl.pallas_call(
            functools.partial(_kernel, (rows, cols, slots, nb, ncol)),
            out_shape=[
                jax.ShapeDtypeStruct(z_loc.shape, jnp.float32),
                jax.ShapeDtypeStruct((2, slots, RING, RING, HALF, lanes), jnp.float32),
            ],
            in_specs=[hbm] * 4,
            out_specs=[vmem, hbm],
            scratch_shapes=[
                buf(2, n_row, n_col),
                buf(2, slots, 2, HALF, n_row),
                buf(2, ncol, n_row),
                buf(rows, EDGE, EDGE),
                buf(2, slots, HALF, lanes),
                buf(ncol, lanes),
                buf(ncol, lanes),
                buf(pairs // 2, rows, EDGE, STEP),
                buf(rows, EDGE, STEP),
                buf(chips, size, LANES),
                buf(size, size),
                buf(size // 2, size),
                buf(size // 4, size),
                buf(peers, size // 4 // chips, size),
                buf(size // 2, size),
                buf(2, size, size),
                buf(2, EDGE, tri),
                buf(2, RING, RING, EDGE, tri),
                buf(DEEP, rows, EDGE, lanes),
                buf(2, size, size),
                buf(2, ncol, size),
                buf(2, peers, sl, size),
                buf(2, ncol, size),
                buf(2, size, size),
                buf(2, 2, peers, gcol, LANES),
                dma((4,)),
                dma((3, pairs)), dma((3, pairs)), dma((3, pairs)),
                dma((slots, pairs)), dma((pairs // 2, rows, 2)),
                dma((slots, 2)), dma((rows, 2)),
                dma((peers,)), dma((peers,)),
                dma((4,)),
                dma((peers,)), dma((peers,)), dma((peers,)), dma((peers,)),
                dma((pairs,)), dma((pairs,)),
                dma((gathers,)), dma((gathers, 8)), dma((gathers, 8)),
                dma((DEEP, rows)), dma((DEEP, rows)), dma((DEEP, rows)),
                dma((2, n128)), dma((2, n128)), dma((2, n128)),
                pltpu.SemaphoreType.REGULAR((DEEP,)), pltpu.SemaphoreType.REGULAR((2,)),
                dma((2, peers)), dma((2, peers)), dma((2, peers)), dma((2, peers)),
                dma((2,)), dma((2,)),
                dma((2, 2, peers)), dma((2, 2, peers)),
                dma((16,)), dma((16,)),
            ],
            compiler_params=pltpu.CompilerParams(collective_id=0, has_side_effects=True, vmem_limit_bytes=67_043_328),
            name="eigvec",
        )(v_loc, t_mine, z_loc, l_loc)[0]

    return jax.shard_map(local_work, mesh=mesh, in_specs=(mat_spec, fac_spec, mat_spec, mat_spec), out_specs=mat_spec, check_vma=False)
```

```python
import functools

import jax
import jax.numpy as jnp
from jax import lax
from jax.experimental import pallas as pl
from jax.experimental.pallas import tpu as pltpu
from jax.sharding import PartitionSpec as P

PREC_HIGH = lax.Precision.HIGHEST
MESH = pl.DeviceIdType.MESH
EDGE = 64
HALF = EDGE // 2
LANES = 128
STEP = 256
RING = 4
LEAD = 9
DEEP = 3


def _dot_nt(a, b):
    return lax.dot_general(a, b, (((1,), (1,)), ((), ())), precision=PREC_HIGH, preferred_element_type=jnp.float32)


def _dot_nn(a, b):
    return lax.dot_general(a, b, (((1,), (0,)), ((), ())), precision=PREC_HIGH, preferred_element_type=jnp.float32)


def _at(i, n):
    return pl.ds(pl.multiple_of(i * n, n), n)


def _loop(lo, hi, body):
    def one(i, carry):
        body(i)
        return carry

    lax.fori_loop(lo, hi, one, 0)


def _gathers(slots):
    early = [(slots - 1, 0), (slots - 2, 0), None, None, ("m", 0)]
    first = early + [(q, 0) for q in range(slots - 3, -1, -1)]
    rest = [(slots - 1, 1), ("m", 1)] + [(q, 1) for q in range(slots - 2, -1, -1)]
    return first + [None] * (LEAD - len(first)) + rest


def _kernel(dims, v_in, t_in, z_in, l_in, out_ref, gath, *scratch):
    (stage, vt, zt, tb, own, ys, xs, vb, ld, lx, gm, pk, gx, r2, ga, pm, mg, blk, mbuf, sbuf, rs, wb, cm, rx,
     in_sem, swap_l, swap_s, swap_r, v_s, v_r, l_s, l_r, lx_s, lx_r, gx_sem, r2_s, r2_r, ga_s, ga_r, fin_s, fin_r,
     ag_loc, ag_s, ag_r, blk_loc, blk_s, blk_r, mat_loc, mat_s, mat_r, free_b, free_m, rs_s, rs_r, ex_s, ex_r, cm_s, cm_r,
     rx_s, rx_r, eg_s, eg_r) = scratch
    xm = cm
    rows, cols, slots, nb, ncol = dims
    row, col = lax.axis_index("row"), lax.axis_index("col")
    x, k = row // 2, row % 2
    chips, groups = rows // 2, cols // rows
    size, lanes = rows * EDGE, nb * LANES
    hsize, qsize, n128 = size // 2, size // 4, size // LANES
    pairs = nb // 2
    gcol = ncol // 2
    sl = gcol // chips
    mate = {"row": row + 1 - 2 * k, "col": col}
    top, whole = nb - 1, nb // 2
    part, grp = col % rows, col // rows
    k_half, m_half = _at(k, HALF), _at(1 - k, HALF)
    s_a, s_b = 1 + (RING - 1) * k, RING - (RING - 1) * k
    a, b = (col // s_a) % RING, (col // s_b) % RING

    def remote(src, dst, ss, rr, to):
        return pltpu.make_async_remote_copy(src, dst, ss, rr, device_id=to, device_id_type=MESH)

    def await_(ref, sem):
        pltpu.make_async_copy(ref, ref, sem).wait()

    def peer(d):
        return lax.rem(x + d, chips)

    def at_peer(d):
        return {"row": 2 * peer(d) + k, "col": col}

    def plane(da, db):
        return {"row": row, "col": lax.rem(a + da, RING) * s_a + lax.rem(b + db, RING) * s_b}

    def low(q):
        return (groups * q // 2) * STEP

    order = _gathers(slots)

    class Slot:
        def __init__(self, kind, w, n):
            self.kind, self.w, self.n = kind, w, n

        def own(self):
            if self.kind == "m":
                return pm.at[self.w]
            return own.at[self.w, self.kind, :, pl.ds(low(self.kind), lanes - low(self.kind))]

        def piece(self, bb, aa, part=None):
            if self.kind == "m":
                return mg.at[self.w, bb, aa] if part is None else mg.at[self.w, bb, aa, pl.ds(part * HALF, HALF)]
            at = pl.ds(low(self.kind), lanes - low(self.kind))
            e = slice(None) if part is None else pl.ds(part * (HALF // 2), HALF // 2)
            return gath.at[self.w, self.kind, bb, aa, e, at]

        def bundle(self, bb, part=None):
            e = slice(None) if part is None else pl.ds(part * (RING // 2), RING // 2)
            if self.kind == "m":
                return mg.at[self.w, bb, e]
            return gath.at[self.w, self.kind, bb, e, :, pl.ds(low(self.kind), lanes - low(self.kind))]

        def copy(self, i):
            d = 1 if i % 2 == 0 else RING - 1
            back = RING - d
            if i < 2:
                src, dst, to = self.own(), self.piece(b, a), plane(d, 0)
            elif i < 4:
                src = dst = self.piece(b, lax.rem(a + back, RING), i % 2)
                to = plane(d, 0)
            elif i < 6:
                src = dst = self.bundle(b)
                to = plane(0, d)
            else:
                src = dst = self.bundle(lax.rem(b + back, RING), i % 2)
                to = plane(0, d)
            return remote(src, dst, ag_s.at[self.n, i], ag_r.at[self.n, i], to)

        def arrived(self, i):
            back = RING - 1 if i % 2 == 0 else 1
            if i < 2:
                dst = self.piece(b, lax.rem(a + back, RING))
            elif i < 4:
                dst = self.piece(b, lax.rem(a + 2, RING), i % 2)
            elif i < 6:
                dst = self.bundle(lax.rem(b + back, RING))
            else:
                dst = self.bundle(lax.rem(b + 2, RING), i % 2)
            await_(dst, ag_r.at[self.n, i])

        def kept(self):
            return pltpu.make_async_copy(self.own(), self.piece(b, a), ag_loc.at[self.n])

        def stage(self, s):
            if s == 0:
                self.copy(0).start()
                self.copy(1).start()
                self.kept().start()
            elif s == 1:
                for i in range(2):
                    self.arrived(i)
                    self.copy(2 + i).start()
            elif s == 2:
                self.kept().wait()
                self.arrived(2)
                self.arrived(3)
                self.copy(4).start()
                self.copy(5).start()
            elif s == 3:
                for i in range(4, 6):
                    self.arrived(i)
                    self.copy(2 + i).start()
            elif s == 4:
                self.arrived(6)
                self.arrived(7)
            else:
                for i in range(8):
                    self.copy(i).wait_send()

    class Eager(Slot):
        def spot(self, db, da, part=None):
            return self.piece(lax.rem(b + db, RING), lax.rem(a + da, RING), part)

        def copy(self, i):
            back = RING - 1
            db, da, part, to_b, to_a = (
                (0, 0, None, 0, 1), (0, 0, None, 0, back), (0, 0, None, 1, 0), (0, 0, None, back, 0),
                (0, back, 0, 0, 1), (0, 1, 1, 0, back),
                (0, back, None, 1, 0), (0, back, None, back, 0), (0, 1, None, 1, 0), (0, 1, None, back, 0),
                (0, 2, None, 1, 0), (0, 2, None, back, 0),
                (back, 0, None, 1, 0), (back, back, None, 1, 0), (1, 1, None, back, 0), (1, 2, None, back, 0),
            )[i]
            dst = self.spot(db, da, part)
            src = self.own() if db == 0 and da == 0 else dst
            sent_ = remote(src, dst, eg_s.at[i], eg_r.at[i], plane(to_a, to_b))
            return sent_, self.spot(db + RING - to_b, da + RING - to_a, part)

        def go(self, *which):
            for i in which:
                self.copy(i)[0].start()

        def got(self, *which):
            for i in which:
                await_(self.copy(i)[1], eg_r.at[i])

        def stage(self, s):
            if s == 0:
                self.go(0, 1, 2, 3)
                self.kept().start()
            elif s == 1:
                self.got(0)
                self.go(4, 6, 7)
                self.got(1)
                self.go(5, 8, 9)
                self.got(2)
                self.go(12)
            elif s == 2:
                self.got(4, 5)
                self.go(10, 11)
                self.got(6)
                self.go(13)
            elif s == 3:
                self.got(9)
                self.go(14)
                self.got(11)
                self.go(15)
            elif s == 4:
                self.got(3, 7, 8, 10, 12, 13, 14, 15)
                self.kept().wait()
                for i in range(16):
                    self.copy(i)[0].wait_send()

    def tick(t):
        for s in (4, 3, 2, 1, 0, 5):
            n = t - s
            if isinstance(n, int):
                if 0 <= n < len(order) and order[n] is not None:
                    (Eager if order[n] == ("m", 0) else Slot)(*order[n], n).stage(s)
                continue
            for kind in list(range(slots)) + ["m"]:
                at_v, at_l = order.index((kind, 0)), order.index((kind, 1))

                @pl.when(n == at_l if kind == "m" else jnp.logical_or(n == at_v, n == at_l))
                def _(s=s, n=n, kind=kind, at_l=at_l):
                    Slot(kind, jnp.where(n == at_l, 1, 0), n).stage(s)

    def block_of(n):
        j = top - n % nb
        return n // nb, j, j // groups, j % groups, n % 2

    run = min(rows, RING)
    runs = rows // run

    def in_blk(n, q, i, half):
        return blk.at[n % DEEP, pl.ds(i * run, run), half, pl.ds(low(q), lanes - low(q))]

    def from_mate(n, q, i):
        await_(in_blk(n, q, i, m_half), blk_r.at[n % DEEP, i])

    def mat_copies(n, i):
        w, j, q, h, s = block_of(n)
        c = h * rows + q
        src = mg.at[w, (c // s_b) % RING, (c // s_a) % RING, :, pl.ds(LANES * (i * (i + 1) // 2), LANES * (i + 1))]
        dst = mbuf.at[s, pl.ds(pl.multiple_of(i * LANES + k * EDGE, EDGE), EDGE), pl.ds(0, LANES * (i + 1))]
        return (
            pltpu.make_async_copy(src, dst, mat_loc.at[s, i]),
            remote(src, dst, mat_s.at[s, i], mat_r.at[s, i], mate),
        )

    def per_piece(n, act):
        q_now = block_of(n)[2]
        for q in range(slots):

            @pl.when(q_now == q)
            def _(q=q):
                for i in range(runs):
                    act(q, i)

    def fetch_blk(n):
        w, _, _, h, _ = block_of(n)
        s = n % DEEP

        def go(q, i):
            c = h * rows + i * run
            z_now, y_run = c // RING, pl.ds(c % RING, run)
            at = pl.ds(low(q), lanes - low(q))
            dst = in_blk(n, q, i, k_half)

            def both(src):
                pltpu.make_async_copy(src, dst, blk_loc.at[s, i]).start()
                remote(src, dst, blk_s.at[s, i], blk_r.at[s, i], mate).start()

            pl.when(k == 0)(lambda: both(gath.at[w, q, z_now, y_run, :, at]))
            pl.when(k == 1)(lambda: both(gath.at[w, q, y_run, z_now, :, at]))

        per_piece(n, go)

    def fetch_mat(n):
        for i in range(n128):
            for c in mat_copies(n, i):
                c.start()

    def wait_blk(n):
        def one(q, i):
            await_(in_blk(n, q, i, k_half), blk_loc.at[n % DEEP, i])
            from_mate(n, q, i)

        per_piece(n, one)

    def wait_mat(n):
        for i in range(n128):
            mat_copies(n, i)[0].wait()
            there = pl.ds(pl.multiple_of(i * LANES + (1 - k) * EDGE, EDGE), EDGE), pl.ds(0, LANES * (i + 1))
            await_(mbuf.at[(n % 2, *there)], mat_r.at[n % 2, i])

    def release_blk(n):
        per_piece(n, lambda q, i: await_(in_blk(n, q, i, k_half), blk_s.at[n % DEEP, i]))

        @pl.when(n + DEEP < 2 * nb)
        def _():
            pl.semaphore_signal(free_b.at[n % DEEP], inc=1, device_id=mate, device_id_type=MESH)
            pl.semaphore_wait(free_b.at[n % DEEP], 1)
            fetch_blk(n + DEEP)

    def release_mat(n):
        for i in range(n128):
            mat_copies(n, i)[1].wait_send()

        @pl.when(n + 2 < 2 * nb)
        def _():
            pl.semaphore_signal(free_m.at[n % 2], inc=1, device_id=mate, device_id_type=MESH)
            pl.semaphore_wait(free_m.at[n % 2], 1)
            fetch_mat(n + 2)

    def over(first, body):
        pl.when(first % 2 == 1)(lambda: body(first * STEP, STEP))
        _loop((first + 1) // 2, whole // 2, lambda i: body(i * 2 * STEP, 2 * STEP))

    def rows_at(off, width):
        return pl.ds(pl.multiple_of(off, STEP), width)

    def cut(n, off, width):
        return blk[n % DEEP, :, :, rows_at(off, width)].reshape(size, width)

    def project(dst, ref, n, first):
        dst[...] = jnp.zeros((ncol, size), jnp.float32)

        def one(off, width):
            dst[...] += _dot_nt(ref[:, rows_at(off, width)], cut(n, off, width))

        if whole % 4 or isinstance(first, int):
            over(first, one)
            return
        half = (first + 1) // 2
        pl.when(first % 2 == 1)(lambda: one(first * STEP, STEP))
        pl.when(half % 2 == 1)(lambda: one(half * 2 * STEP, 2 * STEP))
        _loop((half + 1) // 2, whole // 4, lambda i: one(i * 4 * STEP, 4 * STEP))

    def slice_of(g, x2):
        return pl.ds(pl.multiple_of(g * gcol + x2 * sl, sl), sl)

    def cols_of(g):
        return pl.ds(g * gcol, gcol)

    def rs_copy(par, g, d):
        return remote(sbuf.at[par, slice_of(g, peer(d))], rs.at[g, d - 1], rs_s.at[g, d - 1], rs_r.at[g, d - 1], at_peer(d))

    def w_copy(par, g, d):
        mine = wb.at[par, slice_of(g, x)]
        return remote(mine, mine, ex_s.at[g, d - 1], ex_r.at[g, d - 1], at_peer(d))

    c_half = pl.ds(pl.multiple_of(k * (rows // 2), rows // 2), rows // 2)

    def c_copy(par):
        return remote(cm.at[par, _at(k, hsize)], cm.at[par, _at(k, hsize)], cm_s.at[par], cm_r.at[par], mate)

    def apply(n, off, width):
        ys[:, rows_at(off, width)] = ys[:, rows_at(off, width)] - _dot_nn(wb[n % 2], cut(n, off, width))

    def cross(n, off, width):
        here = blk[n % DEEP, c_half, :, rows_at(off, width)].reshape(hsize, width)
        cm[n % 2, _at(k, hsize)] += _dot_nt(here, cut(n + 1, off, width))

    def cols_in(gs):
        return pl.ds(gs[0] * gcol, len(gs) * gcol)

    barrier = pltpu.get_barrier_semaphore()

    def here_i_am(device):
        pl.semaphore_signal(barrier, inc=1, device_id=device, device_id_type=MESH)

    def group_member(d):
        n = lax.rem(2 * part + k + d, 2 * rows)
        here_i_am({"col": grp * rows + n // 2, "row": 2 * x + n % 2})

    _loop(1, 2 * rows, group_member)
    for d in range(1, chips):
        here_i_am(at_peer(d))
    for d in (1, RING - 1):
        here_i_am(plane(d, 0))
        here_i_am(plane(0, d))

    ins = [
        pltpu.make_async_copy(src, stage.at[i % 2], in_sem.at[i]) for i, src in enumerate((v_in, l_in, z_in))
    ] + [pltpu.make_async_copy(t_in, tb, in_sem.at[3])]
    for i in (0, 1, 3):
        ins[i].start()
    pl.semaphore_wait(barrier, 2 * rows - 1 + chips - 1 + 4)

    def swaps(m, i):
        there = _at(2 * i + k, LANES)
        if m < 2:
            mine, theirs = vt.at[m, :, k, :, _at(i, LANES)], vt.at[m, :, 1 - k, :, _at(i, LANES)]
            dst = own.at[m, :, :, there]
        else:
            mine, theirs = zt.at[k, :, _at(i, LANES)], zt.at[1 - k, :, _at(i, LANES)]
            dst = ys.at[:, there]
        return (
            pltpu.make_async_copy(mine, dst, swap_l.at[m, i]),
            remote(theirs, dst, swap_s.at[m, i], swap_r.at[m, i], mate),
        )

    def arriving(m, i):
        there = _at(2 * i + 1 - k, LANES)
        await_(own.at[m, :, :, there] if m < 2 else ys.at[:, there], swap_r.at[m, i])

    def turn(m, then=None):
        ins[m].wait()

        def one(i):
            block = stage[m % 2, _at(i, LANES), :].T
            if m < 2:
                vt[m, :, :, :, _at(i, LANES)] = block.reshape(slots, 2, HALF, LANES)
            else:
                zt[:, :, _at(i, LANES)] = block.reshape(2, ncol, LANES)
            for c in swaps(m, i):
                c.start()
            if then is not None:
                pl.when(i > 0)(lambda: then(i - 1))

        _loop(0, pairs, one)
        if then is not None:
            then(pairs - 1)

    def swapped(m):
        def one(i):
            swaps(m, i)[0].wait()
            arriving(m, i)

        _loop(0, pairs, one)

    my_q, my_h = part, grp
    my_j = groups * my_q + my_h
    first_t = my_j // 2

    def deal_v(q, t, act):
        to, kk = grp * rows + q, t % 2
        src = own.at[0, q, :, _at(t, STEP)]
        dst = vb.at[t // 2, part, k_half]
        self_ = jnp.logical_and(to == col, k == kk)
        act(
            self_,
            pltpu.make_async_copy(src, dst, v_r.at[t // 2, part, k]),
            remote(src, dst, v_s.at[q, t], v_r.at[t // 2, part, k], {"col": to, "row": 2 * x + kk}),
        )

    def deal_l(q, kk, act):
        to = grp * rows + q
        src = own.at[1, q, :, _at((groups * q + grp) // 2, STEP)]
        dst = ld.at[part, k_half]
        self_ = jnp.logical_and(to == col, k == kk)
        act(
            self_,
            pltpu.make_async_copy(src, dst, l_r.at[part, k]),
            remote(src, dst, l_s.at[q, kk], l_r.at[part, k], {"col": to, "row": 2 * x + kk}),
        )

    def send(self_, here, there):
        pl.when(self_)(here.start)
        pl.when(jnp.logical_not(self_))(there.start)

    def sent(self_, here, there):
        pl.when(jnp.logical_not(self_))(there.wait_send)

    def over_v(act):
        def one(q):
            _loop((groups * q + grp) // 2, pairs, lambda t: deal_v(q, t, act))

        _loop(0, slots, one)

    def over_l(act):
        def one(q):
            deal_l(q, 0, act)
            deal_l(q, 1, act)

        _loop(0, slots, one)

    def deal_chunk(t):
        swaps(0, t)[0].wait()
        arriving(0, t)
        _loop(0, (2 * t + 1 - grp + groups) // groups, lambda q: deal_v(q, t, send))

    turn(0, deal_chunk)
    ins[2].start()
    turn(1)
    swapped(1)
    over_l(send)
    turn(2)
    mbuf[...] = jnp.zeros_like(mbuf)

    gm[...] = jnp.zeros_like(gm)

    def chunk(i):
        def got(n):
            await_(vb.at[i, n // 2, _at(n % 2, HALF)], v_r.at[i, n // 2, n % 2])

        _loop(0, 2 * rows, got)
        all_ = vb[i].reshape(size, STEP)
        gm[pl.ds(0, hsize), pl.ds(0, hsize)] += _dot_nt(all_[:hsize], all_[:hsize])
        gm[pl.ds(hsize, hsize), :] += _dot_nt(all_[hsize:], all_)

    _loop((first_t + 1 - k) // 2, pairs // 2, chunk)
    tick(0)

    widths = []
    w_ = hsize
    while w_ >= EDGE:
        widths.append(w_)
        w_ //= 2

    def packed(w_):
        return pl.ds(size - 2 * w_, w_)

    pk[...] = jnp.zeros_like(pk)
    for w_ in widths:
        for i in range(hsize // w_):
            pk[pl.ds(i * w_, w_), packed(w_)] = gm[pl.ds((2 * i + 1) * w_, w_), pl.ds(2 * i * w_, w_)]

    mine, theirs = _at(k, qsize), _at(1 - k, qsize)
    to_mate = remote(pk.at[theirs], gx, gx_sem.at[0], gx_sem.at[1], mate)
    to_mate.start()
    tick(1)
    to_mate.wait_recv()
    pk[mine] += gx[...]
    rl = qsize // chips

    def r2_copy(d):
        src = pk.at[pl.ds(pl.multiple_of(k * qsize + peer(d) * rl, rl), rl)]
        return remote(src, r2.at[d - 1], r2_s.at[d - 1], r2_r.at[d - 1], at_peer(d))

    for d in range(1, chips):
        r2_copy(d).start()

    def got_l(n):
        await_(ld.at[n // 2, _at(n % 2, HALF)], l_r.at[n // 2, n % 2])

    _loop(0, 2 * rows, got_l)
    ev = my_j % 2 == 0
    lo_half = lax.broadcasted_iota(jnp.int32, (size, LANES), 1) < EDGE
    l_lo, l_hi = ld[:, :, pl.ds(0, LANES)].reshape(size, LANES), ld[:, :, pl.ds(LANES, LANES)].reshape(size, LANES)
    lx[x] = jnp.where(
        lo_half,
        jnp.where(ev, l_lo, pltpu.roll(l_lo, EDGE, 1)),
        jnp.where(ev, pltpu.roll(l_hi, EDGE, 1), l_hi),
    )

    def lx_copy(d):
        return remote(lx.at[x], lx.at[x], lx_s.at[d - 1], lx_r.at[d - 1], at_peer(d))

    tick(2)
    for d in range(1, chips):
        r2_copy(d).wait_recv()
    my_rows = pl.ds(pl.multiple_of(k * qsize + x * rl, rl), rl)
    total = pk[my_rows]
    for d in range(1, chips):
        total = total + r2[d - 1]
    ga[my_rows] = total

    def ga_copy(d):
        return remote(ga.at[my_rows], ga.at[my_rows], ga_s.at[d - 1], ga_r.at[d - 1], at_peer(d))

    for d in range(1, chips):
        ga_copy(d).start()
    for d in range(1, chips):
        lx_copy(d).start()
    tick(3)
    for d in range(1, chips):
        await_(ga.at[pl.ds(pl.multiple_of(k * qsize + peer(chips - d) * rl, rl), rl)], ga_r.at[d - 1])
    half_to_mate = remote(ga.at[mine], ga.at[mine], gx_sem.at[2], gx_sem.at[3], mate)
    half_to_mate.start()

    r_i = lax.broadcasted_iota(jnp.int32, (LANES, LANES), 0)
    c_i = lax.broadcasted_iota(jnp.int32, (LANES, LANES), 1)

    def tile(i):
        return _at(i, LANES), _at(i, LANES)

    def merge_tile(w, i, low_part):
        cur = xm[(w, *tile(i))]
        xm[(w, *tile(i))] = cur - _dot_nn(_dot_nn(cur, low_part), cur)

    def level_l(lev):
        pick = jnp.logical_and(
            lax.shift_right_logical(r_i, lev) % 2 == 1,
            lax.shift_right_logical(c_i, lev) + 1 == lax.shift_right_logical(r_i, lev),
        )
        _loop(0, n128, lambda i: merge_tile(1, i, jnp.where(pick, gm[tile(i)], 0.0)))

    def level_big(w, corner):
        for w_ in reversed(widths[:-1]):
            for i in range(hsize // w_):
                d1 = pl.ds(2 * i * w_, w_)
                d2 = pl.ds((2 * i + 1) * w_, w_)
                xm[w, d2, d1] = -_dot_nn(_dot_nn(xm[w, d2, d2], corner(w_, i)), xm[w, d1, d1])

    def pack_factor(w):
        for i in range(n128):
            pm[w, :, pl.ds(LANES * (i * (i + 1) // 2), LANES * (i + 1))] = xm[
                w, pl.ds(pl.multiple_of(i * LANES + k * EDGE, EDGE), EDGE), pl.ds(0, LANES * (i + 1))
            ]

    xm[...] = jnp.zeros_like(xm)
    ins[3].wait()
    for p in range(0, rows, 2):
        zero = jnp.zeros((EDGE, EDGE), jnp.float32)
        both = jnp.concatenate(
            [jnp.concatenate([tb[p], zero], axis=1), jnp.concatenate([zero, tb[p + 1]], axis=1)], axis=0
        )
        xm[0, pl.ds(p * EDGE, LANES), pl.ds(p * EDGE, LANES)] = both
    await_(ga.at[theirs], gx_sem.at[3])

    def corner64(i):
        block = ga[_at(i, EDGE), packed(EDGE)]
        zero = jnp.zeros((EDGE, EDGE), jnp.float32)
        low_part = jnp.concatenate([block, zero], axis=1)
        merge_tile(0, i, jnp.concatenate([jnp.zeros_like(low_part), low_part], axis=0))

    _loop(0, n128, corner64)
    level_big(0, lambda w_, i: ga[pl.ds(i * w_, w_), packed(w_)])
    pack_factor(0)
    tick(4)

    fetch_blk(0)
    fetch_blk(1)
    for d in range(1, chips):
        await_(lx.at[peer(chips - d)], lx_r.at[d - 1])
    for i in range(chips):
        gm[_at(i, LANES), :] = lx[i].T
    same = r_i == c_i

    def diag(i):
        d = gm[tile(i)]
        xm[(1, *tile(i))] = jnp.where(same, 1.0 / jnp.where(same, d, 1.0), 0.0)

    _loop(0, n128, diag)
    swapped(2)
    tick(5)
    _loop(0, 3, level_l)
    tick(6)
    wait_blk(0)
    project(sbuf.at[0], ys, 0, top // 2)
    for g in range(2):
        for d in range(1, chips):
            rs_copy(0, g, d).start()
    _loop(3, 7, level_l)
    tick(7)
    level_big(1, lambda w_, i: gm[pl.ds((2 * i + 1) * w_, w_), pl.ds(2 * i * w_, w_)])
    pack_factor(1)
    tick(8)
    fetch_mat(0)
    fetch_mat(1)
    fetch_blk(2)

    wait_mat(0)

    def reflect(n):
        j, par, nxt = top - n, n % 2, (n + 1) % 2

        @pl.when(j > 0)
        def _():
            wait_blk(n + 1)
            cm[par, _at(k, hsize)] = jnp.zeros((hsize, size), jnp.float32)
            pl.when(j % 2 == 1)(lambda: cross(n, (j // 2) * STEP, STEP))

            def one(off, width):
                apply(n - 1, off, width)
                cross(n, off, width)

            over((j + 1) // 2, one)
            c_copy(par).start()

        pl.when(j == 0)(lambda: over(0, functools.partial(apply, n - 1)))

        def factor(gs):
            totals = []
            for g in gs:
                for d in range(1, chips):
                    rs_copy(par, g, d).wait_recv()
                total = sbuf[par, slice_of(g, x)]
                for d in range(1, chips):
                    total = total + rs[g, d - 1]
                totals.append(total)
            got = _dot_nn(jnp.concatenate(totals, axis=0), mbuf[par])
            for i, g in enumerate(gs):
                wb[par, slice_of(g, x)] = got[i * sl : (i + 1) * sl]
                for d in range(1, chips):
                    w_copy(par, g, d).start()

        factor((0,))
        factor((1,))

        for g in range(2):
            for d in range(1, chips):
                rs_copy(par, g, d).wait_send()

        pl.when(n > 0)(lambda: release_blk(n - 1))
        release_mat(n)

        @pl.when(j > 0)
        def _():
            project(sbuf.at[nxt], ys, n + 1, (j - 1) // 2)

        @pl.when(jnp.logical_or(n >= 8, par == 0))
        def _():
            tick(jnp.where(n < 8, LEAD + n // 2, LEAD - 4 + n))

        @pl.when(j > 0)
        def _():
            wait_mat(n + 1)
            await_(cm.at[par, _at(1 - k, hsize)], cm_r.at[par])

        def correct(gs):
            for g in gs:
                for d in range(1, chips):
                    await_(wb.at[par, slice_of(g, peer(chips - d))], ex_r.at[g, d - 1])

            @pl.when(j > 0)
            def _():
                sbuf[nxt, cols_in(gs)] = sbuf[nxt, cols_in(gs)] - _dot_nn(wb[par, cols_in(gs)], cm[par])
                for g in gs:
                    for d in range(1, chips):
                        rs_copy(nxt, g, d).start()

        correct((0,))
        correct((1,))

        for g in range(2):
            for d in range(1, chips):
                w_copy(par, g, d).wait_send()

        @pl.when(j > 0)
        def _():
            c_copy(par).wait_send()

    _loop(0, nb, reflect)
    over(0, functools.partial(apply, top))
    release_blk(top)

    xs[...] = jnp.zeros_like(xs)
    def first_half(val):
        return lax.broadcasted_iota(jnp.int32, val.shape, 1) < EDGE


    def take(ref, cols_, j):
        lo = ref[cols_, pl.ds(pl.multiple_of((j // 2) * STEP, LANES), LANES)]
        hi = ref[cols_, pl.ds(pl.multiple_of((j // 2) * STEP + LANES, LANES), LANES)]
        even = j % 2 == 0
        return jnp.where(
            first_half(lo),
            jnp.where(even, lo, pltpu.roll(lo, EDGE, 1)),
            jnp.where(even, pltpu.roll(hi, EDGE, 1), hi),
        )

    def spread(val, j):
        even, first = j % 2 == 0, first_half(val)
        other = pltpu.roll(val, EDGE, 1)
        zero = jnp.zeros_like(val)
        lo = jnp.where(even, jnp.where(first, val, zero), jnp.where(first, zero, other))
        hi = jnp.where(even, jnp.where(first, other, zero), jnp.where(first, zero, val))
        return jnp.concatenate([lo, hi], axis=1)

    def x_copy(par, g, d):
        src = sbuf.at[par, cols_of(g), _at(peer(d), LANES)]
        return remote(src, rx.at[par, g, d - 1], rx_s.at[par, g, d - 1], rx_r.at[par, g, d - 1], at_peer(d))

    def solve_partial(n, gs, j):
        par, cols_ = n % 2, cols_in(gs)
        wb[0, cols_] = -wb[0, cols_]
        wb[0, cols_, _at(x, LANES)] += take(ys, cols_, j)
        sbuf[par, cols_] = _dot_nn(wb[0, cols_], mbuf[par])
        for g in gs:
            for d in range(1, chips):
                x_copy(par, g, d).start()

    def fin_copy(i):
        return remote(
            xs.at[:, _at(2 * i + 1 - k, LANES)], zt.at[k, :, _at(i, LANES)], fin_s.at[i], fin_r.at[i], mate
        )

    def give(i):
        await_(zt.at[1 - k, :, _at(i, LANES)], fin_r.at[i])
        zt[k, :, _at(i, LANES)] = xs[:, _at(2 * i + k, LANES)]
        out_ref[_at(i, LANES), :] = zt[:, :, _at(i, LANES)].reshape(2 * ncol, LANES).T

    for m in range(3):
        _loop(0, pairs, lambda i, m=m: swaps(m, i)[1].wait_send())
    over_v(sent)
    over_l(sent)
    to_mate.wait_send()
    half_to_mate.wait_send()
    for d in range(1, chips):
        r2_copy(d).wait_send()
        ga_copy(d).wait_send()
        lx_copy(d).wait_send()

    wait_blk(nb)
    wait_mat(nb)
    wb[0] = jnp.zeros((ncol, size), jnp.float32)
    for g in range(2):
        solve_partial(nb, (g,), top)
    release_blk(nb)
    release_mat(nb)

    def solve(i):
        n = nb + i
        j, par, nxt = top - i, n % 2, (n + 1) % 2

        @pl.when(j > 0)
        def _():
            wait_blk(n + 1)
            wait_mat(n + 1)
            project(wb.at[0], xs, n + 1, (j + 1) // 2)

        def finish(gs):
            cols_ = cols_in(gs)
            vals = []
            for g in gs:
                for d in range(1, chips):
                    x_copy(par, g, d).wait_recv()
                val = sbuf[par, cols_of(g), _at(x, LANES)]
                for d in range(1, chips):
                    val = val + rx[par, g, d - 1]
                vals.append(val)
            solved = spread(jnp.concatenate(vals, axis=0), j)
            xs[cols_, _at(j // 2, STEP)] += solved

            @pl.when(j > 0)
            def _():
                wb[0, cols_] += _dot_nt(solved, cut(n + 1, (j // 2) * STEP, STEP))
                solve_partial(n + 1, gs, j - 1)

        finish((0,))
        finish((1,))

        pl.when(j % 2 == 0)(lambda: fin_copy(j // 2).start())
        pl.when(jnp.logical_and(j % 2 == 1, j < top))(lambda: give(j // 2 + 1))

        for g in range(2):
            for d in range(1, chips):
                x_copy(par, g, d).wait_send()

        @pl.when(j > 0)
        def _():
            release_blk(n + 1)
            release_mat(n + 1)

        tick(LEAD - 4 + n)

    _loop(0, nb, solve)

    give(0)
    _loop(0, pairs, lambda i: fin_copy(i).wait_send())


def solution(mesh):
    rows, cols = mesh.shape["row"], mesh.shape["col"]
    mat_spec = P(("kpt", "row"), "col")
    fac_spec = P("kpt", None, None)

    def local_work(v_loc, t_loc, z_loc, l_loc):
        n_row, n_col = v_loc.shape
        slots, lanes, chips, size = n_col // EDGE, 2 * n_row, rows // 2, rows * EDGE
        nb, ncol = lanes // LANES, z_loc.shape[1] // 2
        pairs, gcol, peers = nb // 2, ncol // 2, max(chips - 1, 1)
        sl, gathers, n128 = gcol // chips, len(_gathers(slots)), size // LANES
        tri = LANES * (n128 * (n128 + 1) // 2)
        dma = pltpu.SemaphoreType.DMA
        hbm, vmem = pl.BlockSpec(memory_space=pl.ANY), pl.BlockSpec(memory_space=pltpu.VMEM)

        def buf(*shape):
            return pltpu.VMEM(shape, jnp.float32)

        col = lax.axis_index("col")
        t_mine = lax.dynamic_slice_in_dim(t_loc, (cols // rows * (col % rows) + col // rows) * rows, rows, axis=0)
        return pl.pallas_call(
            functools.partial(_kernel, (rows, cols, slots, nb, ncol)),
            out_shape=[
                jax.ShapeDtypeStruct(z_loc.shape, jnp.float32),
                jax.ShapeDtypeStruct((2, slots, RING, RING, HALF, lanes), jnp.float32),
            ],
            in_specs=[hbm] * 4,
            out_specs=[vmem, hbm],
            scratch_shapes=[
                buf(2, n_row, n_col),
                buf(2, slots, 2, HALF, n_row),
                buf(2, ncol, n_row),
                buf(rows, EDGE, EDGE),
                buf(2, slots, HALF, lanes),
                buf(ncol, lanes),
                buf(ncol, lanes),
                buf(pairs // 2, rows, EDGE, STEP),
                buf(rows, EDGE, STEP),
                buf(chips, size, LANES),
                buf(size, size),
                buf(size // 2, size),
                buf(size // 4, size),
                buf(peers, size // 4 // chips, size),
                buf(size // 2, size),
                buf(2, EDGE, tri),
                buf(2, RING, RING, EDGE, tri),
                buf(DEEP, rows, EDGE, lanes),
                buf(2, size, size),
                buf(2, ncol, size),
                buf(2, peers, sl, size),
                buf(2, ncol, size),
                buf(2, size, size),
                buf(2, 2, peers, gcol, LANES),
                dma((4,)),
                dma((3, pairs)), dma((3, pairs)), dma((3, pairs)),
                dma((slots, pairs)), dma((pairs // 2, rows, 2)),
                dma((slots, 2)), dma((rows, 2)),
                dma((peers,)), dma((peers,)),
                dma((4,)),
                dma((peers,)), dma((peers,)), dma((peers,)), dma((peers,)),
                dma((pairs,)), dma((pairs,)),
                dma((gathers,)), dma((gathers, 8)), dma((gathers, 8)),
                dma((DEEP, rows)), dma((DEEP, rows)), dma((DEEP, rows)),
                dma((2, n128)), dma((2, n128)), dma((2, n128)),
                pltpu.SemaphoreType.REGULAR((DEEP,)), pltpu.SemaphoreType.REGULAR((2,)),
                dma((2, peers)), dma((2, peers)), dma((2, peers)), dma((2, peers)),
                dma((2,)), dma((2,)),
                dma((2, 2, peers)), dma((2, 2, peers)),
                dma((16,)), dma((16,)),
            ],
            compiler_params=pltpu.CompilerParams(collective_id=0, has_side_effects=True, vmem_limit_bytes=67_043_328),
            name="eigvec",
        )(v_loc, t_mine, z_loc, l_loc)[0]

    return jax.shard_map(local_work, mesh=mesh, in_specs=(mat_spec, fac_spec, mat_spec, mat_spec), out_specs=mat_spec, check_vma=False)
```

```python
import functools

import jax
import jax.numpy as jnp
from jax import lax
from jax.experimental import pallas as pl
from jax.experimental.pallas import tpu as pltpu
from jax.sharding import PartitionSpec as P

PREC_HIGH = lax.Precision.HIGHEST
MESH = pl.DeviceIdType.MESH
EDGE = 64
HALF = EDGE // 2
LANES = 128
STEP = 256
RING = 4
LEAD = 9
DEEP = 3


def _dot_nt(a, b):
    return lax.dot_general(a, b, (((1,), (1,)), ((), ())), precision=PREC_HIGH, preferred_element_type=jnp.float32)


def _dot_nn(a, b):
    return lax.dot_general(a, b, (((1,), (0,)), ((), ())), precision=PREC_HIGH, preferred_element_type=jnp.float32)


def _at(i, n):
    return pl.ds(pl.multiple_of(i * n, n), n)


def _loop(lo, hi, body):
    def one(i, carry):
        body(i)
        return carry

    lax.fori_loop(lo, hi, one, 0)


def _gathers(slots):
    early = [(slots - 1, 0), (slots - 2, 0), None, None, ("m", 0)]
    first = early + [(q, 0) for q in range(slots - 3, -1, -1)]
    rest = [(slots - 1, 1), ("m", 1)] + [(q, 1) for q in range(slots - 2, -1, -1)]
    return first + [None] * (LEAD - len(first)) + rest


def _kernel(dims, v_in, t_in, z_in, l_in, out_ref, gath, *scratch):
    (stage, vt, zt, tb, own, ys, xs, vb, ld, lx, gm, pk, gx, r2, ga, pm, mg, blk, mbuf, sbuf, rs, wb, cm, rx,
     in_sem, swap_l, swap_s, swap_r, v_s, v_r, l_s, l_r, lx_s, lx_r, gx_sem, r2_s, r2_r, ga_s, ga_r, fin_s, fin_r,
     ag_loc, ag_s, ag_r, blk_loc, blk_s, blk_r, mat_loc, mat_s, mat_r, free_b, free_m, rs_s, rs_r, ex_s, ex_r, cm_s, cm_r,
     rx_s, rx_r, eg_s, eg_r) = scratch
    xm = cm
    rows, cols, slots, nb, ncol = dims
    row, col = lax.axis_index("row"), lax.axis_index("col")
    x, k = row // 2, row % 2
    chips, groups = rows // 2, cols // rows
    size, lanes = rows * EDGE, nb * LANES
    hsize, qsize, n128 = size // 2, size // 4, size // LANES
    pairs = nb // 2
    gcol = ncol // 2
    sl = gcol // chips
    mate = {"row": row + 1 - 2 * k, "col": col}
    top, whole = nb - 1, nb // 2
    part, grp = col % rows, col // rows
    k_half, m_half = _at(k, HALF), _at(1 - k, HALF)
    s_a, s_b = 1 + (RING - 1) * k, RING - (RING - 1) * k
    a, b = (col // s_a) % RING, (col // s_b) % RING

    def remote(src, dst, ss, rr, to):
        return pltpu.make_async_remote_copy(src, dst, ss, rr, device_id=to, device_id_type=MESH)

    def await_(ref, sem):
        pltpu.make_async_copy(ref, ref, sem).wait()

    def peer(d):
        return lax.rem(x + d, chips)

    def at_peer(d):
        return {"row": 2 * peer(d) + k, "col": col}

    def plane(da, db):
        return {"row": row, "col": lax.rem(a + da, RING) * s_a + lax.rem(b + db, RING) * s_b}

    def low(q):
        return (groups * q // 2) * STEP

    order = _gathers(slots)

    class Slot:
        def __init__(self, kind, w, n):
            self.kind, self.w, self.n = kind, w, n

        def own(self):
            if self.kind == "m":
                return pm.at[self.w]
            return own.at[self.w, self.kind, :, pl.ds(low(self.kind), lanes - low(self.kind))]

        def piece(self, bb, aa, part=None):
            if self.kind == "m":
                return mg.at[self.w, bb, aa] if part is None else mg.at[self.w, bb, aa, pl.ds(part * HALF, HALF)]
            at = pl.ds(low(self.kind), lanes - low(self.kind))
            e = slice(None) if part is None else pl.ds(part * (HALF // 2), HALF // 2)
            return gath.at[self.w, self.kind, bb, aa, e, at]

        def bundle(self, bb, part=None):
            e = slice(None) if part is None else pl.ds(part * (RING // 2), RING // 2)
            if self.kind == "m":
                return mg.at[self.w, bb, e]
            return gath.at[self.w, self.kind, bb, e, :, pl.ds(low(self.kind), lanes - low(self.kind))]

        def copy(self, i):
            d = 1 if i % 2 == 0 else RING - 1
            back = RING - d
            if i < 2:
                src, dst, to = self.own(), self.piece(b, a), plane(d, 0)
            elif i < 4:
                src = dst = self.piece(b, lax.rem(a + back, RING), i % 2)
                to = plane(d, 0)
            elif i < 6:
                src = dst = self.bundle(b)
                to = plane(0, d)
            else:
                src = dst = self.bundle(lax.rem(b + back, RING), i % 2)
                to = plane(0, d)
            return remote(src, dst, ag_s.at[self.n, i], ag_r.at[self.n, i], to)

        def arrived(self, i):
            back = RING - 1 if i % 2 == 0 else 1
            if i < 2:
                dst = self.piece(b, lax.rem(a + back, RING))
            elif i < 4:
                dst = self.piece(b, lax.rem(a + 2, RING), i % 2)
            elif i < 6:
                dst = self.bundle(lax.rem(b + back, RING))
            else:
                dst = self.bundle(lax.rem(b + 2, RING), i % 2)
            await_(dst, ag_r.at[self.n, i])

        def kept(self):
            return pltpu.make_async_copy(self.own(), self.piece(b, a), ag_loc.at[self.n])

        def stage(self, s):
            if s == 0:
                self.copy(0).start()
                self.copy(1).start()
                self.kept().start()
            elif s == 1:
                for i in range(2):
                    self.arrived(i)
                    self.copy(2 + i).start()
            elif s == 2:
                self.kept().wait()
                self.arrived(2)
                self.arrived(3)
                self.copy(4).start()
                self.copy(5).start()
            elif s == 3:
                for i in range(4, 6):
                    self.arrived(i)
                    self.copy(2 + i).start()
            elif s == 4:
                self.arrived(6)
                self.arrived(7)
            else:
                for i in range(8):
                    self.copy(i).wait_send()

    class Eager(Slot):
        def spot(self, db, da, part=None):
            return self.piece(lax.rem(b + db, RING), lax.rem(a + da, RING), part)

        def copy(self, i):
            back = RING - 1
            db, da, part, to_b, to_a = (
                (0, 0, None, 0, 1), (0, 0, None, 0, back), (0, 0, None, 1, 0), (0, 0, None, back, 0),
                (0, back, 0, 0, 1), (0, 1, 1, 0, back),
                (0, back, None, 1, 0), (0, back, None, back, 0), (0, 1, None, 1, 0), (0, 1, None, back, 0),
                (0, 2, None, 1, 0), (0, 2, None, back, 0),
                (back, 0, None, 1, 0), (back, back, None, 1, 0), (1, 1, None, back, 0), (1, 2, None, back, 0),
            )[i]
            dst = self.spot(db, da, part)
            src = self.own() if db == 0 and da == 0 else dst
            sent_ = remote(src, dst, eg_s.at[i], eg_r.at[i], plane(to_a, to_b))
            return sent_, self.spot(db + RING - to_b, da + RING - to_a, part)

        def go(self, *which):
            for i in which:
                self.copy(i)[0].start()

        def got(self, *which):
            for i in which:
                await_(self.copy(i)[1], eg_r.at[i])

        def stage(self, s):
            if s == 0:
                self.go(0, 1, 2, 3)
                self.kept().start()
            elif s == 1:
                self.got(0)
                self.go(4, 6, 7)
                self.got(1)
                self.go(5, 8, 9)
                self.got(2)
                self.go(12)
            elif s == 2:
                self.got(4, 5)
                self.go(10, 11)
                self.got(6)
                self.go(13)
            elif s == 3:
                self.got(9)
                self.go(14)
                self.got(11)
                self.go(15)
            elif s == 4:
                self.got(3, 7, 8, 10, 12, 13, 14, 15)
                self.kept().wait()
                for i in range(16):
                    self.copy(i)[0].wait_send()

    def tick(t):
        for s in (4, 3, 2, 1, 0, 5):
            n = t - s
            if isinstance(n, int):
                if 0 <= n < len(order) and order[n] is not None:
                    (Eager if order[n] == ("m", 0) else Slot)(*order[n], n).stage(s)
                continue
            for kind in list(range(slots)) + ["m"]:
                at_v, at_l = order.index((kind, 0)), order.index((kind, 1))

                @pl.when(n == at_l if kind == "m" else jnp.logical_or(n == at_v, n == at_l))
                def _(s=s, n=n, kind=kind, at_l=at_l):
                    Slot(kind, jnp.where(n == at_l, 1, 0), n).stage(s)

    def block_of(n):
        j = top - n % nb
        return n // nb, j, j // groups, j % groups, n % 2

    run = min(rows, RING)
    runs = rows // run

    def in_blk(n, q, i, half):
        return blk.at[n % DEEP, pl.ds(i * run, run), half, pl.ds(low(q), lanes - low(q))]

    def from_mate(n, q, i):
        await_(in_blk(n, q, i, m_half), blk_r.at[n % DEEP, i])

    def mat_copies(n, i):
        w, j, q, h, s = block_of(n)
        c = h * rows + q
        src = mg.at[w, (c // s_b) % RING, (c // s_a) % RING, :, pl.ds(LANES * (i * (i + 1) // 2), LANES * (i + 1))]
        dst = mbuf.at[s, pl.ds(pl.multiple_of(i * LANES + k * EDGE, EDGE), EDGE), pl.ds(0, LANES * (i + 1))]
        return (
            pltpu.make_async_copy(src, dst, mat_loc.at[s, i]),
            remote(src, dst, mat_s.at[s, i], mat_r.at[s, i], mate),
        )

    def per_piece(n, act):
        q_now = block_of(n)[2]
        for q in range(slots):

            @pl.when(q_now == q)
            def _(q=q):
                for i in range(runs):
                    act(q, i)

    def fetch_blk(n):
        w, _, _, h, _ = block_of(n)
        s = n % DEEP

        def go(q, i):
            c = h * rows + i * run
            z_now, y_run = c // RING, pl.ds(c % RING, run)
            at = pl.ds(low(q), lanes - low(q))
            dst = in_blk(n, q, i, k_half)

            def both(src):
                pltpu.make_async_copy(src, dst, blk_loc.at[s, i]).start()
                remote(src, dst, blk_s.at[s, i], blk_r.at[s, i], mate).start()

            pl.when(k == 0)(lambda: both(gath.at[w, q, z_now, y_run, :, at]))
            pl.when(k == 1)(lambda: both(gath.at[w, q, y_run, z_now, :, at]))

        per_piece(n, go)

    def fetch_mat(n):
        for i in range(n128):
            for c in mat_copies(n, i):
                c.start()

    def wait_blk(n):
        def one(q, i):
            await_(in_blk(n, q, i, k_half), blk_loc.at[n % DEEP, i])
            from_mate(n, q, i)

        per_piece(n, one)

    def wait_mat(n):
        for i in range(n128):
            mat_copies(n, i)[0].wait()
            there = pl.ds(pl.multiple_of(i * LANES + (1 - k) * EDGE, EDGE), EDGE), pl.ds(0, LANES * (i + 1))
            await_(mbuf.at[(n % 2, *there)], mat_r.at[n % 2, i])

    def release_blk(n):
        per_piece(n, lambda q, i: await_(in_blk(n, q, i, k_half), blk_s.at[n % DEEP, i]))

        @pl.when(n + DEEP < 2 * nb)
        def _():
            pl.semaphore_signal(free_b.at[n % DEEP], inc=1, device_id=mate, device_id_type=MESH)
            pl.semaphore_wait(free_b.at[n % DEEP], 1)
            fetch_blk(n + DEEP)

    def release_mat(n):
        for i in range(n128):
            mat_copies(n, i)[1].wait_send()

        @pl.when(n + 2 < 2 * nb)
        def _():
            pl.semaphore_signal(free_m.at[n % 2], inc=1, device_id=mate, device_id_type=MESH)
            pl.semaphore_wait(free_m.at[n % 2], 1)
            fetch_mat(n + 2)

    def over(first, body):
        pl.when(first % 2 == 1)(lambda: body(first * STEP, STEP))
        _loop((first + 1) // 2, whole // 2, lambda i: body(i * 2 * STEP, 2 * STEP))

    def rows_at(off, width):
        return pl.ds(pl.multiple_of(off, STEP), width)

    def cut(n, off, width):
        return blk[n % DEEP, :, :, rows_at(off, width)].reshape(size, width)

    def project(dst, ref, n, first):
        dst[...] = jnp.zeros((ncol, size), jnp.float32)

        def one(off, width):
            dst[...] += _dot_nt(ref[:, rows_at(off, width)], cut(n, off, width))

        if whole % 4 or isinstance(first, int):
            over(first, one)
            return
        half = (first + 1) // 2
        pl.when(first % 2 == 1)(lambda: one(first * STEP, STEP))
        pl.when(half % 2 == 1)(lambda: one(half * 2 * STEP, 2 * STEP))
        _loop((half + 1) // 2, whole // 4, lambda i: one(i * 4 * STEP, 4 * STEP))

    def slice_of(g, x2):
        return pl.ds(pl.multiple_of(g * gcol + x2 * sl, sl), sl)

    def cols_of(g):
        return pl.ds(g * gcol, gcol)

    def rs_copy(par, g, d):
        return remote(sbuf.at[par, slice_of(g, peer(d))], rs.at[g, d - 1], rs_s.at[g, d - 1], rs_r.at[g, d - 1], at_peer(d))

    def w_copy(par, g, d):
        mine = wb.at[par, slice_of(g, x)]
        return remote(mine, mine, ex_s.at[g, d - 1], ex_r.at[g, d - 1], at_peer(d))

    c_half = pl.ds(pl.multiple_of(k * (rows // 2), rows // 2), rows // 2)

    def c_copy(par):
        return remote(cm.at[par, _at(k, hsize)], cm.at[par, _at(k, hsize)], cm_s.at[par], cm_r.at[par], mate)

    def apply(n, off, width):
        ys[:, rows_at(off, width)] = ys[:, rows_at(off, width)] - _dot_nn(wb[n % 2], cut(n, off, width))

    def cross(n, off, width):
        here = blk[n % DEEP, c_half, :, rows_at(off, width)].reshape(hsize, width)
        cm[n % 2, _at(k, hsize)] += _dot_nt(here, cut(n + 1, off, width))

    def cols_in(gs):
        return pl.ds(gs[0] * gcol, len(gs) * gcol)

    barrier = pltpu.get_barrier_semaphore()

    def here_i_am(device):
        pl.semaphore_signal(barrier, inc=1, device_id=device, device_id_type=MESH)

    def group_member(d):
        n = lax.rem(2 * part + k + d, 2 * rows)
        here_i_am({"col": grp * rows + n // 2, "row": 2 * x + n % 2})

    _loop(1, 2 * rows, group_member)
    for d in range(1, chips):
        here_i_am(at_peer(d))
    for d in (1, RING - 1):
        here_i_am(plane(d, 0))
        here_i_am(plane(0, d))

    ins = [
        pltpu.make_async_copy(src, stage.at[i % 2], in_sem.at[i]) for i, src in enumerate((v_in, l_in, z_in))
    ] + [pltpu.make_async_copy(t_in, tb, in_sem.at[3])]
    for i in (0, 1, 3):
        ins[i].start()
    pl.semaphore_wait(barrier, 2 * rows - 1 + chips - 1 + 4)

    def swaps(m, i):
        there = _at(2 * i + k, LANES)
        if m < 2:
            mine, theirs = vt.at[m, :, k, :, _at(i, LANES)], vt.at[m, :, 1 - k, :, _at(i, LANES)]
            dst = own.at[m, :, :, there]
        else:
            mine, theirs = zt.at[k, :, _at(i, LANES)], zt.at[1 - k, :, _at(i, LANES)]
            dst = ys.at[:, there]
        return (
            pltpu.make_async_copy(mine, dst, swap_l.at[m, i]),
            remote(theirs, dst, swap_s.at[m, i], swap_r.at[m, i], mate),
        )

    def arriving(m, i):
        there = _at(2 * i + 1 - k, LANES)
        await_(own.at[m, :, :, there] if m < 2 else ys.at[:, there], swap_r.at[m, i])

    def turn(m, then=None):
        ins[m].wait()

        def one(i):
            block = stage[m % 2, _at(i, LANES), :].T
            if m < 2:
                vt[m, :, :, :, _at(i, LANES)] = block.reshape(slots, 2, HALF, LANES)
            else:
                zt[:, :, _at(i, LANES)] = block.reshape(2, ncol, LANES)
            for c in swaps(m, i):
                c.start()
            if then is not None:
                pl.when(i > 0)(lambda: then(i - 1))

        _loop(0, pairs, one)
        if then is not None:
            then(pairs - 1)

    def swapped(m):
        def one(i):
            swaps(m, i)[0].wait()
            arriving(m, i)

        _loop(0, pairs, one)

    my_q, my_h = part, grp
    my_j = groups * my_q + my_h
    first_t = my_j // 2

    def deal_v(q, t, act):
        to, kk = grp * rows + q, t % 2
        src = own.at[0, q, :, _at(t, STEP)]
        dst = vb.at[t // 2, part, k_half]
        self_ = jnp.logical_and(to == col, k == kk)
        act(
            self_,
            pltpu.make_async_copy(src, dst, v_r.at[t // 2, part, k]),
            remote(src, dst, v_s.at[q, t], v_r.at[t // 2, part, k], {"col": to, "row": 2 * x + kk}),
        )

    def deal_l(q, kk, act):
        to = grp * rows + q
        src = own.at[1, q, :, _at((groups * q + grp) // 2, STEP)]
        dst = ld.at[part, k_half]
        self_ = jnp.logical_and(to == col, k == kk)
        act(
            self_,
            pltpu.make_async_copy(src, dst, l_r.at[part, k]),
            remote(src, dst, l_s.at[q, kk], l_r.at[part, k], {"col": to, "row": 2 * x + kk}),
        )

    def send(self_, here, there):
        pl.when(self_)(here.start)
        pl.when(jnp.logical_not(self_))(there.start)

    def sent(self_, here, there):
        pl.when(jnp.logical_not(self_))(there.wait_send)

    def over_v(act):
        def one(q):
            _loop((groups * q + grp) // 2, pairs, lambda t: deal_v(q, t, act))

        _loop(0, slots, one)

    def over_l(act):
        def one(q):
            deal_l(q, 0, act)
            deal_l(q, 1, act)

        _loop(0, slots, one)

    def deal_chunk(t):
        swaps(0, t)[0].wait()
        arriving(0, t)
        _loop(0, (2 * t + 1 - grp + groups) // groups, lambda q: deal_v(q, t, send))

    turn(0, deal_chunk)
    ins[2].start()
    turn(1)
    swapped(1)
    over_l(send)
    turn(2)
    mbuf[...] = jnp.zeros_like(mbuf)

    gm[...] = jnp.zeros_like(gm)

    def chunk(i):
        def got(n):
            await_(vb.at[i, n // 2, _at(n % 2, HALF)], v_r.at[i, n // 2, n % 2])

        _loop(0, 2 * rows, got)
        all_ = vb[i].reshape(size, STEP)
        gm[pl.ds(0, hsize), pl.ds(0, hsize)] += _dot_nt(all_[:hsize], all_[:hsize])
        gm[pl.ds(hsize, hsize), :] += _dot_nt(all_[hsize:], all_)

    _loop((first_t + 1 - k) // 2, pairs // 2, chunk)
    tick(0)

    widths = []
    w_ = hsize
    while w_ >= EDGE:
        widths.append(w_)
        w_ //= 2

    def packed(w_):
        return pl.ds(size - 2 * w_, w_)

    pk[...] = jnp.zeros_like(pk)
    for w_ in widths:
        for i in range(hsize // w_):
            pk[pl.ds(i * w_, w_), packed(w_)] = gm[pl.ds((2 * i + 1) * w_, w_), pl.ds(2 * i * w_, w_)]

    mine, theirs = _at(k, qsize), _at(1 - k, qsize)
    to_mate = remote(pk.at[theirs], gx, gx_sem.at[0], gx_sem.at[1], mate)
    to_mate.start()
    tick(1)
    to_mate.wait_recv()
    pk[mine] += gx[...]
    rl = qsize // chips

    def r2_copy(d):
        src = pk.at[pl.ds(pl.multiple_of(k * qsize + peer(d) * rl, rl), rl)]
        return remote(src, r2.at[d - 1], r2_s.at[d - 1], r2_r.at[d - 1], at_peer(d))

    for d in range(1, chips):
        r2_copy(d).start()

    def got_l(n):
        await_(ld.at[n // 2, _at(n % 2, HALF)], l_r.at[n // 2, n % 2])

    _loop(0, 2 * rows, got_l)
    ev = my_j % 2 == 0
    lo_half = lax.broadcasted_iota(jnp.int32, (size, LANES), 1) < EDGE
    l_lo, l_hi = ld[:, :, pl.ds(0, LANES)].reshape(size, LANES), ld[:, :, pl.ds(LANES, LANES)].reshape(size, LANES)
    lx[x] = jnp.where(
        lo_half,
        jnp.where(ev, l_lo, pltpu.roll(l_lo, EDGE, 1)),
        jnp.where(ev, pltpu.roll(l_hi, EDGE, 1), l_hi),
    )

    def lx_copy(d):
        return remote(lx.at[x], lx.at[x], lx_s.at[d - 1], lx_r.at[d - 1], at_peer(d))

    tick(2)
    for d in range(1, chips):
        r2_copy(d).wait_recv()
    my_rows = pl.ds(pl.multiple_of(k * qsize + x * rl, rl), rl)
    total = pk[my_rows]
    for d in range(1, chips):
        total = total + r2[d - 1]
    ga[my_rows] = total

    def ga_copy(d):
        return remote(ga.at[my_rows], ga.at[my_rows], ga_s.at[d - 1], ga_r.at[d - 1], at_peer(d))

    for d in range(1, chips):
        ga_copy(d).start()
    for d in range(1, chips):
        lx_copy(d).start()
    tick(3)
    for d in range(1, chips):
        await_(ga.at[pl.ds(pl.multiple_of(k * qsize + peer(chips - d) * rl, rl), rl)], ga_r.at[d - 1])
    half_to_mate = remote(ga.at[mine], ga.at[mine], gx_sem.at[2], gx_sem.at[3], mate)
    half_to_mate.start()

    r_i = lax.broadcasted_iota(jnp.int32, (LANES, LANES), 0)
    c_i = lax.broadcasted_iota(jnp.int32, (LANES, LANES), 1)

    def tile(i):
        return _at(i, LANES), _at(i, LANES)

    def merge_tile(w, i, low_part):
        cur = xm[(w, *tile(i))]
        xm[(w, *tile(i))] = cur - _dot_nn(_dot_nn(cur, low_part), cur)

    def level_l(lev):
        pick = jnp.logical_and(
            lax.shift_right_logical(r_i, lev) % 2 == 1,
            lax.shift_right_logical(c_i, lev) + 1 == lax.shift_right_logical(r_i, lev),
        )
        _loop(0, n128, lambda i: merge_tile(1, i, jnp.where(pick, gm[tile(i)], 0.0)))

    def level_big(w, corner):
        for w_ in reversed(widths[:-1]):
            for i in range(hsize // w_):
                d1 = pl.ds(2 * i * w_, w_)
                d2 = pl.ds((2 * i + 1) * w_, w_)
                xm[w, d2, d1] = -_dot_nn(_dot_nn(xm[w, d2, d2], corner(w_, i)), xm[w, d1, d1])

    def pack_factor(w):
        for i in range(n128):
            pm[w, :, pl.ds(LANES * (i * (i + 1) // 2), LANES * (i + 1))] = xm[
                w, pl.ds(pl.multiple_of(i * LANES + k * EDGE, EDGE), EDGE), pl.ds(0, LANES * (i + 1))
            ]

    xm[...] = jnp.zeros_like(xm)
    ins[3].wait()
    for p in range(0, rows, 2):
        zero = jnp.zeros((EDGE, EDGE), jnp.float32)
        both = jnp.concatenate(
            [jnp.concatenate([tb[p], zero], axis=1), jnp.concatenate([zero, tb[p + 1]], axis=1)], axis=0
        )
        xm[0, pl.ds(p * EDGE, LANES), pl.ds(p * EDGE, LANES)] = both
    await_(ga.at[theirs], gx_sem.at[3])

    def corner64(i):
        block = ga[_at(i, EDGE), packed(EDGE)]
        zero = jnp.zeros((EDGE, EDGE), jnp.float32)
        low_part = jnp.concatenate([block, zero], axis=1)
        merge_tile(0, i, jnp.concatenate([jnp.zeros_like(low_part), low_part], axis=0))

    _loop(0, n128, corner64)
    level_big(0, lambda w_, i: ga[pl.ds(i * w_, w_), packed(w_)])
    pack_factor(0)
    tick(4)

    fetch_blk(0)
    fetch_blk(1)
    for d in range(1, chips):
        await_(lx.at[peer(chips - d)], lx_r.at[d - 1])
    for i in range(chips):
        gm[_at(i, LANES), :] = lx[i].T
    same = r_i == c_i

    def diag(i):
        d = gm[tile(i)]
        xm[(1, *tile(i))] = jnp.where(same, 1.0 / jnp.where(same, d, 1.0), 0.0)

    _loop(0, n128, diag)
    swapped(2)
    tick(5)
    _loop(0, 3, level_l)
    tick(6)
    wait_blk(0)
    project(sbuf.at[0], ys, 0, top // 2)
    for g in range(2):
        for d in range(1, chips):
            rs_copy(0, g, d).start()
    _loop(3, 7, level_l)
    tick(7)
    level_big(1, lambda w_, i: gm[pl.ds((2 * i + 1) * w_, w_), pl.ds(2 * i * w_, w_)])
    pack_factor(1)
    tick(8)
    fetch_mat(0)
    fetch_mat(1)
    fetch_blk(2)

    wait_mat(0)

    def reflect(n):
        j, par, nxt = top - n, n % 2, (n + 1) % 2

        @pl.when(j > 0)
        def _():
            wait_blk(n + 1)
            cm[par, _at(k, hsize)] = jnp.zeros((hsize, size), jnp.float32)
            pl.when(j % 2 == 1)(lambda: cross(n, (j // 2) * STEP, STEP))

            def one(off, width):
                apply(n - 1, off, width)
                cross(n, off, width)

            over((j + 1) // 2, one)
            c_copy(par).start()

        pl.when(j == 0)(lambda: over(0, functools.partial(apply, n - 1)))

        def factor(gs):
            totals = []
            for g in gs:
                for d in range(1, chips):
                    rs_copy(par, g, d).wait_recv()
                total = sbuf[par, slice_of(g, x)]
                for d in range(1, chips):
                    total = total + rs[g, d - 1]
                totals.append(total)
            got = _dot_nn(jnp.concatenate(totals, axis=0), mbuf[par])
            for i, g in enumerate(gs):
                wb[par, slice_of(g, x)] = got[i * sl : (i + 1) * sl]
                for d in range(1, chips):
                    w_copy(par, g, d).start()

        factor((0,))
        factor((1,))

        for g in range(2):
            for d in range(1, chips):
                rs_copy(par, g, d).wait_send()

        pl.when(n > 0)(lambda: release_blk(n - 1))
        release_mat(n)

        @pl.when(j > 0)
        def _():
            project(sbuf.at[nxt], ys, n + 1, (j - 1) // 2)

        @pl.when(jnp.where(n < 9, par == 0, par == 1))
        def _():
            tick(LEAD + (n + 1) // 2)

        @pl.when(j > 0)
        def _():
            wait_mat(n + 1)
            await_(cm.at[par, _at(1 - k, hsize)], cm_r.at[par])

        def correct(gs):
            for g in gs:
                for d in range(1, chips):
                    await_(wb.at[par, slice_of(g, peer(chips - d))], ex_r.at[g, d - 1])

            @pl.when(j > 0)
            def _():
                sbuf[nxt, cols_in(gs)] = sbuf[nxt, cols_in(gs)] - _dot_nn(wb[par, cols_in(gs)], cm[par])
                for g in gs:
                    for d in range(1, chips):
                        rs_copy(nxt, g, d).start()

        correct((0,))
        correct((1,))

        for g in range(2):
            for d in range(1, chips):
                w_copy(par, g, d).wait_send()

        @pl.when(j > 0)
        def _():
            c_copy(par).wait_send()

    _loop(0, nb, reflect)
    over(0, functools.partial(apply, top))
    release_blk(top)

    xs[...] = jnp.zeros_like(xs)
    def first_half(val):
        return lax.broadcasted_iota(jnp.int32, val.shape, 1) < EDGE


    def take(ref, cols_, j):
        lo = ref[cols_, pl.ds(pl.multiple_of((j // 2) * STEP, LANES), LANES)]
        hi = ref[cols_, pl.ds(pl.multiple_of((j // 2) * STEP + LANES, LANES), LANES)]
        even = j % 2 == 0
        return jnp.where(
            first_half(lo),
            jnp.where(even, lo, pltpu.roll(lo, EDGE, 1)),
            jnp.where(even, pltpu.roll(hi, EDGE, 1), hi),
        )

    def spread(val, j):
        even, first = j % 2 == 0, first_half(val)
        other = pltpu.roll(val, EDGE, 1)
        zero = jnp.zeros_like(val)
        lo = jnp.where(even, jnp.where(first, val, zero), jnp.where(first, zero, other))
        hi = jnp.where(even, jnp.where(first, other, zero), jnp.where(first, zero, val))
        return jnp.concatenate([lo, hi], axis=1)

    def x_copy(par, g, d):
        src = sbuf.at[par, cols_of(g), _at(peer(d), LANES)]
        return remote(src, rx.at[par, g, d - 1], rx_s.at[par, g, d - 1], rx_r.at[par, g, d - 1], at_peer(d))

    def solve_partial(n, gs, j):
        par, cols_ = n % 2, cols_in(gs)
        wb[0, cols_] = -wb[0, cols_]
        wb[0, cols_, _at(x, LANES)] += take(ys, cols_, j)
        sbuf[par, cols_] = _dot_nn(wb[0, cols_], mbuf[par])
        for g in gs:
            for d in range(1, chips):
                x_copy(par, g, d).start()

    def fin_copy(i):
        return remote(
            xs.at[:, _at(2 * i + 1 - k, LANES)], zt.at[k, :, _at(i, LANES)], fin_s.at[i], fin_r.at[i], mate
        )

    def give(i):
        await_(zt.at[1 - k, :, _at(i, LANES)], fin_r.at[i])
        zt[k, :, _at(i, LANES)] = xs[:, _at(2 * i + k, LANES)]
        out_ref[_at(i, LANES), :] = zt[:, :, _at(i, LANES)].reshape(2 * ncol, LANES).T

    for m in range(3):
        _loop(0, pairs, lambda i, m=m: swaps(m, i)[1].wait_send())
    over_v(sent)
    over_l(sent)
    to_mate.wait_send()
    half_to_mate.wait_send()
    for d in range(1, chips):
        r2_copy(d).wait_send()
        ga_copy(d).wait_send()
        lx_copy(d).wait_send()

    wait_blk(nb)
    wait_mat(nb)
    wb[0] = jnp.zeros((ncol, size), jnp.float32)
    for g in range(2):
        solve_partial(nb, (g,), top)
    release_blk(nb)
    release_mat(nb)

    def solve(i):
        n = nb + i
        j, par, nxt = top - i, n % 2, (n + 1) % 2

        @pl.when(j > 0)
        def _():
            wait_blk(n + 1)
            wait_mat(n + 1)
            project(wb.at[0], xs, n + 1, (j + 1) // 2)

        def finish(gs):
            cols_ = cols_in(gs)
            vals = []
            for g in gs:
                for d in range(1, chips):
                    x_copy(par, g, d).wait_recv()
                val = sbuf[par, cols_of(g), _at(x, LANES)]
                for d in range(1, chips):
                    val = val + rx[par, g, d - 1]
                vals.append(val)
            solved = spread(jnp.concatenate(vals, axis=0), j)
            xs[cols_, _at(j // 2, STEP)] += solved

            @pl.when(j > 0)
            def _():
                wb[0, cols_] += _dot_nt(solved, cut(n + 1, (j // 2) * STEP, STEP))
                solve_partial(n + 1, gs, j - 1)

        finish((0,))
        finish((1,))

        pl.when(j % 2 == 0)(lambda: fin_copy(j // 2).start())
        pl.when(jnp.logical_and(j % 2 == 1, j < top))(lambda: give(j // 2 + 1))

        for g in range(2):
            for d in range(1, chips):
                x_copy(par, g, d).wait_send()

        @pl.when(jnp.logical_or(i == 0, i % 2 == 1))
        def _():
            tick(LEAD + 9 + (i + 1) // 2)

        @pl.when(j > 0)
        def _():
            release_blk(n + 1)
            release_mat(n + 1)

    _loop(0, nb, solve)

    give(0)
    _loop(0, pairs, lambda i: fin_copy(i).wait_send())


def solution(mesh):
    rows, cols = mesh.shape["row"], mesh.shape["col"]
    mat_spec = P(("kpt", "row"), "col")
    fac_spec = P("kpt", None, None)

    def local_work(v_loc, t_loc, z_loc, l_loc):
        n_row, n_col = v_loc.shape
        slots, lanes, chips, size = n_col // EDGE, 2 * n_row, rows // 2, rows * EDGE
        nb, ncol = lanes // LANES, z_loc.shape[1] // 2
        pairs, gcol, peers = nb // 2, ncol // 2, max(chips - 1, 1)
        sl, gathers, n128 = gcol // chips, len(_gathers(slots)), size // LANES
        tri = LANES * (n128 * (n128 + 1) // 2)
        dma = pltpu.SemaphoreType.DMA
        hbm, vmem = pl.BlockSpec(memory_space=pl.ANY), pl.BlockSpec(memory_space=pltpu.VMEM)

        def buf(*shape):
            return pltpu.VMEM(shape, jnp.float32)

        col = lax.axis_index("col")
        t_mine = lax.dynamic_slice_in_dim(t_loc, (cols // rows * (col % rows) + col // rows) * rows, rows, axis=0)
        return pl.pallas_call(
            functools.partial(_kernel, (rows, cols, slots, nb, ncol)),
            out_shape=[
                jax.ShapeDtypeStruct(z_loc.shape, jnp.float32),
                jax.ShapeDtypeStruct((2, slots, RING, RING, HALF, lanes), jnp.float32),
            ],
            in_specs=[hbm] * 4,
            out_specs=[vmem, hbm],
            scratch_shapes=[
                buf(2, n_row, n_col),
                buf(2, slots, 2, HALF, n_row),
                buf(2, ncol, n_row),
                buf(rows, EDGE, EDGE),
                buf(2, slots, HALF, lanes),
                buf(ncol, lanes),
                buf(ncol, lanes),
                buf(pairs // 2, rows, EDGE, STEP),
                buf(rows, EDGE, STEP),
                buf(chips, size, LANES),
                buf(size, size),
                buf(size // 2, size),
                buf(size // 4, size),
                buf(peers, size // 4 // chips, size),
                buf(size // 2, size),
                buf(2, EDGE, tri),
                buf(2, RING, RING, EDGE, tri),
                buf(DEEP, rows, EDGE, lanes),
                buf(2, size, size),
                buf(2, ncol, size),
                buf(2, peers, sl, size),
                buf(2, ncol, size),
                buf(2, size, size),
                buf(2, 2, peers, gcol, LANES),
                dma((4,)),
                dma((3, pairs)), dma((3, pairs)), dma((3, pairs)),
                dma((slots, pairs)), dma((pairs // 2, rows, 2)),
                dma((slots, 2)), dma((rows, 2)),
                dma((peers,)), dma((peers,)),
                dma((4,)),
                dma((peers,)), dma((peers,)), dma((peers,)), dma((peers,)),
                dma((pairs,)), dma((pairs,)),
                dma((gathers,)), dma((gathers, 8)), dma((gathers, 8)),
                dma((DEEP, rows)), dma((DEEP, rows)), dma((DEEP, rows)),
                dma((2, n128)), dma((2, n128)), dma((2, n128)),
                pltpu.SemaphoreType.REGULAR((DEEP,)), pltpu.SemaphoreType.REGULAR((2,)),
                dma((2, peers)), dma((2, peers)), dma((2, peers)), dma((2, peers)),
                dma((2,)), dma((2,)),
                dma((2, 2, peers)), dma((2, 2, peers)),
                dma((16,)), dma((16,)),
            ],
            compiler_params=pltpu.CompilerParams(collective_id=0, has_side_effects=True, vmem_limit_bytes=67_043_328),
            name="eigvec",
        )(v_loc, t_mine, z_loc, l_loc)[0]

    return jax.shard_map(local_work, mesh=mesh, in_specs=(mat_spec, fac_spec, mat_spec, mat_spec), out_specs=mat_spec, check_vma=False)
```

```python
import functools

import jax
import jax.numpy as jnp
from jax import lax
from jax.experimental import pallas as pl
from jax.experimental.pallas import tpu as pltpu
from jax.sharding import PartitionSpec as P

PREC_HIGH = lax.Precision.HIGHEST
MESH = pl.DeviceIdType.MESH
EDGE = 64
HALF = EDGE // 2
LANES = 128
STEP = 256
RING = 4
LEAD = 9
DEEP = 3


def _dot_nt(a, b):
    return lax.dot_general(a, b, (((1,), (1,)), ((), ())), precision=PREC_HIGH, preferred_element_type=jnp.float32)


def _dot_nn(a, b):
    return lax.dot_general(a, b, (((1,), (0,)), ((), ())), precision=PREC_HIGH, preferred_element_type=jnp.float32)


def _at(i, n):
    return pl.ds(pl.multiple_of(i * n, n), n)


def _loop(lo, hi, body):
    def one(i, carry):
        body(i)
        return carry

    lax.fori_loop(lo, hi, one, 0)


def _gathers(slots):
    early = [(slots - 1, 0), (slots - 2, 0), None, None, ("m", 0)]
    first = early + [(q, 0) for q in range(slots - 3, -1, -1)]
    rest = [(slots - 1, 1), ("m", 1)] + [(q, 1) for q in range(slots - 2, -1, -1)]
    return first + [None] * (LEAD - len(first)) + rest


def _kernel(dims, v_in, t_in, z_in, l_in, out_ref, gath, *scratch):
    (stage, vt, zt, tb, own, ys, xs, vb, ld, lx, gm, pk, gx, r2, ga, pm, mg, blk, mbuf, sbuf, rs, wb, cm, rx,
     in_sem, swap_l, swap_s, swap_r, v_s, v_r, l_s, l_r, lx_s, lx_r, gx_sem, r2_s, r2_r, ga_s, ga_r, fin_s, fin_r,
     ag_loc, ag_s, ag_r, blk_loc, blk_s, blk_r, mat_loc, mat_s, mat_r, free_b, free_m, rs_s, rs_r, ex_s, ex_r, cm_s, cm_r,
     rx_s, rx_r, eg_s, eg_r) = scratch
    xm = cm
    rows, cols, slots, nb, ncol = dims
    row, col = lax.axis_index("row"), lax.axis_index("col")
    x, k = row // 2, row % 2
    chips, groups = rows // 2, cols // rows
    size, lanes = rows * EDGE, nb * LANES
    hsize, qsize, n128 = size // 2, size // 4, size // LANES
    pairs = nb // 2
    gcol = ncol // 2
    sl = gcol // chips
    mate = {"row": row + 1 - 2 * k, "col": col}
    top, whole = nb - 1, nb // 2
    part, grp = col % rows, col // rows
    k_half, m_half = _at(k, HALF), _at(1 - k, HALF)
    s_a, s_b = 1 + (RING - 1) * k, RING - (RING - 1) * k
    a, b = (col // s_a) % RING, (col // s_b) % RING

    def remote(src, dst, ss, rr, to):
        return pltpu.make_async_remote_copy(src, dst, ss, rr, device_id=to, device_id_type=MESH)

    def await_(ref, sem):
        pltpu.make_async_copy(ref, ref, sem).wait()

    def peer(d):
        return lax.rem(x + d, chips)

    def at_peer(d):
        return {"row": 2 * peer(d) + k, "col": col}

    def plane(da, db):
        return {"row": row, "col": lax.rem(a + da, RING) * s_a + lax.rem(b + db, RING) * s_b}

    def low(q):
        return (groups * q // 2) * STEP

    order = _gathers(slots)

    class Slot:
        def __init__(self, kind, w, n):
            self.kind, self.w, self.n = kind, w, n

        def own(self):
            if self.kind == "m":
                return pm.at[self.w]
            return own.at[self.w, self.kind, :, pl.ds(low(self.kind), lanes - low(self.kind))]

        def piece(self, bb, aa, part=None):
            if self.kind == "m":
                return mg.at[self.w, bb, aa] if part is None else mg.at[self.w, bb, aa, pl.ds(part * HALF, HALF)]
            at = pl.ds(low(self.kind), lanes - low(self.kind))
            e = slice(None) if part is None else pl.ds(part * (HALF // 2), HALF // 2)
            return gath.at[self.w, self.kind, bb, aa, e, at]

        def bundle(self, bb, part=None):
            e = slice(None) if part is None else pl.ds(part * (RING // 2), RING // 2)
            if self.kind == "m":
                return mg.at[self.w, bb, e]
            return gath.at[self.w, self.kind, bb, e, :, pl.ds(low(self.kind), lanes - low(self.kind))]

        def copy(self, i):
            d = 1 if i % 2 == 0 else RING - 1
            back = RING - d
            if i < 2:
                src, dst, to = self.own(), self.piece(b, a), plane(d, 0)
            elif i < 4:
                src = dst = self.piece(b, lax.rem(a + back, RING), i % 2)
                to = plane(d, 0)
            elif i < 6:
                src = dst = self.bundle(b)
                to = plane(0, d)
            else:
                src = dst = self.bundle(lax.rem(b + back, RING), i % 2)
                to = plane(0, d)
            return remote(src, dst, ag_s.at[self.n, i], ag_r.at[self.n, i], to)

        def arrived(self, i):
            back = RING - 1 if i % 2 == 0 else 1
            if i < 2:
                dst = self.piece(b, lax.rem(a + back, RING))
            elif i < 4:
                dst = self.piece(b, lax.rem(a + 2, RING), i % 2)
            elif i < 6:
                dst = self.bundle(lax.rem(b + back, RING))
            else:
                dst = self.bundle(lax.rem(b + 2, RING), i % 2)
            await_(dst, ag_r.at[self.n, i])

        def kept(self):
            return pltpu.make_async_copy(self.own(), self.piece(b, a), ag_loc.at[self.n])

        def stage(self, s):
            if s == 0:
                self.copy(0).start()
                self.copy(1).start()
                self.kept().start()
            elif s == 1:
                for i in range(2):
                    self.arrived(i)
                    self.copy(2 + i).start()
            elif s == 2:
                self.kept().wait()
                self.arrived(2)
                self.arrived(3)
                self.copy(4).start()
                self.copy(5).start()
            elif s == 3:
                for i in range(4, 6):
                    self.arrived(i)
                    self.copy(2 + i).start()
            elif s == 4:
                self.arrived(6)
                self.arrived(7)
            else:
                for i in range(8):
                    self.copy(i).wait_send()

    class Eager(Slot):
        def spot(self, db, da, part=None):
            return self.piece(lax.rem(b + db, RING), lax.rem(a + da, RING), part)

        def copy(self, i):
            back = RING - 1
            db, da, part, to_b, to_a = (
                (0, 0, None, 0, 1), (0, 0, None, 0, back), (0, 0, None, 1, 0), (0, 0, None, back, 0),
                (0, back, 0, 0, 1), (0, 1, 1, 0, back),
                (0, back, None, 1, 0), (0, back, None, back, 0), (0, 1, None, 1, 0), (0, 1, None, back, 0),
                (0, 2, None, 1, 0), (0, 2, None, back, 0),
                (back, 0, None, 1, 0), (back, back, None, 1, 0), (1, 1, None, back, 0), (1, 2, None, back, 0),
            )[i]
            dst = self.spot(db, da, part)
            src = self.own() if db == 0 and da == 0 else dst
            sent_ = remote(src, dst, eg_s.at[i], eg_r.at[i], plane(to_a, to_b))
            return sent_, self.spot(db + RING - to_b, da + RING - to_a, part)

        def go(self, *which):
            for i in which:
                self.copy(i)[0].start()

        def got(self, *which):
            for i in which:
                await_(self.copy(i)[1], eg_r.at[i])

        def stage(self, s):
            if s == 0:
                self.go(0, 1, 2, 3)
                self.kept().start()
            elif s == 1:
                self.got(0)
                self.go(4, 6, 7)
                self.got(1)
                self.go(5, 8, 9)
                self.got(2)
                self.go(12)
            elif s == 2:
                self.got(4, 5)
                self.go(10, 11)
                self.got(6)
                self.go(13)
            elif s == 3:
                self.got(9)
                self.go(14)
                self.got(11)
                self.go(15)
            elif s == 4:
                self.got(3, 7, 8, 10, 12, 13, 14, 15)
                self.kept().wait()
                for i in range(16):
                    self.copy(i)[0].wait_send()

    def tick(t):
        for s in (4, 3, 2, 1, 0, 5):
            n = t - s
            if isinstance(n, int):
                if 0 <= n < len(order) and order[n] is not None:
                    (Eager if order[n] == ("m", 0) else Slot)(*order[n], n).stage(s)
                continue
            for kind in list(range(slots)) + ["m"]:
                at_v, at_l = order.index((kind, 0)), order.index((kind, 1))

                @pl.when(n == at_l if kind == "m" else jnp.logical_or(n == at_v, n == at_l))
                def _(s=s, n=n, kind=kind, at_l=at_l):
                    Slot(kind, jnp.where(n == at_l, 1, 0), n).stage(s)

    def block_of(n):
        j = top - n % nb
        return n // nb, j, j // groups, j % groups, n % 2

    run = min(rows, RING)
    runs = rows // run

    def in_blk(n, q, i, half):
        return blk.at[n % DEEP, pl.ds(i * run, run), half, pl.ds(low(q), lanes - low(q))]

    def from_mate(n, q, i):
        await_(in_blk(n, q, i, m_half), blk_r.at[n % DEEP, i])

    def mat_copies(n, i):
        w, j, q, h, s = block_of(n)
        c = h * rows + q
        src = mg.at[w, (c // s_b) % RING, (c // s_a) % RING, :, pl.ds(LANES * (i * (i + 1) // 2), LANES * (i + 1))]
        dst = mbuf.at[s, pl.ds(pl.multiple_of(i * LANES + k * EDGE, EDGE), EDGE), pl.ds(0, LANES * (i + 1))]
        return (
            pltpu.make_async_copy(src, dst, mat_loc.at[s, i]),
            remote(src, dst, mat_s.at[s, i], mat_r.at[s, i], mate),
        )

    def per_piece(n, act):
        q_now = block_of(n)[2]
        for q in range(slots):

            @pl.when(q_now == q)
            def _(q=q):
                for i in range(runs):
                    act(q, i)

    def fetch_blk(n):
        w, _, _, h, _ = block_of(n)
        s = n % DEEP

        def go(q, i):
            c = h * rows + i * run
            z_now, y_run = c // RING, pl.ds(c % RING, run)
            at = pl.ds(low(q), lanes - low(q))
            dst = in_blk(n, q, i, k_half)

            def both(src):
                pltpu.make_async_copy(src, dst, blk_loc.at[s, i]).start()
                remote(src, dst, blk_s.at[s, i], blk_r.at[s, i], mate).start()

            pl.when(k == 0)(lambda: both(gath.at[w, q, z_now, y_run, :, at]))
            pl.when(k == 1)(lambda: both(gath.at[w, q, y_run, z_now, :, at]))

        per_piece(n, go)

    def fetch_mat(n):
        for i in range(n128):
            for c in mat_copies(n, i):
                c.start()

    def wait_blk(n):
        def one(q, i):
            await_(in_blk(n, q, i, k_half), blk_loc.at[n % DEEP, i])
            from_mate(n, q, i)

        per_piece(n, one)

    def wait_mat(n):
        for i in range(n128):
            mat_copies(n, i)[0].wait()
            there = pl.ds(pl.multiple_of(i * LANES + (1 - k) * EDGE, EDGE), EDGE), pl.ds(0, LANES * (i + 1))
            await_(mbuf.at[(n % 2, *there)], mat_r.at[n % 2, i])

    def release_blk(n):
        per_piece(n, lambda q, i: await_(in_blk(n, q, i, k_half), blk_s.at[n % DEEP, i]))

        @pl.when(n + DEEP < 2 * nb)
        def _():
            pl.semaphore_signal(free_b.at[n % DEEP], inc=1, device_id=mate, device_id_type=MESH)
            pl.semaphore_wait(free_b.at[n % DEEP], 1)
            fetch_blk(n + DEEP)

    def release_mat(n):
        for i in range(n128):
            mat_copies(n, i)[1].wait_send()

        @pl.when(n + 2 < 2 * nb)
        def _():
            pl.semaphore_signal(free_m.at[n % 2], inc=1, device_id=mate, device_id_type=MESH)
            pl.semaphore_wait(free_m.at[n % 2], 1)
            fetch_mat(n + 2)

    def over(first, body):
        pl.when(first % 2 == 1)(lambda: body(first * STEP, STEP))
        _loop((first + 1) // 2, whole // 2, lambda i: body(i * 2 * STEP, 2 * STEP))

    def rows_at(off, width):
        return pl.ds(pl.multiple_of(off, STEP), width)

    def cut(n, off, width):
        return blk[n % DEEP, :, :, rows_at(off, width)].reshape(size, width)

    def project(dst, ref, n, first):
        dst[...] = jnp.zeros((ncol, size), jnp.float32)

        def one(off, width):
            dst[...] += _dot_nt(ref[:, rows_at(off, width)], cut(n, off, width))

        if whole % 4 or isinstance(first, int):
            over(first, one)
            return
        half = (first + 1) // 2
        pl.when(first % 2 == 1)(lambda: one(first * STEP, STEP))
        pl.when(half % 2 == 1)(lambda: one(half * 2 * STEP, 2 * STEP))
        _loop((half + 1) // 2, whole // 4, lambda i: one(i * 4 * STEP, 4 * STEP))

    def slice_of(g, x2):
        return pl.ds(pl.multiple_of(g * gcol + x2 * sl, sl), sl)

    def cols_of(g):
        return pl.ds(g * gcol, gcol)

    def rs_copy(par, g, d):
        return remote(sbuf.at[par, slice_of(g, peer(d))], rs.at[g, d - 1], rs_s.at[g, d - 1], rs_r.at[g, d - 1], at_peer(d))

    def w_copy(par, g, d):
        mine = wb.at[par, slice_of(g, x)]
        return remote(mine, mine, ex_s.at[g, d - 1], ex_r.at[g, d - 1], at_peer(d))

    c_half = pl.ds(pl.multiple_of(k * (rows // 2), rows // 2), rows // 2)

    def c_copy(n):
        mine = cm.at[n % 3, _at(k, hsize)]
        return remote(mine, mine, cm_s.at[n % 3], cm_r.at[n % 3], mate)

    def apply(n, off, width):
        ys[:, rows_at(off, width)] = ys[:, rows_at(off, width)] - _dot_nn(wb[n % 2], cut(n, off, width))

    def cross(n, off, width):
        here = blk[n % DEEP, c_half, :, rows_at(off, width)].reshape(hsize, width)
        cm[n % 3, _at(k, hsize)] += _dot_nt(here, cut(n + 1, off, width))

    def cross_all(n):
        wait_blk(n + 1)
        cm[n % 3, _at(k, hsize)] = jnp.zeros((hsize, size), jnp.float32)
        over((top - n) // 2, functools.partial(cross, n))
        c_copy(n).start()

    def cols_in(gs):
        return pl.ds(gs[0] * gcol, len(gs) * gcol)

    barrier = pltpu.get_barrier_semaphore()

    def here_i_am(device):
        pl.semaphore_signal(barrier, inc=1, device_id=device, device_id_type=MESH)

    def group_member(d):
        n = lax.rem(2 * part + k + d, 2 * rows)
        here_i_am({"col": grp * rows + n // 2, "row": 2 * x + n % 2})

    _loop(1, 2 * rows, group_member)
    for d in range(1, chips):
        here_i_am(at_peer(d))
    for d in (1, RING - 1):
        here_i_am(plane(d, 0))
        here_i_am(plane(0, d))

    ins = [
        pltpu.make_async_copy(src, stage.at[i % 2], in_sem.at[i]) for i, src in enumerate((v_in, l_in, z_in))
    ] + [pltpu.make_async_copy(t_in, tb, in_sem.at[3])]
    for i in (0, 1, 3):
        ins[i].start()
    pl.semaphore_wait(barrier, 2 * rows - 1 + chips - 1 + 4)

    def swaps(m, i):
        there = _at(2 * i + k, LANES)
        if m < 2:
            mine, theirs = vt.at[m, :, k, :, _at(i, LANES)], vt.at[m, :, 1 - k, :, _at(i, LANES)]
            dst = own.at[m, :, :, there]
        else:
            mine, theirs = zt.at[k, :, _at(i, LANES)], zt.at[1 - k, :, _at(i, LANES)]
            dst = ys.at[:, there]
        return (
            pltpu.make_async_copy(mine, dst, swap_l.at[m, i]),
            remote(theirs, dst, swap_s.at[m, i], swap_r.at[m, i], mate),
        )

    def arriving(m, i):
        there = _at(2 * i + 1 - k, LANES)
        await_(own.at[m, :, :, there] if m < 2 else ys.at[:, there], swap_r.at[m, i])

    def turn(m, then=None):
        ins[m].wait()

        def one(i):
            block = stage[m % 2, _at(i, LANES), :].T
            if m < 2:
                vt[m, :, :, :, _at(i, LANES)] = block.reshape(slots, 2, HALF, LANES)
            else:
                zt[:, :, _at(i, LANES)] = block.reshape(2, ncol, LANES)
            for c in swaps(m, i):
                c.start()
            if then is not None:
                pl.when(i > 0)(lambda: then(i - 1))

        _loop(0, pairs, one)
        if then is not None:
            then(pairs - 1)

    def swapped(m):
        def one(i):
            swaps(m, i)[0].wait()
            arriving(m, i)

        _loop(0, pairs, one)

    my_q, my_h = part, grp
    my_j = groups * my_q + my_h
    first_t = my_j // 2

    def deal_v(q, t, act):
        to, kk = grp * rows + q, t % 2
        src = own.at[0, q, :, _at(t, STEP)]
        dst = vb.at[t // 2, part, k_half]
        self_ = jnp.logical_and(to == col, k == kk)
        act(
            self_,
            pltpu.make_async_copy(src, dst, v_r.at[t // 2, part, k]),
            remote(src, dst, v_s.at[q, t], v_r.at[t // 2, part, k], {"col": to, "row": 2 * x + kk}),
        )

    def deal_l(q, kk, act):
        to = grp * rows + q
        src = own.at[1, q, :, _at((groups * q + grp) // 2, STEP)]
        dst = ld.at[part, k_half]
        self_ = jnp.logical_and(to == col, k == kk)
        act(
            self_,
            pltpu.make_async_copy(src, dst, l_r.at[part, k]),
            remote(src, dst, l_s.at[q, kk], l_r.at[part, k], {"col": to, "row": 2 * x + kk}),
        )

    def send(self_, here, there):
        pl.when(self_)(here.start)
        pl.when(jnp.logical_not(self_))(there.start)

    def sent(self_, here, there):
        pl.when(jnp.logical_not(self_))(there.wait_send)

    def over_v(act):
        def one(q):
            _loop((groups * q + grp) // 2, pairs, lambda t: deal_v(q, t, act))

        _loop(0, slots, one)

    def over_l(act):
        def one(q):
            deal_l(q, 0, act)
            deal_l(q, 1, act)

        _loop(0, slots, one)

    def deal_chunk(t):
        swaps(0, t)[0].wait()
        arriving(0, t)
        _loop(0, (2 * t + 1 - grp + groups) // groups, lambda q: deal_v(q, t, send))

    turn(0, deal_chunk)
    ins[2].start()
    turn(1)
    swapped(1)
    over_l(send)
    turn(2)
    mbuf[...] = jnp.zeros_like(mbuf)

    gm[...] = jnp.zeros_like(gm)

    def chunk(i):
        def got(n):
            await_(vb.at[i, n // 2, _at(n % 2, HALF)], v_r.at[i, n // 2, n % 2])

        _loop(0, 2 * rows, got)
        all_ = vb[i].reshape(size, STEP)
        gm[pl.ds(0, hsize), pl.ds(0, hsize)] += _dot_nt(all_[:hsize], all_[:hsize])
        gm[pl.ds(hsize, hsize), :] += _dot_nt(all_[hsize:], all_)

    _loop((first_t + 1 - k) // 2, pairs // 2, chunk)
    tick(0)

    widths = []
    w_ = hsize
    while w_ >= EDGE:
        widths.append(w_)
        w_ //= 2

    def packed(w_):
        return pl.ds(size - 2 * w_, w_)

    pk[...] = jnp.zeros_like(pk)
    for w_ in widths:
        for i in range(hsize // w_):
            pk[pl.ds(i * w_, w_), packed(w_)] = gm[pl.ds((2 * i + 1) * w_, w_), pl.ds(2 * i * w_, w_)]

    mine, theirs = _at(k, qsize), _at(1 - k, qsize)
    to_mate = remote(pk.at[theirs], gx, gx_sem.at[0], gx_sem.at[1], mate)
    to_mate.start()
    tick(1)
    to_mate.wait_recv()
    pk[mine] += gx[...]
    rl = qsize // chips

    def r2_copy(d):
        src = pk.at[pl.ds(pl.multiple_of(k * qsize + peer(d) * rl, rl), rl)]
        return remote(src, r2.at[d - 1], r2_s.at[d - 1], r2_r.at[d - 1], at_peer(d))

    for d in range(1, chips):
        r2_copy(d).start()

    def got_l(n):
        await_(ld.at[n // 2, _at(n % 2, HALF)], l_r.at[n // 2, n % 2])

    _loop(0, 2 * rows, got_l)
    ev = my_j % 2 == 0
    lo_half = lax.broadcasted_iota(jnp.int32, (size, LANES), 1) < EDGE
    l_lo, l_hi = ld[:, :, pl.ds(0, LANES)].reshape(size, LANES), ld[:, :, pl.ds(LANES, LANES)].reshape(size, LANES)
    lx[x] = jnp.where(
        lo_half,
        jnp.where(ev, l_lo, pltpu.roll(l_lo, EDGE, 1)),
        jnp.where(ev, pltpu.roll(l_hi, EDGE, 1), l_hi),
    )

    def lx_copy(d):
        return remote(lx.at[x], lx.at[x], lx_s.at[d - 1], lx_r.at[d - 1], at_peer(d))

    tick(2)
    for d in range(1, chips):
        r2_copy(d).wait_recv()
    my_rows = pl.ds(pl.multiple_of(k * qsize + x * rl, rl), rl)
    total = pk[my_rows]
    for d in range(1, chips):
        total = total + r2[d - 1]
    ga[my_rows] = total

    def ga_copy(d):
        return remote(ga.at[my_rows], ga.at[my_rows], ga_s.at[d - 1], ga_r.at[d - 1], at_peer(d))

    for d in range(1, chips):
        ga_copy(d).start()
    for d in range(1, chips):
        lx_copy(d).start()
    tick(3)
    for d in range(1, chips):
        await_(ga.at[pl.ds(pl.multiple_of(k * qsize + peer(chips - d) * rl, rl), rl)], ga_r.at[d - 1])
    half_to_mate = remote(ga.at[mine], ga.at[mine], gx_sem.at[2], gx_sem.at[3], mate)
    half_to_mate.start()

    r_i = lax.broadcasted_iota(jnp.int32, (LANES, LANES), 0)
    c_i = lax.broadcasted_iota(jnp.int32, (LANES, LANES), 1)

    def tile(i):
        return _at(i, LANES), _at(i, LANES)

    def merge_tile(w, i, low_part):
        cur = xm[(w, *tile(i))]
        xm[(w, *tile(i))] = cur - _dot_nn(_dot_nn(cur, low_part), cur)

    def level_l(lev):
        pick = jnp.logical_and(
            lax.shift_right_logical(r_i, lev) % 2 == 1,
            lax.shift_right_logical(c_i, lev) + 1 == lax.shift_right_logical(r_i, lev),
        )
        _loop(0, n128, lambda i: merge_tile(1, i, jnp.where(pick, gm[tile(i)], 0.0)))

    def level_big(w, corner):
        for w_ in reversed(widths[:-1]):
            for i in range(hsize // w_):
                d1 = pl.ds(2 * i * w_, w_)
                d2 = pl.ds((2 * i + 1) * w_, w_)
                xm[w, d2, d1] = -_dot_nn(_dot_nn(xm[w, d2, d2], corner(w_, i)), xm[w, d1, d1])

    def pack_factor(w):
        for i in range(n128):
            pm[w, :, pl.ds(LANES * (i * (i + 1) // 2), LANES * (i + 1))] = xm[
                w, pl.ds(pl.multiple_of(i * LANES + k * EDGE, EDGE), EDGE), pl.ds(0, LANES * (i + 1))
            ]

    xm[...] = jnp.zeros_like(xm)
    ins[3].wait()
    for p in range(0, rows, 2):
        zero = jnp.zeros((EDGE, EDGE), jnp.float32)
        both = jnp.concatenate(
            [jnp.concatenate([tb[p], zero], axis=1), jnp.concatenate([zero, tb[p + 1]], axis=1)], axis=0
        )
        xm[0, pl.ds(p * EDGE, LANES), pl.ds(p * EDGE, LANES)] = both
    await_(ga.at[theirs], gx_sem.at[3])

    def corner64(i):
        block = ga[_at(i, EDGE), packed(EDGE)]
        zero = jnp.zeros((EDGE, EDGE), jnp.float32)
        low_part = jnp.concatenate([block, zero], axis=1)
        merge_tile(0, i, jnp.concatenate([jnp.zeros_like(low_part), low_part], axis=0))

    _loop(0, n128, corner64)
    level_big(0, lambda w_, i: ga[pl.ds(i * w_, w_), packed(w_)])
    pack_factor(0)
    tick(4)

    fetch_blk(0)
    fetch_blk(1)
    for d in range(1, chips):
        await_(lx.at[peer(chips - d)], lx_r.at[d - 1])
    for i in range(chips):
        gm[_at(i, LANES), :] = lx[i].T
    same = r_i == c_i

    def diag(i):
        d = gm[tile(i)]
        xm[(1, *tile(i))] = jnp.where(same, 1.0 / jnp.where(same, d, 1.0), 0.0)

    _loop(0, n128, diag)
    swapped(2)
    tick(5)
    _loop(0, 3, level_l)
    tick(6)
    wait_blk(0)
    project(sbuf.at[0], ys, 0, top // 2)
    for g in range(2):
        for d in range(1, chips):
            rs_copy(0, g, d).start()
    _loop(3, 7, level_l)
    tick(7)
    level_big(1, lambda w_, i: gm[pl.ds((2 * i + 1) * w_, w_), pl.ds(2 * i * w_, w_)])
    pack_factor(1)
    tick(8)
    fetch_mat(0)
    fetch_mat(1)
    fetch_blk(2)

    wait_mat(0)
    wait_blk(1)
    cm[0, _at(k, hsize)] = jnp.zeros((hsize, size), jnp.float32)
    cross(0, (whole - 1) * STEP, STEP)
    c_copy(0).start()

    def reflect(n):
        j, par, nxt = top - n, n % 2, (n + 1) % 2

        pl.when(n > 0)(lambda: over((j + 1) // 2, functools.partial(apply, n - 1)))

        def factor(gs):
            totals = []
            for g in gs:
                for d in range(1, chips):
                    rs_copy(par, g, d).wait_recv()
                total = sbuf[par, slice_of(g, x)]
                for d in range(1, chips):
                    total = total + rs[g, d - 1]
                totals.append(total)
            got = _dot_nn(jnp.concatenate(totals, axis=0), mbuf[par])
            for i, g in enumerate(gs):
                wb[par, slice_of(g, x)] = got[i * sl : (i + 1) * sl]
                for d in range(1, chips):
                    w_copy(par, g, d).start()

        factor((0,))
        factor((1,))

        for g in range(2):
            for d in range(1, chips):
                rs_copy(par, g, d).wait_send()

        pl.when(n > 0)(lambda: release_blk(n - 1))
        release_mat(n)

        @pl.when(j > 0)
        def _():
            project(sbuf.at[nxt], ys, n + 1, (j - 1) // 2)

        @pl.when(jnp.where(n < 9, par == 0, par == 1))
        def _():
            tick(LEAD + (n + 1) // 2)

        @pl.when(j > 0)
        def _():
            wait_mat(n + 1)
            await_(cm.at[n % 3, _at(1 - k, hsize)], cm_r.at[n % 3])

        def correct(gs):
            for g in gs:
                for d in range(1, chips):
                    await_(wb.at[par, slice_of(g, peer(chips - d))], ex_r.at[g, d - 1])

            @pl.when(j > 0)
            def _():
                sbuf[nxt, cols_in(gs)] = sbuf[nxt, cols_in(gs)] - _dot_nn(wb[par, cols_in(gs)], cm[n % 3])
                for g in gs:
                    for d in range(1, chips):
                        rs_copy(nxt, g, d).start()

        correct((0,))
        pl.when(j > 1)(lambda: cross_all(n + 1))
        correct((1,))

        for g in range(2):
            for d in range(1, chips):
                w_copy(par, g, d).wait_send()

        @pl.when(j > 0)
        def _():
            c_copy(n).wait_send()

    _loop(0, nb, reflect)
    over(0, functools.partial(apply, top))
    release_blk(top)

    xs[...] = jnp.zeros_like(xs)
    def first_half(val):
        return lax.broadcasted_iota(jnp.int32, val.shape, 1) < EDGE


    def take(ref, cols_, j):
        lo = ref[cols_, pl.ds(pl.multiple_of((j // 2) * STEP, LANES), LANES)]
        hi = ref[cols_, pl.ds(pl.multiple_of((j // 2) * STEP + LANES, LANES), LANES)]
        even = j % 2 == 0
        return jnp.where(
            first_half(lo),
            jnp.where(even, lo, pltpu.roll(lo, EDGE, 1)),
            jnp.where(even, pltpu.roll(hi, EDGE, 1), hi),
        )

    def spread(val, j):
        even, first = j % 2 == 0, first_half(val)
        other = pltpu.roll(val, EDGE, 1)
        zero = jnp.zeros_like(val)
        lo = jnp.where(even, jnp.where(first, val, zero), jnp.where(first, zero, other))
        hi = jnp.where(even, jnp.where(first, other, zero), jnp.where(first, zero, val))
        return jnp.concatenate([lo, hi], axis=1)

    def x_copy(par, g, d):
        src = sbuf.at[par, cols_of(g), _at(peer(d), LANES)]
        return remote(src, rx.at[par, g, d - 1], rx_s.at[par, g, d - 1], rx_r.at[par, g, d - 1], at_peer(d))

    def solve_partial(n, gs, j):
        par, cols_ = n % 2, cols_in(gs)
        wb[0, cols_] = -wb[0, cols_]
        wb[0, cols_, _at(x, LANES)] += take(ys, cols_, j)
        sbuf[par, cols_] = _dot_nn(wb[0, cols_], mbuf[par])
        for g in gs:
            for d in range(1, chips):
                x_copy(par, g, d).start()

    def fin_copy(i):
        return remote(
            xs.at[:, _at(2 * i + 1 - k, LANES)], zt.at[k, :, _at(i, LANES)], fin_s.at[i], fin_r.at[i], mate
        )

    def give(i):
        await_(zt.at[1 - k, :, _at(i, LANES)], fin_r.at[i])
        zt[k, :, _at(i, LANES)] = xs[:, _at(2 * i + k, LANES)]
        out_ref[_at(i, LANES), :] = zt[:, :, _at(i, LANES)].reshape(2 * ncol, LANES).T

    for m in range(3):
        _loop(0, pairs, lambda i, m=m: swaps(m, i)[1].wait_send())
    over_v(sent)
    over_l(sent)
    to_mate.wait_send()
    half_to_mate.wait_send()
    for d in range(1, chips):
        r2_copy(d).wait_send()
        ga_copy(d).wait_send()
        lx_copy(d).wait_send()

    wait_blk(nb)
    wait_mat(nb)
    wb[0] = jnp.zeros((ncol, size), jnp.float32)
    for g in range(2):
        solve_partial(nb, (g,), top)
    release_blk(nb)
    release_mat(nb)

    def solve(i):
        n = nb + i
        j, par, nxt = top - i, n % 2, (n + 1) % 2

        @pl.when(j > 0)
        def _():
            wait_blk(n + 1)
            wait_mat(n + 1)
            project(wb.at[0], xs, n + 1, (j + 1) // 2)

        def finish(gs):
            cols_ = cols_in(gs)
            vals = []
            for g in gs:
                for d in range(1, chips):
                    x_copy(par, g, d).wait_recv()
                val = sbuf[par, cols_of(g), _at(x, LANES)]
                for d in range(1, chips):
                    val = val + rx[par, g, d - 1]
                vals.append(val)
            solved = spread(jnp.concatenate(vals, axis=0), j)
            xs[cols_, _at(j // 2, STEP)] += solved

            @pl.when(j > 0)
            def _():
                wb[0, cols_] += _dot_nt(solved, cut(n + 1, (j // 2) * STEP, STEP))
                solve_partial(n + 1, gs, j - 1)

        finish((0,))
        finish((1,))

        pl.when(j % 2 == 0)(lambda: fin_copy(j // 2).start())
        pl.when(jnp.logical_and(j % 2 == 1, j < top))(lambda: give(j // 2 + 1))

        for g in range(2):
            for d in range(1, chips):
                x_copy(par, g, d).wait_send()

        @pl.when(jnp.logical_or(i == 0, i % 2 == 1))
        def _():
            tick(LEAD + 9 + (i + 1) // 2)

        @pl.when(j > 0)
        def _():
            release_blk(n + 1)
            release_mat(n + 1)

    _loop(0, nb, solve)

    give(0)
    _loop(0, pairs, lambda i: fin_copy(i).wait_send())


def solution(mesh):
    rows, cols = mesh.shape["row"], mesh.shape["col"]
    mat_spec = P(("kpt", "row"), "col")
    fac_spec = P("kpt", None, None)

    def local_work(v_loc, t_loc, z_loc, l_loc):
        n_row, n_col = v_loc.shape
        slots, lanes, chips, size = n_col // EDGE, 2 * n_row, rows // 2, rows * EDGE
        nb, ncol = lanes // LANES, z_loc.shape[1] // 2
        pairs, gcol, peers = nb // 2, ncol // 2, max(chips - 1, 1)
        sl, gathers, n128 = gcol // chips, len(_gathers(slots)), size // LANES
        tri = LANES * (n128 * (n128 + 1) // 2)
        dma = pltpu.SemaphoreType.DMA
        hbm, vmem = pl.BlockSpec(memory_space=pl.ANY), pl.BlockSpec(memory_space=pltpu.VMEM)

        def buf(*shape):
            return pltpu.VMEM(shape, jnp.float32)

        col = lax.axis_index("col")
        t_mine = lax.dynamic_slice_in_dim(t_loc, (cols // rows * (col % rows) + col // rows) * rows, rows, axis=0)
        return pl.pallas_call(
            functools.partial(_kernel, (rows, cols, slots, nb, ncol)),
            out_shape=[
                jax.ShapeDtypeStruct(z_loc.shape, jnp.float32),
                jax.ShapeDtypeStruct((2, slots, RING, RING, HALF, lanes), jnp.float32),
            ],
            in_specs=[hbm] * 4,
            out_specs=[vmem, hbm],
            scratch_shapes=[
                buf(2, n_row, n_col),
                buf(2, slots, 2, HALF, n_row),
                buf(2, ncol, n_row),
                buf(rows, EDGE, EDGE),
                buf(2, slots, HALF, lanes),
                buf(ncol, lanes),
                buf(ncol, lanes),
                buf(pairs // 2, rows, EDGE, STEP),
                buf(rows, EDGE, STEP),
                buf(chips, size, LANES),
                buf(size, size),
                buf(size // 2, size),
                buf(size // 4, size),
                buf(peers, size // 4 // chips, size),
                buf(size // 2, size),
                buf(2, EDGE, tri),
                buf(2, RING, RING, EDGE, tri),
                buf(DEEP, rows, EDGE, lanes),
                buf(2, size, size),
                buf(2, ncol, size),
                buf(2, peers, sl, size),
                buf(2, ncol, size),
                buf(3, size, size),
                buf(2, 2, peers, gcol, LANES),
                dma((4,)),
                dma((3, pairs)), dma((3, pairs)), dma((3, pairs)),
                dma((slots, pairs)), dma((pairs // 2, rows, 2)),
                dma((slots, 2)), dma((rows, 2)),
                dma((peers,)), dma((peers,)),
                dma((4,)),
                dma((peers,)), dma((peers,)), dma((peers,)), dma((peers,)),
                dma((pairs,)), dma((pairs,)),
                dma((gathers,)), dma((gathers, 8)), dma((gathers, 8)),
                dma((DEEP, rows)), dma((DEEP, rows)), dma((DEEP, rows)),
                dma((2, n128)), dma((2, n128)), dma((2, n128)),
                pltpu.SemaphoreType.REGULAR((DEEP,)), pltpu.SemaphoreType.REGULAR((2,)),
                dma((2, peers)), dma((2, peers)), dma((2, peers)), dma((2, peers)),
                dma((3,)), dma((3,)),
                dma((2, 2, peers)), dma((2, 2, peers)),
                dma((16,)), dma((16,)),
            ],
            compiler_params=pltpu.CompilerParams(collective_id=0, has_side_effects=True, vmem_limit_bytes=67_043_328),
            name="eigvec",
        )(v_loc, t_mine, z_loc, l_loc)[0]

    return jax.shard_map(local_work, mesh=mesh, in_specs=(mat_spec, fac_spec, mat_spec, mat_spec), out_specs=mat_spec, check_vma=False)
```

```python
import functools

import jax
import jax.numpy as jnp
from jax import lax
from jax.experimental import pallas as pl
from jax.experimental.pallas import tpu as pltpu
from jax.sharding import PartitionSpec as P

PREC_HIGH = lax.Precision.HIGHEST
MESH = pl.DeviceIdType.MESH
EDGE = 64
HALF = EDGE // 2
LANES = 128
STEP = 256
RING = 4
LEAD = 9
DEEP = 3


def _dot_nt(a, b):
    return lax.dot_general(a, b, (((1,), (1,)), ((), ())), precision=PREC_HIGH, preferred_element_type=jnp.float32)


def _dot_nn(a, b):
    return lax.dot_general(a, b, (((1,), (0,)), ((), ())), precision=PREC_HIGH, preferred_element_type=jnp.float32)


def _at(i, n):
    return pl.ds(pl.multiple_of(i * n, n), n)


def _loop(lo, hi, body):
    def one(i, carry):
        body(i)
        return carry

    lax.fori_loop(lo, hi, one, 0)


def _gathers(slots):
    early = [(slots - 1, 0), (slots - 2, 0), None, None, ("m", 0)]
    first = early + [(q, 0) for q in range(slots - 3, -1, -1)]
    rest = [(slots - 1, 1), ("m", 1)] + [(q, 1) for q in range(slots - 2, -1, -1)]
    return first + [None] * (LEAD - len(first)) + rest


def _kernel(dims, v_in, t_in, z_in, l_in, out_ref, gath, *scratch):
    (stage, vt, zt, tb, own, ys, xs, vb, ld, lx, gm, pk, gx, r2, ga, pm, mg, blk, mbuf, sbuf, rs, wb, cm, rx,
     in_sem, swap_l, swap_s, swap_r, v_s, v_r, l_s, l_r, lx_s, lx_r, gx_sem, r2_s, r2_r, ga_s, ga_r, fin_s, fin_r,
     ag_loc, ag_s, ag_r, blk_loc, blk_s, blk_r, mat_loc, mat_s, mat_r, free_b, free_m, rs_s, rs_r, ex_s, ex_r, cm_s, cm_r,
     rx_s, rx_r, eg_s, eg_r) = scratch
    xm = cm
    rows, cols, slots, nb, ncol = dims
    row, col = lax.axis_index("row"), lax.axis_index("col")
    x, k = row // 2, row % 2
    chips, groups = rows // 2, cols // rows
    size, lanes = rows * EDGE, nb * LANES
    hsize, qsize, n128 = size // 2, size // 4, size // LANES
    pairs = nb // 2
    gcol = ncol // 2
    sl = gcol // chips
    mate = {"row": row + 1 - 2 * k, "col": col}
    top, whole = nb - 1, nb // 2
    part, grp = col % rows, col // rows
    k_half, m_half = _at(k, HALF), _at(1 - k, HALF)
    s_a, s_b = 1 + (RING - 1) * k, RING - (RING - 1) * k
    a, b = (col // s_a) % RING, (col // s_b) % RING

    def remote(src, dst, ss, rr, to):
        return pltpu.make_async_remote_copy(src, dst, ss, rr, device_id=to, device_id_type=MESH)

    def await_(ref, sem):
        pltpu.make_async_copy(ref, ref, sem).wait()

    def peer(d):
        return lax.rem(x + d, chips)

    def at_peer(d):
        return {"row": 2 * peer(d) + k, "col": col}

    def plane(da, db):
        return {"row": row, "col": lax.rem(a + da, RING) * s_a + lax.rem(b + db, RING) * s_b}

    def low(q):
        return (groups * q // 2) * STEP

    order = _gathers(slots)

    class Slot:
        def __init__(self, kind, w, n):
            self.kind, self.w, self.n = kind, w, n

        def own(self):
            if self.kind == "m":
                return pm.at[self.w]
            return own.at[self.w, self.kind, :, pl.ds(low(self.kind), lanes - low(self.kind))]

        def piece(self, bb, aa, part=None):
            if self.kind == "m":
                return mg.at[self.w, bb, aa] if part is None else mg.at[self.w, bb, aa, pl.ds(part * HALF, HALF)]
            at = pl.ds(low(self.kind), lanes - low(self.kind))
            e = slice(None) if part is None else pl.ds(part * (HALF // 2), HALF // 2)
            return gath.at[self.w, self.kind, bb, aa, e, at]

        def bundle(self, bb, part=None):
            e = slice(None) if part is None else pl.ds(part * (RING // 2), RING // 2)
            if self.kind == "m":
                return mg.at[self.w, bb, e]
            return gath.at[self.w, self.kind, bb, e, :, pl.ds(low(self.kind), lanes - low(self.kind))]

        def copy(self, i):
            d = 1 if i % 2 == 0 else RING - 1
            back = RING - d
            if i < 2:
                src, dst, to = self.own(), self.piece(b, a), plane(d, 0)
            elif i < 4:
                src = dst = self.piece(b, lax.rem(a + back, RING), i % 2)
                to = plane(d, 0)
            elif i < 6:
                src = dst = self.bundle(b)
                to = plane(0, d)
            else:
                src = dst = self.bundle(lax.rem(b + back, RING), i % 2)
                to = plane(0, d)
            return remote(src, dst, ag_s.at[self.n, i], ag_r.at[self.n, i], to)

        def arrived(self, i):
            back = RING - 1 if i % 2 == 0 else 1
            if i < 2:
                dst = self.piece(b, lax.rem(a + back, RING))
            elif i < 4:
                dst = self.piece(b, lax.rem(a + 2, RING), i % 2)
            elif i < 6:
                dst = self.bundle(lax.rem(b + back, RING))
            else:
                dst = self.bundle(lax.rem(b + 2, RING), i % 2)
            await_(dst, ag_r.at[self.n, i])

        def kept(self):
            return pltpu.make_async_copy(self.own(), self.piece(b, a), ag_loc.at[self.n])

        def stage(self, s):
            if s == 0:
                self.copy(0).start()
                self.copy(1).start()
                self.kept().start()
            elif s == 1:
                for i in range(2):
                    self.arrived(i)
                    self.copy(2 + i).start()
            elif s == 2:
                self.kept().wait()
                self.arrived(2)
                self.arrived(3)
                self.copy(4).start()
                self.copy(5).start()
            elif s == 3:
                for i in range(4, 6):
                    self.arrived(i)
                    self.copy(2 + i).start()
            elif s == 4:
                self.arrived(6)
                self.arrived(7)
            else:
                for i in range(8):
                    self.copy(i).wait_send()

    class Eager(Slot):
        def spot(self, db, da, part=None):
            return self.piece(lax.rem(b + db, RING), lax.rem(a + da, RING), part)

        def copy(self, i):
            back = RING - 1
            db, da, part, to_b, to_a = (
                (0, 0, None, 0, 1), (0, 0, None, 0, back), (0, 0, None, 1, 0), (0, 0, None, back, 0),
                (0, back, 0, 0, 1), (0, 1, 1, 0, back),
                (0, back, None, 1, 0), (0, back, None, back, 0), (0, 1, None, 1, 0), (0, 1, None, back, 0),
                (0, 2, None, 1, 0), (0, 2, None, back, 0),
                (back, 0, None, 1, 0), (back, back, None, 1, 0), (1, 1, None, back, 0), (1, 2, None, back, 0),
            )[i]
            dst = self.spot(db, da, part)
            src = self.own() if db == 0 and da == 0 else dst
            sent_ = remote(src, dst, eg_s.at[i], eg_r.at[i], plane(to_a, to_b))
            return sent_, self.spot(db + RING - to_b, da + RING - to_a, part)

        def go(self, *which):
            for i in which:
                self.copy(i)[0].start()

        def got(self, *which):
            for i in which:
                await_(self.copy(i)[1], eg_r.at[i])

        def stage(self, s):
            if s == 0:
                self.go(0, 1, 2, 3)
                self.kept().start()
            elif s == 1:
                self.got(0)
                self.go(4, 6, 7)
                self.got(1)
                self.go(5, 8, 9)
                self.got(2)
                self.go(12)
            elif s == 2:
                self.got(4, 5)
                self.go(10, 11)
                self.got(6)
                self.go(13)
            elif s == 3:
                self.got(9)
                self.go(14)
                self.got(11)
                self.go(15)
            elif s == 4:
                self.got(3, 7, 8, 10, 12, 13, 14, 15)
                self.kept().wait()
                for i in range(16):
                    self.copy(i)[0].wait_send()

    def tick(t):
        for s in (4, 3, 2, 1, 0, 5):
            n = t - s
            if isinstance(n, int):
                if 0 <= n < len(order) and order[n] is not None:
                    (Eager if order[n] == ("m", 0) else Slot)(*order[n], n).stage(s)
                continue
            for kind in list(range(slots)) + ["m"]:
                at_v, at_l = order.index((kind, 0)), order.index((kind, 1))

                @pl.when(n == at_l if kind == "m" else jnp.logical_or(n == at_v, n == at_l))
                def _(s=s, n=n, kind=kind, at_l=at_l):
                    Slot(kind, jnp.where(n == at_l, 1, 0), n).stage(s)

    def block_of(n):
        j = top - n % nb
        return n // nb, j, j // groups, j % groups, n % 2

    run = min(rows, RING)
    runs = rows // run

    def in_blk(n, q, i, half):
        return blk.at[n % DEEP, pl.ds(i * run, run), half, pl.ds(low(q), lanes - low(q))]

    def from_mate(n, q, i):
        await_(in_blk(n, q, i, m_half), blk_r.at[n % DEEP, i])

    def mat_copies(n, i):
        w, j, q, h, s = block_of(n)
        c = h * rows + q
        src = mg.at[w, (c // s_b) % RING, (c // s_a) % RING, :, pl.ds(LANES * (i * (i + 1) // 2), LANES * (i + 1))]
        dst = mbuf.at[s, pl.ds(pl.multiple_of(i * LANES + k * EDGE, EDGE), EDGE), pl.ds(0, LANES * (i + 1))]
        return (
            pltpu.make_async_copy(src, dst, mat_loc.at[s, i]),
            remote(src, dst, mat_s.at[s, i], mat_r.at[s, i], mate),
        )

    def per_piece(n, act):
        q_now = block_of(n)[2]
        for q in range(slots):

            @pl.when(q_now == q)
            def _(q=q):
                for i in range(runs):
                    act(q, i)

    def fetch_blk(n):
        w, _, _, h, _ = block_of(n)
        s = n % DEEP

        def go(q, i):
            c = h * rows + i * run
            z_now, y_run = c // RING, pl.ds(c % RING, run)
            at = pl.ds(low(q), lanes - low(q))
            dst = in_blk(n, q, i, k_half)

            def both(src):
                pltpu.make_async_copy(src, dst, blk_loc.at[s, i]).start()
                remote(src, dst, blk_s.at[s, i], blk_r.at[s, i], mate).start()

            pl.when(k == 0)(lambda: both(gath.at[w, q, z_now, y_run, :, at]))
            pl.when(k == 1)(lambda: both(gath.at[w, q, y_run, z_now, :, at]))

        per_piece(n, go)

    def fetch_mat(n):
        for i in range(n128):
            for c in mat_copies(n, i):
                c.start()

    def wait_blk(n):
        def one(q, i):
            await_(in_blk(n, q, i, k_half), blk_loc.at[n % DEEP, i])
            from_mate(n, q, i)

        per_piece(n, one)

    def wait_mat(n):
        for i in range(n128):
            mat_copies(n, i)[0].wait()
            there = pl.ds(pl.multiple_of(i * LANES + (1 - k) * EDGE, EDGE), EDGE), pl.ds(0, LANES * (i + 1))
            await_(mbuf.at[(n % 2, *there)], mat_r.at[n % 2, i])

    def release_blk(n):
        per_piece(n, lambda q, i: await_(in_blk(n, q, i, k_half), blk_s.at[n % DEEP, i]))

        @pl.when(n + DEEP < 2 * nb)
        def _():
            pl.semaphore_signal(free_b.at[n % DEEP], inc=1, device_id=mate, device_id_type=MESH)
            pl.semaphore_wait(free_b.at[n % DEEP], 1)
            fetch_blk(n + DEEP)

    def release_mat(n):
        for i in range(n128):
            mat_copies(n, i)[1].wait_send()

        @pl.when(n + 2 < 2 * nb)
        def _():
            pl.semaphore_signal(free_m.at[n % 2], inc=1, device_id=mate, device_id_type=MESH)
            pl.semaphore_wait(free_m.at[n % 2], 1)
            fetch_mat(n + 2)

    def over(first, body):
        pl.when(first % 2 == 1)(lambda: body(first * STEP, STEP))
        _loop((first + 1) // 2, whole // 2, lambda i: body(i * 2 * STEP, 2 * STEP))

    def rows_at(off, width):
        return pl.ds(pl.multiple_of(off, STEP), width)

    def cut(n, off, width):
        return blk[n % DEEP, :, :, rows_at(off, width)].reshape(size, width)

    def project(dst, ref, n, first):
        dst[...] = jnp.zeros((ncol, size), jnp.float32)

        def one(off, width):
            dst[...] += _dot_nt(ref[:, rows_at(off, width)], cut(n, off, width))

        if whole % 4 or isinstance(first, int):
            over(first, one)
            return
        half = (first + 1) // 2
        pl.when(first % 2 == 1)(lambda: one(first * STEP, STEP))
        pl.when(half % 2 == 1)(lambda: one(half * 2 * STEP, 2 * STEP))
        _loop((half + 1) // 2, whole // 4, lambda i: one(i * 4 * STEP, 4 * STEP))

    def slice_of(g, x2):
        return pl.ds(pl.multiple_of(g * gcol + x2 * sl, sl), sl)

    def cols_of(g):
        return pl.ds(g * gcol, gcol)

    def rs_copy(par, g, d):
        return remote(sbuf.at[par, slice_of(g, peer(d))], rs.at[g, d - 1], rs_s.at[g, d - 1], rs_r.at[g, d - 1], at_peer(d))

    def w_copy(par, g, d):
        mine = wb.at[par, slice_of(g, x)]
        return remote(mine, mine, ex_s.at[g, d - 1], ex_r.at[g, d - 1], at_peer(d))

    c_half = pl.ds(pl.multiple_of(k * (rows // 2), rows // 2), rows // 2)

    def c_copy(par):
        return remote(cm.at[par, _at(k, hsize)], cm.at[par, _at(k, hsize)], cm_s.at[par], cm_r.at[par], mate)

    def summed(par, g):
        for d in range(1, chips):
            rs_copy(par, g, d).wait_recv()
        total = sbuf[par, slice_of(g, x)]
        for d in range(1, chips):
            total = total + rs[g, d - 1]
        return total

    def apply(n, off, width):
        ys[:, rows_at(off, width)] = ys[:, rows_at(off, width)] - _dot_nn(wb[n % 2], cut(n, off, width))

    def cross(n, off, width):
        here = blk[n % DEEP, c_half, :, rows_at(off, width)].reshape(hsize, width)
        cm[n % 2, _at(k, hsize)] += _dot_nt(here, cut(n + 1, off, width))

    def cols_in(gs):
        return pl.ds(gs[0] * gcol, len(gs) * gcol)

    barrier = pltpu.get_barrier_semaphore()

    def here_i_am(device):
        pl.semaphore_signal(barrier, inc=1, device_id=device, device_id_type=MESH)

    def group_member(d):
        n = lax.rem(2 * part + k + d, 2 * rows)
        here_i_am({"col": grp * rows + n // 2, "row": 2 * x + n % 2})

    _loop(1, 2 * rows, group_member)
    for d in range(1, chips):
        here_i_am(at_peer(d))
    for d in (1, RING - 1):
        here_i_am(plane(d, 0))
        here_i_am(plane(0, d))

    ins = [
        pltpu.make_async_copy(src, stage.at[i % 2], in_sem.at[i]) for i, src in enumerate((v_in, l_in, z_in))
    ] + [pltpu.make_async_copy(t_in, tb, in_sem.at[3])]
    for i in (0, 1, 3):
        ins[i].start()
    pl.semaphore_wait(barrier, 2 * rows - 1 + chips - 1 + 4)

    def swaps(m, i):
        there = _at(2 * i + k, LANES)
        if m < 2:
            mine, theirs = vt.at[m, :, k, :, _at(i, LANES)], vt.at[m, :, 1 - k, :, _at(i, LANES)]
            dst = own.at[m, :, :, there]
        else:
            mine, theirs = zt.at[k, :, _at(i, LANES)], zt.at[1 - k, :, _at(i, LANES)]
            dst = ys.at[:, there]
        return (
            pltpu.make_async_copy(mine, dst, swap_l.at[m, i]),
            remote(theirs, dst, swap_s.at[m, i], swap_r.at[m, i], mate),
        )

    def arriving(m, i):
        there = _at(2 * i + 1 - k, LANES)
        await_(own.at[m, :, :, there] if m < 2 else ys.at[:, there], swap_r.at[m, i])

    def turn(m, then=None):
        ins[m].wait()

        def one(i):
            block = stage[m % 2, _at(i, LANES), :].T
            if m < 2:
                vt[m, :, :, :, _at(i, LANES)] = block.reshape(slots, 2, HALF, LANES)
            else:
                zt[:, :, _at(i, LANES)] = block.reshape(2, ncol, LANES)
            for c in swaps(m, i):
                c.start()
            if then is not None:
                pl.when(i > 0)(lambda: then(i - 1))

        _loop(0, pairs, one)
        if then is not None:
            then(pairs - 1)

    def swapped(m):
        def one(i):
            swaps(m, i)[0].wait()
            arriving(m, i)

        _loop(0, pairs, one)

    my_q, my_h = part, grp
    my_j = groups * my_q + my_h
    first_t = my_j // 2

    def deal_v(q, t, act):
        to, kk = grp * rows + q, t % 2
        src = own.at[0, q, :, _at(t, STEP)]
        dst = vb.at[t // 2, part, k_half]
        self_ = jnp.logical_and(to == col, k == kk)
        act(
            self_,
            pltpu.make_async_copy(src, dst, v_r.at[t // 2, part, k]),
            remote(src, dst, v_s.at[q, t], v_r.at[t // 2, part, k], {"col": to, "row": 2 * x + kk}),
        )

    def deal_l(q, kk, act):
        to = grp * rows + q
        src = own.at[1, q, :, _at((groups * q + grp) // 2, STEP)]
        dst = ld.at[part, k_half]
        self_ = jnp.logical_and(to == col, k == kk)
        act(
            self_,
            pltpu.make_async_copy(src, dst, l_r.at[part, k]),
            remote(src, dst, l_s.at[q, kk], l_r.at[part, k], {"col": to, "row": 2 * x + kk}),
        )

    def send(self_, here, there):
        pl.when(self_)(here.start)
        pl.when(jnp.logical_not(self_))(there.start)

    def sent(self_, here, there):
        pl.when(jnp.logical_not(self_))(there.wait_send)

    def over_v(act):
        def one(q):
            _loop((groups * q + grp) // 2, pairs, lambda t: deal_v(q, t, act))

        _loop(0, slots, one)

    def over_l(act):
        def one(q):
            deal_l(q, 0, act)
            deal_l(q, 1, act)

        _loop(0, slots, one)

    def deal_chunk(t):
        swaps(0, t)[0].wait()
        arriving(0, t)
        _loop(0, (2 * t + 1 - grp + groups) // groups, lambda q: deal_v(q, t, send))

    turn(0, deal_chunk)
    ins[2].start()
    turn(1)
    swapped(1)
    over_l(send)
    turn(2)
    mbuf[...] = jnp.zeros_like(mbuf)

    gm[...] = jnp.zeros_like(gm)

    def chunk(i):
        def got(n):
            await_(vb.at[i, n // 2, _at(n % 2, HALF)], v_r.at[i, n // 2, n % 2])

        _loop(0, 2 * rows, got)
        all_ = vb[i].reshape(size, STEP)
        gm[pl.ds(0, hsize), pl.ds(0, hsize)] += _dot_nt(all_[:hsize], all_[:hsize])
        gm[pl.ds(hsize, hsize), :] += _dot_nt(all_[hsize:], all_)

    _loop((first_t + 1 - k) // 2, pairs // 2, chunk)
    tick(0)

    widths = []
    w_ = hsize
    while w_ >= EDGE:
        widths.append(w_)
        w_ //= 2

    def packed(w_):
        return pl.ds(size - 2 * w_, w_)

    pk[...] = jnp.zeros_like(pk)
    for w_ in widths:
        for i in range(hsize // w_):
            pk[pl.ds(i * w_, w_), packed(w_)] = gm[pl.ds((2 * i + 1) * w_, w_), pl.ds(2 * i * w_, w_)]

    mine, theirs = _at(k, qsize), _at(1 - k, qsize)
    to_mate = remote(pk.at[theirs], gx, gx_sem.at[0], gx_sem.at[1], mate)
    to_mate.start()
    tick(1)
    to_mate.wait_recv()
    pk[mine] += gx[...]
    rl = qsize // chips

    def r2_copy(d):
        src = pk.at[pl.ds(pl.multiple_of(k * qsize + peer(d) * rl, rl), rl)]
        return remote(src, r2.at[d - 1], r2_s.at[d - 1], r2_r.at[d - 1], at_peer(d))

    for d in range(1, chips):
        r2_copy(d).start()

    def got_l(n):
        await_(ld.at[n // 2, _at(n % 2, HALF)], l_r.at[n // 2, n % 2])

    _loop(0, 2 * rows, got_l)
    ev = my_j % 2 == 0
    lo_half = lax.broadcasted_iota(jnp.int32, (size, LANES), 1) < EDGE
    l_lo, l_hi = ld[:, :, pl.ds(0, LANES)].reshape(size, LANES), ld[:, :, pl.ds(LANES, LANES)].reshape(size, LANES)
    lx[x] = jnp.where(
        lo_half,
        jnp.where(ev, l_lo, pltpu.roll(l_lo, EDGE, 1)),
        jnp.where(ev, pltpu.roll(l_hi, EDGE, 1), l_hi),
    )

    def lx_copy(d):
        return remote(lx.at[x], lx.at[x], lx_s.at[d - 1], lx_r.at[d - 1], at_peer(d))

    tick(2)
    for d in range(1, chips):
        r2_copy(d).wait_recv()
    my_rows = pl.ds(pl.multiple_of(k * qsize + x * rl, rl), rl)
    total = pk[my_rows]
    for d in range(1, chips):
        total = total + r2[d - 1]
    ga[my_rows] = total

    def ga_copy(d):
        return remote(ga.at[my_rows], ga.at[my_rows], ga_s.at[d - 1], ga_r.at[d - 1], at_peer(d))

    for d in range(1, chips):
        ga_copy(d).start()
    for d in range(1, chips):
        lx_copy(d).start()
    tick(3)
    for d in range(1, chips):
        await_(ga.at[pl.ds(pl.multiple_of(k * qsize + peer(chips - d) * rl, rl), rl)], ga_r.at[d - 1])
    half_to_mate = remote(ga.at[mine], ga.at[mine], gx_sem.at[2], gx_sem.at[3], mate)
    half_to_mate.start()

    r_i = lax.broadcasted_iota(jnp.int32, (LANES, LANES), 0)
    c_i = lax.broadcasted_iota(jnp.int32, (LANES, LANES), 1)

    def tile(i):
        return _at(i, LANES), _at(i, LANES)

    def merge_tile(w, i, low_part):
        cur = xm[(w, *tile(i))]
        xm[(w, *tile(i))] = cur - _dot_nn(_dot_nn(cur, low_part), cur)

    def level_l(lev):
        pick = jnp.logical_and(
            lax.shift_right_logical(r_i, lev) % 2 == 1,
            lax.shift_right_logical(c_i, lev) + 1 == lax.shift_right_logical(r_i, lev),
        )
        _loop(0, n128, lambda i: merge_tile(1, i, jnp.where(pick, gm[tile(i)], 0.0)))

    def level_big(w, corner):
        for w_ in reversed(widths[:-1]):
            for i in range(hsize // w_):
                d1 = pl.ds(2 * i * w_, w_)
                d2 = pl.ds((2 * i + 1) * w_, w_)
                xm[w, d2, d1] = -_dot_nn(_dot_nn(xm[w, d2, d2], corner(w_, i)), xm[w, d1, d1])

    def pack_factor(w):
        for i in range(n128):
            pm[w, :, pl.ds(LANES * (i * (i + 1) // 2), LANES * (i + 1))] = xm[
                w, pl.ds(pl.multiple_of(i * LANES + k * EDGE, EDGE), EDGE), pl.ds(0, LANES * (i + 1))
            ]

    xm[...] = jnp.zeros_like(xm)
    ins[3].wait()
    for p in range(0, rows, 2):
        zero = jnp.zeros((EDGE, EDGE), jnp.float32)
        both = jnp.concatenate(
            [jnp.concatenate([tb[p], zero], axis=1), jnp.concatenate([zero, tb[p + 1]], axis=1)], axis=0
        )
        xm[0, pl.ds(p * EDGE, LANES), pl.ds(p * EDGE, LANES)] = both
    await_(ga.at[theirs], gx_sem.at[3])

    def corner64(i):
        block = ga[_at(i, EDGE), packed(EDGE)]
        zero = jnp.zeros((EDGE, EDGE), jnp.float32)
        low_part = jnp.concatenate([block, zero], axis=1)
        merge_tile(0, i, jnp.concatenate([jnp.zeros_like(low_part), low_part], axis=0))

    _loop(0, n128, corner64)
    level_big(0, lambda w_, i: ga[pl.ds(i * w_, w_), packed(w_)])
    pack_factor(0)
    tick(4)

    fetch_blk(0)
    fetch_blk(1)
    for d in range(1, chips):
        await_(lx.at[peer(chips - d)], lx_r.at[d - 1])
    for i in range(chips):
        gm[_at(i, LANES), :] = lx[i].T
    same = r_i == c_i

    def diag(i):
        d = gm[tile(i)]
        xm[(1, *tile(i))] = jnp.where(same, 1.0 / jnp.where(same, d, 1.0), 0.0)

    _loop(0, n128, diag)
    swapped(2)
    tick(5)
    _loop(0, 3, level_l)
    tick(6)
    wait_blk(0)
    project(sbuf.at[0], ys, 0, top // 2)
    for g in range(2):
        for d in range(1, chips):
            rs_copy(0, g, d).start()
    _loop(3, 7, level_l)
    tick(7)
    for g in range(2):
        wb[1, slice_of(g, x)] = summed(0, g)
        for d in range(1, chips):
            w_copy(1, g, d).start()
    level_big(1, lambda w_, i: gm[pl.ds((2 * i + 1) * w_, w_), pl.ds(2 * i * w_, w_)])
    pack_factor(1)
    tick(8)
    fetch_mat(0)
    fetch_mat(1)
    fetch_blk(2)
    for g in range(2):
        for d in range(1, chips):
            await_(wb.at[1, slice_of(g, peer(chips - d))], ex_r.at[g, d - 1])
            w_copy(1, g, d).wait_send()
            rs_copy(0, g, d).wait_send()

    wait_mat(0)
    wb[0] = _dot_nn(wb[1], mbuf[0])

    def reflect(n):
        j, par, nxt = top - n, n % 2, (n + 1) % 2

        @pl.when(j > 0)
        def _():
            wait_blk(n + 1)
            cm[par, _at(k, hsize)] = jnp.zeros((hsize, size), jnp.float32)
            pl.when(j % 2 == 1)(lambda: cross(n, (j // 2) * STEP, STEP))

            def one(off, width):
                apply(n - 1, off, width)
                cross(n, off, width)

            over((j + 1) // 2, one)
            c_copy(par).start()

        pl.when(j == 0)(lambda: over(0, functools.partial(apply, n - 1)))

        def factor(gs):
            got = _dot_nn(jnp.concatenate([summed(par, g) for g in gs], axis=0), mbuf[par])
            for i, g in enumerate(gs):
                wb[par, slice_of(g, x)] = got[i * sl : (i + 1) * sl]
                for d in range(1, chips):
                    w_copy(par, g, d).start()

        @pl.when(jnp.logical_and(n > 0, j >= 7))
        def _():
            factor((0,))
            factor((1,))

        pl.when(jnp.logical_and(n > 0, j < 7))(lambda: factor((0, 1)))

        @pl.when(n > 0)
        def _():
            for g in range(2):
                for d in range(1, chips):
                    rs_copy(par, g, d).wait_send()

        pl.when(n > 0)(lambda: release_blk(n - 1))
        release_mat(n)

        @pl.when(j > 0)
        def _():
            project(sbuf.at[nxt], ys, n + 1, (j - 1) // 2)

        @pl.when(jnp.where(n < 9, par == 0, par == 1))
        def _():
            tick(LEAD + (n + 1) // 2)

        @pl.when(j > 0)
        def _():
            wait_mat(n + 1)
            await_(cm.at[par, _at(1 - k, hsize)], cm_r.at[par])

        def correct(gs):
            @pl.when(n > 0)
            def _():
                for g in gs:
                    for d in range(1, chips):
                        await_(wb.at[par, slice_of(g, peer(chips - d))], ex_r.at[g, d - 1])

            @pl.when(j > 0)
            def _():
                sbuf[nxt, cols_in(gs)] = sbuf[nxt, cols_in(gs)] - _dot_nn(wb[par, cols_in(gs)], cm[par])
                for g in gs:
                    for d in range(1, chips):
                        rs_copy(nxt, g, d).start()

        correct((0,))
        correct((1,))

        @pl.when(n > 0)
        def _():
            for g in range(2):
                for d in range(1, chips):
                    w_copy(par, g, d).wait_send()

        @pl.when(j > 0)
        def _():
            c_copy(par).wait_send()

    _loop(0, nb, reflect)
    over(0, functools.partial(apply, top))
    release_blk(top)

    xs[...] = jnp.zeros_like(xs)
    def first_half(val):
        return lax.broadcasted_iota(jnp.int32, val.shape, 1) < EDGE


    def take(ref, cols_, j):
        lo = ref[cols_, pl.ds(pl.multiple_of((j // 2) * STEP, LANES), LANES)]
        hi = ref[cols_, pl.ds(pl.multiple_of((j // 2) * STEP + LANES, LANES), LANES)]
        even = j % 2 == 0
        return jnp.where(
            first_half(lo),
            jnp.where(even, lo, pltpu.roll(lo, EDGE, 1)),
            jnp.where(even, pltpu.roll(hi, EDGE, 1), hi),
        )

    def spread(val, j):
        even, first = j % 2 == 0, first_half(val)
        other = pltpu.roll(val, EDGE, 1)
        zero = jnp.zeros_like(val)
        lo = jnp.where(even, jnp.where(first, val, zero), jnp.where(first, zero, other))
        hi = jnp.where(even, jnp.where(first, other, zero), jnp.where(first, zero, val))
        return jnp.concatenate([lo, hi], axis=1)

    def x_copy(par, g, d):
        src = sbuf.at[par, cols_of(g), _at(peer(d), LANES)]
        return remote(src, rx.at[par, g, d - 1], rx_s.at[par, g, d - 1], rx_r.at[par, g, d - 1], at_peer(d))

    def solve_partial(n, gs, j):
        par, cols_ = n % 2, cols_in(gs)
        wb[0, cols_] = -wb[0, cols_]
        wb[0, cols_, _at(x, LANES)] += take(ys, cols_, j)
        sbuf[par, cols_] = _dot_nn(wb[0, cols_], mbuf[par])
        for g in gs:
            for d in range(1, chips):
                x_copy(par, g, d).start()

    def fin_copy(i):
        return remote(
            xs.at[:, _at(2 * i + 1 - k, LANES)], zt.at[k, :, _at(i, LANES)], fin_s.at[i], fin_r.at[i], mate
        )

    def give(i):
        await_(zt.at[1 - k, :, _at(i, LANES)], fin_r.at[i])
        zt[k, :, _at(i, LANES)] = xs[:, _at(2 * i + k, LANES)]
        out_ref[_at(i, LANES), :] = zt[:, :, _at(i, LANES)].reshape(2 * ncol, LANES).T

    for m in range(3):
        _loop(0, pairs, lambda i, m=m: swaps(m, i)[1].wait_send())
    over_v(sent)
    over_l(sent)
    to_mate.wait_send()
    half_to_mate.wait_send()
    for d in range(1, chips):
        r2_copy(d).wait_send()
        ga_copy(d).wait_send()
        lx_copy(d).wait_send()

    wait_blk(nb)
    wait_mat(nb)
    wb[0] = jnp.zeros((ncol, size), jnp.float32)
    for g in range(2):
        solve_partial(nb, (g,), top)
    release_blk(nb)
    release_mat(nb)

    def solve(i):
        n = nb + i
        j, par, nxt = top - i, n % 2, (n + 1) % 2

        @pl.when(j > 0)
        def _():
            wait_blk(n + 1)
            wait_mat(n + 1)
            project(wb.at[0], xs, n + 1, (j + 1) // 2)

        def finish(gs):
            cols_ = cols_in(gs)
            vals = []
            for g in gs:
                for d in range(1, chips):
                    x_copy(par, g, d).wait_recv()
                val = sbuf[par, cols_of(g), _at(x, LANES)]
                for d in range(1, chips):
                    val = val + rx[par, g, d - 1]
                vals.append(val)
            solved = spread(jnp.concatenate(vals, axis=0), j)
            xs[cols_, _at(j // 2, STEP)] += solved

            @pl.when(j > 0)
            def _():
                wb[0, cols_] += _dot_nt(solved, cut(n + 1, (j // 2) * STEP, STEP))
                solve_partial(n + 1, gs, j - 1)

        finish((0,))
        finish((1,))

        pl.when(j % 2 == 0)(lambda: fin_copy(j // 2).start())
        pl.when(jnp.logical_and(j % 2 == 1, j < top))(lambda: give(j // 2 + 1))

        for g in range(2):
            for d in range(1, chips):
                x_copy(par, g, d).wait_send()

        @pl.when(jnp.logical_or(i == 0, i % 2 == 1))
        def _():
            tick(LEAD + 9 + (i + 1) // 2)

        @pl.when(j > 0)
        def _():
            release_blk(n + 1)
            release_mat(n + 1)

    _loop(0, nb, solve)

    give(0)
    _loop(0, pairs, lambda i: fin_copy(i).wait_send())


def solution(mesh):
    rows, cols = mesh.shape["row"], mesh.shape["col"]
    mat_spec = P(("kpt", "row"), "col")
    fac_spec = P("kpt", None, None)

    def local_work(v_loc, t_loc, z_loc, l_loc):
        n_row, n_col = v_loc.shape
        slots, lanes, chips, size = n_col // EDGE, 2 * n_row, rows // 2, rows * EDGE
        nb, ncol = lanes // LANES, z_loc.shape[1] // 2
        pairs, gcol, peers = nb // 2, ncol // 2, max(chips - 1, 1)
        sl, gathers, n128 = gcol // chips, len(_gathers(slots)), size // LANES
        tri = LANES * (n128 * (n128 + 1) // 2)
        dma = pltpu.SemaphoreType.DMA
        hbm, vmem = pl.BlockSpec(memory_space=pl.ANY), pl.BlockSpec(memory_space=pltpu.VMEM)

        def buf(*shape):
            return pltpu.VMEM(shape, jnp.float32)

        col = lax.axis_index("col")
        t_mine = lax.dynamic_slice_in_dim(t_loc, (cols // rows * (col % rows) + col // rows) * rows, rows, axis=0)
        return pl.pallas_call(
            functools.partial(_kernel, (rows, cols, slots, nb, ncol)),
            out_shape=[
                jax.ShapeDtypeStruct(z_loc.shape, jnp.float32),
                jax.ShapeDtypeStruct((2, slots, RING, RING, HALF, lanes), jnp.float32),
            ],
            in_specs=[hbm] * 4,
            out_specs=[vmem, hbm],
            scratch_shapes=[
                buf(2, n_row, n_col),
                buf(2, slots, 2, HALF, n_row),
                buf(2, ncol, n_row),
                buf(rows, EDGE, EDGE),
                buf(2, slots, HALF, lanes),
                buf(ncol, lanes),
                buf(ncol, lanes),
                buf(pairs // 2, rows, EDGE, STEP),
                buf(rows, EDGE, STEP),
                buf(chips, size, LANES),
                buf(size, size),
                buf(size // 2, size),
                buf(size // 4, size),
                buf(peers, size // 4 // chips, size),
                buf(size // 2, size),
                buf(2, EDGE, tri),
                buf(2, RING, RING, EDGE, tri),
                buf(DEEP, rows, EDGE, lanes),
                buf(2, size, size),
                buf(2, ncol, size),
                buf(2, peers, sl, size),
                buf(2, ncol, size),
                buf(2, size, size),
                buf(2, 2, peers, gcol, LANES),
                dma((4,)),
                dma((3, pairs)), dma((3, pairs)), dma((3, pairs)),
                dma((slots, pairs)), dma((pairs // 2, rows, 2)),
                dma((slots, 2)), dma((rows, 2)),
                dma((peers,)), dma((peers,)),
                dma((4,)),
                dma((peers,)), dma((peers,)), dma((peers,)), dma((peers,)),
                dma((pairs,)), dma((pairs,)),
                dma((gathers,)), dma((gathers, 8)), dma((gathers, 8)),
                dma((DEEP, rows)), dma((DEEP, rows)), dma((DEEP, rows)),
                dma((2, n128)), dma((2, n128)), dma((2, n128)),
                pltpu.SemaphoreType.REGULAR((DEEP,)), pltpu.SemaphoreType.REGULAR((2,)),
                dma((2, peers)), dma((2, peers)), dma((2, peers)), dma((2, peers)),
                dma((2,)), dma((2,)),
                dma((2, 2, peers)), dma((2, 2, peers)),
                dma((16,)), dma((16,)),
            ],
            compiler_params=pltpu.CompilerParams(collective_id=0, has_side_effects=True, vmem_limit_bytes=67_043_328),
            name="eigvec",
        )(v_loc, t_mine, z_loc, l_loc)[0]

    return jax.shard_map(local_work, mesh=mesh, in_specs=(mat_spec, fac_spec, mat_spec, mat_spec), out_specs=mat_spec, check_vma=False)
```

```python
import functools

import jax
import jax.numpy as jnp
from jax import lax
from jax.experimental import pallas as pl
from jax.experimental.pallas import tpu as pltpu
from jax.sharding import PartitionSpec as P

PREC_HIGH = lax.Precision.HIGHEST
MESH = pl.DeviceIdType.MESH
EDGE = 64
HALF = EDGE // 2
LANES = 128
STEP = 256
RING = 4
LEAD = 9
DEEP = 3


def _dot_nt(a, b):
    return lax.dot_general(a, b, (((1,), (1,)), ((), ())), precision=PREC_HIGH, preferred_element_type=jnp.float32)


def _dot_nn(a, b):
    return lax.dot_general(a, b, (((1,), (0,)), ((), ())), precision=PREC_HIGH, preferred_element_type=jnp.float32)


def _at(i, n):
    return pl.ds(pl.multiple_of(i * n, n), n)


def _loop(lo, hi, body):
    def one(i, carry):
        body(i)
        return carry

    lax.fori_loop(lo, hi, one, 0)


def _gathers(slots):
    early = [(slots - 1, 0), (slots - 2, 0), None, None, ("m", 0), None]
    first = early + [(q, 0) for q in range(slots - 3, -1, -1)]
    rest = [(slots - 1, 1), ("m", 1)] + [(q, 1) for q in range(slots - 2, -1, -1)]
    return first + [None] * (LEAD - len(first)) + rest


def _kernel(dims, v_in, t_in, z_in, l_in, out_ref, gath, *scratch):
    (stage, vt, zt, tb, own, ys, xs, vb, ld, lx, gm, pk, gx, r2, ga, pm, mg, blk, mbuf, sbuf, rs, wb, cm, rx,
     in_sem, swap_l, swap_s, swap_r, v_s, v_r, l_s, l_r, lx_s, lx_r, gx_sem, r2_s, r2_r, ga_s, ga_r, fin_s, fin_r,
     ag_loc, ag_s, ag_r, blk_loc, blk_s, blk_r, mat_loc, mat_s, mat_r, free_b, free_m, rs_s, rs_r, ex_s, ex_r, cm_s, cm_r,
     rx_s, rx_r, eg_s, eg_r) = scratch
    xm = cm
    rows, cols, slots, nb, ncol = dims
    row, col = lax.axis_index("row"), lax.axis_index("col")
    x, k = row // 2, row % 2
    chips, groups = rows // 2, cols // rows
    size, lanes = rows * EDGE, nb * LANES
    hsize, qsize, n128 = size // 2, size // 4, size // LANES
    pairs = nb // 2
    gcol = ncol // 2
    sl = gcol // chips
    mate = {"row": row + 1 - 2 * k, "col": col}
    top, whole = nb - 1, nb // 2
    part, grp = col % rows, col // rows
    k_half, m_half = _at(k, HALF), _at(1 - k, HALF)
    s_a, s_b = 1 + (RING - 1) * k, RING - (RING - 1) * k
    a, b = (col // s_a) % RING, (col // s_b) % RING

    def remote(src, dst, ss, rr, to):
        return pltpu.make_async_remote_copy(src, dst, ss, rr, device_id=to, device_id_type=MESH)

    def await_(ref, sem):
        pltpu.make_async_copy(ref, ref, sem).wait()

    def peer(d):
        return lax.rem(x + d, chips)

    def at_peer(d):
        return {"row": 2 * peer(d) + k, "col": col}

    def plane(da, db):
        return {"row": row, "col": lax.rem(a + da, RING) * s_a + lax.rem(b + db, RING) * s_b}

    def low(q):
        return (groups * q // 2) * STEP

    order = _gathers(slots)

    class Slot:
        def __init__(self, kind, w, n):
            self.kind, self.w, self.n = kind, w, n

        def own(self):
            if self.kind == "m":
                return pm.at[self.w]
            return own.at[self.w, self.kind, :, pl.ds(low(self.kind), lanes - low(self.kind))]

        def piece(self, bb, aa, part=None):
            if self.kind == "m":
                return mg.at[self.w, bb, aa] if part is None else mg.at[self.w, bb, aa, pl.ds(part * HALF, HALF)]
            at = pl.ds(low(self.kind), lanes - low(self.kind))
            e = slice(None) if part is None else pl.ds(part * (HALF // 2), HALF // 2)
            return gath.at[self.w, self.kind, bb, aa, e, at]

        def bundle(self, bb, part=None):
            e = slice(None) if part is None else pl.ds(part * (RING // 2), RING // 2)
            if self.kind == "m":
                return mg.at[self.w, bb, e]
            return gath.at[self.w, self.kind, bb, e, :, pl.ds(low(self.kind), lanes - low(self.kind))]

        def copy(self, i):
            d = 1 if i % 2 == 0 else RING - 1
            back = RING - d
            if i < 2:
                src, dst, to = self.own(), self.piece(b, a), plane(d, 0)
            elif i < 4:
                src = dst = self.piece(b, lax.rem(a + back, RING), i % 2)
                to = plane(d, 0)
            elif i < 6:
                src = dst = self.bundle(b)
                to = plane(0, d)
            else:
                src = dst = self.bundle(lax.rem(b + back, RING), i % 2)
                to = plane(0, d)
            return remote(src, dst, ag_s.at[self.n, i], ag_r.at[self.n, i], to)

        def arrived(self, i):
            back = RING - 1 if i % 2 == 0 else 1
            if i < 2:
                dst = self.piece(b, lax.rem(a + back, RING))
            elif i < 4:
                dst = self.piece(b, lax.rem(a + 2, RING), i % 2)
            elif i < 6:
                dst = self.bundle(lax.rem(b + back, RING))
            else:
                dst = self.bundle(lax.rem(b + 2, RING), i % 2)
            await_(dst, ag_r.at[self.n, i])

        def kept(self):
            return pltpu.make_async_copy(self.own(), self.piece(b, a), ag_loc.at[self.n])

        def stage(self, s):
            if s == 0:
                self.copy(0).start()
                self.copy(1).start()
                self.kept().start()
            elif s == 1:
                for i in range(2):
                    self.arrived(i)
                    self.copy(2 + i).start()
            elif s == 2:
                self.kept().wait()
                self.arrived(2)
                self.arrived(3)
                self.copy(4).start()
                self.copy(5).start()
            elif s == 3:
                for i in range(4, 6):
                    self.arrived(i)
                    self.copy(2 + i).start()
            elif s == 4:
                self.arrived(6)
                self.arrived(7)
            else:
                for i in range(8):
                    self.copy(i).wait_send()

    class Eager(Slot):
        def spot(self, db, da, part=None):
            return self.piece(lax.rem(b + db, RING), lax.rem(a + da, RING), part)

        def copy(self, i):
            back = RING - 1
            db, da, part, to_b, to_a = (
                (0, 0, None, 0, 1), (0, 0, None, 0, back), (0, 0, None, 1, 0), (0, 0, None, back, 0),
                (0, back, 0, 0, 1), (0, 1, 1, 0, back),
                (0, back, None, 1, 0), (0, back, None, back, 0), (0, 1, None, 1, 0), (0, 1, None, back, 0),
                (0, 2, None, 1, 0), (0, 2, None, back, 0),
                (back, 0, None, 1, 0), (back, back, None, 1, 0), (1, 1, None, back, 0), (1, 2, None, back, 0),
            )[i]
            dst = self.spot(db, da, part)
            src = self.own() if db == 0 and da == 0 else dst
            sent_ = remote(src, dst, eg_s.at[i], eg_r.at[i], plane(to_a, to_b))
            return sent_, self.spot(db + RING - to_b, da + RING - to_a, part)

        def go(self, *which):
            for i in which:
                self.copy(i)[0].start()

        def got(self, *which):
            for i in which:
                await_(self.copy(i)[1], eg_r.at[i])

        def stage(self, s):
            if s == 0:
                self.go(0, 1, 2, 3)
                self.kept().start()
            elif s == 1:
                self.got(0)
                self.go(4, 6, 7)
                self.got(1)
                self.go(5, 8, 9)
                self.got(2)
                self.go(12)
            elif s == 2:
                self.got(4, 5)
                self.go(10, 11)
                self.got(6)
                self.go(13)
            elif s == 3:
                self.got(9)
                self.go(14)
                self.got(11)
                self.go(15)
            elif s == 4:
                self.got(3, 7, 8, 10, 12, 13, 14, 15)
                self.kept().wait()
                for i in range(16):
                    self.copy(i)[0].wait_send()

    def tick(t):
        for s in (4, 3, 2, 1, 0, 5):
            n = t - s
            if isinstance(n, int):
                if 0 <= n < len(order) and order[n] is not None:
                    (Eager if order[n] == ("m", 0) else Slot)(*order[n], n).stage(s)
                continue
            for kind in list(range(slots)) + ["m"]:
                at_v, at_l = order.index((kind, 0)), order.index((kind, 1))

                @pl.when(n == at_l if kind == "m" else jnp.logical_or(n == at_v, n == at_l))
                def _(s=s, n=n, kind=kind, at_l=at_l):
                    Slot(kind, jnp.where(n == at_l, 1, 0), n).stage(s)

    def block_of(n):
        j = top - n % nb
        return n // nb, j, j // groups, j % groups, n % 2

    run = min(rows, RING)
    runs = rows // run

    def in_blk(n, q, i, half):
        return blk.at[n % DEEP, pl.ds(i * run, run), half, pl.ds(low(q), lanes - low(q))]

    def from_mate(n, q, i):
        await_(in_blk(n, q, i, m_half), blk_r.at[n % DEEP, i])

    def mat_copies(n, i):
        w, j, q, h, s = block_of(n)
        c = h * rows + q
        src = mg.at[w, (c // s_b) % RING, (c // s_a) % RING, :, pl.ds(LANES * (i * (i + 1) // 2), LANES * (i + 1))]
        dst = mbuf.at[s, pl.ds(pl.multiple_of(i * LANES + k * EDGE, EDGE), EDGE), pl.ds(0, LANES * (i + 1))]
        return (
            pltpu.make_async_copy(src, dst, mat_loc.at[s, i]),
            remote(src, dst, mat_s.at[s, i], mat_r.at[s, i], mate),
        )

    def per_piece(n, act):
        q_now = block_of(n)[2]
        for q in range(slots):

            @pl.when(q_now == q)
            def _(q=q):
                for i in range(runs):
                    act(q, i)

    def fetch_blk(n):
        w, _, _, h, _ = block_of(n)
        s = n % DEEP

        def go(q, i):
            c = h * rows + i * run
            z_now, y_run = c // RING, pl.ds(c % RING, run)
            at = pl.ds(low(q), lanes - low(q))
            dst = in_blk(n, q, i, k_half)

            def both(src):
                pltpu.make_async_copy(src, dst, blk_loc.at[s, i]).start()
                remote(src, dst, blk_s.at[s, i], blk_r.at[s, i], mate).start()

            pl.when(k == 0)(lambda: both(gath.at[w, q, z_now, y_run, :, at]))
            pl.when(k == 1)(lambda: both(gath.at[w, q, y_run, z_now, :, at]))

        per_piece(n, go)

    def fetch_mat(n):
        for i in range(n128):
            for c in mat_copies(n, i):
                c.start()

    def wait_blk(n):
        def one(q, i):
            await_(in_blk(n, q, i, k_half), blk_loc.at[n % DEEP, i])
            from_mate(n, q, i)

        per_piece(n, one)

    def wait_mat(n):
        for i in range(n128):
            mat_copies(n, i)[0].wait()
            there = pl.ds(pl.multiple_of(i * LANES + (1 - k) * EDGE, EDGE), EDGE), pl.ds(0, LANES * (i + 1))
            await_(mbuf.at[(n % 2, *there)], mat_r.at[n % 2, i])

    def release_blk(n):
        per_piece(n, lambda q, i: await_(in_blk(n, q, i, k_half), blk_s.at[n % DEEP, i]))

        @pl.when(n + DEEP < 2 * nb)
        def _():
            pl.semaphore_signal(free_b.at[n % DEEP], inc=1, device_id=mate, device_id_type=MESH)
            pl.semaphore_wait(free_b.at[n % DEEP], 1)
            fetch_blk(n + DEEP)

    def release_mat(n):
        for i in range(n128):
            mat_copies(n, i)[1].wait_send()

        @pl.when(n + 2 < 2 * nb)
        def _():
            pl.semaphore_signal(free_m.at[n % 2], inc=1, device_id=mate, device_id_type=MESH)
            pl.semaphore_wait(free_m.at[n % 2], 1)
            fetch_mat(n + 2)

    def over(first, body):
        pl.when(first % 2 == 1)(lambda: body(first * STEP, STEP))
        _loop((first + 1) // 2, whole // 2, lambda i: body(i * 2 * STEP, 2 * STEP))

    def rows_at(off, width):
        return pl.ds(pl.multiple_of(off, STEP), width)

    def cut(n, off, width):
        return blk[n % DEEP, :, :, rows_at(off, width)].reshape(size, width)

    def project(dst, ref, n, first):
        dst[...] = jnp.zeros((ncol, size), jnp.float32)

        def one(off, width):
            dst[...] += _dot_nt(ref[:, rows_at(off, width)], cut(n, off, width))

        if whole % 4 or isinstance(first, int):
            over(first, one)
            return
        half = (first + 1) // 2
        pl.when(first % 2 == 1)(lambda: one(first * STEP, STEP))
        pl.when(half % 2 == 1)(lambda: one(half * 2 * STEP, 2 * STEP))
        _loop((half + 1) // 2, whole // 4, lambda i: one(i * 4 * STEP, 4 * STEP))

    def slice_of(g, x2):
        return pl.ds(pl.multiple_of(g * gcol + x2 * sl, sl), sl)

    def cols_of(g):
        return pl.ds(g * gcol, gcol)

    def rs_copy(par, g, d):
        return remote(sbuf.at[par, slice_of(g, peer(d))], rs.at[g, d - 1], rs_s.at[g, d - 1], rs_r.at[g, d - 1], at_peer(d))

    def w_copy(par, g, d):
        mine = wb.at[par, slice_of(g, x)]
        return remote(mine, mine, ex_s.at[g, d - 1], ex_r.at[g, d - 1], at_peer(d))

    c_half = pl.ds(pl.multiple_of(k * (rows // 2), rows // 2), rows // 2)

    def c_copy(par):
        return remote(cm.at[par, _at(k, hsize)], cm.at[par, _at(k, hsize)], cm_s.at[par], cm_r.at[par], mate)

    def summed(par, g):
        for d in range(1, chips):
            rs_copy(par, g, d).wait_recv()
        total = sbuf[par, slice_of(g, x)]
        for d in range(1, chips):
            total = total + rs[g, d - 1]
        return total

    def apply(n, off, width):
        ys[:, rows_at(off, width)] = ys[:, rows_at(off, width)] - _dot_nn(wb[n % 2], cut(n, off, width))

    def cross(n, off, width):
        here = blk[n % DEEP, c_half, :, rows_at(off, width)].reshape(hsize, width)
        cm[n % 2, _at(k, hsize)] += _dot_nt(here, cut(n + 1, off, width))

    def cols_in(gs):
        return pl.ds(gs[0] * gcol, len(gs) * gcol)

    barrier = pltpu.get_barrier_semaphore()

    def here_i_am(device):
        pl.semaphore_signal(barrier, inc=1, device_id=device, device_id_type=MESH)

    def group_member(d):
        n = lax.rem(2 * part + k + d, 2 * rows)
        here_i_am({"col": grp * rows + n // 2, "row": 2 * x + n % 2})

    _loop(1, 2 * rows, group_member)
    for d in range(1, chips):
        here_i_am(at_peer(d))
    for d in (1, RING - 1):
        here_i_am(plane(d, 0))
        here_i_am(plane(0, d))

    ins = [
        pltpu.make_async_copy(src, stage.at[i % 2], in_sem.at[i]) for i, src in enumerate((v_in, l_in, z_in))
    ] + [pltpu.make_async_copy(t_in, tb, in_sem.at[3])]
    for i in (0, 1, 3):
        ins[i].start()
    pl.semaphore_wait(barrier, 2 * rows - 1 + chips - 1 + 4)

    def swaps(m, i):
        there = _at(2 * i + k, LANES)
        if m < 2:
            mine, theirs = vt.at[m, :, k, :, _at(i, LANES)], vt.at[m, :, 1 - k, :, _at(i, LANES)]
            dst = own.at[m, :, :, there]
        else:
            mine, theirs = zt.at[k, :, _at(i, LANES)], zt.at[1 - k, :, _at(i, LANES)]
            dst = ys.at[:, there]
        return (
            pltpu.make_async_copy(mine, dst, swap_l.at[m, i]),
            remote(theirs, dst, swap_s.at[m, i], swap_r.at[m, i], mate),
        )

    def arriving(m, i):
        there = _at(2 * i + 1 - k, LANES)
        await_(own.at[m, :, :, there] if m < 2 else ys.at[:, there], swap_r.at[m, i])

    def turn(m, then=None):
        ins[m].wait()

        def one(i):
            block = stage[m % 2, _at(i, LANES), :].T
            if m < 2:
                vt[m, :, :, :, _at(i, LANES)] = block.reshape(slots, 2, HALF, LANES)
            else:
                zt[:, :, _at(i, LANES)] = block.reshape(2, ncol, LANES)
            for c in swaps(m, i):
                c.start()
            if then is not None:
                pl.when(i > 0)(lambda: then(i - 1))

        _loop(0, pairs, one)
        if then is not None:
            then(pairs - 1)

    def swapped(m):
        def one(i):
            swaps(m, i)[0].wait()
            arriving(m, i)

        _loop(0, pairs, one)

    my_q, my_h = part, grp
    my_j = groups * my_q + my_h
    first_t = my_j // 2

    def deal_v(q, t, act):
        to, kk = grp * rows + q, t % 2
        src = own.at[0, q, :, _at(t, STEP)]
        dst = vb.at[t // 2, part, k_half]
        self_ = jnp.logical_and(to == col, k == kk)
        act(
            self_,
            pltpu.make_async_copy(src, dst, v_r.at[t // 2, part, k]),
            remote(src, dst, v_s.at[q, t], v_r.at[t // 2, part, k], {"col": to, "row": 2 * x + kk}),
        )

    def deal_l(q, kk, act):
        to = grp * rows + q
        src = own.at[1, q, :, _at((groups * q + grp) // 2, STEP)]
        dst = ld.at[part, k_half]
        self_ = jnp.logical_and(to == col, k == kk)
        act(
            self_,
            pltpu.make_async_copy(src, dst, l_r.at[part, k]),
            remote(src, dst, l_s.at[q, kk], l_r.at[part, k], {"col": to, "row": 2 * x + kk}),
        )

    def send(self_, here, there):
        pl.when(self_)(here.start)
        pl.when(jnp.logical_not(self_))(there.start)

    def sent(self_, here, there):
        pl.when(jnp.logical_not(self_))(there.wait_send)

    def over_v(act):
        def one(q):
            _loop((groups * q + grp) // 2, pairs, lambda t: deal_v(q, t, act))

        _loop(0, slots, one)

    def over_l(act):
        def one(q):
            deal_l(q, 0, act)
            deal_l(q, 1, act)

        _loop(0, slots, one)

    def deal_chunk(t):
        swaps(0, t)[0].wait()
        arriving(0, t)
        _loop(0, (2 * t + 1 - grp + groups) // groups, lambda q: deal_v(q, t, send))

    turn(0, deal_chunk)
    ins[2].start()
    turn(1)
    swapped(1)
    over_l(send)
    turn(2)
    mbuf[...] = jnp.zeros_like(mbuf)

    gm[...] = jnp.zeros_like(gm)

    def chunk(i):
        def got(n):
            await_(vb.at[i, n // 2, _at(n % 2, HALF)], v_r.at[i, n // 2, n % 2])

        _loop(0, 2 * rows, got)
        all_ = vb[i].reshape(size, STEP)
        gm[pl.ds(0, hsize), pl.ds(0, hsize)] += _dot_nt(all_[:hsize], all_[:hsize])
        gm[pl.ds(hsize, hsize), :] += _dot_nt(all_[hsize:], all_)

    _loop((first_t + 1 - k) // 2, pairs // 2, chunk)
    tick(0)

    widths = []
    w_ = hsize
    while w_ >= EDGE:
        widths.append(w_)
        w_ //= 2

    def packed(w_):
        return pl.ds(size - 2 * w_, w_)

    pk[...] = jnp.zeros_like(pk)
    for w_ in widths:
        for i in range(hsize // w_):
            pk[pl.ds(i * w_, w_), packed(w_)] = gm[pl.ds((2 * i + 1) * w_, w_), pl.ds(2 * i * w_, w_)]

    mine, theirs = _at(k, qsize), _at(1 - k, qsize)
    to_mate = remote(pk.at[theirs], gx, gx_sem.at[0], gx_sem.at[1], mate)
    to_mate.start()
    tick(1)
    to_mate.wait_recv()
    pk[mine] += gx[...]
    rl = qsize // chips

    def r2_copy(d):
        src = pk.at[pl.ds(pl.multiple_of(k * qsize + peer(d) * rl, rl), rl)]
        return remote(src, r2.at[d - 1], r2_s.at[d - 1], r2_r.at[d - 1], at_peer(d))

    for d in range(1, chips):
        r2_copy(d).start()

    def got_l(n):
        await_(ld.at[n // 2, _at(n % 2, HALF)], l_r.at[n // 2, n % 2])

    _loop(0, 2 * rows, got_l)
    ev = my_j % 2 == 0
    lo_half = lax.broadcasted_iota(jnp.int32, (size, LANES), 1) < EDGE
    l_lo, l_hi = ld[:, :, pl.ds(0, LANES)].reshape(size, LANES), ld[:, :, pl.ds(LANES, LANES)].reshape(size, LANES)
    lx[x] = jnp.where(
        lo_half,
        jnp.where(ev, l_lo, pltpu.roll(l_lo, EDGE, 1)),
        jnp.where(ev, pltpu.roll(l_hi, EDGE, 1), l_hi),
    )

    def lx_copy(d):
        return remote(lx.at[x], lx.at[x], lx_s.at[d - 1], lx_r.at[d - 1], at_peer(d))

    tick(2)
    for d in range(1, chips):
        r2_copy(d).wait_recv()
    my_rows = pl.ds(pl.multiple_of(k * qsize + x * rl, rl), rl)
    total = pk[my_rows]
    for d in range(1, chips):
        total = total + r2[d - 1]
    ga[my_rows] = total

    def ga_copy(d):
        return remote(ga.at[my_rows], ga.at[my_rows], ga_s.at[d - 1], ga_r.at[d - 1], at_peer(d))

    for d in range(1, chips):
        ga_copy(d).start()
    for d in range(1, chips):
        lx_copy(d).start()
    tick(3)
    for d in range(1, chips):
        await_(ga.at[pl.ds(pl.multiple_of(k * qsize + peer(chips - d) * rl, rl), rl)], ga_r.at[d - 1])
    half_to_mate = remote(ga.at[mine], ga.at[mine], gx_sem.at[2], gx_sem.at[3], mate)
    half_to_mate.start()

    r_i = lax.broadcasted_iota(jnp.int32, (LANES, LANES), 0)
    c_i = lax.broadcasted_iota(jnp.int32, (LANES, LANES), 1)

    def tile(i):
        return _at(i, LANES), _at(i, LANES)

    def merge_tile(w, i, low_part):
        cur = xm[(w, *tile(i))]
        xm[(w, *tile(i))] = cur - _dot_nn(_dot_nn(cur, low_part), cur)

    def level_l(lev):
        pick = jnp.logical_and(
            lax.shift_right_logical(r_i, lev) % 2 == 1,
            lax.shift_right_logical(c_i, lev) + 1 == lax.shift_right_logical(r_i, lev),
        )
        _loop(0, n128, lambda i: merge_tile(1, i, jnp.where(pick, gm[tile(i)], 0.0)))

    def level_big(w, corner):
        for w_ in reversed(widths[:-1]):
            for i in range(hsize // w_):
                d1 = pl.ds(2 * i * w_, w_)
                d2 = pl.ds((2 * i + 1) * w_, w_)
                xm[w, d2, d1] = -_dot_nn(_dot_nn(xm[w, d2, d2], corner(w_, i)), xm[w, d1, d1])

    def pack_factor(w):
        for i in range(n128):
            pm[w, :, pl.ds(LANES * (i * (i + 1) // 2), LANES * (i + 1))] = xm[
                w, pl.ds(pl.multiple_of(i * LANES + k * EDGE, EDGE), EDGE), pl.ds(0, LANES * (i + 1))
            ]

    xm[...] = jnp.zeros_like(xm)
    ins[3].wait()
    for p in range(0, rows, 2):
        zero = jnp.zeros((EDGE, EDGE), jnp.float32)
        both = jnp.concatenate(
            [jnp.concatenate([tb[p], zero], axis=1), jnp.concatenate([zero, tb[p + 1]], axis=1)], axis=0
        )
        xm[0, pl.ds(p * EDGE, LANES), pl.ds(p * EDGE, LANES)] = both
    await_(ga.at[theirs], gx_sem.at[3])

    def corner64(i):
        block = ga[_at(i, EDGE), packed(EDGE)]
        zero = jnp.zeros((EDGE, EDGE), jnp.float32)
        low_part = jnp.concatenate([block, zero], axis=1)
        merge_tile(0, i, jnp.concatenate([jnp.zeros_like(low_part), low_part], axis=0))

    _loop(0, n128, corner64)
    level_big(0, lambda w_, i: ga[pl.ds(i * w_, w_), packed(w_)])
    pack_factor(0)
    tick(4)

    fetch_blk(0)
    fetch_blk(1)
    for d in range(1, chips):
        await_(lx.at[peer(chips - d)], lx_r.at[d - 1])
    for i in range(chips):
        gm[_at(i, LANES), :] = lx[i].T
    same = r_i == c_i

    def diag(i):
        d = gm[tile(i)]
        xm[(1, *tile(i))] = jnp.where(same, 1.0 / jnp.where(same, d, 1.0), 0.0)

    _loop(0, n128, diag)
    swapped(2)
    tick(5)
    _loop(0, 3, level_l)
    tick(6)
    wait_blk(0)
    project(sbuf.at[0], ys, 0, top // 2)
    for g in range(2):
        for d in range(1, chips):
            rs_copy(0, g, d).start()
    _loop(3, 7, level_l)
    tick(7)
    for g in range(2):
        wb[1, slice_of(g, x)] = summed(0, g)
        for d in range(1, chips):
            w_copy(1, g, d).start()
    level_big(1, lambda w_, i: gm[pl.ds((2 * i + 1) * w_, w_), pl.ds(2 * i * w_, w_)])
    pack_factor(1)
    tick(8)
    fetch_mat(0)
    fetch_mat(1)
    fetch_blk(2)
    for g in range(2):
        for d in range(1, chips):
            await_(wb.at[1, slice_of(g, peer(chips - d))], ex_r.at[g, d - 1])
            w_copy(1, g, d).wait_send()
            rs_copy(0, g, d).wait_send()

    wait_mat(0)
    wb[0] = _dot_nn(wb[1], mbuf[0])

    def reflect(n):
        j, par, nxt = top - n, n % 2, (n + 1) % 2

        @pl.when(j > 0)
        def _():
            wait_blk(n + 1)
            cm[par, _at(k, hsize)] = jnp.zeros((hsize, size), jnp.float32)
            pl.when(j % 2 == 1)(lambda: cross(n, (j // 2) * STEP, STEP))

            def one(off, width):
                apply(n - 1, off, width)
                cross(n, off, width)

            over((j + 1) // 2, one)
            c_copy(par).start()

        pl.when(j == 0)(lambda: over(0, functools.partial(apply, n - 1)))

        def factor(gs):
            got = _dot_nn(jnp.concatenate([summed(par, g) for g in gs], axis=0), mbuf[par])
            for i, g in enumerate(gs):
                wb[par, slice_of(g, x)] = got[i * sl : (i + 1) * sl]
                for d in range(1, chips):
                    w_copy(par, g, d).start()

        @pl.when(jnp.logical_and(n > 0, j >= 7))
        def _():
            factor((0,))
            factor((1,))

        pl.when(jnp.logical_and(n > 0, j < 7))(lambda: factor((0, 1)))

        @pl.when(n > 0)
        def _():
            for g in range(2):
                for d in range(1, chips):
                    rs_copy(par, g, d).wait_send()

        pl.when(n > 0)(lambda: release_blk(n - 1))
        release_mat(n)

        @pl.when(j > 0)
        def _():
            project(sbuf.at[nxt], ys, n + 1, (j - 1) // 2)

        @pl.when(jnp.logical_or(par == 1, jnp.logical_or(n == 0, n == 12)))
        def _():
            tick(LEAD + (n + 1) // 2 + jnp.where(n >= 12, 1, 0))

        @pl.when(j > 0)
        def _():
            wait_mat(n + 1)
            await_(cm.at[par, _at(1 - k, hsize)], cm_r.at[par])

        def correct(gs):
            @pl.when(n > 0)
            def _():
                for g in gs:
                    for d in range(1, chips):
                        await_(wb.at[par, slice_of(g, peer(chips - d))], ex_r.at[g, d - 1])

            @pl.when(j > 0)
            def _():
                sbuf[nxt, cols_in(gs)] = sbuf[nxt, cols_in(gs)] - _dot_nn(wb[par, cols_in(gs)], cm[par])
                for g in gs:
                    for d in range(1, chips):
                        rs_copy(nxt, g, d).start()

        correct((0,))
        correct((1,))

        @pl.when(n > 0)
        def _():
            for g in range(2):
                for d in range(1, chips):
                    w_copy(par, g, d).wait_send()

        @pl.when(j > 0)
        def _():
            c_copy(par).wait_send()

    _loop(0, nb, reflect)
    over(0, functools.partial(apply, top))
    release_blk(top)

    xs[...] = jnp.zeros_like(xs)
    def first_half(val):
        return lax.broadcasted_iota(jnp.int32, val.shape, 1) < EDGE


    def take(ref, cols_, j):
        lo = ref[cols_, pl.ds(pl.multiple_of((j // 2) * STEP, LANES), LANES)]
        hi = ref[cols_, pl.ds(pl.multiple_of((j // 2) * STEP + LANES, LANES), LANES)]
        even = j % 2 == 0
        return jnp.where(
            first_half(lo),
            jnp.where(even, lo, pltpu.roll(lo, EDGE, 1)),
            jnp.where(even, pltpu.roll(hi, EDGE, 1), hi),
        )

    def spread(val, j):
        even, first = j % 2 == 0, first_half(val)
        other = pltpu.roll(val, EDGE, 1)
        zero = jnp.zeros_like(val)
        lo = jnp.where(even, jnp.where(first, val, zero), jnp.where(first, zero, other))
        hi = jnp.where(even, jnp.where(first, other, zero), jnp.where(first, zero, val))
        return jnp.concatenate([lo, hi], axis=1)

    def x_copy(par, g, d):
        src = sbuf.at[par, cols_of(g), _at(peer(d), LANES)]
        return remote(src, rx.at[par, g, d - 1], rx_s.at[par, g, d - 1], rx_r.at[par, g, d - 1], at_peer(d))

    def solve_partial(n, gs, j):
        par, cols_ = n % 2, cols_in(gs)
        wb[0, cols_] = -wb[0, cols_]
        wb[0, cols_, _at(x, LANES)] += take(ys, cols_, j)
        sbuf[par, cols_] = _dot_nn(wb[0, cols_], mbuf[par])
        for g in gs:
            for d in range(1, chips):
                x_copy(par, g, d).start()

    def fin_copy(i):
        return remote(
            xs.at[:, _at(2 * i + 1 - k, LANES)], zt.at[k, :, _at(i, LANES)], fin_s.at[i], fin_r.at[i], mate
        )

    def give(i):
        await_(zt.at[1 - k, :, _at(i, LANES)], fin_r.at[i])
        zt[k, :, _at(i, LANES)] = xs[:, _at(2 * i + k, LANES)]
        out_ref[_at(i, LANES), :] = zt[:, :, _at(i, LANES)].reshape(2 * ncol, LANES).T

    for m in range(3):
        _loop(0, pairs, lambda i, m=m: swaps(m, i)[1].wait_send())
    over_v(sent)
    over_l(sent)
    to_mate.wait_send()
    half_to_mate.wait_send()
    for d in range(1, chips):
        r2_copy(d).wait_send()
        ga_copy(d).wait_send()
        lx_copy(d).wait_send()

    wait_blk(nb)
    wait_mat(nb)
    wb[0] = jnp.zeros((ncol, size), jnp.float32)
    for g in range(2):
        solve_partial(nb, (g,), top)
    release_blk(nb)
    release_mat(nb)

    def solve(i):
        n = nb + i
        j, par, nxt = top - i, n % 2, (n + 1) % 2

        @pl.when(j > 0)
        def _():
            wait_blk(n + 1)
            wait_mat(n + 1)
            project(wb.at[0], xs, n + 1, (j + 1) // 2)

        def finish(gs):
            cols_ = cols_in(gs)
            vals = []
            for g in gs:
                for d in range(1, chips):
                    x_copy(par, g, d).wait_recv()
                val = sbuf[par, cols_of(g), _at(x, LANES)]
                for d in range(1, chips):
                    val = val + rx[par, g, d - 1]
                vals.append(val)
            solved = spread(jnp.concatenate(vals, axis=0), j)
            xs[cols_, _at(j // 2, STEP)] += solved

            @pl.when(j > 0)
            def _():
                wb[0, cols_] += _dot_nt(solved, cut(n + 1, (j // 2) * STEP, STEP))
                solve_partial(n + 1, gs, j - 1)

        finish((0,))
        finish((1,))

        pl.when(j % 2 == 0)(lambda: fin_copy(j // 2).start())
        pl.when(jnp.logical_and(j % 2 == 1, j < top))(lambda: give(j // 2 + 1))

        for g in range(2):
            for d in range(1, chips):
                x_copy(par, g, d).wait_send()

        @pl.when(jnp.logical_or(i == 0, i % 2 == 1))
        def _():
            tick(LEAD + 10 + (i + 1) // 2)

        @pl.when(j > 0)
        def _():
            release_blk(n + 1)
            release_mat(n + 1)

    _loop(0, nb, solve)

    give(0)
    _loop(0, pairs, lambda i: fin_copy(i).wait_send())


def solution(mesh):
    rows, cols = mesh.shape["row"], mesh.shape["col"]
    mat_spec = P(("kpt", "row"), "col")
    fac_spec = P("kpt", None, None)

    def local_work(v_loc, t_loc, z_loc, l_loc):
        n_row, n_col = v_loc.shape
        slots, lanes, chips, size = n_col // EDGE, 2 * n_row, rows // 2, rows * EDGE
        nb, ncol = lanes // LANES, z_loc.shape[1] // 2
        pairs, gcol, peers = nb // 2, ncol // 2, max(chips - 1, 1)
        sl, gathers, n128 = gcol // chips, len(_gathers(slots)), size // LANES
        tri = LANES * (n128 * (n128 + 1) // 2)
        dma = pltpu.SemaphoreType.DMA
        hbm, vmem = pl.BlockSpec(memory_space=pl.ANY), pl.BlockSpec(memory_space=pltpu.VMEM)

        def buf(*shape):
            return pltpu.VMEM(shape, jnp.float32)

        col = lax.axis_index("col")
        t_mine = lax.dynamic_slice_in_dim(t_loc, (cols // rows * (col % rows) + col // rows) * rows, rows, axis=0)
        return pl.pallas_call(
            functools.partial(_kernel, (rows, cols, slots, nb, ncol)),
            out_shape=[
                jax.ShapeDtypeStruct(z_loc.shape, jnp.float32),
                jax.ShapeDtypeStruct((2, slots, RING, RING, HALF, lanes), jnp.float32),
            ],
            in_specs=[hbm] * 4,
            out_specs=[vmem, hbm],
            scratch_shapes=[
                buf(2, n_row, n_col),
                buf(2, slots, 2, HALF, n_row),
                buf(2, ncol, n_row),
                buf(rows, EDGE, EDGE),
                buf(2, slots, HALF, lanes),
                buf(ncol, lanes),
                buf(ncol, lanes),
                buf(pairs // 2, rows, EDGE, STEP),
                buf(rows, EDGE, STEP),
                buf(chips, size, LANES),
                buf(size, size),
                buf(size // 2, size),
                buf(size // 4, size),
                buf(peers, size // 4 // chips, size),
                buf(size // 2, size),
                buf(2, EDGE, tri),
                buf(2, RING, RING, EDGE, tri),
                buf(DEEP, rows, EDGE, lanes),
                buf(2, size, size),
                buf(2, ncol, size),
                buf(2, peers, sl, size),
                buf(2, ncol, size),
                buf(2, size, size),
                buf(2, 2, peers, gcol, LANES),
                dma((4,)),
                dma((3, pairs)), dma((3, pairs)), dma((3, pairs)),
                dma((slots, pairs)), dma((pairs // 2, rows, 2)),
                dma((slots, 2)), dma((rows, 2)),
                dma((peers,)), dma((peers,)),
                dma((4,)),
                dma((peers,)), dma((peers,)), dma((peers,)), dma((peers,)),
                dma((pairs,)), dma((pairs,)),
                dma((gathers,)), dma((gathers, 8)), dma((gathers, 8)),
                dma((DEEP, rows)), dma((DEEP, rows)), dma((DEEP, rows)),
                dma((2, n128)), dma((2, n128)), dma((2, n128)),
                pltpu.SemaphoreType.REGULAR((DEEP,)), pltpu.SemaphoreType.REGULAR((2,)),
                dma((2, peers)), dma((2, peers)), dma((2, peers)), dma((2, peers)),
                dma((2,)), dma((2,)),
                dma((2, 2, peers)), dma((2, 2, peers)),
                dma((16,)), dma((16,)),
            ],
            compiler_params=pltpu.CompilerParams(collective_id=0, has_side_effects=True, vmem_limit_bytes=67_043_328),
            name="eigvec",
        )(v_loc, t_mine, z_loc, l_loc)[0]

    return jax.shard_map(local_work, mesh=mesh, in_specs=(mat_spec, fac_spec, mat_spec, mat_spec), out_specs=mat_spec, check_vma=False)
```

```python
import functools

import jax
import jax.numpy as jnp
from jax import lax
from jax.experimental import pallas as pl
from jax.experimental.pallas import tpu as pltpu
from jax.sharding import PartitionSpec as P

PREC_HIGH = lax.Precision.HIGHEST
MESH = pl.DeviceIdType.MESH
EDGE = 64
HALF = EDGE // 2
LANES = 128
STEP = 256
RING = 4
LEAD = 9
DEEP = 3


def _dot_nt(a, b):
    return lax.dot_general(a, b, (((1,), (1,)), ((), ())), precision=PREC_HIGH, preferred_element_type=jnp.float32)


def _dot_nn(a, b):
    return lax.dot_general(a, b, (((1,), (0,)), ((), ())), precision=PREC_HIGH, preferred_element_type=jnp.float32)


def _at(i, n):
    return pl.ds(pl.multiple_of(i * n, n), n)


def _loop(lo, hi, body):
    def one(i, carry):
        body(i)
        return carry

    lax.fori_loop(lo, hi, one, 0)


def _gathers(slots):
    early = [(slots - 1, 0), (slots - 2, 0), None, None, ("m", 0), None]
    first = early + [(q, 0) for q in range(slots - 3, -1, -1)]
    rest = [(slots - 1, 1), ("m", 1)] + [(q, 1) for q in range(slots - 2, -1, -1)]
    return first + [None] * (LEAD - len(first)) + rest


def _kernel(dims, v_in, t_in, z_in, l_in, out_ref, gath, *scratch):
    (stage, vt, zt, tb, own, ys, xs, vb, ld, lx, gm, pk, gx, r2, ga, pm, mg, blk, mbuf, sbuf, rs, wb, cm, rx,
     in_sem, swap_l, swap_s, swap_r, v_s, v_r, l_s, l_r, lx_s, lx_r, gx_sem, r2_s, r2_r, ga_s, ga_r, fin_s, fin_r,
     ag_loc, ag_s, ag_r, blk_loc, blk_s, blk_r, mat_loc, mat_s, mat_r, free_b, free_m, rs_s, rs_r, ex_s, ex_r, cm_s, cm_r,
     rx_s, rx_r, eg_s, eg_r) = scratch
    xm = cm
    rows, cols, slots, nb, ncol = dims
    row, col = lax.axis_index("row"), lax.axis_index("col")
    x, k = row // 2, row % 2
    chips, groups = rows // 2, cols // rows
    size, lanes = rows * EDGE, nb * LANES
    hsize, qsize, n128 = size // 2, size // 4, size // LANES
    pairs = nb // 2
    gcol = ncol // 2
    sl = gcol // chips
    mate = {"row": row + 1 - 2 * k, "col": col}
    top, whole = nb - 1, nb // 2
    part, grp = col % rows, col // rows
    k_half, m_half = _at(k, HALF), _at(1 - k, HALF)
    s_a, s_b = 1 + (RING - 1) * k, RING - (RING - 1) * k
    a, b = (col // s_a) % RING, (col // s_b) % RING

    def remote(src, dst, ss, rr, to):
        return pltpu.make_async_remote_copy(src, dst, ss, rr, device_id=to, device_id_type=MESH)

    def await_(ref, sem):
        pltpu.make_async_copy(ref, ref, sem).wait()

    def peer(d):
        return lax.rem(x + d, chips)

    def at_peer(d):
        return {"row": 2 * peer(d) + k, "col": col}

    def plane(da, db):
        return {"row": row, "col": lax.rem(a + da, RING) * s_a + lax.rem(b + db, RING) * s_b}

    def low(q):
        return (groups * q // 2) * STEP

    order = _gathers(slots)

    class Slot:
        def __init__(self, kind, w, n):
            self.kind, self.w, self.n = kind, w, n

        def own(self):
            if self.kind == "m":
                return pm.at[self.w]
            return own.at[self.w, self.kind, :, pl.ds(low(self.kind), lanes - low(self.kind))]

        def piece(self, bb, aa, part=None):
            if self.kind == "m":
                return mg.at[self.w, bb, aa] if part is None else mg.at[self.w, bb, aa, pl.ds(part * HALF, HALF)]
            at = pl.ds(low(self.kind), lanes - low(self.kind))
            e = slice(None) if part is None else pl.ds(part * (HALF // 2), HALF // 2)
            return gath.at[self.w, self.kind, bb, aa, e, at]

        def bundle(self, bb, part=None):
            e = slice(None) if part is None else pl.ds(part * (RING // 2), RING // 2)
            if self.kind == "m":
                return mg.at[self.w, bb, e]
            return gath.at[self.w, self.kind, bb, e, :, pl.ds(low(self.kind), lanes - low(self.kind))]

        def copy(self, i):
            d = 1 if i % 2 == 0 else RING - 1
            back = RING - d
            if i < 2:
                src, dst, to = self.own(), self.piece(b, a), plane(d, 0)
            elif i < 4:
                src = dst = self.piece(b, lax.rem(a + back, RING), i % 2)
                to = plane(d, 0)
            elif i < 6:
                src = dst = self.bundle(b)
                to = plane(0, d)
            else:
                src = dst = self.bundle(lax.rem(b + back, RING), i % 2)
                to = plane(0, d)
            return remote(src, dst, ag_s.at[self.n, i], ag_r.at[self.n, i], to)

        def arrived(self, i):
            back = RING - 1 if i % 2 == 0 else 1
            if i < 2:
                dst = self.piece(b, lax.rem(a + back, RING))
            elif i < 4:
                dst = self.piece(b, lax.rem(a + 2, RING), i % 2)
            elif i < 6:
                dst = self.bundle(lax.rem(b + back, RING))
            else:
                dst = self.bundle(lax.rem(b + 2, RING), i % 2)
            await_(dst, ag_r.at[self.n, i])

        def kept(self):
            return pltpu.make_async_copy(self.own(), self.piece(b, a), ag_loc.at[self.n])

        def stage(self, s):
            if s == 0:
                self.copy(0).start()
                self.copy(1).start()
                self.kept().start()
            elif s == 1:
                for i in range(2):
                    self.arrived(i)
                    self.copy(2 + i).start()
            elif s == 2:
                self.kept().wait()
                self.arrived(2)
                self.arrived(3)
                self.copy(4).start()
                self.copy(5).start()
            elif s == 3:
                for i in range(4, 6):
                    self.arrived(i)
                    self.copy(2 + i).start()
            elif s == 4:
                self.arrived(6)
                self.arrived(7)
            else:
                for i in range(8):
                    self.copy(i).wait_send()

    class Eager(Slot):
        def spot(self, db, da, part=None):
            return self.piece(lax.rem(b + db, RING), lax.rem(a + da, RING), part)

        def copy(self, i):
            back = RING - 1
            db, da, part, to_b, to_a = (
                (0, 0, None, 0, 1), (0, 0, None, 0, back), (0, 0, None, 1, 0), (0, 0, None, back, 0),
                (0, back, 0, 0, 1), (0, 1, 1, 0, back),
                (0, back, None, 1, 0), (0, back, None, back, 0), (0, 1, None, 1, 0), (0, 1, None, back, 0),
                (0, 2, None, 1, 0), (0, 2, None, back, 0),
                (back, 0, None, 1, 0), (back, back, None, 1, 0), (1, 1, None, back, 0), (1, 2, None, back, 0),
            )[i]
            dst = self.spot(db, da, part)
            src = self.own() if db == 0 and da == 0 else dst
            sent_ = remote(src, dst, eg_s.at[i], eg_r.at[i], plane(to_a, to_b))
            return sent_, self.spot(db + RING - to_b, da + RING - to_a, part)

        def go(self, *which):
            for i in which:
                self.copy(i)[0].start()

        def got(self, *which):
            for i in which:
                await_(self.copy(i)[1], eg_r.at[i])

        def stage(self, s):
            if s == 0:
                self.go(0, 1, 2, 3)
                self.kept().start()
            elif s == 1:
                self.got(0)
                self.go(4, 6, 7)
                self.got(1)
                self.go(5, 8, 9)
                self.got(2)
                self.go(12)
            elif s == 2:
                self.got(4, 5)
                self.go(10, 11)
                self.got(6)
                self.go(13)
            elif s == 3:
                self.got(9)
                self.go(14)
                self.got(11)
                self.go(15)
            elif s == 4:
                self.got(3, 7, 8, 10, 12, 13, 14, 15)
                self.kept().wait()
                for i in range(16):
                    self.copy(i)[0].wait_send()

    def tick(t):
        for s in (4, 3, 2, 1, 0, 5):
            n = t - s
            if isinstance(n, int):
                if 0 <= n < len(order) and order[n] is not None:
                    (Eager if order[n] == ("m", 0) else Slot)(*order[n], n).stage(s)
                continue
            for kind in list(range(slots)) + ["m"]:
                at_v, at_l = order.index((kind, 0)), order.index((kind, 1))

                @pl.when(n == at_l if kind == "m" else jnp.logical_or(n == at_v, n == at_l))
                def _(s=s, n=n, kind=kind, at_l=at_l):
                    Slot(kind, jnp.where(n == at_l, 1, 0), n).stage(s)

    def block_of(n):
        j = top - n % nb
        return n // nb, j, j // groups, j % groups, n % 2

    run = min(rows, RING)
    runs = rows // run

    def in_blk(n, q, i, half):
        return blk.at[n % DEEP, pl.ds(i * run, run), half, pl.ds(low(q), lanes - low(q))]

    def from_mate(n, q, i):
        await_(in_blk(n, q, i, m_half), blk_r.at[n % DEEP, i])

    def mat_copies(n, i):
        w, j, q, h, s = block_of(n)
        c = h * rows + q
        src = mg.at[w, (c // s_b) % RING, (c // s_a) % RING, :, pl.ds(LANES * (i * (i + 1) // 2), LANES * (i + 1))]
        dst = mbuf.at[s, pl.ds(pl.multiple_of(i * LANES + k * EDGE, EDGE), EDGE), pl.ds(0, LANES * (i + 1))]
        return (
            pltpu.make_async_copy(src, dst, mat_loc.at[s, i]),
            remote(src, dst, mat_s.at[s, i], mat_r.at[s, i], mate),
        )

    def per_piece(n, act):
        q_now = block_of(n)[2]
        for q in range(slots):

            @pl.when(q_now == q)
            def _(q=q):
                for i in range(runs):
                    act(q, i)

    def fetch_blk(n):
        w, _, _, h, _ = block_of(n)
        s = n % DEEP

        def go(q, i):
            c = h * rows + i * run
            z_now, y_run = c // RING, pl.ds(c % RING, run)
            at = pl.ds(low(q), lanes - low(q))
            dst = in_blk(n, q, i, k_half)

            def both(src):
                pltpu.make_async_copy(src, dst, blk_loc.at[s, i]).start()
                remote(src, dst, blk_s.at[s, i], blk_r.at[s, i], mate).start()

            pl.when(k == 0)(lambda: both(gath.at[w, q, z_now, y_run, :, at]))
            pl.when(k == 1)(lambda: both(gath.at[w, q, y_run, z_now, :, at]))

        per_piece(n, go)

    def fetch_mat(n):
        for i in range(n128):
            for c in mat_copies(n, i):
                c.start()

    def wait_blk(n):
        def one(q, i):
            await_(in_blk(n, q, i, k_half), blk_loc.at[n % DEEP, i])
            from_mate(n, q, i)

        per_piece(n, one)

    def wait_mat(n):
        for i in range(n128):
            mat_copies(n, i)[0].wait()
            there = pl.ds(pl.multiple_of(i * LANES + (1 - k) * EDGE, EDGE), EDGE), pl.ds(0, LANES * (i + 1))
            await_(mbuf.at[(n % 2, *there)], mat_r.at[n % 2, i])

    def release_blk(n):
        per_piece(n, lambda q, i: await_(in_blk(n, q, i, k_half), blk_s.at[n % DEEP, i]))

        @pl.when(n + DEEP < 2 * nb)
        def _():
            pl.semaphore_signal(free_b.at[n % DEEP], inc=1, device_id=mate, device_id_type=MESH)
            pl.semaphore_wait(free_b.at[n % DEEP], 1)
            fetch_blk(n + DEEP)

    def release_mat(n):
        for i in range(n128):
            mat_copies(n, i)[1].wait_send()

        @pl.when(n + 2 < 2 * nb)
        def _():
            pl.semaphore_signal(free_m.at[n % 2], inc=1, device_id=mate, device_id_type=MESH)
            pl.semaphore_wait(free_m.at[n % 2], 1)
            fetch_mat(n + 2)

    def over(first, body):
        pl.when(first % 2 == 1)(lambda: body(first * STEP, STEP))
        _loop((first + 1) // 2, whole // 2, lambda i: body(i * 2 * STEP, 2 * STEP))

    def rows_at(off, width):
        return pl.ds(pl.multiple_of(off, STEP), width)

    def cut(n, off, width):
        return blk[n % DEEP, :, :, rows_at(off, width)].reshape(size, width)

    def project(dst, ref, n, first):
        dst[...] = jnp.zeros((ncol, size), jnp.float32)

        def one(off, width):
            dst[...] += _dot_nt(ref[:, rows_at(off, width)], cut(n, off, width))

        if whole % 4 or isinstance(first, int):
            over(first, one)
            return
        half = (first + 1) // 2
        pl.when(first % 2 == 1)(lambda: one(first * STEP, STEP))
        pl.when(half % 2 == 1)(lambda: one(half * 2 * STEP, 2 * STEP))
        _loop((half + 1) // 2, whole // 4, lambda i: one(i * 4 * STEP, 4 * STEP))

    def slice_of(g, x2):
        return pl.ds(pl.multiple_of(g * gcol + x2 * sl, sl), sl)

    def cols_of(g):
        return pl.ds(g * gcol, gcol)

    def rs_copy(par, g, d):
        return remote(sbuf.at[par, slice_of(g, peer(d))], rs.at[g, d - 1], rs_s.at[g, d - 1], rs_r.at[g, d - 1], at_peer(d))

    def w_copy(par, g, d):
        mine = wb.at[par, slice_of(g, x)]
        return remote(mine, mine, ex_s.at[g, d - 1], ex_r.at[g, d - 1], at_peer(d))

    c_half = pl.ds(pl.multiple_of(k * (rows // 2), rows // 2), rows // 2)

    def c_copy(par):
        return remote(cm.at[par, _at(k, hsize)], cm.at[par, _at(k, hsize)], cm_s.at[par], cm_r.at[par], mate)

    def summed(par, g):
        for d in range(1, chips):
            rs_copy(par, g, d).wait_recv()
        total = sbuf[par, slice_of(g, x)]
        for d in range(1, chips):
            total = total + rs[g, d - 1]
        return total

    def apply(n, off, width):
        ys[:, rows_at(off, width)] = ys[:, rows_at(off, width)] - _dot_nn(wb[n % 2], cut(n, off, width))

    def cross(n, off, width):
        here = blk[n % DEEP, c_half, :, rows_at(off, width)].reshape(hsize, width)
        cm[n % 2, _at(k, hsize)] += _dot_nt(here, cut(n + 1, off, width))

    def cols_in(gs):
        return pl.ds(gs[0] * gcol, len(gs) * gcol)

    barrier = pltpu.get_barrier_semaphore()

    def here_i_am(device):
        pl.semaphore_signal(barrier, inc=1, device_id=device, device_id_type=MESH)

    def group_member(d):
        n = lax.rem(2 * part + k + d, 2 * rows)
        here_i_am({"col": grp * rows + n // 2, "row": 2 * x + n % 2})

    _loop(1, 2 * rows, group_member)
    for d in range(1, chips):
        here_i_am(at_peer(d))
    for d in (1, RING - 1):
        here_i_am(plane(d, 0))
        here_i_am(plane(0, d))

    ins = [
        pltpu.make_async_copy(src, stage.at[i % 2], in_sem.at[i]) for i, src in enumerate((v_in, l_in, z_in))
    ] + [pltpu.make_async_copy(t_in, tb, in_sem.at[3])]
    for i in (0, 1, 3):
        ins[i].start()
    pl.semaphore_wait(barrier, 2 * rows - 1 + chips - 1 + 4)

    def swaps(m, i):
        there = _at(2 * i + k, LANES)
        if m < 2:
            mine, theirs = vt.at[m, :, k, :, _at(i, LANES)], vt.at[m, :, 1 - k, :, _at(i, LANES)]
            dst = own.at[m, :, :, there]
        else:
            mine, theirs = zt.at[k, :, _at(i, LANES)], zt.at[1 - k, :, _at(i, LANES)]
            dst = ys.at[:, there]
        return (
            pltpu.make_async_copy(mine, dst, swap_l.at[m, i]),
            remote(theirs, dst, swap_s.at[m, i], swap_r.at[m, i], mate),
        )

    def arriving(m, i):
        there = _at(2 * i + 1 - k, LANES)
        await_(own.at[m, :, :, there] if m < 2 else ys.at[:, there], swap_r.at[m, i])

    def turn(m, then=None):
        ins[m].wait()

        def one(i):
            block = stage[m % 2, _at(i, LANES), :].T
            if m < 2:
                vt[m, :, :, :, _at(i, LANES)] = block.reshape(slots, 2, HALF, LANES)
            else:
                zt[:, :, _at(i, LANES)] = block.reshape(2, ncol, LANES)
            for c in swaps(m, i):
                c.start()
            if then is not None:
                pl.when(i > 0)(lambda: then(i - 1))

        _loop(0, pairs, one)
        if then is not None:
            then(pairs - 1)

    def swapped(m):
        def one(i):
            swaps(m, i)[0].wait()
            arriving(m, i)

        _loop(0, pairs, one)

    my_q, my_h = part, grp
    my_j = groups * my_q + my_h
    first_t = my_j // 2

    def deal_v(q, t, act):
        to, kk = grp * rows + q, t % 2
        src = own.at[0, q, :, _at(t, STEP)]
        dst = vb.at[t // 2, part, k_half]
        self_ = jnp.logical_and(to == col, k == kk)
        act(
            self_,
            pltpu.make_async_copy(src, dst, v_r.at[t // 2, part, k]),
            remote(src, dst, v_s.at[q, t], v_r.at[t // 2, part, k], {"col": to, "row": 2 * x + kk}),
        )

    def deal_l(q, kk, act):
        to = grp * rows + q
        src = own.at[1, q, :, _at((groups * q + grp) // 2, STEP)]
        dst = ld.at[part, k_half]
        self_ = jnp.logical_and(to == col, k == kk)
        act(
            self_,
            pltpu.make_async_copy(src, dst, l_r.at[part, k]),
            remote(src, dst, l_s.at[q, kk], l_r.at[part, k], {"col": to, "row": 2 * x + kk}),
        )

    def send(self_, here, there):
        pl.when(self_)(here.start)
        pl.when(jnp.logical_not(self_))(there.start)

    def sent(self_, here, there):
        pl.when(jnp.logical_not(self_))(there.wait_send)

    def over_v(act):
        def one(q):
            _loop((groups * q + grp) // 2, pairs, lambda t: deal_v(q, t, act))

        _loop(0, slots, one)

    def over_l(act):
        def one(q):
            deal_l(q, 0, act)
            deal_l(q, 1, act)

        _loop(0, slots, one)

    def deal_chunk(t):
        swaps(0, t)[0].wait()
        arriving(0, t)
        _loop(0, (2 * t + 1 - grp + groups) // groups, lambda q: deal_v(q, t, send))

    turn(0, deal_chunk)
    ins[2].start()
    turn(1)
    swapped(1)
    over_l(send)
    turn(2)
    mbuf[...] = jnp.zeros_like(mbuf)

    gm[...] = jnp.zeros_like(gm)

    def chunk(i):
        def got(n):
            await_(vb.at[i, n // 2, _at(n % 2, HALF)], v_r.at[i, n // 2, n % 2])

        _loop(0, 2 * rows, got)
        all_ = vb[i].reshape(size, STEP)
        gm[pl.ds(0, hsize), pl.ds(0, hsize)] += _dot_nt(all_[:hsize], all_[:hsize])
        gm[pl.ds(hsize, hsize), :] += _dot_nt(all_[hsize:], all_)

    _loop((first_t + 1 - k) // 2, pairs // 2, chunk)
    tick(0)

    widths = []
    w_ = hsize
    while w_ >= EDGE:
        widths.append(w_)
        w_ //= 2

    def packed(w_):
        return pl.ds(size - 2 * w_, w_)

    pk[...] = jnp.zeros_like(pk)
    for w_ in widths:
        for i in range(hsize // w_):
            pk[pl.ds(i * w_, w_), packed(w_)] = gm[pl.ds((2 * i + 1) * w_, w_), pl.ds(2 * i * w_, w_)]

    mine, theirs = _at(k, qsize), _at(1 - k, qsize)
    to_mate = remote(pk.at[theirs], gx, gx_sem.at[0], gx_sem.at[1], mate)
    to_mate.start()
    tick(1)
    to_mate.wait_recv()
    pk[mine] += gx[...]
    rl = qsize // chips

    def r2_copy(d):
        src = pk.at[pl.ds(pl.multiple_of(k * qsize + peer(d) * rl, rl), rl)]
        return remote(src, r2.at[d - 1], r2_s.at[d - 1], r2_r.at[d - 1], at_peer(d))

    for d in range(1, chips):
        r2_copy(d).start()

    def got_l(n):
        await_(ld.at[n // 2, _at(n % 2, HALF)], l_r.at[n // 2, n % 2])

    _loop(0, 2 * rows, got_l)
    ev = my_j % 2 == 0
    lo_half = lax.broadcasted_iota(jnp.int32, (size, LANES), 1) < EDGE
    l_lo, l_hi = ld[:, :, pl.ds(0, LANES)].reshape(size, LANES), ld[:, :, pl.ds(LANES, LANES)].reshape(size, LANES)
    lx[x] = jnp.where(
        lo_half,
        jnp.where(ev, l_lo, pltpu.roll(l_lo, EDGE, 1)),
        jnp.where(ev, pltpu.roll(l_hi, EDGE, 1), l_hi),
    )

    def lx_copy(d):
        return remote(lx.at[x], lx.at[x], lx_s.at[d - 1], lx_r.at[d - 1], at_peer(d))

    tick(2)
    for d in range(1, chips):
        r2_copy(d).wait_recv()
    my_rows = pl.ds(pl.multiple_of(k * qsize + x * rl, rl), rl)
    total = pk[my_rows]
    for d in range(1, chips):
        total = total + r2[d - 1]
    ga[my_rows] = total

    def ga_copy(d):
        return remote(ga.at[my_rows], ga.at[my_rows], ga_s.at[d - 1], ga_r.at[d - 1], at_peer(d))

    for d in range(1, chips):
        ga_copy(d).start()
    for d in range(1, chips):
        lx_copy(d).start()
    tick(3)
    for d in range(1, chips):
        await_(ga.at[pl.ds(pl.multiple_of(k * qsize + peer(chips - d) * rl, rl), rl)], ga_r.at[d - 1])
    half_to_mate = remote(ga.at[mine], ga.at[mine], gx_sem.at[2], gx_sem.at[3], mate)
    half_to_mate.start()

    r_i = lax.broadcasted_iota(jnp.int32, (LANES, LANES), 0)
    c_i = lax.broadcasted_iota(jnp.int32, (LANES, LANES), 1)

    def tile(i):
        return _at(i, LANES), _at(i, LANES)

    def merge_tile(w, i, low_part):
        cur = xm[(w, *tile(i))]
        xm[(w, *tile(i))] = cur - _dot_nn(_dot_nn(cur, low_part), cur)

    def level_l(lev):
        pick = jnp.logical_and(
            lax.shift_right_logical(r_i, lev) % 2 == 1,
            lax.shift_right_logical(c_i, lev) + 1 == lax.shift_right_logical(r_i, lev),
        )
        _loop(0, n128, lambda i: merge_tile(1, i, jnp.where(pick, gm[tile(i)], 0.0)))

    def level_big(w, corner):
        for w_ in reversed(widths[:-1]):
            for i in range(hsize // w_):
                d1 = pl.ds(2 * i * w_, w_)
                d2 = pl.ds((2 * i + 1) * w_, w_)
                xm[w, d2, d1] = -_dot_nn(_dot_nn(xm[w, d2, d2], corner(w_, i)), xm[w, d1, d1])

    def pack_factor(w):
        for i in range(n128):
            pm[w, :, pl.ds(LANES * (i * (i + 1) // 2), LANES * (i + 1))] = xm[
                w, pl.ds(pl.multiple_of(i * LANES + k * EDGE, EDGE), EDGE), pl.ds(0, LANES * (i + 1))
            ]

    xm[...] = jnp.zeros_like(xm)
    ins[3].wait()
    for p in range(0, rows, 2):
        zero = jnp.zeros((EDGE, EDGE), jnp.float32)
        both = jnp.concatenate(
            [jnp.concatenate([tb[p], zero], axis=1), jnp.concatenate([zero, tb[p + 1]], axis=1)], axis=0
        )
        xm[0, pl.ds(p * EDGE, LANES), pl.ds(p * EDGE, LANES)] = both
    await_(ga.at[theirs], gx_sem.at[3])

    def corner64(i):
        block = ga[_at(i, EDGE), packed(EDGE)]
        zero = jnp.zeros((EDGE, EDGE), jnp.float32)
        low_part = jnp.concatenate([block, zero], axis=1)
        merge_tile(0, i, jnp.concatenate([jnp.zeros_like(low_part), low_part], axis=0))

    _loop(0, n128, corner64)
    level_big(0, lambda w_, i: ga[pl.ds(i * w_, w_), packed(w_)])
    pack_factor(0)
    tick(4)

    fetch_blk(0)
    fetch_blk(1)
    for d in range(1, chips):
        await_(lx.at[peer(chips - d)], lx_r.at[d - 1])
    for i in range(chips):
        gm[_at(i, LANES), :] = lx[i].T
    same = r_i == c_i

    def diag(i):
        d = gm[tile(i)]
        xm[(1, *tile(i))] = jnp.where(same, 1.0 / jnp.where(same, d, 1.0), 0.0)

    _loop(0, n128, diag)
    swapped(2)
    tick(5)
    _loop(0, 3, level_l)
    tick(6)
    wait_blk(0)
    project(sbuf.at[0], ys, 0, top // 2)
    for g in range(2):
        for d in range(1, chips):
            rs_copy(0, g, d).start()
    _loop(3, 7, level_l)
    tick(7)
    for g in range(2):
        wb[1, slice_of(g, x)] = summed(0, g)
        for d in range(1, chips):
            w_copy(1, g, d).start()
    level_big(1, lambda w_, i: gm[pl.ds((2 * i + 1) * w_, w_), pl.ds(2 * i * w_, w_)])
    pack_factor(1)
    tick(8)
    fetch_mat(0)
    fetch_mat(1)
    fetch_blk(2)
    for g in range(2):
        for d in range(1, chips):
            await_(wb.at[1, slice_of(g, peer(chips - d))], ex_r.at[g, d - 1])
            w_copy(1, g, d).wait_send()
            rs_copy(0, g, d).wait_send()

    wait_mat(0)
    wb[0] = _dot_nn(wb[1], mbuf[0])

    def reflect(n):
        j, par, nxt = top - n, n % 2, (n + 1) % 2

        @pl.when(j > 0)
        def _():
            wait_blk(n + 1)
            cm[par, _at(k, hsize)] = jnp.zeros((hsize, size), jnp.float32)
            pl.when(j % 2 == 1)(lambda: cross(n, (j // 2) * STEP, STEP))

            def one(off, width):
                apply(n - 1, off, width)
                cross(n, off, width)

            over((j + 1) // 2, one)
            c_copy(par).start()

        pl.when(j == 0)(lambda: over(0, functools.partial(apply, n - 1)))

        def factor(gs):
            got = _dot_nn(jnp.concatenate([summed(par, g) for g in gs], axis=0), mbuf[par])
            for i, g in enumerate(gs):
                wb[par, slice_of(g, x)] = got[i * sl : (i + 1) * sl]
                for d in range(1, chips):
                    w_copy(par, g, d).start()

        @pl.when(jnp.logical_and(n > 0, j >= 7))
        def _():
            factor((0,))
            factor((1,))

        pl.when(jnp.logical_and(n > 0, j < 7))(lambda: factor((0, 1)))

        @pl.when(n > 0)
        def _():
            for g in range(2):
                for d in range(1, chips):
                    rs_copy(par, g, d).wait_send()

        pl.when(n > 0)(lambda: release_blk(n - 1))
        release_mat(n)

        @pl.when(j > 0)
        def _():
            project(sbuf.at[nxt], ys, n + 1, (j - 1) // 2)

        @pl.when(jnp.logical_or(par == 1, n == 12))
        def _():
            tick(LEAD + (n + 1) // 2 + jnp.where(n >= 12, 1, 0))

        @pl.when(j > 0)
        def _():
            wait_mat(n + 1)
            await_(cm.at[par, _at(1 - k, hsize)], cm_r.at[par])

        def correct(gs):
            @pl.when(n > 0)
            def _():
                for g in gs:
                    for d in range(1, chips):
                        await_(wb.at[par, slice_of(g, peer(chips - d))], ex_r.at[g, d - 1])

            @pl.when(j > 0)
            def _():
                sbuf[nxt, cols_in(gs)] = sbuf[nxt, cols_in(gs)] - _dot_nn(wb[par, cols_in(gs)], cm[par])
                for g in gs:
                    for d in range(1, chips):
                        rs_copy(nxt, g, d).start()

        correct((0,))
        correct((1,))
        pl.when(n == 0)(lambda: tick(LEAD))

        @pl.when(n > 0)
        def _():
            for g in range(2):
                for d in range(1, chips):
                    w_copy(par, g, d).wait_send()

        @pl.when(j > 0)
        def _():
            c_copy(par).wait_send()

    _loop(0, nb, reflect)
    over(0, functools.partial(apply, top))
    release_blk(top)

    xs[...] = jnp.zeros_like(xs)
    def first_half(val):
        return lax.broadcasted_iota(jnp.int32, val.shape, 1) < EDGE


    def take(ref, cols_, j):
        lo = ref[cols_, pl.ds(pl.multiple_of((j // 2) * STEP, LANES), LANES)]
        hi = ref[cols_, pl.ds(pl.multiple_of((j // 2) * STEP + LANES, LANES), LANES)]
        even = j % 2 == 0
        return jnp.where(
            first_half(lo),
            jnp.where(even, lo, pltpu.roll(lo, EDGE, 1)),
            jnp.where(even, pltpu.roll(hi, EDGE, 1), hi),
        )

    def spread(val, j):
        even, first = j % 2 == 0, first_half(val)
        other = pltpu.roll(val, EDGE, 1)
        zero = jnp.zeros_like(val)
        lo = jnp.where(even, jnp.where(first, val, zero), jnp.where(first, zero, other))
        hi = jnp.where(even, jnp.where(first, other, zero), jnp.where(first, zero, val))
        return jnp.concatenate([lo, hi], axis=1)

    def x_copy(par, g, d):
        src = sbuf.at[par, cols_of(g), _at(peer(d), LANES)]
        return remote(src, rx.at[par, g, d - 1], rx_s.at[par, g, d - 1], rx_r.at[par, g, d - 1], at_peer(d))

    def solve_partial(n, gs, j):
        par, cols_ = n % 2, cols_in(gs)
        wb[0, cols_] = -wb[0, cols_]
        wb[0, cols_, _at(x, LANES)] += take(ys, cols_, j)
        sbuf[par, cols_] = _dot_nn(wb[0, cols_], mbuf[par])
        for g in gs:
            for d in range(1, chips):
                x_copy(par, g, d).start()

    def fin_copy(i):
        return remote(
            xs.at[:, _at(2 * i + 1 - k, LANES)], zt.at[k, :, _at(i, LANES)], fin_s.at[i], fin_r.at[i], mate
        )

    def give(i):
        await_(zt.at[1 - k, :, _at(i, LANES)], fin_r.at[i])
        zt[k, :, _at(i, LANES)] = xs[:, _at(2 * i + k, LANES)]
        out_ref[_at(i, LANES), :] = zt[:, :, _at(i, LANES)].reshape(2 * ncol, LANES).T

    for m in range(3):
        _loop(0, pairs, lambda i, m=m: swaps(m, i)[1].wait_send())
    over_v(sent)
    over_l(sent)
    to_mate.wait_send()
    half_to_mate.wait_send()
    for d in range(1, chips):
        r2_copy(d).wait_send()
        ga_copy(d).wait_send()
        lx_copy(d).wait_send()

    wait_blk(nb)
    wait_mat(nb)
    wb[0] = jnp.zeros((ncol, size), jnp.float32)
    for g in range(2):
        solve_partial(nb, (g,), top)
    release_blk(nb)
    release_mat(nb)

    def solve(i):
        n = nb + i
        j, par, nxt = top - i, n % 2, (n + 1) % 2

        @pl.when(j > 0)
        def _():
            wait_blk(n + 1)
            wait_mat(n + 1)
            project(wb.at[0], xs, n + 1, (j + 1) // 2)

        def finish(gs):
            cols_ = cols_in(gs)
            vals = []
            for g in gs:
                for d in range(1, chips):
                    x_copy(par, g, d).wait_recv()
                val = sbuf[par, cols_of(g), _at(x, LANES)]
                for d in range(1, chips):
                    val = val + rx[par, g, d - 1]
                vals.append(val)
            solved = spread(jnp.concatenate(vals, axis=0), j)
            xs[cols_, _at(j // 2, STEP)] += solved

            @pl.when(j > 0)
            def _():
                wb[0, cols_] += _dot_nt(solved, cut(n + 1, (j // 2) * STEP, STEP))
                solve_partial(n + 1, gs, j - 1)

        finish((0,))
        finish((1,))

        pl.when(j % 2 == 0)(lambda: fin_copy(j // 2).start())
        pl.when(jnp.logical_and(j % 2 == 1, j < top))(lambda: give(j // 2 + 1))

        for g in range(2):
            for d in range(1, chips):
                x_copy(par, g, d).wait_send()

        @pl.when(jnp.logical_or(i == 0, i % 2 == 1))
        def _():
            tick(LEAD + 10 + (i + 1) // 2)

        @pl.when(j > 0)
        def _():
            release_blk(n + 1)
            release_mat(n + 1)

    _loop(0, nb, solve)

    give(0)
    _loop(0, pairs, lambda i: fin_copy(i).wait_send())


def solution(mesh):
    rows, cols = mesh.shape["row"], mesh.shape["col"]
    mat_spec = P(("kpt", "row"), "col")
    fac_spec = P("kpt", None, None)

    def local_work(v_loc, t_loc, z_loc, l_loc):
        n_row, n_col = v_loc.shape
        slots, lanes, chips, size = n_col // EDGE, 2 * n_row, rows // 2, rows * EDGE
        nb, ncol = lanes // LANES, z_loc.shape[1] // 2
        pairs, gcol, peers = nb // 2, ncol // 2, max(chips - 1, 1)
        sl, gathers, n128 = gcol // chips, len(_gathers(slots)), size // LANES
        tri = LANES * (n128 * (n128 + 1) // 2)
        dma = pltpu.SemaphoreType.DMA
        hbm, vmem = pl.BlockSpec(memory_space=pl.ANY), pl.BlockSpec(memory_space=pltpu.VMEM)

        def buf(*shape):
            return pltpu.VMEM(shape, jnp.float32)

        col = lax.axis_index("col")
        t_mine = lax.dynamic_slice_in_dim(t_loc, (cols // rows * (col % rows) + col // rows) * rows, rows, axis=0)
        return pl.pallas_call(
            functools.partial(_kernel, (rows, cols, slots, nb, ncol)),
            out_shape=[
                jax.ShapeDtypeStruct(z_loc.shape, jnp.float32),
                jax.ShapeDtypeStruct((2, slots, RING, RING, HALF, lanes), jnp.float32),
            ],
            in_specs=[hbm] * 4,
            out_specs=[vmem, hbm],
            scratch_shapes=[
                buf(2, n_row, n_col),
                buf(2, slots, 2, HALF, n_row),
                buf(2, ncol, n_row),
                buf(rows, EDGE, EDGE),
                buf(2, slots, HALF, lanes),
                buf(ncol, lanes),
                buf(ncol, lanes),
                buf(pairs // 2, rows, EDGE, STEP),
                buf(rows, EDGE, STEP),
                buf(chips, size, LANES),
                buf(size, size),
                buf(size // 2, size),
                buf(size // 4, size),
                buf(peers, size // 4 // chips, size),
                buf(size // 2, size),
                buf(2, EDGE, tri),
                buf(2, RING, RING, EDGE, tri),
                buf(DEEP, rows, EDGE, lanes),
                buf(2, size, size),
                buf(2, ncol, size),
                buf(2, peers, sl, size),
                buf(2, ncol, size),
                buf(2, size, size),
                buf(2, 2, peers, gcol, LANES),
                dma((4,)),
                dma((3, pairs)), dma((3, pairs)), dma((3, pairs)),
                dma((slots, pairs)), dma((pairs // 2, rows, 2)),
                dma((slots, 2)), dma((rows, 2)),
                dma((peers,)), dma((peers,)),
                dma((4,)),
                dma((peers,)), dma((peers,)), dma((peers,)), dma((peers,)),
                dma((pairs,)), dma((pairs,)),
                dma((gathers,)), dma((gathers, 8)), dma((gathers, 8)),
                dma((DEEP, rows)), dma((DEEP, rows)), dma((DEEP, rows)),
                dma((2, n128)), dma((2, n128)), dma((2, n128)),
                pltpu.SemaphoreType.REGULAR((DEEP,)), pltpu.SemaphoreType.REGULAR((2,)),
                dma((2, peers)), dma((2, peers)), dma((2, peers)), dma((2, peers)),
                dma((2,)), dma((2,)),
                dma((2, 2, peers)), dma((2, 2, peers)),
                dma((16,)), dma((16,)),
            ],
            compiler_params=pltpu.CompilerParams(collective_id=0, has_side_effects=True, vmem_limit_bytes=67_043_328),
            name="eigvec",
        )(v_loc, t_mine, z_loc, l_loc)[0]

    return jax.shard_map(local_work, mesh=mesh, in_specs=(mat_spec, fac_spec, mat_spec, mat_spec), out_specs=mat_spec, check_vma=False)
```

```python
import functools

import jax
import jax.numpy as jnp
from jax import lax
from jax.experimental import pallas as pl
from jax.experimental.pallas import tpu as pltpu
from jax.sharding import PartitionSpec as P

PREC_HIGH = lax.Precision.HIGHEST
MESH = pl.DeviceIdType.MESH
EDGE = 64
HALF = EDGE // 2
LANES = 128
STEP = 256
RING = 4
LEAD = 9
DEEP = 3


def _dot_nt(a, b):
    return lax.dot_general(a, b, (((1,), (1,)), ((), ())), precision=PREC_HIGH, preferred_element_type=jnp.float32)


def _dot_nn(a, b):
    return lax.dot_general(a, b, (((1,), (0,)), ((), ())), precision=PREC_HIGH, preferred_element_type=jnp.float32)


def _at(i, n):
    return pl.ds(pl.multiple_of(i * n, n), n)


def _loop(lo, hi, body):
    def one(i, carry):
        body(i)
        return carry

    lax.fori_loop(lo, hi, one, 0)


def _gathers(slots):
    early = [(slots - 1, 0), (slots - 2, 0), None, None, ("m", 0), None]
    first = early + [(q, 0) for q in range(slots - 3, -1, -1)]
    rest = [(slots - 1, 1), ("m", 1)] + [(q, 1) for q in range(slots - 2, -1, -1)]
    return first + [None] * (LEAD - len(first)) + rest


def _kernel(dims, v_in, t_in, z_in, l_in, out_ref, gath, *scratch):
    (stage, vt, zt, tb, own, ys, xs, vb, ld, lx, gm, pk, gx, r2, ga, pm, mg, blk, mbuf, sbuf, rs, wb, cm, rx,
     in_sem, swap_l, swap_s, swap_r, v_s, v_r, l_s, l_r, lx_s, lx_r, gx_sem, r2_s, r2_r, ga_s, ga_r, fin_s, fin_r,
     ag_loc, ag_s, ag_r, blk_loc, blk_s, blk_r, mat_loc, mat_s, mat_r, free_b, free_m, rs_s, rs_r, ex_s, ex_r, cm_s, cm_r,
     rx_s, rx_r, eg_s, eg_r) = scratch
    xm = cm
    rows, cols, slots, nb, ncol = dims
    row, col = lax.axis_index("row"), lax.axis_index("col")
    x, k = row // 2, row % 2
    chips, groups = rows // 2, cols // rows
    size, lanes = rows * EDGE, nb * LANES
    hsize, qsize, n128 = size // 2, size // 4, size // LANES
    pairs = nb // 2
    gcol = ncol // 2
    sl = gcol // chips
    mate = {"row": row + 1 - 2 * k, "col": col}
    top, whole = nb - 1, nb // 2
    part, grp = col % rows, col // rows
    k_half, m_half = _at(k, HALF), _at(1 - k, HALF)
    s_a, s_b = 1 + (RING - 1) * k, RING - (RING - 1) * k
    a, b = (col // s_a) % RING, (col // s_b) % RING

    def remote(src, dst, ss, rr, to):
        return pltpu.make_async_remote_copy(src, dst, ss, rr, device_id=to, device_id_type=MESH)

    def await_(ref, sem):
        pltpu.make_async_copy(ref, ref, sem).wait()

    def peer(d):
        return lax.rem(x + d, chips)

    def at_peer(d):
        return {"row": 2 * peer(d) + k, "col": col}

    def plane(da, db):
        return {"row": row, "col": lax.rem(a + da, RING) * s_a + lax.rem(b + db, RING) * s_b}

    def low(q):
        return (groups * q // 2) * STEP

    order = _gathers(slots)

    class Slot:
        def __init__(self, kind, w, n):
            self.kind, self.w, self.n = kind, w, n

        def own(self):
            if self.kind == "m":
                return pm.at[self.w]
            return own.at[self.w, self.kind, :, pl.ds(low(self.kind), lanes - low(self.kind))]

        def piece(self, bb, aa, part=None):
            if self.kind == "m":
                return mg.at[self.w, bb, aa] if part is None else mg.at[self.w, bb, aa, pl.ds(part * HALF, HALF)]
            at = pl.ds(low(self.kind), lanes - low(self.kind))
            e = slice(None) if part is None else pl.ds(part * (HALF // 2), HALF // 2)
            return gath.at[self.w, self.kind, bb, aa, e, at]

        def bundle(self, bb, part=None):
            e = slice(None) if part is None else pl.ds(part * (RING // 2), RING // 2)
            if self.kind == "m":
                return mg.at[self.w, bb, e]
            return gath.at[self.w, self.kind, bb, e, :, pl.ds(low(self.kind), lanes - low(self.kind))]

        def copy(self, i):
            d = 1 if i % 2 == 0 else RING - 1
            back = RING - d
            if i < 2:
                src, dst, to = self.own(), self.piece(b, a), plane(d, 0)
            elif i < 4:
                src = dst = self.piece(b, lax.rem(a + back, RING), i % 2)
                to = plane(d, 0)
            elif i < 6:
                src = dst = self.bundle(b)
                to = plane(0, d)
            else:
                src = dst = self.bundle(lax.rem(b + back, RING), i % 2)
                to = plane(0, d)
            return remote(src, dst, ag_s.at[self.n, i], ag_r.at[self.n, i], to)

        def arrived(self, i):
            back = RING - 1 if i % 2 == 0 else 1
            if i < 2:
                dst = self.piece(b, lax.rem(a + back, RING))
            elif i < 4:
                dst = self.piece(b, lax.rem(a + 2, RING), i % 2)
            elif i < 6:
                dst = self.bundle(lax.rem(b + back, RING))
            else:
                dst = self.bundle(lax.rem(b + 2, RING), i % 2)
            await_(dst, ag_r.at[self.n, i])

        def kept(self):
            return pltpu.make_async_copy(self.own(), self.piece(b, a), ag_loc.at[self.n])

        def stage(self, s):
            if s == 0:
                self.copy(0).start()
                self.copy(1).start()
                self.kept().start()
            elif s == 1:
                for i in range(2):
                    self.arrived(i)
                    self.copy(2 + i).start()
            elif s == 2:
                self.kept().wait()
                self.arrived(2)
                self.arrived(3)
                self.copy(4).start()
                self.copy(5).start()
            elif s == 3:
                for i in range(4, 6):
                    self.arrived(i)
                    self.copy(2 + i).start()
            elif s == 4:
                self.arrived(6)
                self.arrived(7)
            else:
                for i in range(8):
                    self.copy(i).wait_send()

    class Eager(Slot):
        def spot(self, db, da, part=None):
            return self.piece(lax.rem(b + db, RING), lax.rem(a + da, RING), part)

        def copy(self, i):
            back = RING - 1
            db, da, part, to_b, to_a = (
                (0, 0, None, 0, 1), (0, 0, None, 0, back), (0, 0, None, 1, 0), (0, 0, None, back, 0),
                (0, back, 0, 0, 1), (0, 1, 1, 0, back),
                (0, back, None, 1, 0), (0, back, None, back, 0), (0, 1, None, 1, 0), (0, 1, None, back, 0),
                (0, 2, None, 1, 0), (0, 2, None, back, 0),
                (back, 0, None, 1, 0), (back, back, None, 1, 0), (1, 1, None, back, 0), (1, 2, None, back, 0),
            )[i]
            dst = self.spot(db, da, part)
            src = self.own() if db == 0 and da == 0 else dst
            sent_ = remote(src, dst, eg_s.at[i], eg_r.at[i], plane(to_a, to_b))
            return sent_, self.spot(db + RING - to_b, da + RING - to_a, part)

        def go(self, *which):
            for i in which:
                self.copy(i)[0].start()

        def got(self, *which):
            for i in which:
                await_(self.copy(i)[1], eg_r.at[i])

        def stage(self, s):
            if s == 0:
                self.go(0, 1, 2, 3)
                self.kept().start()
            elif s == 1:
                self.got(0)
                self.go(4, 6, 7)
                self.got(1)
                self.go(5, 8, 9)
                self.got(2)
                self.go(12)
            elif s == 2:
                self.got(4, 5)
                self.go(10, 11)
                self.got(6)
                self.go(13)
            elif s == 3:
                self.got(9)
                self.go(14)
                self.got(11)
                self.go(15)
            elif s == 4:
                self.got(3, 7, 8, 10, 12, 13, 14, 15)
                self.kept().wait()
                for i in range(16):
                    self.copy(i)[0].wait_send()

    def tick(t, stages=(4, 3, 2, 1, 0, 5)):
        for s in stages:
            n = t - s
            if isinstance(n, int):
                if 0 <= n < len(order) and order[n] is not None:
                    (Eager if order[n] == ("m", 0) else Slot)(*order[n], n).stage(s)
                continue
            for kind in list(range(slots)) + ["m"]:
                at_v, at_l = order.index((kind, 0)), order.index((kind, 1))

                @pl.when(n == at_l if kind == "m" else jnp.logical_or(n == at_v, n == at_l))
                def _(s=s, n=n, kind=kind, at_l=at_l):
                    Slot(kind, jnp.where(n == at_l, 1, 0), n).stage(s)

    def block_of(n):
        j = top - n % nb
        return n // nb, j, j // groups, j % groups, n % 2

    run = min(rows, RING)
    runs = rows // run

    def in_blk(n, q, i, half):
        return blk.at[n % DEEP, pl.ds(i * run, run), half, pl.ds(low(q), lanes - low(q))]

    def from_mate(n, q, i):
        await_(in_blk(n, q, i, m_half), blk_r.at[n % DEEP, i])

    def mat_copies(n, i):
        w, j, q, h, s = block_of(n)
        c = h * rows + q
        src = mg.at[w, (c // s_b) % RING, (c // s_a) % RING, :, pl.ds(LANES * (i * (i + 1) // 2), LANES * (i + 1))]
        dst = mbuf.at[s, pl.ds(pl.multiple_of(i * LANES + k * EDGE, EDGE), EDGE), pl.ds(0, LANES * (i + 1))]
        return (
            pltpu.make_async_copy(src, dst, mat_loc.at[s, i]),
            remote(src, dst, mat_s.at[s, i], mat_r.at[s, i], mate),
        )

    def per_piece(n, act):
        q_now = block_of(n)[2]
        for q in range(slots):

            @pl.when(q_now == q)
            def _(q=q):
                for i in range(runs):
                    act(q, i)

    def fetch_blk(n):
        w, _, _, h, _ = block_of(n)
        s = n % DEEP

        def go(q, i):
            c = h * rows + i * run
            z_now, y_run = c // RING, pl.ds(c % RING, run)
            at = pl.ds(low(q), lanes - low(q))
            dst = in_blk(n, q, i, k_half)

            def both(src):
                pltpu.make_async_copy(src, dst, blk_loc.at[s, i]).start()
                remote(src, dst, blk_s.at[s, i], blk_r.at[s, i], mate).start()

            pl.when(k == 0)(lambda: both(gath.at[w, q, z_now, y_run, :, at]))
            pl.when(k == 1)(lambda: both(gath.at[w, q, y_run, z_now, :, at]))

        per_piece(n, go)

    def fetch_mat(n):
        for i in range(n128):
            for c in mat_copies(n, i):
                c.start()

    def wait_blk(n):
        def one(q, i):
            await_(in_blk(n, q, i, k_half), blk_loc.at[n % DEEP, i])
            from_mate(n, q, i)

        per_piece(n, one)

    def wait_mat(n):
        for i in range(n128):
            mat_copies(n, i)[0].wait()
            there = pl.ds(pl.multiple_of(i * LANES + (1 - k) * EDGE, EDGE), EDGE), pl.ds(0, LANES * (i + 1))
            await_(mbuf.at[(n % 2, *there)], mat_r.at[n % 2, i])

    def release_blk(n):
        per_piece(n, lambda q, i: await_(in_blk(n, q, i, k_half), blk_s.at[n % DEEP, i]))

        @pl.when(n + DEEP < 2 * nb)
        def _():
            pl.semaphore_signal(free_b.at[n % DEEP], inc=1, device_id=mate, device_id_type=MESH)
            pl.semaphore_wait(free_b.at[n % DEEP], 1)
            fetch_blk(n + DEEP)

    def release_mat(n):
        for i in range(n128):
            mat_copies(n, i)[1].wait_send()

        @pl.when(n + 2 < 2 * nb)
        def _():
            pl.semaphore_signal(free_m.at[n % 2], inc=1, device_id=mate, device_id_type=MESH)
            pl.semaphore_wait(free_m.at[n % 2], 1)
            fetch_mat(n + 2)

    def over(first, body):
        pl.when(first % 2 == 1)(lambda: body(first * STEP, STEP))
        _loop((first + 1) // 2, whole // 2, lambda i: body(i * 2 * STEP, 2 * STEP))

    def rows_at(off, width):
        return pl.ds(pl.multiple_of(off, STEP), width)

    def cut(n, off, width):
        return blk[n % DEEP, :, :, rows_at(off, width)].reshape(size, width)

    def project(dst, ref, n, first):
        dst[...] = jnp.zeros((ncol, size), jnp.float32)

        def one(off, width):
            dst[...] += _dot_nt(ref[:, rows_at(off, width)], cut(n, off, width))

        if whole % 4 or isinstance(first, int):
            over(first, one)
            return
        half = (first + 1) // 2
        pl.when(first % 2 == 1)(lambda: one(first * STEP, STEP))
        pl.when(half % 2 == 1)(lambda: one(half * 2 * STEP, 2 * STEP))
        _loop((half + 1) // 2, whole // 4, lambda i: one(i * 4 * STEP, 4 * STEP))

    def slice_of(g, x2):
        return pl.ds(pl.multiple_of(g * gcol + x2 * sl, sl), sl)

    def cols_of(g):
        return pl.ds(g * gcol, gcol)

    def rs_copy(par, g, d):
        return remote(sbuf.at[par, slice_of(g, peer(d))], rs.at[g, d - 1], rs_s.at[g, d - 1], rs_r.at[g, d - 1], at_peer(d))

    def w_copy(par, g, d):
        mine = wb.at[par, slice_of(g, x)]
        return remote(mine, mine, ex_s.at[g, d - 1], ex_r.at[g, d - 1], at_peer(d))

    c_half = pl.ds(pl.multiple_of(k * (rows // 2), rows // 2), rows // 2)

    def c_copy(par):
        return remote(cm.at[par, _at(k, hsize)], cm.at[par, _at(k, hsize)], cm_s.at[par], cm_r.at[par], mate)

    def summed(par, g):
        for d in range(1, chips):
            rs_copy(par, g, d).wait_recv()
        total = sbuf[par, slice_of(g, x)]
        for d in range(1, chips):
            total = total + rs[g, d - 1]
        return total

    def apply(n, off, width):
        ys[:, rows_at(off, width)] = ys[:, rows_at(off, width)] - _dot_nn(wb[n % 2], cut(n, off, width))

    def cross(n, off, width):
        here = blk[n % DEEP, c_half, :, rows_at(off, width)].reshape(hsize, width)
        cm[n % 2, _at(k, hsize)] += _dot_nt(here, cut(n + 1, off, width))

    def cols_in(gs):
        return pl.ds(gs[0] * gcol, len(gs) * gcol)

    barrier = pltpu.get_barrier_semaphore()

    def here_i_am(device):
        pl.semaphore_signal(barrier, inc=1, device_id=device, device_id_type=MESH)

    def group_member(d):
        n = lax.rem(2 * part + k + d, 2 * rows)
        here_i_am({"col": grp * rows + n // 2, "row": 2 * x + n % 2})

    _loop(1, 2 * rows, group_member)
    for d in range(1, chips):
        here_i_am(at_peer(d))
    for d in (1, RING - 1):
        here_i_am(plane(d, 0))
        here_i_am(plane(0, d))

    ins = [
        pltpu.make_async_copy(src, stage.at[i % 2], in_sem.at[i]) for i, src in enumerate((v_in, l_in, z_in))
    ] + [pltpu.make_async_copy(t_in, tb, in_sem.at[3])]
    for i in (0, 1, 3):
        ins[i].start()
    pl.semaphore_wait(barrier, 2 * rows - 1 + chips - 1 + 4)

    def swaps(m, i):
        there = _at(2 * i + k, LANES)
        if m < 2:
            mine, theirs = vt.at[m, :, k, :, _at(i, LANES)], vt.at[m, :, 1 - k, :, _at(i, LANES)]
            dst = own.at[m, :, :, there]
        else:
            mine, theirs = zt.at[k, :, _at(i, LANES)], zt.at[1 - k, :, _at(i, LANES)]
            dst = ys.at[:, there]
        return (
            pltpu.make_async_copy(mine, dst, swap_l.at[m, i]),
            remote(theirs, dst, swap_s.at[m, i], swap_r.at[m, i], mate),
        )

    def arriving(m, i):
        there = _at(2 * i + 1 - k, LANES)
        await_(own.at[m, :, :, there] if m < 2 else ys.at[:, there], swap_r.at[m, i])

    def turn(m, then=None):
        ins[m].wait()

        def one(i):
            block = stage[m % 2, _at(i, LANES), :].T
            if m < 2:
                vt[m, :, :, :, _at(i, LANES)] = block.reshape(slots, 2, HALF, LANES)
            else:
                zt[:, :, _at(i, LANES)] = block.reshape(2, ncol, LANES)
            for c in swaps(m, i):
                c.start()
            if then is not None:
                pl.when(i > 0)(lambda: then(i - 1))

        _loop(0, pairs, one)
        if then is not None:
            then(pairs - 1)

    def swapped(m):
        def one(i):
            swaps(m, i)[0].wait()
            arriving(m, i)

        _loop(0, pairs, one)

    my_q, my_h = part, grp
    my_j = groups * my_q + my_h
    first_t = my_j // 2

    def deal_v(q, t, act):
        to, kk = grp * rows + q, t % 2
        src = own.at[0, q, :, _at(t, STEP)]
        dst = vb.at[t // 2, part, k_half]
        self_ = jnp.logical_and(to == col, k == kk)
        act(
            self_,
            pltpu.make_async_copy(src, dst, v_r.at[t // 2, part, k]),
            remote(src, dst, v_s.at[q, t], v_r.at[t // 2, part, k], {"col": to, "row": 2 * x + kk}),
        )

    def deal_l(q, kk, act):
        to = grp * rows + q
        src = own.at[1, q, :, _at((groups * q + grp) // 2, STEP)]
        dst = ld.at[part, k_half]
        self_ = jnp.logical_and(to == col, k == kk)
        act(
            self_,
            pltpu.make_async_copy(src, dst, l_r.at[part, k]),
            remote(src, dst, l_s.at[q, kk], l_r.at[part, k], {"col": to, "row": 2 * x + kk}),
        )

    def send(self_, here, there):
        pl.when(self_)(here.start)
        pl.when(jnp.logical_not(self_))(there.start)

    def sent(self_, here, there):
        pl.when(jnp.logical_not(self_))(there.wait_send)

    def over_v(act):
        def one(q):
            _loop((groups * q + grp) // 2, pairs, lambda t: deal_v(q, t, act))

        _loop(0, slots, one)

    def over_l(act):
        def one(q):
            deal_l(q, 0, act)
            deal_l(q, 1, act)

        _loop(0, slots, one)

    def deal_chunk(t):
        swaps(0, t)[0].wait()
        arriving(0, t)
        _loop(0, (2 * t + 1 - grp + groups) // groups, lambda q: deal_v(q, t, send))

    turn(0, deal_chunk)
    ins[2].start()
    turn(1)
    swapped(1)
    over_l(send)
    turn(2)
    mbuf[...] = jnp.zeros_like(mbuf)

    gm[...] = jnp.zeros_like(gm)

    def chunk(i):
        def got(n):
            await_(vb.at[i, n // 2, _at(n % 2, HALF)], v_r.at[i, n // 2, n % 2])

        _loop(0, 2 * rows, got)
        all_ = vb[i].reshape(size, STEP)
        gm[pl.ds(0, hsize), pl.ds(0, hsize)] += _dot_nt(all_[:hsize], all_[:hsize])
        gm[pl.ds(hsize, hsize), :] += _dot_nt(all_[hsize:], all_)

    _loop((first_t + 1 - k) // 2, pairs // 2, chunk)
    tick(0)

    widths = []
    w_ = hsize
    while w_ >= EDGE:
        widths.append(w_)
        w_ //= 2

    def packed(w_):
        return pl.ds(size - 2 * w_, w_)

    pk[...] = jnp.zeros_like(pk)
    for w_ in widths:
        for i in range(hsize // w_):
            pk[pl.ds(i * w_, w_), packed(w_)] = gm[pl.ds((2 * i + 1) * w_, w_), pl.ds(2 * i * w_, w_)]

    mine, theirs = _at(k, qsize), _at(1 - k, qsize)
    to_mate = remote(pk.at[theirs], gx, gx_sem.at[0], gx_sem.at[1], mate)
    to_mate.start()
    tick(1)
    to_mate.wait_recv()
    pk[mine] += gx[...]
    rl = qsize // chips

    def r2_copy(d):
        src = pk.at[pl.ds(pl.multiple_of(k * qsize + peer(d) * rl, rl), rl)]
        return remote(src, r2.at[d - 1], r2_s.at[d - 1], r2_r.at[d - 1], at_peer(d))

    for d in range(1, chips):
        r2_copy(d).start()

    def got_l(n):
        await_(ld.at[n // 2, _at(n % 2, HALF)], l_r.at[n // 2, n % 2])

    _loop(0, 2 * rows, got_l)
    ev = my_j % 2 == 0
    lo_half = lax.broadcasted_iota(jnp.int32, (size, LANES), 1) < EDGE
    l_lo, l_hi = ld[:, :, pl.ds(0, LANES)].reshape(size, LANES), ld[:, :, pl.ds(LANES, LANES)].reshape(size, LANES)
    lx[x] = jnp.where(
        lo_half,
        jnp.where(ev, l_lo, pltpu.roll(l_lo, EDGE, 1)),
        jnp.where(ev, pltpu.roll(l_hi, EDGE, 1), l_hi),
    )

    def lx_copy(d):
        return remote(lx.at[x], lx.at[x], lx_s.at[d - 1], lx_r.at[d - 1], at_peer(d))

    tick(2)
    for d in range(1, chips):
        r2_copy(d).wait_recv()
    my_rows = pl.ds(pl.multiple_of(k * qsize + x * rl, rl), rl)
    total = pk[my_rows]
    for d in range(1, chips):
        total = total + r2[d - 1]
    ga[my_rows] = total

    def ga_copy(d):
        return remote(ga.at[my_rows], ga.at[my_rows], ga_s.at[d - 1], ga_r.at[d - 1], at_peer(d))

    for d in range(1, chips):
        ga_copy(d).start()
    for d in range(1, chips):
        lx_copy(d).start()
    tick(3)
    for d in range(1, chips):
        await_(ga.at[pl.ds(pl.multiple_of(k * qsize + peer(chips - d) * rl, rl), rl)], ga_r.at[d - 1])
    half_to_mate = remote(ga.at[mine], ga.at[mine], gx_sem.at[2], gx_sem.at[3], mate)
    half_to_mate.start()

    r_i = lax.broadcasted_iota(jnp.int32, (LANES, LANES), 0)
    c_i = lax.broadcasted_iota(jnp.int32, (LANES, LANES), 1)

    def tile(i):
        return _at(i, LANES), _at(i, LANES)

    def merge_tile(w, i, low_part):
        cur = xm[(w, *tile(i))]
        xm[(w, *tile(i))] = cur - _dot_nn(_dot_nn(cur, low_part), cur)

    def level_l(lev):
        pick = jnp.logical_and(
            lax.shift_right_logical(r_i, lev) % 2 == 1,
            lax.shift_right_logical(c_i, lev) + 1 == lax.shift_right_logical(r_i, lev),
        )
        _loop(0, n128, lambda i: merge_tile(1, i, jnp.where(pick, gm[tile(i)], 0.0)))

    def level_big(w, corner):
        for w_ in reversed(widths[:-1]):
            for i in range(hsize // w_):
                d1 = pl.ds(2 * i * w_, w_)
                d2 = pl.ds((2 * i + 1) * w_, w_)
                xm[w, d2, d1] = -_dot_nn(_dot_nn(xm[w, d2, d2], corner(w_, i)), xm[w, d1, d1])

    def pack_factor(w):
        for i in range(n128):
            pm[w, :, pl.ds(LANES * (i * (i + 1) // 2), LANES * (i + 1))] = xm[
                w, pl.ds(pl.multiple_of(i * LANES + k * EDGE, EDGE), EDGE), pl.ds(0, LANES * (i + 1))
            ]

    xm[...] = jnp.zeros_like(xm)
    ins[3].wait()
    for p in range(0, rows, 2):
        zero = jnp.zeros((EDGE, EDGE), jnp.float32)
        both = jnp.concatenate(
            [jnp.concatenate([tb[p], zero], axis=1), jnp.concatenate([zero, tb[p + 1]], axis=1)], axis=0
        )
        xm[0, pl.ds(p * EDGE, LANES), pl.ds(p * EDGE, LANES)] = both
    await_(ga.at[theirs], gx_sem.at[3])

    def corner64(i):
        block = ga[_at(i, EDGE), packed(EDGE)]
        zero = jnp.zeros((EDGE, EDGE), jnp.float32)
        low_part = jnp.concatenate([block, zero], axis=1)
        merge_tile(0, i, jnp.concatenate([jnp.zeros_like(low_part), low_part], axis=0))

    _loop(0, n128, corner64)
    level_big(0, lambda w_, i: ga[pl.ds(i * w_, w_), packed(w_)])
    pack_factor(0)
    tick(4)

    fetch_blk(0)
    fetch_blk(1)
    for d in range(1, chips):
        await_(lx.at[peer(chips - d)], lx_r.at[d - 1])
    for i in range(chips):
        gm[_at(i, LANES), :] = lx[i].T
    same = r_i == c_i

    def diag(i):
        d = gm[tile(i)]
        xm[(1, *tile(i))] = jnp.where(same, 1.0 / jnp.where(same, d, 1.0), 0.0)

    _loop(0, n128, diag)
    swapped(2)
    tick(5)
    _loop(0, 3, level_l)
    tick(6)
    wait_blk(0)
    project(sbuf.at[0], ys, 0, top // 2)
    for g in range(2):
        for d in range(1, chips):
            rs_copy(0, g, d).start()
    _loop(3, 7, level_l)
    tick(7)
    for g in range(2):
        wb[1, slice_of(g, x)] = summed(0, g)
        for d in range(1, chips):
            w_copy(1, g, d).start()
    level_big(1, lambda w_, i: gm[pl.ds((2 * i + 1) * w_, w_), pl.ds(2 * i * w_, w_)])
    pack_factor(1)
    tick(8, (4,))
    fetch_mat(0)
    fetch_mat(1)
    fetch_blk(2)
    for g in range(2):
        for d in range(1, chips):
            await_(wb.at[1, slice_of(g, peer(chips - d))], ex_r.at[g, d - 1])
            w_copy(1, g, d).wait_send()
            rs_copy(0, g, d).wait_send()

    wait_mat(0)
    wb[0] = _dot_nn(wb[1], mbuf[0])

    def reflect(n):
        j, par, nxt = top - n, n % 2, (n + 1) % 2

        @pl.when(j > 0)
        def _():
            wait_blk(n + 1)
            cm[par, _at(k, hsize)] = jnp.zeros((hsize, size), jnp.float32)
            pl.when(j % 2 == 1)(lambda: cross(n, (j // 2) * STEP, STEP))

            def one(off, width):
                apply(n - 1, off, width)
                cross(n, off, width)

            over((j + 1) // 2, one)
            c_copy(par).start()

        pl.when(j == 0)(lambda: over(0, functools.partial(apply, n - 1)))

        def factor(gs):
            got = _dot_nn(jnp.concatenate([summed(par, g) for g in gs], axis=0), mbuf[par])
            for i, g in enumerate(gs):
                wb[par, slice_of(g, x)] = got[i * sl : (i + 1) * sl]
                for d in range(1, chips):
                    w_copy(par, g, d).start()

        @pl.when(jnp.logical_and(n > 0, j >= 7))
        def _():
            factor((0,))
            factor((1,))

        pl.when(jnp.logical_and(n > 0, j < 7))(lambda: factor((0, 1)))

        @pl.when(n > 0)
        def _():
            for g in range(2):
                for d in range(1, chips):
                    rs_copy(par, g, d).wait_send()

        pl.when(n > 0)(lambda: release_blk(n - 1))
        release_mat(n)

        @pl.when(j > 0)
        def _():
            project(sbuf.at[nxt], ys, n + 1, (j - 1) // 2)

        @pl.when(jnp.logical_or(par == 1, n == 12))
        def _():
            tick(LEAD + (n + 1) // 2 + jnp.where(n >= 12, 1, 0) - jnp.where(n == 1, 1, 0))

        @pl.when(j > 0)
        def _():
            wait_mat(n + 1)
            await_(cm.at[par, _at(1 - k, hsize)], cm_r.at[par])

        def correct(gs):
            @pl.when(n > 0)
            def _():
                for g in gs:
                    for d in range(1, chips):
                        await_(wb.at[par, slice_of(g, peer(chips - d))], ex_r.at[g, d - 1])

            @pl.when(j > 0)
            def _():
                sbuf[nxt, cols_in(gs)] = sbuf[nxt, cols_in(gs)] - _dot_nn(wb[par, cols_in(gs)], cm[par])
                for g in gs:
                    for d in range(1, chips):
                        rs_copy(nxt, g, d).start()

        correct((0,))
        correct((1,))
        pl.when(n == 0)(lambda: tick(8, (3, 2, 1, 0, 5)))
        pl.when(n == 1)(lambda: tick(10))

        @pl.when(n > 0)
        def _():
            for g in range(2):
                for d in range(1, chips):
                    w_copy(par, g, d).wait_send()

        @pl.when(j > 0)
        def _():
            c_copy(par).wait_send()

    _loop(0, nb, reflect)
    over(0, functools.partial(apply, top))
    release_blk(top)

    xs[...] = jnp.zeros_like(xs)
    def first_half(val):
        return lax.broadcasted_iota(jnp.int32, val.shape, 1) < EDGE


    def take(ref, cols_, j):
        lo = ref[cols_, pl.ds(pl.multiple_of((j // 2) * STEP, LANES), LANES)]
        hi = ref[cols_, pl.ds(pl.multiple_of((j // 2) * STEP + LANES, LANES), LANES)]
        even = j % 2 == 0
        return jnp.where(
            first_half(lo),
            jnp.where(even, lo, pltpu.roll(lo, EDGE, 1)),
            jnp.where(even, pltpu.roll(hi, EDGE, 1), hi),
        )

    def spread(val, j):
        even, first = j % 2 == 0, first_half(val)
        other = pltpu.roll(val, EDGE, 1)
        zero = jnp.zeros_like(val)
        lo = jnp.where(even, jnp.where(first, val, zero), jnp.where(first, zero, other))
        hi = jnp.where(even, jnp.where(first, other, zero), jnp.where(first, zero, val))
        return jnp.concatenate([lo, hi], axis=1)

    def x_copy(par, g, d):
        src = sbuf.at[par, cols_of(g), _at(peer(d), LANES)]
        return remote(src, rx.at[par, g, d - 1], rx_s.at[par, g, d - 1], rx_r.at[par, g, d - 1], at_peer(d))

    def solve_partial(n, gs, j):
        par, cols_ = n % 2, cols_in(gs)
        wb[0, cols_] = -wb[0, cols_]
        wb[0, cols_, _at(x, LANES)] += take(ys, cols_, j)
        sbuf[par, cols_] = _dot_nn(wb[0, cols_], mbuf[par])
        for g in gs:
            for d in range(1, chips):
                x_copy(par, g, d).start()

    def fin_copy(i):
        return remote(
            xs.at[:, _at(2 * i + 1 - k, LANES)], zt.at[k, :, _at(i, LANES)], fin_s.at[i], fin_r.at[i], mate
        )

    def give(i):
        await_(zt.at[1 - k, :, _at(i, LANES)], fin_r.at[i])
        zt[k, :, _at(i, LANES)] = xs[:, _at(2 * i + k, LANES)]
        out_ref[_at(i, LANES), :] = zt[:, :, _at(i, LANES)].reshape(2 * ncol, LANES).T

    for m in range(3):
        _loop(0, pairs, lambda i, m=m: swaps(m, i)[1].wait_send())
    over_v(sent)
    over_l(sent)
    to_mate.wait_send()
    half_to_mate.wait_send()
    for d in range(1, chips):
        r2_copy(d).wait_send()
        ga_copy(d).wait_send()
        lx_copy(d).wait_send()

    wait_blk(nb)
    wait_mat(nb)
    wb[0] = jnp.zeros((ncol, size), jnp.float32)
    for g in range(2):
        solve_partial(nb, (g,), top)
    release_blk(nb)
    release_mat(nb)

    def solve(i):
        n = nb + i
        j, par, nxt = top - i, n % 2, (n + 1) % 2

        @pl.when(j > 0)
        def _():
            wait_blk(n + 1)
            wait_mat(n + 1)
            project(wb.at[0], xs, n + 1, (j + 1) // 2)

        def finish(gs):
            cols_ = cols_in(gs)
            vals = []
            for g in gs:
                for d in range(1, chips):
                    x_copy(par, g, d).wait_recv()
                val = sbuf[par, cols_of(g), _at(x, LANES)]
                for d in range(1, chips):
                    val = val + rx[par, g, d - 1]
                vals.append(val)
            solved = spread(jnp.concatenate(vals, axis=0), j)
            xs[cols_, _at(j // 2, STEP)] += solved

            @pl.when(j > 0)
            def _():
                wb[0, cols_] += _dot_nt(solved, cut(n + 1, (j // 2) * STEP, STEP))
                solve_partial(n + 1, gs, j - 1)

        finish((0,))
        finish((1,))

        pl.when(j % 2 == 0)(lambda: fin_copy(j // 2).start())
        pl.when(jnp.logical_and(j % 2 == 1, j < top))(lambda: give(j // 2 + 1))

        for g in range(2):
            for d in range(1, chips):
                x_copy(par, g, d).wait_send()

        @pl.when(jnp.logical_or(i == 0, i % 2 == 1))
        def _():
            tick(LEAD + 10 + (i + 1) // 2)

        @pl.when(j > 0)
        def _():
            release_blk(n + 1)
            release_mat(n + 1)

    _loop(0, nb, solve)

    give(0)
    _loop(0, pairs, lambda i: fin_copy(i).wait_send())


def solution(mesh):
    rows, cols = mesh.shape["row"], mesh.shape["col"]
    mat_spec = P(("kpt", "row"), "col")
    fac_spec = P("kpt", None, None)

    def local_work(v_loc, t_loc, z_loc, l_loc):
        n_row, n_col = v_loc.shape
        slots, lanes, chips, size = n_col // EDGE, 2 * n_row, rows // 2, rows * EDGE
        nb, ncol = lanes // LANES, z_loc.shape[1] // 2
        pairs, gcol, peers = nb // 2, ncol // 2, max(chips - 1, 1)
        sl, gathers, n128 = gcol // chips, len(_gathers(slots)), size // LANES
        tri = LANES * (n128 * (n128 + 1) // 2)
        dma = pltpu.SemaphoreType.DMA
        hbm, vmem = pl.BlockSpec(memory_space=pl.ANY), pl.BlockSpec(memory_space=pltpu.VMEM)

        def buf(*shape):
            return pltpu.VMEM(shape, jnp.float32)

        col = lax.axis_index("col")
        t_mine = lax.dynamic_slice_in_dim(t_loc, (cols // rows * (col % rows) + col // rows) * rows, rows, axis=0)
        return pl.pallas_call(
            functools.partial(_kernel, (rows, cols, slots, nb, ncol)),
            out_shape=[
                jax.ShapeDtypeStruct(z_loc.shape, jnp.float32),
                jax.ShapeDtypeStruct((2, slots, RING, RING, HALF, lanes), jnp.float32),
            ],
            in_specs=[hbm] * 4,
            out_specs=[vmem, hbm],
            scratch_shapes=[
                buf(2, n_row, n_col),
                buf(2, slots, 2, HALF, n_row),
                buf(2, ncol, n_row),
                buf(rows, EDGE, EDGE),
                buf(2, slots, HALF, lanes),
                buf(ncol, lanes),
                buf(ncol, lanes),
                buf(pairs // 2, rows, EDGE, STEP),
                buf(rows, EDGE, STEP),
                buf(chips, size, LANES),
                buf(size, size),
                buf(size // 2, size),
                buf(size // 4, size),
                buf(peers, size // 4 // chips, size),
                buf(size // 2, size),
                buf(2, EDGE, tri),
                buf(2, RING, RING, EDGE, tri),
                buf(DEEP, rows, EDGE, lanes),
                buf(2, size, size),
                buf(2, ncol, size),
                buf(2, peers, sl, size),
                buf(2, ncol, size),
                buf(2, size, size),
                buf(2, 2, peers, gcol, LANES),
                dma((4,)),
                dma((3, pairs)), dma((3, pairs)), dma((3, pairs)),
                dma((slots, pairs)), dma((pairs // 2, rows, 2)),
                dma((slots, 2)), dma((rows, 2)),
                dma((peers,)), dma((peers,)),
                dma((4,)),
                dma((peers,)), dma((peers,)), dma((peers,)), dma((peers,)),
                dma((pairs,)), dma((pairs,)),
                dma((gathers,)), dma((gathers, 8)), dma((gathers, 8)),
                dma((DEEP, rows)), dma((DEEP, rows)), dma((DEEP, rows)),
                dma((2, n128)), dma((2, n128)), dma((2, n128)),
                pltpu.SemaphoreType.REGULAR((DEEP,)), pltpu.SemaphoreType.REGULAR((2,)),
                dma((2, peers)), dma((2, peers)), dma((2, peers)), dma((2, peers)),
                dma((2,)), dma((2,)),
                dma((2, 2, peers)), dma((2, 2, peers)),
                dma((16,)), dma((16,)),
            ],
            compiler_params=pltpu.CompilerParams(collective_id=0, has_side_effects=True, vmem_limit_bytes=67_043_328),
            name="eigvec",
        )(v_loc, t_mine, z_loc, l_loc)[0]

    return jax.shard_map(local_work, mesh=mesh, in_specs=(mat_spec, fac_spec, mat_spec, mat_spec), out_specs=mat_spec, check_vma=False)
```
